128 devices in a mesh: band: 4 (over z), lev: 32 (over y, x, core).
Axes of the slice: x: 4, y: 4, z: 4, core: 2. Of those that a mesh axis runs over, the one named last changes fastest.
Arguments:
- neutrals: float32 [5, 64, 32, 2880], P(None, 'lev', 'band'), may hold values from -6 to 6
- wind_lon: float32 [64, 32, 2880], P('lev', 'band'), may hold values from -0.15 to 0.15
- wind_lat: float32 [64, 32, 2880], P('lev', 'band'), may hold values from -0.15 to 0.15
- wind_lev: float32 [64, 32, 2880], P('lev', 'band'), may hold values from -0.15 to 0.15
- eddy_coupling: float32 [5, 64], replicated, may hold values from 0.3 to 6
- pair_weight: float32 [32, 32, 2880], P(None, 'band'), may hold values from 0 to 1
- ion_yield: float32 [7, 5], replicated, may hold values from -2.5 to 2.5
- ion_spread: float32 [7], replicated, may hold values from 0.02 to 0.4
- ion_loss: float32 [7], replicated, may hold values from 0.005 to 0.1
- column_order: int32 [4, 23040], P('band'), may hold values from 0 to 23039, each once within a row
- column_units: int32 [32], replicated, may hold values from 1 to 270, 5760 in all
- tube_owner: int32 [32, 270, 1], replicated, may hold values from 0 to 127; in each aligned block of 270 rows (0 to 269, 270 to 539, ..., all dimensions but the last counted through in order) at most 3 rows name the same one
Outputs:
- column_state: float32 [4, 32, 5, 64, 1080], P('band', 'lev')
- ion_lines: float32 [128, 96, 7, 512], P(('band', 'lev'))
The draws below stay inside these ranges and needn't reach their ends.
Inputs may be any that keep to these rules, and one draw needn't show every extreme that they name: `column_order`: each row lists every column of its band once. `column_units`: the counts sum to 5760; the largest is 270. `tube_owner`: among the 270 slots of one owner no tube owner is named more than 3 times, and some is named exactly that often.
All inputs are finite; a program needn't handle non-finite values.
Results may differ from the reference program's by a relative error of at most 0.0003.
Values sent between devices are 32-bit elements; how exact they have to be, the bound alone decides.
No kernel may reach another device: no remote copies, remote signals or barrier semaphores. Data moves between devices by JAX's collectives and lax.ppermute only.
A program may use at most 192 MiB of HBM per device.

```python
import math
import jax
import jax.numpy as jnp
import numpy as np
from jax import lax

SPECIES = 5
IONS = 7
NLON = 2880
NLEV = 64
TUBE_COLS = 4
TSTEPS = 2
SWEEPS = 8
SECTIONS = 20
BANDS = 4
OWNERS = 32
PEERS = 128
NLAT = 32
COLS = 23040
BAND_TUBES = 5760
TUBE_CAP = 270
COL_CAP = 1080
PEER_SLOTS = 3
PAIRS = 32
LINE_PTS = 512


def block_scale(own_key, shape, shards, least, top_value):
    level = 1.0
    for position, shards_of in shards:
        heights = jax.random.uniform(jax.random.fold_in(jax.random.fold_in(own_key, 6), position), (shards_of,), jnp.float32, least / len(shards), top_value / len(shards))
        level = level * jnp.repeat(jnp.exp(heights), shape[position] // shards_of).reshape((-1,) + (1,) * (len(shape) - 1 - position))
    return level


def split_up(count, total, limit, skew):
    portions = [(1 << 20) // math.isqrt(standing ** skew) + 1 for standing in range(2, count + 1)]
    surplus, counts = total - limit - (count - 1), [1] * (count - 1)
    while surplus > 0:
        candidates = [i for i in range(count - 1) if counts[i] < limit]
        pool, remaining = sum([portions[i] for i in candidates]), surplus
        for i in candidates:
            addition = min(limit - counts[i], max(1, remaining * portions[i] // pool), surplus)
            counts[i] = counts[i] + addition
            surplus = surplus - addition
    return np.array([limit] + counts)


def uneven_parts(stream_key, amount, total, reach, skew):
    if amount == 2:
        one = jax.random.randint(stream_key, (), max(1, total - reach), min(reach, total - 1) + 1)
        return jnp.stack([one, total - one])
    tallies = jnp.asarray(split_up(amount, total, reach, skew), jnp.int32)
    pairs = (amount - 1) // 2
    giver, taker = tallies[1:1 + 2 * pairs:2], tallies[2:2 + 2 * pairs:2]
    margin = jnp.minimum(giver - 1, reach - taker)
    shifted = jax.random.randint(jax.random.fold_in(stream_key, 1), (pairs,), 0, 1 << 20) % (margin + 1)
    tallies = tallies.at[1:1 + 2 * pairs:2].set(giver - shifted).at[2:2 + 2 * pairs:2].set(taker + shifted)
    return tallies[jax.random.permutation(jax.random.fold_in(stream_key, 2), amount)]


def deal_out(rng, own, number, rows, number_of, top, limit, skew):
    order = jax.random.permutation(rng, number_of)
    packed, common = load_shares(number_of, rows * top, limit, skew, True), load_shares(number_of, rows * top, limit, skew, False)
    places = jnp.arange(number_of)

    def named(lengths, rotation):
        used = int((lengths > 0).sum())
        fixed = max(1, used // 4)
        moved = fixed + (places - fixed + rotation * (used - fixed)) % max(1, number_of - fixed)
        return jnp.zeros((number_of,), jnp.int32).at[order[jnp.where(places < fixed, places, moved)]].set(jnp.asarray(lengths, jnp.int32))

    lengths = jnp.where(number % 4 == 0, named(packed, number // 4), named(common, number - number // 4 - 1))
    mixed = jax.random.permutation(jax.random.fold_in(own, 3), number_of)
    source_of, sink = mixed[0:number_of // 2 * 2:2], mixed[1:number_of // 2 * 2:2]
    margin = jnp.minimum(lengths[source_of] - 1, limit - lengths[sink]) // 2
    margin = jnp.where((source_of == order[0]) | (sink == order[0]) | (lengths[sink] == 0), 0, jnp.maximum(margin, 0))
    moved = jax.random.randint(jax.random.fold_in(own, 4), (number_of // 2,), 0, 1 << 20) % (margin + 1)
    lengths = lengths.at[source_of].add(-moved).at[sink].add(moved)
    labels = jnp.searchsorted(jnp.cumsum(lengths), jnp.arange(rows * top), side="right").astype(jnp.int32)
    listing = labels.reshape(top, rows).T
    listing = listing[jax.random.permutation(jax.random.fold_in(own, 1), rows)]
    rotation = jax.random.randint(jax.random.fold_in(own, 2), (rows, 1), 0, top)
    return jnp.take_along_axis(listing, (jnp.arange(top)[None, :] + rotation) % top, axis=1)


def load_shares(number_of, total, bound, slope, full):
    loads = [(1 << 20) // math.isqrt(standing ** slope) + 1 for standing in range(1, number_of + 1)]
    largest = bound if full else min(bound, max(-(-total // number_of), total * loads[0] // sum(loads)))
    least = 1 if total - largest >= number_of - 1 else 0
    counts, rest = [largest] + [least] * (number_of - 1), total - largest - least * (number_of - 1)
    while rest > 0:
        movable = [i for i in range(1, number_of) if counts[i] < largest] or [i for i in range(1, number_of) if counts[i] < bound]
        pool, budget = sum([loads[i] for i in movable]), rest
        for i in movable:
            more = min(bound - counts[i], max(1, budget * loads[i] // pool), rest)
            counts[i] = counts[i] + more
            rest = rest - more
    return np.array(counts)


def bell_draw(key, extent, scale, bound, shards=(), kind=jnp.bfloat16):
    values = scale * jax.random.normal(key, extent, jnp.float32)
    if shards:
        values = values * block_scale(key, extent, shards, -0.22, 0.18)
    return jnp.clip(values, -bound, bound).astype(kind)


def setup_inputs(seed: int = 0) -> dict:
    key_list = jax.random.split(jax.random.key(seed), 13)
    neutrals = bell_draw(key_list[0], (SPECIES, NLEV, NLAT, NLON), 1.0, 6.0, ((1, 32), (2, 4)), jnp.float32)
    wind_lon = jnp.clip(jax.random.uniform(key_list[1], (NLEV, NLAT, NLON), jnp.float32, -0.15, 0.15) * block_scale(key_list[1], (NLEV, NLAT, NLON), ((0, 32), (1, 4)), -0.4, 0.0), -0.15, 0.15)
    wind_lat = jnp.clip(jax.random.uniform(key_list[2], (NLEV, NLAT, NLON), jnp.float32, -0.15, 0.15) * block_scale(key_list[2], (NLEV, NLAT, NLON), ((0, 32), (1, 4)), -0.4, 0.0), -0.15, 0.15)
    wind_lev = jnp.clip(jax.random.uniform(key_list[3], (NLEV, NLAT, NLON), jnp.float32, -0.15, 0.15) * block_scale(key_list[3], (NLEV, NLAT, NLON), ((0, 32), (1, 4)), -0.4, 0.0), -0.15, 0.15)
    eddy_coupling = jnp.clip(jnp.exp(jax.random.uniform(key_list[4], (SPECIES, NLEV), jnp.float32, math.log(0.3), math.log(6.0))), 0.3, 6.0)
    pair_weight = jnp.clip(1.0 * jax.random.uniform(key_list[5], (PAIRS, NLAT, NLON), jnp.float32) ** block_scale(key_list[5], (PAIRS, NLAT, NLON), ((1, 4),), -0.2, 0.2), 0.0, 1.0)
    ion_yield = bell_draw(key_list[6], (IONS, SPECIES), SPECIES ** -0.5, 2.5, (), jnp.float32)
    ion_spread = jnp.clip(jnp.exp(jax.random.uniform(key_list[7], (IONS,), jnp.float32, math.log(0.02), math.log(0.4))), 0.02, 0.4)
    ion_loss = jnp.clip(jnp.exp(jax.random.uniform(key_list[8], (IONS,), jnp.float32, math.log(0.005), math.log(0.1))), 0.005, 0.1)
    column_order = jax.vmap(lambda own: jax.random.permutation(own, COLS))(jax.random.split(key_list[9], BANDS)).reshape((BANDS, COLS)).astype(jnp.int32)
    column_units = uneven_parts(key_list[10], OWNERS, BAND_TUBES, TUBE_CAP, 2).astype(jnp.int32)
    tube_owner_keys = jax.random.split(jax.random.fold_in(key_list[11], 1), OWNERS * TUBE_CAP // TUBE_CAP)
    tube_owner_turns = jax.random.permutation(jax.random.fold_in(key_list[11], 3), OWNERS * TUBE_CAP // TUBE_CAP)
    tube_owner = jax.vmap(lambda own, number: deal_out(jax.random.fold_in(key_list[11], 2), own, number, TUBE_CAP, PEERS, 1, PEER_SLOTS, 2))(tube_owner_keys, tube_owner_turns).reshape((OWNERS, TUBE_CAP, 1))
    return {"neutrals": neutrals, "wind_lon": wind_lon, "wind_lat": wind_lat, "wind_lev": wind_lev, "eddy_coupling": eddy_coupling, "pair_weight": pair_weight, "ion_yield": ion_yield, "ion_spread": ion_spread, "ion_loss": ion_loss, "column_order": column_order, "column_units": column_units, "tube_owner": tube_owner}


HIGHEST = lax.Precision.HIGHEST


def upwind_faces(courant, upstream, downstream):
    return jnp.maximum(courant, 0.0) * upstream + jnp.minimum(courant, 0.0) * downstream


def transport_once(density, wind_lon, wind_lat, wind_lev):
    western = jnp.roll(density, 1, axis=3)
    flux_lon = upwind_faces(wind_lon, western, density)
    change = flux_lon - jnp.roll(flux_lon, -1, axis=3)
    across = jnp.pad(density, ((0, 0), (0, 0), (1, 1), (0, 0)))
    courant = jnp.pad(wind_lat, ((0, 0), (1, 1), (0, 0)))
    flux_lat = upwind_faces(courant[:, 1:], across[:, :, :-1], across[:, :, 1:])
    change = change + flux_lat[:, :, :-1] - flux_lat[:, :, 1:]
    upward = jnp.pad(density, ((0, 0), (1, 1), (0, 0), (0, 0)))
    courant = jnp.pad(wind_lev, ((1, 1), (0, 0), (0, 0)))
    flux_lev = upwind_faces(courant[1:], upward[:, :-1], upward[:, 1:])
    change = change + flux_lev[:, :-1] - flux_lev[:, 1:]
    return density + change


def vertical_solve(density, eddy_coupling):
    zero_edge = jnp.zeros((eddy_coupling.shape[0], 1), jnp.float32)
    coupling_below = jnp.concatenate([zero_edge, eddy_coupling[:, 1:]], 1)[:, :, None]
    coupling_above = jnp.concatenate([eddy_coupling[:, 1:], zero_edge], 1)[:, :, None]
    diagonal = 1.0 + coupling_below + coupling_above
    iterate = density
    zero_layer = jnp.zeros_like(density[:, :1])
    for sweep_index in range(SWEEPS):
        beneath = jnp.concatenate([zero_layer, iterate[:, :-1]], 1)
        overhead = jnp.concatenate([iterate[:, 1:], zero_layer], 1)
        iterate = (density + coupling_below * beneath + coupling_above * overhead) / diagonal
    return iterate


def interpolate(ion_yield, neutral_block, weight_block):
    paired = weight_block * neutral_block[..., 0::2] + (1.0 - weight_block) * neutral_block[..., 1::2]
    return jnp.einsum("is,...scp->...icp", ion_yield, paired, precision=HIGHEST)


def line_diffusion(source, ion_spread, ion_loss):
    spread_rate = ion_spread[:, None]
    loss_rate = ion_loss[:, None]

    def advance(section_index, density):
        left_side = jnp.concatenate([density[..., :1], density[..., :-1]], -1)
        right_side = jnp.concatenate([density[..., 1:], density[..., -1:]], -1)
        return density + spread_rate * (left_side - 2.0 * density + right_side) + source - loss_rate * density

    return lax.fori_loop(0, SECTIONS, advance, jnp.zeros_like(source))


def owner_table(destinations):
    device_ids = jnp.arange(PEERS, dtype=jnp.int32)
    matches = (destinations[:, None] == device_ids[None, :]).astype(jnp.int32)
    rank_of = jnp.sum(jnp.cumsum(matches, 0) * matches, 1) - 1
    flat_slot = (destinations * PEER_SLOTS + rank_of).astype(jnp.int32)
    empty_table = jnp.full((PEERS * PEER_SLOTS,), TUBE_CAP, jnp.int32)
    return empty_table.at[flat_slot].set(jnp.arange(TUBE_CAP, dtype=jnp.int32))


def reference(neutrals, wind_lon, wind_lat, wind_lev, eddy_coupling, pair_weight, ion_yield, ion_spread, ion_loss, column_order, column_units, tube_owner):
    species = neutrals.shape[0]
    ion_count = ion_yield.shape[0]
    density = neutrals
    for substep in range(TSTEPS):
        density = transport_once(density, wind_lon, wind_lat, wind_lev)
    solved = vertical_solve(density.reshape(species, NLEV, NLAT * NLON), eddy_coupling)
    by_band = solved.reshape(species, NLEV, BANDS, COLS)
    starts = jnp.cumsum(column_units) - column_units
    slot_ids = jnp.arange(COL_CAP, dtype=jnp.int32)
    positions = jnp.minimum(TUBE_COLS * starts[:, None] + slot_ids[None, :], COLS - 1).astype(jnp.int32)
    live_slots = (slot_ids[None, :] < TUBE_COLS * column_units[:, None]).astype(jnp.float32)
    column_ids = column_order[:, positions]

    def band_columns(band_index):
        gathered = jnp.take(by_band[:, :, band_index], column_ids[band_index], axis=2)
        return jnp.transpose(gathered, (2, 0, 1, 3)) * live_slots[:, None, None, :]

    column_state = lax.map(band_columns, jnp.arange(BANDS, dtype=jnp.int32))
    weight_band = pair_weight.reshape(PAIRS, BANDS, COLS)

    def band_weights(band_index):
        return jnp.transpose(jnp.take(weight_band[:, band_index], column_ids[band_index], axis=1), (1, 0, 2))

    weight_state = lax.map(band_weights, jnp.arange(BANDS, dtype=jnp.int32))
    slot_table = jax.vmap(owner_table)(tube_owner[:, :, 0]).reshape(OWNERS, PEERS, PEER_SLOTS)
    state_blocks = column_state.reshape(BANDS, OWNERS, species, NLEV, TUBE_CAP, TUBE_COLS)
    weight_blocks = weight_state.reshape(BANDS, OWNERS, PAIRS, TUBE_CAP, TUBE_COLS)
    owner_ids = jnp.arange(OWNERS, dtype=jnp.int32)[:, None]

    def device_lines(device):
        picked = slot_table[:, device]
        alive_mask = (picked < column_units[:, None]).astype(jnp.float32)
        clipped = jnp.minimum(picked, TUBE_CAP - 1)
        neutral_part = state_blocks[:, owner_ids, :, :, clipped, :]
        neutral_part = jnp.swapaxes(neutral_part, 4, 5) * alive_mask[:, :, None, None, None, None]
        weight_part = jnp.swapaxes(weight_blocks[:, owner_ids, :, clipped, :], 3, 4)[:, :, :, None]
        sources = interpolate(ion_yield, neutral_part, weight_part)
        sources = jnp.transpose(sources, (0, 1, 3, 2, 4, 5)).reshape(OWNERS * PEER_SLOTS, ion_count, LINE_PTS)
        return line_diffusion(sources, ion_spread, ion_loss)

    ion_lines = lax.map(device_lines, jnp.arange(PEERS, dtype=jnp.int32))
    return column_state, ion_lines
```

```python
import functools

import jax
import jax.numpy as jnp
import numpy as np
from jax import lax
from jax.experimental import pallas as pl
from jax.experimental.pallas import tpu as pltpu
from jax.sharding import PartitionSpec as P

SPECIES = 5
IONS = 7
NLON = 2880
NLEV = 64
PAIRS = 32
BAND_LATS = 8
TSTEPS = 2
SWEEPS = 8
SECTIONS = 20
TUBE_COLS = 4
PEERS = 128
PEER_SLOTS = 3
COL_CAP = 1080
TUBE_CAP = 270
BAND_COLS = BAND_LATS * NLON
LINE_PTS = 512

LANES = 128
LON_BLOCKS = 23
LON_PAD = LON_BLOCKS * LANES
CHIP_LEVS = 4
PLANES = 12
GROUPS = 6
MSG_ROWS = 192
SLOT_BLOCKS = 9
SLOTS_PAD = SLOT_BLOCKS * LANES
ORDER_PAD = BAND_COLS + LANES
UNROLL = 64
ZERO_TUBE = SLOT_BLOCKS * 32
ITEM_ROWS = 16

f32 = jnp.float32
VMEM = pl.BlockSpec(memory_space=pltpu.VMEM)
SMEM = pl.BlockSpec(memory_space=pltpu.SMEM)
ANY = pl.BlockSpec(memory_space=pl.ANY)


def call(kernel, out_shape, in_specs, out_specs, scratch=(), name=None, flops=0):
    return pl.pallas_call(
        kernel,
        out_shape=out_shape,
        in_specs=in_specs,
        out_specs=out_specs,
        scratch_shapes=list(scratch),
        name=name,
        cost_estimate=pl.CostEstimate(flops=flops, bytes_accessed=1 << 20, transcendentals=0),
        compiler_params=pltpu.CompilerParams(vmem_limit_bytes=60 * 1024 * 1024),
    )


def sds(shape, dtype=f32):
    return jax.ShapeDtypeStruct(shape, dtype)


def upwind(courant_plus, courant_minus, upstream, downstream):
    return courant_plus * upstream + courant_minus * downstream


def transport_kernel(
    n_ref, wlon_ref, wlat_ref, wlev_ref, south_ref, north_ref, below_ref, above_ref, wlat_n_ref, wlev_up_ref,
    *outs, last,
):
    def split(c):
        return jnp.maximum(c, 0.0), jnp.minimum(c, 0.0)

    def shift_west(x):
        return jnp.concatenate([x[:, NLON - 1 :], x[:, : NLON - 1]], axis=1)

    def shift_east(x):
        return jnp.concatenate([x[:, 1:], x[:, :1]], axis=1)

    for j in range(2):

        @pl.loop(0, SPECIES)
        def _(s):
            x = n_ref[s, j]
            flux = upwind(*split(wlon_ref[j]), shift_west(x), x)
            total = x + (flux - shift_east(flux))
            southern = jnp.concatenate([south_ref[s, j], x[: BAND_LATS - 1]], axis=0)
            flux = upwind(*split(wlat_ref[j]), southern, x)
            edge = upwind(*split(wlat_n_ref[j]), x[BAND_LATS - 1 :], north_ref[s, j])
            total = total + (flux - jnp.concatenate([flux[1:], edge], axis=0))
            beneath = below_ref[s] if j == 0 else n_ref[s, 0]
            overhead = n_ref[s, 1] if j == 0 else above_ref[s]
            over_wind = wlev_ref[1] if j == 0 else wlev_up_ref[...]
            flux = upwind(*split(wlev_ref[j]), beneath, x)
            total = total + (flux - upwind(*split(over_wind), x, overhead))
            if last:
                row = pl.multiple_of((j * SPECIES + s) * BAND_LATS, BAND_LATS)
                for blk in range(LON_BLOCKS):
                    wide = min(LANES, NLON - blk * LANES)
                    outs[0][blk, pl.ds(row, BAND_LATS), :wide] = total[:, blk * LANES : blk * LANES + wide]
            else:
                outs[0][s, j] = total
                outs[1 + j][s] = total
                outs[3][s, j] = total[:1]
                outs[4][s, j] = total[BAND_LATS - 1 :]


def transport_step(density, winds, halo, last):
    if last:
        out_shape = (sds((LON_BLOCKS, 2 * SPECIES * BAND_LATS, LANES)),)
    else:
        out_shape = (
            sds((SPECIES, 2, BAND_LATS, NLON)),
            sds((SPECIES, BAND_LATS, NLON)),
            sds((SPECIES, BAND_LATS, NLON)),
            sds((SPECIES, 2, 1, NLON)),
            sds((SPECIES, 2, 1, NLON)),
        )
    return call(
        functools.partial(transport_kernel, last=last),
        out_shape,
        [VMEM] * 10,
        tuple([VMEM] * len(out_shape)),
        name="transport",
        flops=4_000_000,
    )(density, *winds, *halo)


def prepare_kernel(units_ref, owner_ref, rows_ref, sel_ref, weight_ref, table_ref, own_ref, count, blocks, table, picked):
    @pl.loop(0, PEERS * PEER_SLOTS)
    def _(i):
        table_ref[i] = ZERO_TUBE

    @pl.loop(0, PEERS)
    def _(i):
        count[i] = 0

    @pl.loop(0, units_ref[0])
    def _(u):
        dest = owner_ref[u]
        rank = count[dest]
        count[dest] = rank + 1
        table_ref[dest * PEER_SLOTS + rank] = u

    for blk in range(LON_BLOCKS):
        wide = min(LANES, NLON - blk * LANES)
        blocks[blk, :, :wide] = weight_ref[:, blk * LANES : blk * LANES + wide]

    @pl.loop(0, BAND_LATS)
    def _(lat):
        for g in range(6):
            parts = [
                blocks[min(4 * g + i, LON_BLOCKS - 1), pl.ds(lat, PAIRS, stride=BAND_LATS), :] for i in range(4)
            ]
            start = pl.multiple_of((lat * 6 + g) * LANES, LANES)
            table[pl.ds(start, LANES), :] = jnp.concatenate(parts, axis=0).T

    @pl.loop(0, SLOTS_PAD // UNROLL)
    def _(step):
        base = pl.multiple_of(step * UNROLL, UNROLL)
        for i in range(UNROLL):
            picked[pl.ds(base + i, 1), :] = table[pl.ds(rows_ref[base + i], 1), :]

    for blk in range(SLOT_BLOCKS):
        turned = picked[blk * LANES : (blk + 1) * LANES, :].T
        which = sel_ref[blk : blk + 1, :]
        kept = turned[:PAIRS]
        for i in range(1, 4):
            kept = jnp.where(which == i, turned[i * PAIRS : (i + 1) * PAIRS], kept)
        own_ref[blk] = kept


def prepare(units, owners, rows, sel, weights):
    return call(
        prepare_kernel,
        (sds((PEERS * PEER_SLOTS,), jnp.int32), sds((SLOT_BLOCKS, PAIRS, LANES))),
        [SMEM, SMEM, SMEM, VMEM, VMEM],
        (SMEM, VMEM),
        [
            pltpu.SMEM((PEERS,), jnp.int32),
            pltpu.VMEM((LON_BLOCKS, PAIRS * BAND_LATS, LANES), f32),
            pltpu.VMEM((BAND_LATS * 6 * LANES, LANES), f32),
            pltpu.VMEM((SLOTS_PAD, LANES), f32),
        ],
        name="prepare",
        flops=20_000_000,
    )(units, owners, rows, sel, weights)


def pack_kernel(core_ref, starts_ref, units_ref, order_hbm, mine_ref, other_ref, msg_ref, order, planes, table, sem):
    fetch = pltpu.make_async_copy(order_hbm, order, sem)
    fetch.start()
    core = core_ref[0]
    for source, side in ((mine_ref, core), (other_ref, 1 - core)):

        @pl.loop(0, LON_BLOCKS)
        def _(blk):
            for j in range(2):
                for i in range(PLANES):
                    row = pl.multiple_of(((2 * side + j) * PLANES + i) * BAND_LATS, BAND_LATS)
                    from_row = (j * SPECIES + i % SPECIES) * BAND_LATS
                    planes[blk, pl.ds(row, BAND_LATS), :] = source[blk, from_row : from_row + BAND_LATS, :]

    @pl.loop(0, LON_BLOCKS)
    def _(blk):
        for lat in range(BAND_LATS):
            parts = [
                planes[blk, pl.ds((jj * PLANES + first) * BAND_LATS + lat, 8, stride=BAND_LATS), :]
                for jj in range(CHIP_LEVS)
                for first in (0, 3, 1, 4)
            ]
            start = pl.multiple_of((lat * LON_BLOCKS + blk) * LANES, LANES)
            table[pl.ds(start, LANES), :] = jnp.concatenate(parts, axis=0).T

    fetch.wait()
    lane = lax.broadcasted_iota(jnp.int32, (1, LANES), 1)
    group_of = lax.div(lax.rem(lane, 32), SPECIES)

    @pl.loop(0, 16 * GROUPS)
    def _(turn):
        peer = lax.div(turn, GROUPS)
        group = turn - peer * GROUPS
        owner = 2 * peer + core
        live = jnp.clip(TUBE_COLS * units_ref[owner] - MSG_ROWS * group, 0, MSG_ROWS)
        first = TUBE_COLS * starts_ref[owner] + MSG_ROWS * group
        mask = group_of == group

        @pl.loop(0, lax.div(live + (UNROLL - 1), UNROLL))
        def _(step):
            base = first + step * UNROLL
            row = pl.multiple_of(peer * MSG_ROWS + step * UNROLL, UNROLL)
            for i in range(UNROLL):
                value = table[pl.ds(order[base + i], 1), :]
                pltpu.store(msg_ref.at[pl.ds(row + i, 1), :], value, mask=mask)


def pack(core, starts, units, order, mine, other):
    return call(
        pack_kernel,
        sds((16 * MSG_ROWS, LANES)),
        [SMEM, SMEM, SMEM, ANY, VMEM, VMEM],
        VMEM,
        [
            pltpu.SMEM((ORDER_PAD,), jnp.int32),
            pltpu.VMEM((LON_BLOCKS, CHIP_LEVS * PLANES * BAND_LATS, LANES), f32),
            pltpu.VMEM((BAND_LATS * LON_PAD, LANES), f32),
            pltpu.SemaphoreType.DMA,
        ],
        name="pack",
        flops=40_000_000,
    )(core, starts, units, order, mine, other)


def solve_kernel(
    units_ref, table_ref, got_ref, lower_ref, upper_ref, inv_ref, weight_ref,
    state_ref, items_ref, turned, solved, wide, tubes,
):
    live = TUBE_COLS * units_ref[0]
    lane = lax.broadcasted_iota(jnp.int32, (1, LANES), 1)

    @pl.loop(0, 16)
    def _(m):
        row = pl.multiple_of(m * MSG_ROWS, MSG_ROWS)
        out = pl.multiple_of(m * LANES, LANES)
        turned[0, pl.ds(out, LANES), :] = got_ref[pl.ds(row, LANES), :].T
        rest = jnp.concatenate([got_ref[pl.ds(row + LANES, 64), :]] * 2, axis=0)
        turned[1, pl.ds(out, LANES), :] = rest.T

    low = lane < 64
    for pair in range(3):

        @pl.loop(0, SPECIES)
        def _(s):
            lower, upper, inv = lower_ref[s], upper_ref[s], inv_ref[s]

            def levels(half, group):
                return turned[half, pl.ds(group * SPECIES + s, NLEV, stride=32), :]

            first = levels(0, 2 * pair)
            odd = pltpu.roll(levels(0, 2 * pair + 1), 64, axis=1)
            second = jnp.where(low, levels(1, 2 * pair), odd)
            third = jnp.where(low, odd, levels(1, 2 * pair + 1))
            for i, rhs in enumerate((first, second, third)):
                blk = 3 * pair + i
                scaled = rhs * inv
                x = rhs
                for _ in range(SWEEPS):
                    x = scaled + lower * pltpu.roll(x, 1, axis=0) + upper * pltpu.roll(x, NLEV - 1, axis=0)
                x = jnp.where(lane + blk * LANES < live, x, 0.0)
                solved[s * SLOT_BLOCKS + blk] = x
                width = min(LANES, COL_CAP - blk * LANES)
                state_ref[0, 0, s, :, blk * LANES : blk * LANES + width] = x[:, :width]

    quarter = lax.div(lane, 32)

    @pl.loop(0, SLOT_BLOCKS)
    def _(blk):
        weight = weight_ref[blk]
        for s in range(SPECIES):
            where = s * SLOT_BLOCKS + blk
            even = solved[where, pl.ds(0, PAIRS, stride=2), :]
            odd = solved[where, pl.ds(1, PAIRS, stride=2), :]
            paired = weight * even + (1.0 - weight) * odd
            wide[s] = jnp.concatenate([paired] * 4, axis=0).T
            item = wide[s, pl.ds(0, 32, stride=TUBE_COLS), :]
            for c in range(1, TUBE_COLS):
                item = jnp.where(quarter == c, wide[s, pl.ds(c, 32, stride=TUBE_COLS), :], item)
            tubes[pl.ds(blk * 256 + s, 32, stride=8), :] = item

    tubes[ZERO_TUBE * 8 :, :] = jnp.zeros((8, LANES), f32)
    sub = lax.broadcasted_iota(jnp.int32, (8, LANES), 0)

    @pl.loop(0, PEERS // 4)
    def _(step):
        for i in range(4):
            d = step * 4 + i
            tiles = [
                tubes[pl.ds(pl.multiple_of(table_ref[d * PEER_SLOTS + r] * 8, 8), 8), :] for r in range(PEER_SLOTS)
            ]
            mid = pltpu.roll(tiles[1], 5, axis=0)
            top = pltpu.roll(tiles[2], 2, axis=0)
            row = pl.multiple_of(d * ITEM_ROWS, ITEM_ROWS)
            items_ref[pl.ds(row, 8), :] = jnp.where(sub < 5, tiles[0], mid)
            items_ref[pl.ds(row + 8, 8), :] = jnp.where(sub < 2, mid, jnp.where(sub < 7, top, 0.0))


def solve(units, table, got, lower, upper, inv, weights):
    return call(
        solve_kernel,
        (sds((1, 1, SPECIES, NLEV, COL_CAP)), sds((PEERS * ITEM_ROWS, LANES))),
        [SMEM, SMEM] + [VMEM] * 5,
        (VMEM, VMEM),
        [
            pltpu.VMEM((2, 16 * LANES, LANES), f32),
            pltpu.VMEM((SPECIES * SLOT_BLOCKS, NLEV, LANES), f32),
            pltpu.VMEM((SPECIES, LANES, LANES), f32),
            pltpu.VMEM((ZERO_TUBE * 8 + 8, LANES), f32),
        ],
        name="solve",
        flops=40_000_000,
    )(units, table, got, lower, upper, inv, weights)


def halves(x):
    high = x.astype(jnp.bfloat16)
    return high, (x - high.astype(f32)).astype(jnp.bfloat16)


def product(x, high, low):
    x_high, x_low = halves(x)
    dot = functools.partial(jnp.dot, preferred_element_type=f32)
    return dot(x_high, high) + (dot(x_low, high) + dot(x_high, low))


def lines_kernel(
    items_ref, yield_ref, rates_ref, waves_ref, fwd_high, fwd_low, inv_high, inv_low, out_ref, spec_in, spec, mixed
):
    tubes = 32 * PEER_SLOTS
    for b in range(4):
        for s in range(SPECIES):
            for r in range(PEER_SLOTS):
                rows = items_ref[pl.ds(b * 32 * ITEM_ROWS + r * SPECIES + s, 32, stride=ITEM_ROWS), :]
                spec_in[b, pl.ds(s * tubes + r, 32, stride=PEER_SLOTS), :] = rows

    @pl.loop(0, SPECIES)
    def _(s):
        row = pl.multiple_of(s * tubes, tubes)
        x = jnp.concatenate([spec_in[b, pl.ds(row, tubes), :] for b in range(4)], axis=1)
        y = product(x, fwd_high[...], fwd_low[...])
        for b in range(4):
            spec[b, pl.ds(row, tubes), :] = y[:, b * LANES : (b + 1) * LANES]

    keep = (1.0 - rates_ref[1]) + rates_ref[0] * waves_ref[...]
    gain = jnp.ones((8, LINE_PTS), f32)
    for _ in range(SECTIONS - 1):
        gain = gain * keep + 1.0
    for b in range(4):
        part = gain[:, b * LANES : (b + 1) * LANES]
        scale = [yield_ref[s] * part for s in range(SPECIES)]

        @pl.loop(0, tubes // 8)
        def _(step):
            base = step * 8
            for i in range(8):
                t = base + i
                total = scale[0] * spec[b, pl.ds(t, 1), :]
                for s in range(1, SPECIES):
                    total = total + scale[s] * spec[b, pl.ds(s * tubes + t, 1), :]
                mixed[b, pl.ds(pl.multiple_of(t * 8, 8), 8), :] = total

    chunk = 96

    @pl.loop(0, tubes * 8 // chunk)
    def _(step):
        row = pl.multiple_of(step * chunk, chunk)
        x = jnp.concatenate([mixed[b, pl.ds(row, chunk), :] for b in range(4)], axis=1)
        y = product(x, inv_high[...], inv_low[...])
        y = y.reshape(chunk // 8, 8, LINE_PTS)
        out_ref[0, pl.ds(step * (chunk // 8), chunk // 8)] = y[:, :IONS, :]


def cosine_basis():
    k = np.arange(LINE_PTS)[:, None]
    n = np.arange(LINE_PTS)[None, :]
    basis = np.cos(np.pi * k * (n + 0.5) / LINE_PTS) * np.sqrt(2.0 / LINE_PTS)
    basis[0] *= np.sqrt(0.5)
    waves = 2.0 * np.cos(np.pi * np.arange(LINE_PTS) / LINE_PTS) - 2.0
    return basis, waves


def lines(items, ion_yield, ion_spread, ion_loss):
    basis, waves = cosine_basis()

    def parts(matrix):
        matrix = matrix.astype(np.float32)
        high = matrix.astype(jnp.bfloat16)
        low = (matrix - high.astype(np.float32)).astype(jnp.bfloat16)
        return jnp.asarray(high), jnp.asarray(low)

    fill = ((0, 8 - IONS),)
    yields = jnp.pad(ion_yield, fill + ((0, 0),)).T[:, :, None]
    yields = jnp.broadcast_to(yields, (SPECIES, 8, LANES))
    rates = jnp.stack([jnp.pad(ion_spread, fill), jnp.pad(ion_loss, fill)])[:, :, None]
    rates = jnp.broadcast_to(rates, (2, 8, LINE_PTS))
    waves = jnp.asarray(waves.astype(np.float32))[None]
    tubes = 32 * PEER_SLOTS
    return call(
        lines_kernel,
        sds((1, tubes, IONS, LINE_PTS)),
        [VMEM] * 8,
        VMEM,
        [
            pltpu.VMEM((4, SPECIES * tubes, LANES), f32),
            pltpu.VMEM((4, SPECIES * tubes, LANES), f32),
            pltpu.VMEM((4, tubes * 8, LANES), f32),
        ],
        name="lines",
        flops=2_000_000_000,
    )(items, yields, rates, waves, *parts(basis.T), *parts(basis))


def up(x, axis):
    ends = lax.axis_size(axis) - 1
    return lax.ppermute(x, axis, [(i, i + 1) for i in range(ends)])


def down(x, axis):
    ends = lax.axis_size(axis) - 1
    return lax.ppermute(x, axis, [(i + 1, i) for i in range(ends)])


def on_device(
    neutrals,
    wind_lon,
    wind_lat,
    wind_lev,
    eddy_coupling,
    pair_weight,
    ion_yield,
    ion_spread,
    ion_loss,
    column_order,
    column_units,
    tube_owner,
):
    lev = lax.axis_index("lev")
    winds = (wind_lon, wind_lat, wind_lev)

    below = up(neutrals[:, 1], "lev")
    got = down(jnp.concatenate([neutrals[:, 0], wind_lev[:1]], 0), "lev")
    above, wlev_up = got[:SPECIES], got[SPECIES]
    south = up(neutrals[:, :, BAND_LATS - 1 :], "band")
    got = down(jnp.concatenate([neutrals[:, :, :1], wind_lat[None, :, :1]], 0), "band")
    north, wlat_n = got[:SPECIES], got[SPECIES]

    starts = jnp.cumsum(column_units) - column_units
    order = column_order[0]
    lat = jnp.zeros_like(order)
    for i in range(1, BAND_LATS):
        lat = lat + (order >= i * NLON).astype(jnp.int32)
    rows = jnp.pad(order + lat * (LON_PAD - NLON), (0, ORDER_PAD - BAND_COLS))
    own_units = column_units[lev].reshape(1)
    padded = jnp.pad(order, (0, SLOTS_PAD))
    own = lax.dynamic_slice(padded, (TUBE_COLS * starts[lev],), (SLOTS_PAD,))
    own_lat = jnp.zeros_like(own)
    for i in range(1, BAND_LATS):
        own_lat = own_lat + (own >= i * NLON).astype(jnp.int32)
    own_lon = own - own_lat * NLON
    own_rows = (own_lat * 6 + own_lon // 512) * LANES + own_lon % LANES
    own_sel = ((own_lon // LANES) % 4).reshape(SLOT_BLOCKS, LANES)
    table, own_weights = prepare(
        own_units, tube_owner[lev, :, 0], own_rows, own_sel, pair_weight.reshape(PAIRS * BAND_LATS, NLON)
    )
    zero = jnp.zeros((SPECIES, 1), f32)
    lower = jnp.concatenate([zero, eddy_coupling[:, 1:]], 1)
    upper = jnp.concatenate([eddy_coupling[:, 1:], zero], 1)
    inv = 1.0 / (1.0 + lower + upper)
    lower, upper, inv = (
        jnp.broadcast_to(x[:, :, None], (SPECIES, NLEV, LANES)) for x in (lower * inv, upper * inv, inv)
    )

    halo = (south, north, below, above, wlat_n, wlev_up)
    density, bottom, top, first_row, last_row = transport_step(neutrals, winds, halo, False)
    halo = (
        up(last_row, "band"),
        down(first_row, "band"),
        up(top, "lev"),
        down(bottom, "lev"),
        wlat_n,
        wlev_up,
    )
    (mine,) = transport_step(density, winds, halo, True)
    owners = lax.axis_size("lev")
    other = lax.ppermute(mine, "lev", [(i, i ^ 1) for i in range(owners)])

    core = (lev % 2).reshape(1)
    outgoing = pack(core, starts, column_units, rows, mine, other)
    parity = [[2 * i + c for i in range(owners // 2)] for c in range(2)]
    got = lax.all_to_all(
        outgoing.reshape(16, MSG_ROWS, LANES), "lev", 0, 0, axis_index_groups=parity, tiled=True
    ).reshape(16 * MSG_ROWS, LANES)

    column_state, items = solve(own_units, table, got, lower, upper, inv, own_weights)
    items = lax.all_to_all(
        items.reshape(PEERS, ITEM_ROWS, LANES), ("band", "lev"), 0, 0, tiled=True
    ).reshape(PEERS * ITEM_ROWS, LANES)
    return column_state, lines(items, ion_yield, ion_spread, ion_loss)


def solution(mesh):
    placed = (
        P(None, "lev", "band", None),
        P("lev", "band", None),
        P("lev", "band", None),
        P("lev", "band", None),
        P(),
        P(None, "band", None),
        P(),
        P(),
        P(),
        P("band", None),
        P(),
        P(),
    )
    return jax.shard_map(
        on_device,
        mesh=mesh,
        in_specs=placed,
        out_specs=(P("band", "lev", None, None, None), P(("band", "lev"), None, None, None)),
        check_vma=False,
    )
```

```python
import functools

import jax
import jax.numpy as jnp
import numpy as np
from jax import lax
from jax.experimental import pallas as pl
from jax.experimental.pallas import tpu as pltpu
from jax.sharding import PartitionSpec as P

SPECIES = 5
IONS = 7
NLON = 2880
NLEV = 64
PAIRS = 32
BAND_LATS = 8
TSTEPS = 2
SWEEPS = 8
SECTIONS = 20
TUBE_COLS = 4
PEERS = 128
PEER_SLOTS = 3
COL_CAP = 1080
TUBE_CAP = 270
BAND_COLS = BAND_LATS * NLON
LINE_PTS = 512

LANES = 128
LON_BLOCKS = 23
LON_PAD = LON_BLOCKS * LANES
CHIP_LEVS = 4
PITCH = 9
LEVEL_PITCH = 257
PLANES = 12
GROUPS = 6
MSG_ROWS = 192
SLOT_BLOCKS = 9
SLOTS_PAD = SLOT_BLOCKS * LANES
ORDER_PAD = BAND_COLS + LANES
UNROLL = 64
ZERO_TUBE = SLOT_BLOCKS * 32
ITEM_ROWS = 16

f32 = jnp.float32
VMEM = pl.BlockSpec(memory_space=pltpu.VMEM)
HELD = pl.BlockSpec(memory_space=pltpu.VMEM)
SMEM = pl.BlockSpec(memory_space=pltpu.SMEM)
ANY = pl.BlockSpec(memory_space=pl.ANY)


def on_chip(shape, dtype=f32):
    return pltpu.VMEM(shape, dtype)


def call(kernel, out_shape, in_specs, out_specs, scratch=(), name=None, flops=0, vmem=16):
    run = pl.pallas_call(
        kernel,
        out_shape=out_shape,
        in_specs=in_specs,
        out_specs=out_specs,
        scratch_shapes=list(scratch),
        name=name,
        cost_estimate=pl.CostEstimate(flops=flops, bytes_accessed=1 << 20, transcendentals=0),
        compiler_params=pltpu.CompilerParams(vmem_limit_bytes=vmem * 1024 * 1024),
    )

    def placed(*args):
        return run(
            *(pltpu.with_memory_space_constraint(x, pltpu.VMEM) if spec is HELD else x for x, spec in zip(args, in_specs))
        )

    return placed


def sds(shape, dtype=f32):
    return jax.ShapeDtypeStruct(shape, dtype)


def upwind(courant_plus, courant_minus, upstream, downstream):
    return courant_plus * upstream + courant_minus * downstream


def edges_kernel(n_ref, wlat_ref, wlev_ref, low_ref, high_ref, first_ref, last_ref):
    low_ref[SPECIES] = wlev_ref[0]
    for j in range(2):
        first_ref[SPECIES, j] = wlat_ref[j, :1]

    @pl.loop(0, SPECIES)
    def _(s):
        low_ref[s] = n_ref[s, 0]
        high_ref[s] = n_ref[s, 1]
        for j in range(2):
            first_ref[s, j] = n_ref[s, j, :1]
            last_ref[s, j] = n_ref[s, j, BAND_LATS - 1 :]


def edges(density, wind_lat, wind_lev):
    return call(
        edges_kernel,
        (
            on_chip((SPECIES + 1, BAND_LATS, NLON)),
            on_chip((SPECIES, BAND_LATS, NLON)),
            on_chip((SPECIES + 1, 2, 1, NLON)),
            on_chip((SPECIES, 2, 1, NLON)),
        ),
        [HELD] * 3,
        (VMEM,) * 4,
        name="edges",
        flops=1_000_000,
    )(density, wind_lat, wind_lev)


def transport_kernel(
    n_ref, wlon_ref, wlat_ref, wlev_ref, south_ref, north_ref, below_ref, above_ref, wlat_n_ref, wlev_up_ref,
    *outs, last,
):
    def split(c):
        return jnp.maximum(c, 0.0), jnp.minimum(c, 0.0)

    def shift_west(x):
        return jnp.concatenate([x[:, NLON - 1 :], x[:, : NLON - 1]], axis=1)

    def shift_east(x):
        return jnp.concatenate([x[:, 1:], x[:, :1]], axis=1)

    for j in range(2):

        @pl.loop(0, SPECIES)
        def _(s):
            x = n_ref[s, j]
            flux = upwind(*split(wlon_ref[j]), shift_west(x), x)
            total = x + (flux - shift_east(flux))
            southern = jnp.concatenate([south_ref[s, j], x[: BAND_LATS - 1]], axis=0)
            flux = upwind(*split(wlat_ref[j]), southern, x)
            edge = upwind(*split(wlat_n_ref[SPECIES, j]), x[BAND_LATS - 1 :], north_ref[s, j])
            total = total + (flux - jnp.concatenate([flux[1:], edge], axis=0))
            beneath = below_ref[s] if j == 0 else n_ref[s, 0]
            overhead = n_ref[s, 1] if j == 0 else above_ref[s]
            over_wind = wlev_ref[1] if j == 0 else wlev_up_ref[SPECIES]
            flux = upwind(*split(wlev_ref[j]), beneath, x)
            total = total + (flux - upwind(*split(over_wind), x, overhead))
            if last:
                row = pl.multiple_of((j * SPECIES + s) * BAND_LATS, BAND_LATS)
                for blk in range(LON_BLOCKS):
                    wide = min(LANES, NLON - blk * LANES)
                    outs[0][blk, pl.ds(row, BAND_LATS), :wide] = total[:, blk * LANES : blk * LANES + wide]
            else:
                outs[0][s, j] = total
                outs[1 + j][s] = total
                outs[3][s, j] = total[:1]
                outs[4][s, j] = total[BAND_LATS - 1 :]


def transport_step(density, winds, halo, last):
    if last:
        out_shape = (on_chip((LON_BLOCKS, 2 * SPECIES * BAND_LATS, LANES)),)
    else:
        out_shape = (
            on_chip((SPECIES, 2, BAND_LATS, NLON)),
            on_chip((SPECIES, BAND_LATS, NLON)),
            on_chip((SPECIES, BAND_LATS, NLON)),
            on_chip((SPECIES, 2, 1, NLON)),
            on_chip((SPECIES, 2, 1, NLON)),
        )
    return call(
        functools.partial(transport_kernel, last=last),
        out_shape,
        [HELD] * 10,
        (VMEM,) * len(out_shape),
        name="transport",
        flops=4_000_000,
    )(density, *winds, *halo)


def prepare_kernel(
    units_ref, owner_ref, rows_ref, sel_ref, weight_ref, column_ref,
    table_ref, own_ref, coef_ref, count, blocks, table, picked,
):
    @pl.loop(0, PEERS * PEER_SLOTS // 8)
    def _(i):
        for k in range(8):
            table_ref[i * 8 + k] = ZERO_TUBE

    @pl.loop(0, PEERS // 8)
    def _(i):
        for k in range(8):
            count[i * 8 + k] = 0

    @pl.loop(0, units_ref[0])
    def _(u):
        dest = owner_ref[u]
        rank = count[dest]
        count[dest] = rank + 1
        table_ref[dest * PEER_SLOTS + rank] = u

    coef_ref[...] = jnp.broadcast_to(column_ref[...], coef_ref.shape)

    for blk in range(LON_BLOCKS):
        wide = min(LANES, NLON - blk * LANES)
        blocks[blk, :, :wide] = weight_ref[:, blk * LANES : blk * LANES + wide]

    @pl.loop(0, BAND_LATS)
    def _(lat):
        for g in range(6):
            parts = [
                blocks[min(4 * g + i, LON_BLOCKS - 1), pl.ds(lat + h * BAND_LATS, 8, stride=4 * BAND_LATS), :]
                for i in range(4)
                for h in range(4)
            ]
            start = pl.multiple_of((lat * 6 + g) * LANES, LANES)
            table[pl.ds(start, LANES), :] = jnp.concatenate(parts, axis=0).T

    @pl.loop(0, SLOTS_PAD // UNROLL)
    def _(step):
        base = pl.multiple_of(step * UNROLL, UNROLL)
        places = rows_ref.at[pl.ds(base, UNROLL)]
        for i in range(UNROLL):
            picked[pl.ds(base + i, 1), :] = table[pl.ds(places[i], 1), :]

    for blk in range(SLOT_BLOCKS):
        turned = picked[blk * LANES : (blk + 1) * LANES, :].T
        which = sel_ref[blk : blk + 1, :]
        kept = turned[:PAIRS]
        for i in range(1, 4):
            kept = jnp.where(which == i, turned[i * PAIRS : (i + 1) * PAIRS], kept)
        own_ref[blk] = kept


def prepare(units, owners, rows, sel, weights, column):
    return call(
        prepare_kernel,
        (
            sds((PEERS * PEER_SLOTS,), jnp.int32),
            on_chip((SLOT_BLOCKS, PAIRS, LANES)),
            on_chip((3 * SPECIES * NLEV, LANES)),
        ),
        [SMEM, SMEM, SMEM, VMEM, VMEM, VMEM],
        (SMEM, VMEM, VMEM),
        [
            pltpu.SMEM((PEERS,), jnp.int32),
            pltpu.VMEM((LON_BLOCKS, PAIRS * BAND_LATS, LANES), f32),
            pltpu.VMEM((BAND_LATS * 6 * LANES, LANES), f32),
            pltpu.VMEM((SLOTS_PAD, LANES), f32),
        ],
        name="prepare",
        flops=20_000_000,
    )(units, owners, rows, sel, weights, column)


def pack_kernel(core_ref, starts_ref, units_ref, order_hbm, mine_ref, other_ref, msg_ref, order, planes, table, sem):
    fetch = pltpu.make_async_copy(order_hbm, order, sem)
    fetch.start()
    core = core_ref[0]
    for source, side in ((mine_ref, core), (other_ref, 1 - core)):

        @pl.loop(0, LON_BLOCKS)
        def _(blk):
            for j in range(2):
                for i in range(PLANES):
                    row = ((2 * side + j) * PLANES + i) * PITCH
                    from_row = (j * SPECIES + i % SPECIES) * BAND_LATS
                    planes[blk, pl.ds(row, BAND_LATS), :] = source[blk, from_row : from_row + BAND_LATS, :]

    @pl.loop(0, LON_BLOCKS)
    def _(blk):
        for lat in range(BAND_LATS):
            parts = [
                planes[blk, pl.ds((jj * PLANES + first) * PITCH + lat, 8, stride=PITCH), :]
                for jj in range(CHIP_LEVS)
                for first in (0, 3, 1, 4)
            ]
            start = pl.multiple_of((lat * LON_BLOCKS + blk) * LANES, LANES)
            table[pl.ds(start, LANES), :] = jnp.concatenate(parts, axis=0).T

    fetch.wait()
    lane = lax.broadcasted_iota(jnp.int32, (1, LANES), 1)
    group_of = lax.div(lax.rem(lane, 32), SPECIES)

    @pl.loop(0, 16 * GROUPS)
    def _(turn):
        peer = lax.div(turn, GROUPS)
        group = turn - peer * GROUPS
        owner = 2 * peer + core
        live = jnp.clip(TUBE_COLS * units_ref[owner] - MSG_ROWS * group, 0, MSG_ROWS)
        first = TUBE_COLS * starts_ref[owner] + MSG_ROWS * group
        mask = group_of == group

        @pl.loop(0, lax.div(live + (UNROLL - 1), UNROLL))
        def _(step):
            base = first + step * UNROLL
            row = pl.multiple_of(peer * MSG_ROWS + step * UNROLL, UNROLL)
            places = order.at[pl.ds(base, UNROLL)]
            for i in range(UNROLL):
                value = table[pl.ds(places[i], 1), :]
                pltpu.store(msg_ref.at[pl.ds(row + i, 1), :], value, mask=mask)


def pack(core, starts, units, order, mine, other):
    return call(
        pack_kernel,
        on_chip((16 * MSG_ROWS, LANES)),
        [SMEM, SMEM, SMEM, ANY, HELD, HELD],
        VMEM,
        [
            pltpu.SMEM((ORDER_PAD,), jnp.int32),
            pltpu.VMEM((LON_BLOCKS, CHIP_LEVS * PLANES * PITCH, LANES), f32),
            pltpu.VMEM((BAND_LATS * LON_PAD, LANES), f32),
            pltpu.SemaphoreType.DMA,
        ],
        name="pack",
        flops=40_000_000,
        vmem=32,
    )(core, starts, units, order, mine, other)


def solve_kernel(
    units_ref, table_ref, got_ref, coef_ref, weight_ref, state_ref, items_ref, turned, natural, pairs, wide, tubes
):
    live = TUBE_COLS * units_ref[0]
    lane = lax.broadcasted_iota(jnp.int32, (1, LANES), 1)
    low = lane < 64
    quarter = lax.div(lane, 32)

    @pl.loop(0, 8)
    def _(i):
        for side in range(2):
            row = pl.multiple_of((2 * i + side) * MSG_ROWS, MSG_ROWS)
            out = i * LEVEL_PITCH + side * LANES
            turned[0, pl.ds(out, LANES), :] = got_ref[pl.ds(row, LANES), :].T
            rest = jnp.concatenate([got_ref[pl.ds(row + LANES, 64), :]] * 2, axis=0)
            turned[1, pl.ds(out, LANES), :] = rest.T

    for pair in range(3):

        @pl.loop(0, SPECIES)
        def _(s):
            def coefs(which):
                row = pl.multiple_of((which * SPECIES + s) * NLEV, NLEV)
                return [coef_ref[pl.ds(row + 8 * v, 8), :] for v in range(8)]

            lower, upper, inv = coefs(0), coefs(1), coefs(2)

            def levels(half, group, v):
                return turned[half, pl.ds(32 * v + group * SPECIES + s, 8, stride=LEVEL_PITCH), :]

            first = [levels(0, 2 * pair, v) for v in range(8)]
            odd = [pltpu.roll(levels(0, 2 * pair + 1, v), 64, axis=1) for v in range(8)]
            second = [jnp.where(low, levels(1, 2 * pair, v), odd[v]) for v in range(8)]
            third = [jnp.where(low, odd[v], levels(1, 2 * pair + 1, v)) for v in range(8)]
            for i, rhs in enumerate((first, second, third)):
                blk = 3 * pair + i
                scaled = [rhs[v] * inv[v] for v in range(8)]
                x = rhs
                for _ in range(SWEEPS):
                    beneath = [pltpu.roll(x[7], 1, axis=0)] + x[:7]
                    overhead = x[1:] + [pltpu.roll(x[0], 7, axis=0)]
                    x = [scaled[v] + lower[v] * beneath[v] + upper[v] * overhead[v] for v in range(8)]
                keep = lane + blk * LANES < live
                for v in range(8):
                    natural[i, pl.ds(v, 8, stride=PITCH), :] = jnp.where(keep, x[v], 0.0)
                width = min(LANES, COL_CAP - blk * LANES)
                for g in range(8):
                    state_ref[0, 0, s, g * 8 : g * 8 + 8, blk * LANES : blk * LANES + width] = natural[
                        i, g * PITCH : g * PITCH + 8, :width
                    ]
                for h in range(4):
                    weight = weight_ref[blk, 8 * h : 8 * h + 8, :]
                    paired = weight * x[2 * h] + (1.0 - weight) * x[2 * h + 1]
                    pairs[i, pl.ds(h, 8, stride=4), :] = paired
                wide[i] = jnp.concatenate([pairs[i]] * 4, axis=0).T
                item = wide[i, pl.ds(0, 32, stride=TUBE_COLS), :]
                for c in range(1, TUBE_COLS):
                    item = jnp.where(quarter == c, wide[i, pl.ds(c, 32, stride=TUBE_COLS), :], item)
                tubes[pl.ds(blk * 256 + s, 32, stride=8), :] = item

    tubes[ZERO_TUBE * 8 :, :] = jnp.zeros((8, LANES), f32)
    sub = lax.broadcasted_iota(jnp.int32, (8, LANES), 0)

    @pl.loop(0, PEERS // 4)
    def _(step):
        for i in range(4):
            d = step * 4 + i
            tiles = [
                tubes[pl.ds(pl.multiple_of(table_ref[d * PEER_SLOTS + r] * 8, 8), 8), :] for r in range(PEER_SLOTS)
            ]
            mid = pltpu.roll(tiles[1], 5, axis=0)
            top = pltpu.roll(tiles[2], 2, axis=0)
            row = pl.multiple_of(d * ITEM_ROWS, ITEM_ROWS)
            items_ref[pl.ds(row, 8), :] = jnp.where(sub < 5, tiles[0], mid)
            items_ref[pl.ds(row + 8, 8), :] = jnp.where(sub < 2, mid, jnp.where(sub < 7, top, 0.0))


def solve(units, table, got, coefs, weights):
    return call(
        solve_kernel,
        (sds((1, 1, SPECIES, NLEV, COL_CAP)), on_chip((PEERS * ITEM_ROWS, LANES))),
        [SMEM, SMEM] + [HELD] * 3,
        (VMEM, VMEM),
        [
            pltpu.VMEM((2, 8 * LEVEL_PITCH, LANES), f32),
            pltpu.VMEM((3, 8 * PITCH, LANES), f32),
            pltpu.VMEM((3, PAIRS, LANES), f32),
            pltpu.VMEM((3, LANES, LANES), f32),
            pltpu.VMEM((ZERO_TUBE * 8 + 8, LANES), f32),
        ],
        name="solve",
        flops=40_000_000,
    )(units, table, got, coefs, weights)


def halves(x):
    high = x.astype(jnp.bfloat16)
    return high, (x - high.astype(f32)).astype(jnp.bfloat16)


def product(x, high, low):
    x_high, x_low = halves(x)
    dot = functools.partial(jnp.dot, preferred_element_type=f32)
    return dot(x_high, high) + (dot(x_low, high) + dot(x_high, low))


def lines_kernel(
    items_ref, yield_ref, rates_ref, waves_ref, fwd_high, fwd_low, inv_high, inv_low, out_ref, spec_in, spec, mixed
):
    tubes = 32 * PEER_SLOTS
    for b in range(4):
        for s in range(SPECIES):
            for r in range(PEER_SLOTS):
                rows = items_ref[pl.ds(b * 32 * ITEM_ROWS + r * SPECIES + s, 32, stride=ITEM_ROWS), :]
                spec_in[b, pl.ds(s * tubes + r, 32, stride=PEER_SLOTS), :] = rows

    half = SPECIES * tubes // 2

    @pl.loop(0, 2)
    def _(step):
        row = pl.multiple_of(step * half, half)
        x = jnp.concatenate([spec_in[b, pl.ds(row, half), :] for b in range(4)], axis=1)
        spec[pl.ds(row, half), :] = product(x, fwd_high[...], fwd_low[...])

    waves = waves_ref[...]
    for i in range(IONS):
        keep = (1.0 - rates_ref[IONS + i]) + rates_ref[i] * waves
        gain = jnp.ones_like(waves)
        for _ in range(SECTIONS - 1):
            gain = gain * keep + 1.0
        total = (yield_ref[i * SPECIES] * gain) * spec[:tubes, :]
        for s in range(1, SPECIES):
            total = total + (yield_ref[i * SPECIES + s] * gain) * spec[s * tubes : (s + 1) * tubes, :]
        mixed[i] = total

    @pl.loop(0, IONS)
    def _(i):
        out_ref[0, i] = product(mixed[i], inv_high[...], inv_low[...])


def cosine_basis():
    k = np.arange(LINE_PTS)[:, None]
    n = np.arange(LINE_PTS)[None, :]
    basis = np.cos(np.pi * k * (n + 0.5) / LINE_PTS) * np.sqrt(2.0 / LINE_PTS)
    basis[0] *= np.sqrt(0.5)
    waves = 2.0 * np.cos(np.pi * np.arange(LINE_PTS) / LINE_PTS) - 2.0
    return basis, waves


def lines(items, ion_yield, ion_spread, ion_loss):
    basis, waves = cosine_basis()

    def parts(matrix):
        matrix = matrix.astype(np.float32)
        high = matrix.astype(jnp.bfloat16)
        low = (matrix - high.astype(np.float32)).astype(jnp.bfloat16)
        return jnp.asarray(high), jnp.asarray(low)

    waves = jnp.asarray(waves.astype(np.float32))[None]
    tubes = 32 * PEER_SLOTS
    by_ion = call(
        lines_kernel,
        sds((1, IONS, tubes, LINE_PTS)),
        [HELD, SMEM, SMEM] + [HELD] * 5,
        VMEM,
        [
            pltpu.VMEM((4, SPECIES * tubes, LANES), f32),
            pltpu.VMEM((SPECIES * tubes, LINE_PTS), f32),
            pltpu.VMEM((IONS, tubes, LINE_PTS), f32),
        ],
        name="lines",
        flops=2_000_000_000,
    )(items, ion_yield.reshape(-1), jnp.concatenate([ion_spread, ion_loss]), waves, *parts(basis.T), *parts(basis))
    return jnp.swapaxes(by_ion, 1, 2)


def up(x, axis):
    ends = lax.axis_size(axis) - 1
    return lax.ppermute(x, axis, [(i, i + 1) for i in range(ends)])


def down(x, axis):
    ends = lax.axis_size(axis) - 1
    return lax.ppermute(x, axis, [(i + 1, i) for i in range(ends)])


def on_device(
    neutrals,
    wind_lon,
    wind_lat,
    wind_lev,
    eddy_coupling,
    pair_weight,
    ion_yield,
    ion_spread,
    ion_loss,
    column_order,
    column_units,
    tube_owner,
):
    lev = lax.axis_index("lev")
    winds = (wind_lon, wind_lat, wind_lev)

    low, high, first, last = edges(neutrals, wind_lat, wind_lev)
    below, above = up(high, "lev"), down(low, "lev")
    south, north = up(last, "band"), down(first, "band")

    starts = jnp.cumsum(column_units) - column_units
    order = column_order[0]
    lat = jnp.zeros_like(order)
    for i in range(1, BAND_LATS):
        lat = lat + (order >= i * NLON).astype(jnp.int32)
    rows = jnp.pad(order + lat * (LON_PAD - NLON), (0, ORDER_PAD - BAND_COLS))
    own_units = column_units[lev].reshape(1)
    padded = jnp.pad(order, (0, SLOTS_PAD))
    own = lax.dynamic_slice(padded, (TUBE_COLS * starts[lev],), (SLOTS_PAD,))
    own_lat = jnp.zeros_like(own)
    for i in range(1, BAND_LATS):
        own_lat = own_lat + (own >= i * NLON).astype(jnp.int32)
    own_lon = own - own_lat * NLON
    own_rows = (own_lat * 6 + own_lon // 512) * LANES + own_lon % LANES
    own_sel = ((own_lon // LANES) % 4).reshape(SLOT_BLOCKS, LANES)
    zero = jnp.zeros((SPECIES, 1), f32)
    lower = jnp.concatenate([zero, eddy_coupling[:, 1:]], 1)
    upper = jnp.concatenate([eddy_coupling[:, 1:], zero], 1)
    inv = 1.0 / (1.0 + lower + upper)
    coefs = jnp.stack([lower * inv, upper * inv, inv]).reshape(3, SPECIES, 8, 8)
    table, own_weights, coefs = prepare(
        own_units,
        tube_owner[lev, :, 0],
        own_rows,
        own_sel,
        pair_weight.reshape(PAIRS * BAND_LATS, NLON),
        jnp.swapaxes(coefs, 2, 3).reshape(-1, 1),
    )

    halo = (south, north, below, above, north, above)
    density, bottom, top, first_row, last_row = transport_step(neutrals, winds, halo, False)
    halo = (up(last_row, "band"), down(first_row, "band"), up(top, "lev"), down(bottom, "lev"), north, above)
    (mine,) = transport_step(density, winds, halo, True)
    owners = lax.axis_size("lev")
    other = lax.ppermute(mine, "lev", [(i, i ^ 1) for i in range(owners)])

    core = (lev % 2).reshape(1)
    outgoing = pack(core, starts, column_units, rows, mine, other)
    parity = [[2 * i + c for i in range(owners // 2)] for c in range(2)]
    got = lax.all_to_all(
        outgoing.reshape(16, MSG_ROWS, LANES), "lev", 0, 0, axis_index_groups=parity, tiled=True
    ).reshape(16 * MSG_ROWS, LANES)

    column_state, items = solve(own_units, table, got, coefs, own_weights)
    items = lax.all_to_all(
        items.reshape(PEERS, ITEM_ROWS, LANES), ("band", "lev"), 0, 0, tiled=True
    ).reshape(PEERS * ITEM_ROWS, LANES)
    return column_state, lines(items, ion_yield, ion_spread, ion_loss)


def solution(mesh):
    placed = (
        P(None, "lev", "band", None),
        P("lev", "band", None),
        P("lev", "band", None),
        P("lev", "band", None),
        P(),
        P(None, "band", None),
        P(),
        P(),
        P(),
        P("band", None),
        P(),
        P(),
    )
    return jax.shard_map(
        on_device,
        mesh=mesh,
        in_specs=placed,
        out_specs=(P("band", "lev", None, None, None), P(("band", "lev"), None, None, None)),
        check_vma=False,
    )
```

```python
import functools

import jax
import jax.numpy as jnp
import numpy as np
from jax import lax
from jax.experimental import pallas as pl
from jax.experimental.pallas import tpu as pltpu
from jax.sharding import PartitionSpec as P

SPECIES = 5
IONS = 7
NLON = 2880
NLEV = 64
PAIRS = 32
BAND_LATS = 8
TSTEPS = 2
SWEEPS = 8
SECTIONS = 20
TUBE_COLS = 4
PEERS = 128
PEER_SLOTS = 3
COL_CAP = 1080
TUBE_CAP = 270
BAND_COLS = BAND_LATS * NLON
LINE_PTS = 512

LANES = 128
LON_BLOCKS = 23
LON_PAD = LON_BLOCKS * LANES
CHIP_LEVS = 4
PITCH = 9
LEVEL_PITCH = 257
PLANES = 12
GROUPS = 6
CHUNKS = 3
MSG_ROWS = 64
PEER_ROWS = CHUNKS * MSG_ROWS
CHUNK_BLOCKS = 3
CHUNK_SLOTS = GROUPS * MSG_ROWS
SLOT_BLOCKS = 9
SLOTS_PAD = SLOT_BLOCKS * LANES
ORDER_PAD = BAND_COLS + LANES
UNROLL = 64
ZERO_TUBE = SLOT_BLOCKS * 32
ITEM_ROWS = 16

f32 = jnp.float32
VMEM = pl.BlockSpec(memory_space=pltpu.VMEM)
HELD = pl.BlockSpec(memory_space=pltpu.VMEM)
SMEM = pl.BlockSpec(memory_space=pltpu.SMEM)
HBM = pl.BlockSpec(memory_space=pltpu.HBM)


def on_chip(shape, dtype=f32):
    return pltpu.VMEM(shape, dtype)


def call(kernel, out_shape, in_specs, out_specs, scratch=(), name=None, flops=0, vmem=16, aliases=()):
    run = pl.pallas_call(
        kernel,
        out_shape=out_shape,
        in_specs=in_specs,
        out_specs=out_specs,
        scratch_shapes=list(scratch),
        name=name,
        input_output_aliases=dict(aliases),
        cost_estimate=pl.CostEstimate(flops=flops, bytes_accessed=1 << 20, transcendentals=0),
        compiler_params=pltpu.CompilerParams(vmem_limit_bytes=vmem * 1024 * 1024),
    )

    def place(x, spec):
        space = pltpu.VMEM if spec is HELD else pltpu.HBM if spec is HBM else None
        return x if space is None else pltpu.with_memory_space_constraint(x, space)

    def placed(*args):
        return run(*(place(x, spec) for x, spec in zip(args, in_specs)))

    return placed


def sds(shape, dtype=f32):
    return jax.ShapeDtypeStruct(shape, dtype)


def upwind(courant_plus, courant_minus, upstream, downstream):
    return courant_plus * upstream + courant_minus * downstream


def edges_kernel(
    n_hbm, wlon_hbm, wlat_hbm, wlev_hbm,
    n_ref, wlon_ref, wlat_ref, wlev_ref, low_ref, high_ref, first_ref, last_ref, sems,
):
    fetches = [
        pltpu.make_async_copy(n_hbm.at[s], n_ref.at[s], sems.at[s]) for s in range(SPECIES)
    ]
    fetches.append(pltpu.make_async_copy(wlat_hbm, wlat_ref, sems.at[SPECIES]))
    fetches.append(pltpu.make_async_copy(wlev_hbm, wlev_ref, sems.at[SPECIES + 1]))
    fetches.append(pltpu.make_async_copy(wlon_hbm, wlon_ref, sems.at[SPECIES + 2]))
    for fetch in fetches:
        fetch.start()
    for fetch in fetches[:-1]:
        fetch.wait()
    low_ref[SPECIES] = wlev_ref[0]
    for j in range(2):
        first_ref[SPECIES, j] = wlat_ref[j, :1]

    @pl.loop(0, SPECIES)
    def _(s):
        low_ref[s] = n_ref[s, 0]
        high_ref[s] = n_ref[s, 1]
        for j in range(2):
            first_ref[s, j] = n_ref[s, j, :1]
            last_ref[s, j] = n_ref[s, j, BAND_LATS - 1 :]

    fetches[-1].wait()


def edges(density, wind_lon, wind_lat, wind_lev):
    return call(
        edges_kernel,
        (
            on_chip(density.shape),
            on_chip(wind_lon.shape),
            on_chip(wind_lat.shape),
            on_chip(wind_lev.shape),
            on_chip((SPECIES + 1, BAND_LATS, NLON)),
            on_chip((SPECIES, BAND_LATS, NLON)),
            on_chip((SPECIES + 1, 2, 1, NLON)),
            on_chip((SPECIES, 2, 1, NLON)),
        ),
        [HBM] * 4,
        (VMEM,) * 8,
        [pltpu.SemaphoreType.DMA((SPECIES + 3,))],
        name="edges",
        flops=1_000_000,
    )(density, wind_lon, wind_lat, wind_lev)


def transport_kernel(
    n_ref, wlon_ref, wlat_ref, wlev_ref, south_ref, north_ref, below_ref, above_ref, wlat_n_ref, wlev_up_ref,
    *outs, last,
):
    def split(c):
        return jnp.maximum(c, 0.0), jnp.minimum(c, 0.0)

    def shift_west(x):
        return jnp.concatenate([x[:, NLON - 1 :], x[:, : NLON - 1]], axis=1)

    def shift_east(x):
        return jnp.concatenate([x[:, 1:], x[:, :1]], axis=1)

    for j in range(2):

        @pl.loop(0, SPECIES)
        def _(s):
            x = n_ref[s, j]
            flux = upwind(*split(wlon_ref[j]), shift_west(x), x)
            total = x + (flux - shift_east(flux))
            southern = jnp.concatenate([south_ref[s, j], x[: BAND_LATS - 1]], axis=0)
            flux = upwind(*split(wlat_ref[j]), southern, x)
            edge = upwind(*split(wlat_n_ref[SPECIES, j]), x[BAND_LATS - 1 :], north_ref[s, j])
            total = total + (flux - jnp.concatenate([flux[1:], edge], axis=0))
            beneath = below_ref[s] if j == 0 else n_ref[s, 0]
            overhead = n_ref[s, 1] if j == 0 else above_ref[s]
            over_wind = wlev_ref[1] if j == 0 else wlev_up_ref[SPECIES]
            flux = upwind(*split(wlev_ref[j]), beneath, x)
            total = total + (flux - upwind(*split(over_wind), x, overhead))
            if last:
                row = pl.multiple_of((j * SPECIES + s) * BAND_LATS, BAND_LATS)
                for blk in range(LON_BLOCKS):
                    wide = min(LANES, NLON - blk * LANES)
                    outs[0][blk, pl.ds(row, BAND_LATS), :wide] = total[:, blk * LANES : blk * LANES + wide]
            else:
                outs[0][s, j] = total
                outs[1 + j][s] = total
                outs[3][s, j] = total[:1]
                outs[4][s, j] = total[BAND_LATS - 1 :]


def transport_step(density, winds, halo, last):
    if last:
        out_shape = (on_chip((LON_BLOCKS, 2 * SPECIES * BAND_LATS, LANES)),)
    else:
        out_shape = (
            on_chip((SPECIES, 2, BAND_LATS, NLON)),
            on_chip((SPECIES, BAND_LATS, NLON)),
            on_chip((SPECIES, BAND_LATS, NLON)),
            on_chip((SPECIES, 2, 1, NLON)),
            on_chip((SPECIES, 2, 1, NLON)),
        )
    return call(
        functools.partial(transport_kernel, last=last),
        out_shape,
        [HELD] * 10,
        (VMEM,) * len(out_shape),
        name="transport",
        flops=4_000_000,
    )(density, *winds, *halo)


def prepare_kernel(
    units_ref, owner_ref, rows_ref, sel_ref, weight_ref, column_ref,
    table_ref, own_ref, coef_ref, count, blocks, table, picked,
):
    @pl.loop(0, PEERS * PEER_SLOTS // 8)
    def _(i):
        for k in range(8):
            table_ref[i * 8 + k] = ZERO_TUBE

    @pl.loop(0, PEERS // 8)
    def _(i):
        for k in range(8):
            count[i * 8 + k] = 0

    @pl.loop(0, units_ref[0])
    def _(u):
        dest = owner_ref[u]
        rank = count[dest]
        count[dest] = rank + 1
        table_ref[dest * PEER_SLOTS + rank] = u

    coef_ref[...] = jnp.broadcast_to(column_ref[...], coef_ref.shape)

    for blk in range(LON_BLOCKS):
        wide = min(LANES, NLON - blk * LANES)
        blocks[blk, :, :wide] = weight_ref[:, blk * LANES : blk * LANES + wide]

    @pl.loop(0, BAND_LATS)
    def _(lat):
        for g in range(6):
            parts = [
                blocks[min(4 * g + i, LON_BLOCKS - 1), pl.ds(lat + h * BAND_LATS, 8, stride=4 * BAND_LATS), :]
                for i in range(4)
                for h in range(4)
            ]
            start = pl.multiple_of((lat * 6 + g) * LANES, LANES)
            table[pl.ds(start, LANES), :] = jnp.concatenate(parts, axis=0).T

    @pl.loop(0, SLOTS_PAD // UNROLL)
    def _(step):
        base = pl.multiple_of(step * UNROLL, UNROLL)
        places = rows_ref.at[pl.ds(base, UNROLL)]
        for i in range(UNROLL):
            picked[pl.ds(base + i, 1), :] = table[pl.ds(places[i], 1), :]

    for blk in range(SLOT_BLOCKS):
        turned = picked[blk * LANES : (blk + 1) * LANES, :].T
        which = sel_ref[blk : blk + 1, :]
        kept = turned[:PAIRS]
        for i in range(1, 4):
            kept = jnp.where(which == i, turned[i * PAIRS : (i + 1) * PAIRS], kept)
        own_ref[blk] = kept


def prepare(units, owners, rows, sel, weights, column):
    return call(
        prepare_kernel,
        (
            sds((PEERS * PEER_SLOTS,), jnp.int32),
            on_chip((SLOT_BLOCKS, PAIRS, LANES)),
            on_chip((3 * SPECIES * NLEV, LANES)),
        ),
        [SMEM, SMEM, SMEM, VMEM, VMEM, VMEM],
        (SMEM, VMEM, VMEM),
        [
            pltpu.SMEM((PEERS,), jnp.int32),
            pltpu.VMEM((LON_BLOCKS, PAIRS * BAND_LATS, LANES), f32),
            pltpu.VMEM((BAND_LATS * 6 * LANES, LANES), f32),
            pltpu.VMEM((SLOTS_PAD, LANES), f32),
        ],
        name="prepare",
        flops=20_000_000,
    )(units, owners, rows, sel, weights, column)


def turn_kernel(source_ref, *refs, side):
    table, planes = refs[-2:]
    half = LANES // 2

    @pl.loop(0, LON_BLOCKS)
    def _(blk):
        for j in range(2):
            for i in range(PLANES):
                from_row = (j * SPECIES + i % SPECIES) * BAND_LATS
                planes[blk, pl.ds((j * PLANES + i) * PITCH, BAND_LATS), :] = source_ref[
                    blk, from_row : from_row + BAND_LATS, :
                ]

    @pl.loop(0, LON_BLOCKS)
    def _(blk):
        for lat in range(BAND_LATS):
            parts = [
                planes[blk, pl.ds((j * PLANES + first) * PITCH + lat, 8, stride=PITCH), :]
                for j in range(2)
                for first in (0, 3, 1, 4)
            ]
            start = pl.multiple_of((lat * LON_BLOCKS + blk) * LANES, LANES)
            table[pl.ds(start, LANES), side * half : (side + 1) * half] = jnp.concatenate(parts, axis=0).T


def turn(side, source, *table):
    return call(
        functools.partial(turn_kernel, side=side),
        on_chip((BAND_LATS * LON_PAD, LANES)),
        [HELD] * (1 + len(table)),
        VMEM,
        [pltpu.VMEM((LON_BLOCKS, 2 * PLANES * PITCH, LANES), f32)],
        name="turn",
        flops=8_000_000,
        aliases={1: 0} if table else {},
    )(source, *table)


def pack_kernel(core_ref, starts_ref, units_ref, order_ref, table_ref, out_hbm, msg_ref, sems):
    core = core_ref[0]
    lane = lax.broadcasted_iota(jnp.int32, (1, LANES), 1)
    group_of = lax.div(lax.rem(lane, 32), SPECIES)

    def send(peer):
        rows = pl.ds(pl.multiple_of(peer * PEER_ROWS, PEER_ROWS), PEER_ROWS)
        return pltpu.make_async_copy(msg_ref.at[rows, :], out_hbm.at[rows, :], sems.at[peer])

    @pl.loop(0, 16)
    def _(peer):
        owner = 2 * peer + core
        live = TUBE_COLS * units_ref[owner]
        first = TUBE_COLS * starts_ref[owner]

        @pl.loop(0, lax.div(live + (MSG_ROWS - 1), MSG_ROWS))
        def _(piece):
            chunk = lax.div(piece, GROUPS)
            mask = group_of == piece - chunk * GROUPS
            row = pl.multiple_of(peer * PEER_ROWS + chunk * MSG_ROWS, MSG_ROWS)
            places = order_ref.at[pl.ds(first + piece * MSG_ROWS, MSG_ROWS)]
            for i in range(MSG_ROWS):
                value = table_ref[pl.ds(places[i], 1), :]
                pltpu.store(msg_ref.at[pl.ds(row + i, 1), :], value, mask=mask)

        send(peer).start()

    @pl.loop(0, 16)
    def _(peer):
        send(peer).wait()


def pack(core, starts, units, order, table):
    return call(
        pack_kernel,
        sds((16 * PEER_ROWS, LANES)),
        [SMEM, SMEM, SMEM, SMEM, HELD],
        HBM,
        [pltpu.VMEM((16 * PEER_ROWS, LANES), f32), pltpu.SemaphoreType.DMA((16,))],
        name="pack",
        flops=30_000_000,
    )(core, starts, units, order, table)


def solve_kernel(
    core_ref, units_ref, table_ref, got_ref, coef_ref, weight_ref, state_hbm, items_ref,
    turned, natural, pairs, wide, tubes, state, sems,
):
    core = core_ref[0]
    live = TUBE_COLS * units_ref[0]
    lane = lax.broadcasted_iota(jnp.int32, (1, LANES), 1)
    low = lane < 64
    quarter = lax.div(lane, 32)

    @pl.loop(0, 8)
    def _(i):
        for side in range(2):
            out = i * LEVEL_PITCH + side * LANES
            for chunk in range(CHUNKS):
                row = pl.multiple_of((2 * i + side) * PEER_ROWS + chunk * MSG_ROWS, MSG_ROWS)
                flipped = jnp.concatenate([got_ref[pl.ds(row, MSG_ROWS), :]] * 2, axis=0).T
                turned[chunk, pl.ds(out + 64 * core, 64), :] = flipped[:64]
                turned[chunk, pl.ds(out + 64 - 64 * core, 64), :] = flipped[64:]

    def leave(s):
        return pltpu.make_async_copy(state.at[s], state_hbm.at[0, 0, s], sems.at[s])

    @pl.loop(0, SPECIES)
    def _(s):
        def coefs(which):
            row = pl.multiple_of((which * SPECIES + s) * NLEV, NLEV)
            return [coef_ref[pl.ds(row + 8 * v, 8), :] for v in range(8)]

        lower, upper, inv = coefs(0), coefs(1), coefs(2)
        for blk in range(SLOT_BLOCKS):
            chunk, i = divmod(blk, 3)

            def levels(group, v):
                return turned[chunk, pl.ds(32 * v + group * SPECIES + s, 8, stride=LEVEL_PITCH), :]

            rhs = [jnp.where(low, levels(2 * i, v), levels(2 * i + 1, v)) for v in range(8)]
            scaled = [rhs[v] * inv[v] for v in range(8)]
            x = rhs
            for _ in range(SWEEPS):
                beneath = [pltpu.roll(x[7], 1, axis=0)] + x[:7]
                overhead = x[1:] + [pltpu.roll(x[0], 7, axis=0)]
                x = [scaled[v] + lower[v] * beneath[v] + upper[v] * overhead[v] for v in range(8)]
            keep = lane + blk * LANES < live
            for v in range(8):
                natural[i, pl.ds(v, 8, stride=PITCH), :] = jnp.where(keep, x[v], 0.0)
            width = min(LANES, COL_CAP - blk * LANES)
            for g in range(8):
                state[s, g * 8 : g * 8 + 8, blk * LANES : blk * LANES + width] = natural[
                    i, g * PITCH : g * PITCH + 8, :width
                ]
            for h in range(4):
                weight = weight_ref[blk, 8 * h : 8 * h + 8, :]
                paired = weight * x[2 * h] + (1.0 - weight) * x[2 * h + 1]
                pairs[i, pl.ds(h, 8, stride=4), :] = paired
            wide[i] = jnp.concatenate([pairs[i]] * 4, axis=0).T
            item = wide[i, pl.ds(0, 32, stride=TUBE_COLS), :]
            for c in range(1, TUBE_COLS):
                item = jnp.where(quarter == c, wide[i, pl.ds(c, 32, stride=TUBE_COLS), :], item)
            tubes[pl.ds(blk * 256 + s, 32, stride=8), :] = item
        leave(s).start()

    tubes[ZERO_TUBE * 8 :, :] = jnp.zeros((8, LANES), f32)
    sub = lax.broadcasted_iota(jnp.int32, (8, LANES), 0)

    @pl.loop(0, PEERS // 4)
    def _(step):
        for i in range(4):
            d = step * 4 + i
            tiles = [
                tubes[pl.ds(pl.multiple_of(table_ref[d * PEER_SLOTS + r] * 8, 8), 8), :] for r in range(PEER_SLOTS)
            ]
            mid = pltpu.roll(tiles[1], 5, axis=0)
            top = pltpu.roll(tiles[2], 2, axis=0)
            row = pl.multiple_of(d * ITEM_ROWS, ITEM_ROWS)
            items_ref[pl.ds(row, 8), :] = jnp.where(sub < 5, tiles[0], mid)
            items_ref[pl.ds(row + 8, 8), :] = jnp.where(sub < 2, mid, jnp.where(sub < 7, top, 0.0))

    for s in range(SPECIES):
        leave(s).wait()


def solve(core, units, table, got, coefs, weights):
    return call(
        solve_kernel,
        (sds((1, 1, SPECIES, NLEV, COL_CAP)), sds((PEERS * ITEM_ROWS, LANES))),
        [SMEM, SMEM, SMEM] + [HELD] * 3,
        (HBM, VMEM),
        [
            pltpu.VMEM((CHUNKS, 8 * LEVEL_PITCH, LANES), f32),
            pltpu.VMEM((3, 8 * PITCH, LANES), f32),
            pltpu.VMEM((3, PAIRS, LANES), f32),
            pltpu.VMEM((3, LANES, LANES), f32),
            pltpu.VMEM((ZERO_TUBE * 8 + 8, LANES), f32),
            pltpu.VMEM((SPECIES, NLEV, COL_CAP), f32),
            pltpu.SemaphoreType.DMA((SPECIES,)),
        ],
        name="solve",
        flops=40_000_000,
    )(core, units, table, got, coefs, weights)


def halves(x):
    high = x.astype(jnp.bfloat16)
    return high, (x - high.astype(f32)).astype(jnp.bfloat16)


def product(x, high, low):
    x_high, x_low = halves(x)
    dot = functools.partial(jnp.dot, preferred_element_type=f32)
    return dot(x_high, high) + (dot(x_low, high) + dot(x_high, low))


def lines_kernel(
    items_ref, yield_ref, rates_ref, waves_ref, fwd_high, fwd_low, inv_high, inv_low, out_hbm,
    spec_in, spec, mixed, done, sems,
):
    tubes = 32 * PEER_SLOTS
    for b in range(4):
        for s in range(SPECIES):
            for r in range(PEER_SLOTS):
                rows = items_ref[pl.ds(b * 32 * ITEM_ROWS + r * SPECIES + s, 32, stride=ITEM_ROWS), :]
                spec_in[b, pl.ds(s * tubes + r, 32, stride=PEER_SLOTS), :] = rows

    half = SPECIES * tubes // 2

    @pl.loop(0, 2)
    def _(step):
        row = pl.multiple_of(step * half, half)
        x = jnp.concatenate([spec_in[b, pl.ds(row, half), :] for b in range(4)], axis=1)
        spec[pl.ds(row, half), :] = product(x, fwd_high[...], fwd_low[...])

    waves = waves_ref[...]
    for i in range(IONS):
        keep = (1.0 - rates_ref[IONS + i]) + rates_ref[i] * waves
        gain = jnp.ones_like(waves)
        for _ in range(SECTIONS - 1):
            gain = gain * keep + 1.0
        total = (yield_ref[i * SPECIES] * gain) * spec[:tubes, :]
        for s in range(1, SPECIES):
            total = total + (yield_ref[i * SPECIES + s] * gain) * spec[s * tubes : (s + 1) * tubes, :]
        mixed[i] = total

    def leave(i):
        return pltpu.make_async_copy(done.at[i], out_hbm.at[0, i], sems.at[i])

    @pl.loop(0, IONS)
    def _(i):
        done[i] = product(mixed[i], inv_high[...], inv_low[...])
        leave(i).start()

    for i in range(IONS):
        leave(i).wait()


def cosine_basis():
    k = np.arange(LINE_PTS)[:, None]
    n = np.arange(LINE_PTS)[None, :]
    basis = np.cos(np.pi * k * (n + 0.5) / LINE_PTS) * np.sqrt(2.0 / LINE_PTS)
    basis[0] *= np.sqrt(0.5)
    waves = 2.0 * np.cos(np.pi * np.arange(LINE_PTS) / LINE_PTS) - 2.0
    return basis, waves


def lines(items, ion_yield, ion_spread, ion_loss):
    basis, waves = cosine_basis()

    def parts(matrix):
        matrix = matrix.astype(np.float32)
        high = matrix.astype(jnp.bfloat16)
        low = (matrix - high.astype(np.float32)).astype(jnp.bfloat16)
        return jnp.asarray(high), jnp.asarray(low)

    waves = jnp.asarray(waves.astype(np.float32))[None]
    tubes = 32 * PEER_SLOTS
    by_ion = call(
        lines_kernel,
        sds((1, IONS, tubes, LINE_PTS)),
        [HELD, SMEM, SMEM] + [HELD] * 5,
        HBM,
        [
            pltpu.VMEM((4, SPECIES * tubes, LANES), f32),
            pltpu.VMEM((SPECIES * tubes, LINE_PTS), f32),
            pltpu.VMEM((IONS, tubes, LINE_PTS), f32),
            pltpu.VMEM((IONS, tubes, LINE_PTS), f32),
            pltpu.SemaphoreType.DMA((IONS,)),
        ],
        name="lines",
        flops=2_000_000_000,
    )(items, ion_yield.reshape(-1), jnp.concatenate([ion_spread, ion_loss]), waves, *parts(basis.T), *parts(basis))
    return jnp.swapaxes(by_ion, 1, 2)


def up(x, axis):
    ends = lax.axis_size(axis) - 1
    return lax.ppermute(x, axis, [(i, i + 1) for i in range(ends)])


def down(x, axis):
    ends = lax.axis_size(axis) - 1
    return lax.ppermute(x, axis, [(i + 1, i) for i in range(ends)])


def on_device(
    neutrals,
    wind_lon,
    wind_lat,
    wind_lev,
    eddy_coupling,
    pair_weight,
    ion_yield,
    ion_spread,
    ion_loss,
    column_order,
    column_units,
    tube_owner,
):
    lev = lax.axis_index("lev")

    neutrals, *winds, low, high, first, last = edges(neutrals, wind_lon, wind_lat, wind_lev)
    below, above = up(high, "lev"), down(low, "lev")
    south, north = up(last, "band"), down(first, "band")

    starts = jnp.cumsum(column_units) - column_units
    order = column_order[0]
    lat = jnp.zeros_like(order)
    for i in range(1, BAND_LATS):
        lat = lat + (order >= i * NLON).astype(jnp.int32)
    rows = jnp.pad(order + lat * (LON_PAD - NLON), (0, ORDER_PAD - BAND_COLS))
    own_units = column_units[lev].reshape(1)
    padded = jnp.pad(order, (0, SLOTS_PAD))
    own = lax.dynamic_slice(padded, (TUBE_COLS * starts[lev],), (SLOTS_PAD,))
    own_lat = jnp.zeros_like(own)
    for i in range(1, BAND_LATS):
        own_lat = own_lat + (own >= i * NLON).astype(jnp.int32)
    own_lon = own - own_lat * NLON
    own_rows = (own_lat * 6 + own_lon // 512) * LANES + own_lon % LANES
    own_sel = ((own_lon // LANES) % 4).reshape(SLOT_BLOCKS, LANES)
    zero = jnp.zeros((SPECIES, 1), f32)
    lower = jnp.concatenate([zero, eddy_coupling[:, 1:]], 1)
    upper = jnp.concatenate([eddy_coupling[:, 1:], zero], 1)
    inv = 1.0 / (1.0 + lower + upper)
    coefs = jnp.stack([lower * inv, upper * inv, inv]).reshape(3, SPECIES, 8, 8)
    table, own_weights, coefs = prepare(
        own_units,
        tube_owner[lev, :, 0],
        own_rows,
        own_sel,
        pair_weight.reshape(PAIRS * BAND_LATS, NLON),
        jnp.swapaxes(coefs, 2, 3).reshape(-1, 1),
    )

    halo = (south, north, below, above, north, above)
    density, bottom, top, first_row, last_row = transport_step(neutrals, winds, halo, False)
    halo = (up(last_row, "band"), down(first_row, "band"), up(top, "lev"), down(bottom, "lev"), north, above)
    (mine,) = transport_step(density, winds, halo, True)
    owners = lax.axis_size("lev")
    other = lax.ppermute(mine, "lev", [(i, i ^ 1) for i in range(owners)])
    turned = turn(1, other, turn(0, mine))

    core = (lev % 2).reshape(1)
    parity = [[2 * i + c for i in range(owners // 2)] for c in range(2)]
    outgoing = pack(core, starts, column_units, rows, turned)
    got = lax.all_to_all(
        outgoing.reshape(16, PEER_ROWS, LANES), "lev", 0, 0, axis_index_groups=parity, tiled=True
    ).reshape(16 * PEER_ROWS, LANES)
    column_state, items = solve(core, own_units, table, got, coefs, own_weights)

    items = lax.all_to_all(
        items.reshape(PEERS, ITEM_ROWS, LANES), ("band", "lev"), 0, 0, tiled=True
    ).reshape(PEERS * ITEM_ROWS, LANES)
    return column_state, lines(items, ion_yield, ion_spread, ion_loss)


def solution(mesh):
    placed = (
        P(None, "lev", "band", None),
        P("lev", "band", None),
        P("lev", "band", None),
        P("lev", "band", None),
        P(),
        P(None, "band", None),
        P(),
        P(),
        P(),
        P("band", None),
        P(),
        P(),
    )
    return jax.shard_map(
        on_device,
        mesh=mesh,
        in_specs=placed,
        out_specs=(P("band", "lev", None, None, None), P(("band", "lev"), None, None, None)),
        check_vma=False,
    )
```

```python
import functools

import jax
import jax.numpy as jnp
import numpy as np
from jax import lax
from jax.experimental import pallas as pl
from jax.experimental.pallas import tpu as pltpu
from jax.sharding import PartitionSpec as P

SPECIES = 5
IONS = 7
NLON = 2880
NLEV = 64
PAIRS = 32
BAND_LATS = 8
TSTEPS = 2
SWEEPS = 8
SECTIONS = 20
TUBE_COLS = 4
PEERS = 128
PEER_SLOTS = 3
COL_CAP = 1080
TUBE_CAP = 270
BAND_COLS = BAND_LATS * NLON
LINE_PTS = 512

LANES = 128
LON_BLOCKS = 23
LON_PAD = LON_BLOCKS * LANES
CHIP_LEVS = 4
PITCH = 9
LEVEL_PITCH = 257
PLANES = 12
GROUPS = 6
CHUNKS = 3
MSG_ROWS = 64
PEER_ROWS = CHUNKS * MSG_ROWS
CHUNK_BLOCKS = 3
CHUNK_SLOTS = GROUPS * MSG_ROWS
SLOT_BLOCKS = 9
SLOTS_PAD = SLOT_BLOCKS * LANES
ORDER_PAD = BAND_COLS + 2 * LANES
UNROLL = 64
ZERO_TUBE = SLOT_BLOCKS * 32
ITEM_ROWS = 16

f32 = jnp.float32
VMEM = pl.BlockSpec(memory_space=pltpu.VMEM)
HELD = pl.BlockSpec(memory_space=pltpu.VMEM)
SMEM = pl.BlockSpec(memory_space=pltpu.SMEM)
HBM = pl.BlockSpec(memory_space=pltpu.HBM)


def on_chip(shape, dtype=f32):
    return pltpu.VMEM(shape, dtype)


def call(kernel, out_shape, in_specs, out_specs, scratch=(), name=None, flops=0, vmem=16):
    run = pl.pallas_call(
        kernel,
        out_shape=out_shape,
        in_specs=in_specs,
        out_specs=out_specs,
        scratch_shapes=list(scratch),
        name=name,
        cost_estimate=pl.CostEstimate(flops=flops, bytes_accessed=1 << 20, transcendentals=0),
        compiler_params=pltpu.CompilerParams(vmem_limit_bytes=vmem * 1024 * 1024),
    )

    def place(x, spec):
        space = pltpu.VMEM if spec is HELD else pltpu.HBM if spec is HBM else None
        return x if space is None else pltpu.with_memory_space_constraint(x, space)

    def placed(*args):
        return run(*(place(x, spec) for x, spec in zip(args, in_specs)))

    return placed


def sds(shape, dtype=f32):
    return jax.ShapeDtypeStruct(shape, dtype)


def upwind(courant_plus, courant_minus, upstream, downstream):
    return courant_plus * upstream + courant_minus * downstream


def edges_kernel(
    n_hbm, wlon_hbm, wlat_hbm, wlev_hbm,
    n_ref, wlon_ref, wlat_ref, wlev_ref, low_ref, high_ref, first_ref, last_ref, sems,
):
    fetches = [
        pltpu.make_async_copy(n_hbm.at[s], n_ref.at[s], sems.at[s]) for s in range(SPECIES)
    ]
    fetches.append(pltpu.make_async_copy(wlat_hbm, wlat_ref, sems.at[SPECIES]))
    fetches.append(pltpu.make_async_copy(wlev_hbm, wlev_ref, sems.at[SPECIES + 1]))
    fetches.append(pltpu.make_async_copy(wlon_hbm, wlon_ref, sems.at[SPECIES + 2]))
    for fetch in fetches:
        fetch.start()
    for fetch in fetches[:-1]:
        fetch.wait()
    low_ref[SPECIES] = wlev_ref[0]
    for j in range(2):
        first_ref[SPECIES, j] = wlat_ref[j, :1]

    @pl.loop(0, SPECIES)
    def _(s):
        low_ref[s] = n_ref[s, 0]
        high_ref[s] = n_ref[s, 1]
        for j in range(2):
            first_ref[s, j] = n_ref[s, j, :1]
            last_ref[s, j] = n_ref[s, j, BAND_LATS - 1 :]

    fetches[-1].wait()


def edges(density, wind_lon, wind_lat, wind_lev):
    return call(
        edges_kernel,
        (
            on_chip(density.shape),
            on_chip(wind_lon.shape),
            on_chip(wind_lat.shape),
            on_chip(wind_lev.shape),
            on_chip((SPECIES + 1, BAND_LATS, NLON)),
            on_chip((SPECIES, BAND_LATS, NLON)),
            on_chip((SPECIES + 1, 2, 1, NLON)),
            on_chip((SPECIES, 2, 1, NLON)),
        ),
        [HBM] * 4,
        (VMEM,) * 8,
        [pltpu.SemaphoreType.DMA((SPECIES + 3,))],
        name="edges",
        flops=1_000_000,
    )(density, wind_lon, wind_lat, wind_lev)


def transport_kernel(
    n_ref, wlon_ref, wlat_ref, wlev_ref, south_ref, north_ref, below_ref, above_ref, wlat_n_ref, wlev_up_ref,
    *outs, last,
):
    def split(c):
        return jnp.maximum(c, 0.0), jnp.minimum(c, 0.0)

    def shift_west(x):
        return jnp.concatenate([x[:, NLON - 1 :], x[:, : NLON - 1]], axis=1)

    def shift_east(x):
        return jnp.concatenate([x[:, 1:], x[:, :1]], axis=1)

    for j in range(2):

        @pl.loop(0, SPECIES)
        def _(s):
            x = n_ref[s, j]
            flux = upwind(*split(wlon_ref[j]), shift_west(x), x)
            total = x + (flux - shift_east(flux))
            southern = jnp.concatenate([south_ref[s, j], x[: BAND_LATS - 1]], axis=0)
            flux = upwind(*split(wlat_ref[j]), southern, x)
            edge = upwind(*split(wlat_n_ref[SPECIES, j]), x[BAND_LATS - 1 :], north_ref[s, j])
            total = total + (flux - jnp.concatenate([flux[1:], edge], axis=0))
            beneath = below_ref[s] if j == 0 else n_ref[s, 0]
            overhead = n_ref[s, 1] if j == 0 else above_ref[s]
            over_wind = wlev_ref[1] if j == 0 else wlev_up_ref[SPECIES]
            flux = upwind(*split(wlev_ref[j]), beneath, x)
            total = total + (flux - upwind(*split(over_wind), x, overhead))
            if last:
                row = pl.multiple_of((j * SPECIES + s) * BAND_LATS, BAND_LATS)
                for blk in range(LON_BLOCKS):
                    wide = min(LANES, NLON - blk * LANES)
                    outs[0][blk, pl.ds(row, BAND_LATS), :wide] = total[:, blk * LANES : blk * LANES + wide]
            else:
                outs[0][s, j] = total
                outs[1 + j][s] = total
                outs[3][s, j] = total[:1]
                outs[4][s, j] = total[BAND_LATS - 1 :]


def transport_step(density, winds, halo, last):
    if last:
        out_shape = (on_chip((LON_BLOCKS, 2 * SPECIES * BAND_LATS, LANES)),)
    else:
        out_shape = (
            on_chip((SPECIES, 2, BAND_LATS, NLON)),
            on_chip((SPECIES, BAND_LATS, NLON)),
            on_chip((SPECIES, BAND_LATS, NLON)),
            on_chip((SPECIES, 2, 1, NLON)),
            on_chip((SPECIES, 2, 1, NLON)),
        )
    return call(
        functools.partial(transport_kernel, last=last),
        out_shape,
        [HELD] * 10,
        (VMEM,) * len(out_shape),
        name="transport",
        flops=4_000_000,
    )(density, *winds, *halo)


def prepare_kernel(
    units_ref, owner_ref, rows_ref, sel_ref, weight_ref, column_ref,
    table_ref, own_ref, coef_ref, count, blocks, table, picked,
):
    @pl.loop(0, PEERS * PEER_SLOTS // 8)
    def _(i):
        for k in range(8):
            table_ref[i * 8 + k] = ZERO_TUBE

    @pl.loop(0, PEERS // 8)
    def _(i):
        for k in range(8):
            count[i * 8 + k] = 0

    @pl.loop(0, units_ref[0])
    def _(u):
        dest = owner_ref[u]
        rank = count[dest]
        count[dest] = rank + 1
        table_ref[dest * PEER_SLOTS + rank] = u

    coef_ref[...] = jnp.broadcast_to(column_ref[...], coef_ref.shape)

    for blk in range(LON_BLOCKS):
        wide = min(LANES, NLON - blk * LANES)
        blocks[blk, :, :wide] = weight_ref[:, blk * LANES : blk * LANES + wide]

    @pl.loop(0, BAND_LATS)
    def _(lat):
        for g in range(6):
            parts = [
                blocks[min(4 * g + i, LON_BLOCKS - 1), pl.ds(lat + h * BAND_LATS, 8, stride=4 * BAND_LATS), :]
                for i in range(4)
                for h in range(4)
            ]
            start = pl.multiple_of((lat * 6 + g) * LANES, LANES)
            table[pl.ds(start, LANES), :] = jnp.concatenate(parts, axis=0).T

    @pl.loop(0, SLOTS_PAD // UNROLL)
    def _(step):
        base = pl.multiple_of(step * UNROLL, UNROLL)
        places = rows_ref.at[pl.ds(base, UNROLL)]
        for i in range(UNROLL):
            picked[pl.ds(base + i, 1), :] = table[pl.ds(places[i], 1), :]

    for blk in range(SLOT_BLOCKS):
        turned = picked[blk * LANES : (blk + 1) * LANES, :].T
        which = sel_ref[blk : blk + 1, :]
        kept = turned[:PAIRS]
        for i in range(1, 4):
            kept = jnp.where(which == i, turned[i * PAIRS : (i + 1) * PAIRS], kept)
        own_ref[blk] = kept


def prepare(units, owners, rows, sel, weights, column):
    return call(
        prepare_kernel,
        (
            sds((PEERS * PEER_SLOTS,), jnp.int32),
            on_chip((SLOT_BLOCKS, PAIRS, LANES)),
            on_chip((3 * SPECIES * NLEV, LANES)),
        ),
        [SMEM, SMEM, SMEM, VMEM, VMEM, VMEM],
        (SMEM, VMEM, VMEM),
        [
            pltpu.SMEM((PEERS,), jnp.int32),
            pltpu.VMEM((LON_BLOCKS, PAIRS * BAND_LATS, LANES), f32),
            pltpu.VMEM((BAND_LATS * 6 * LANES, LANES), f32),
            pltpu.VMEM((SLOTS_PAD, LANES), f32),
        ],
        name="prepare",
        flops=20_000_000,
    )(units, owners, rows, sel, weights, column)


def pack_kernel(
    core_ref, starts_ref, units_ref, order_ref, mine_ref, other_ref, out_hbm, planes, table_ref, msg_ref, sems
):
    @pl.loop(0, LON_BLOCKS)
    def _(blk):
        for side, source in enumerate((mine_ref, other_ref)):
            for j in range(2):
                for i in range(PLANES):
                    from_row = (j * SPECIES + i % SPECIES) * BAND_LATS
                    planes[blk, pl.ds(((2 * side + j) * PLANES + i) * PITCH, BAND_LATS), :] = source[
                        blk, from_row : from_row + BAND_LATS, :
                    ]

    @pl.loop(0, LON_BLOCKS)
    def _(blk):
        for lat in range(BAND_LATS):
            parts = [
                planes[blk, pl.ds((jj * PLANES + first) * PITCH + lat, 8, stride=PITCH), :]
                for jj in range(CHIP_LEVS)
                for first in (0, 3, 1, 4)
            ]
            start = pl.multiple_of((lat * LON_BLOCKS + blk) * LANES, LANES)
            table_ref[pl.ds(start, LANES), :] = jnp.concatenate(parts, axis=0).T

    core = core_ref[0]
    lane = lax.broadcasted_iota(jnp.int32, (1, LANES), 1)
    group_of = lax.div(lax.rem(lane, 32), SPECIES)

    def send(peer):
        rows = pl.ds(pl.multiple_of(peer * PEER_ROWS, PEER_ROWS), PEER_ROWS)
        return pltpu.make_async_copy(msg_ref.at[rows, :], out_hbm.at[rows, :], sems.at[peer])

    @pl.loop(0, 16)
    def _(peer):
        owner = 2 * peer + core
        live = TUBE_COLS * units_ref[owner]
        first = TUBE_COLS * starts_ref[owner]

        @pl.loop(0, lax.div(live + (MSG_ROWS - 1), MSG_ROWS))
        def _(piece):
            chunk = lax.div(piece, GROUPS)
            mask = group_of == piece - chunk * GROUPS
            row = pl.multiple_of(peer * PEER_ROWS + chunk * MSG_ROWS, MSG_ROWS)
            base = first + piece * MSG_ROWS
            for i in range(MSG_ROWS):
                place = order_ref.at[pl.ds(i, ORDER_PAD - MSG_ROWS)][base]
                value = table_ref[pl.ds(place, 1), :]
                pltpu.store(msg_ref.at[pl.ds(row + i, 1), :], value, mask=mask)

        send(peer).start()

    @pl.loop(0, 16)
    def _(peer):
        send(peer).wait()


def pack(core, starts, units, order, mine, other):
    return call(
        pack_kernel,
        sds((16 * PEER_ROWS, LANES)),
        [SMEM, SMEM, SMEM, SMEM, HELD, HELD],
        HBM,
        [
            pltpu.VMEM((LON_BLOCKS, CHIP_LEVS * PLANES * PITCH, LANES), f32),
            pltpu.VMEM((BAND_LATS * LON_PAD, LANES), f32),
            pltpu.VMEM((16 * PEER_ROWS, LANES), f32),
            pltpu.SemaphoreType.DMA((16,)),
        ],
        name="pack",
        flops=30_000_000,
        vmem=32,
    )(core, starts, units, order, mine, other)


def solve_kernel(
    core_ref, units_ref, table_ref, got_ref, coef_ref, weight_ref, state_hbm, items_ref,
    turned, natural, pairs, wide, tubes, state, sems,
):
    core = core_ref[0]
    live = TUBE_COLS * units_ref[0]
    lane = lax.broadcasted_iota(jnp.int32, (1, LANES), 1)
    low = lane < 64
    quarter = lax.div(lane, 32)

    @pl.loop(0, 8)
    def _(i):
        for side in range(2):
            out = i * LEVEL_PITCH + side * LANES
            for chunk in range(CHUNKS):
                row = pl.multiple_of((2 * i + side) * PEER_ROWS + chunk * MSG_ROWS, MSG_ROWS)
                flipped = jnp.concatenate([got_ref[pl.ds(row, MSG_ROWS), :]] * 2, axis=0).T
                turned[chunk, pl.ds(out + 64 * core, 64), :] = flipped[:64]
                turned[chunk, pl.ds(out + 64 - 64 * core, 64), :] = flipped[64:]

    def leave(s):
        return pltpu.make_async_copy(state.at[s], state_hbm.at[0, 0, s], sems.at[s])

    @pl.loop(0, SPECIES)
    def _(s):
        def coefs(which):
            row = pl.multiple_of((which * SPECIES + s) * NLEV, NLEV)
            return [coef_ref[pl.ds(row + 8 * v, 8), :] for v in range(8)]

        lower, upper, inv = coefs(0), coefs(1), coefs(2)
        for blk in range(SLOT_BLOCKS):
            chunk, i = divmod(blk, 3)

            def levels(group, v):
                return turned[chunk, pl.ds(32 * v + group * SPECIES + s, 8, stride=LEVEL_PITCH), :]

            rhs = [jnp.where(low, levels(2 * i, v), levels(2 * i + 1, v)) for v in range(8)]
            scaled = [rhs[v] * inv[v] for v in range(8)]
            x = rhs
            for _ in range(SWEEPS):
                beneath = [pltpu.roll(x[7], 1, axis=0)] + x[:7]
                overhead = x[1:] + [pltpu.roll(x[0], 7, axis=0)]
                x = [scaled[v] + lower[v] * beneath[v] + upper[v] * overhead[v] for v in range(8)]
            keep = lane + blk * LANES < live
            for v in range(8):
                natural[i, pl.ds(v, 8, stride=PITCH), :] = jnp.where(keep, x[v], 0.0)
            width = min(LANES, COL_CAP - blk * LANES)
            for g in range(8):
                state[s, g * 8 : g * 8 + 8, blk * LANES : blk * LANES + width] = natural[
                    i, g * PITCH : g * PITCH + 8, :width
                ]
            for h in range(4):
                weight = weight_ref[blk, 8 * h : 8 * h + 8, :]
                paired = weight * x[2 * h] + (1.0 - weight) * x[2 * h + 1]
                pairs[i, pl.ds(h, 8, stride=4), :] = paired
            wide[i] = jnp.concatenate([pairs[i]] * 4, axis=0).T
            item = wide[i, pl.ds(0, 32, stride=TUBE_COLS), :]
            for c in range(1, TUBE_COLS):
                item = jnp.where(quarter == c, wide[i, pl.ds(c, 32, stride=TUBE_COLS), :], item)
            tubes[pl.ds(blk * 256 + s, 32, stride=8), :] = item
        leave(s).start()

    tubes[ZERO_TUBE * 8 :, :] = jnp.zeros((8, LANES), f32)
    sub = lax.broadcasted_iota(jnp.int32, (8, LANES), 0)

    @pl.loop(0, PEERS // 4)
    def _(step):
        for i in range(4):
            d = step * 4 + i
            tiles = [
                tubes[pl.ds(pl.multiple_of(table_ref[d * PEER_SLOTS + r] * 8, 8), 8), :] for r in range(PEER_SLOTS)
            ]
            mid = pltpu.roll(tiles[1], 5, axis=0)
            top = pltpu.roll(tiles[2], 2, axis=0)
            row = pl.multiple_of(d * ITEM_ROWS, ITEM_ROWS)
            items_ref[pl.ds(row, 8), :] = jnp.where(sub < 5, tiles[0], mid)
            items_ref[pl.ds(row + 8, 8), :] = jnp.where(sub < 2, mid, jnp.where(sub < 7, top, 0.0))

    for s in range(SPECIES):
        leave(s).wait()


def solve(core, units, table, got, coefs, weights):
    return call(
        solve_kernel,
        (sds((1, 1, SPECIES, NLEV, COL_CAP)), sds((PEERS * ITEM_ROWS, LANES))),
        [SMEM, SMEM, SMEM] + [HELD] * 3,
        (HBM, VMEM),
        [
            pltpu.VMEM((CHUNKS, 8 * LEVEL_PITCH, LANES), f32),
            pltpu.VMEM((3, 8 * PITCH, LANES), f32),
            pltpu.VMEM((3, PAIRS, LANES), f32),
            pltpu.VMEM((3, LANES, LANES), f32),
            pltpu.VMEM((ZERO_TUBE * 8 + 8, LANES), f32),
            pltpu.VMEM((SPECIES, NLEV, COL_CAP), f32),
            pltpu.SemaphoreType.DMA((SPECIES,)),
        ],
        name="solve",
        flops=40_000_000,
    )(core, units, table, got, coefs, weights)


def halves(x):
    high = x.astype(jnp.bfloat16)
    return high, (x - high.astype(f32)).astype(jnp.bfloat16)


def product(x, high, low):
    x_high, x_low = halves(x)
    dot = functools.partial(jnp.dot, preferred_element_type=f32)
    return dot(x_high, high) + (dot(x_low, high) + dot(x_high, low))


def lines_kernel(
    items_ref, yield_ref, rates_ref, waves_ref, fwd_high, fwd_low, inv_high, inv_low, out_hbm,
    spec_in, spec, mixed, done, sems,
):
    tubes = 32 * PEER_SLOTS
    for b in range(4):
        for s in range(SPECIES):
            for r in range(PEER_SLOTS):
                rows = items_ref[pl.ds(b * 32 * ITEM_ROWS + r * SPECIES + s, 32, stride=ITEM_ROWS), :]
                spec_in[b, pl.ds(s * tubes + r, 32, stride=PEER_SLOTS), :] = rows

    half = SPECIES * tubes // 2

    @pl.loop(0, 2)
    def _(step):
        row = pl.multiple_of(step * half, half)
        x = jnp.concatenate([spec_in[b, pl.ds(row, half), :] for b in range(4)], axis=1)
        spec[pl.ds(row, half), :] = product(x, fwd_high[...], fwd_low[...])

    waves = waves_ref[...]
    for i in range(IONS):
        keep = (1.0 - rates_ref[IONS + i]) + rates_ref[i] * waves
        gain = jnp.ones_like(waves)
        for _ in range(SECTIONS - 1):
            gain = gain * keep + 1.0
        total = (yield_ref[i * SPECIES] * gain) * spec[:tubes, :]
        for s in range(1, SPECIES):
            total = total + (yield_ref[i * SPECIES + s] * gain) * spec[s * tubes : (s + 1) * tubes, :]
        mixed[i] = total

    def leave(i):
        return pltpu.make_async_copy(done.at[i], out_hbm.at[0, i], sems.at[i])

    @pl.loop(0, IONS)
    def _(i):
        done[i] = product(mixed[i], inv_high[...], inv_low[...])
        leave(i).start()

    for i in range(IONS):
        leave(i).wait()


def cosine_basis():
    k = np.arange(LINE_PTS)[:, None]
    n = np.arange(LINE_PTS)[None, :]
    basis = np.cos(np.pi * k * (n + 0.5) / LINE_PTS) * np.sqrt(2.0 / LINE_PTS)
    basis[0] *= np.sqrt(0.5)
    waves = 2.0 * np.cos(np.pi * np.arange(LINE_PTS) / LINE_PTS) - 2.0
    return basis, waves


def lines(items, ion_yield, ion_spread, ion_loss):
    basis, waves = cosine_basis()

    def parts(matrix):
        matrix = matrix.astype(np.float32)
        high = matrix.astype(jnp.bfloat16)
        low = (matrix - high.astype(np.float32)).astype(jnp.bfloat16)
        return jnp.asarray(high), jnp.asarray(low)

    waves = jnp.asarray(waves.astype(np.float32))[None]
    tubes = 32 * PEER_SLOTS
    by_ion = call(
        lines_kernel,
        sds((1, IONS, tubes, LINE_PTS)),
        [HELD, SMEM, SMEM] + [HELD] * 5,
        HBM,
        [
            pltpu.VMEM((4, SPECIES * tubes, LANES), f32),
            pltpu.VMEM((SPECIES * tubes, LINE_PTS), f32),
            pltpu.VMEM((IONS, tubes, LINE_PTS), f32),
            pltpu.VMEM((IONS, tubes, LINE_PTS), f32),
            pltpu.SemaphoreType.DMA((IONS,)),
        ],
        name="lines",
        flops=2_000_000_000,
    )(items, ion_yield.reshape(-1), jnp.concatenate([ion_spread, ion_loss]), waves, *parts(basis.T), *parts(basis))
    return jnp.swapaxes(by_ion, 1, 2)


def up(x, axis):
    ends = lax.axis_size(axis) - 1
    return lax.ppermute(x, axis, [(i, i + 1) for i in range(ends)])


def down(x, axis):
    ends = lax.axis_size(axis) - 1
    return lax.ppermute(x, axis, [(i + 1, i) for i in range(ends)])


def on_device(
    neutrals,
    wind_lon,
    wind_lat,
    wind_lev,
    eddy_coupling,
    pair_weight,
    ion_yield,
    ion_spread,
    ion_loss,
    column_order,
    column_units,
    tube_owner,
):
    lev = lax.axis_index("lev")

    neutrals, *winds, low, high, first, last = edges(neutrals, wind_lon, wind_lat, wind_lev)
    below, above = up(high, "lev"), down(low, "lev")
    south, north = up(last, "band"), down(first, "band")

    starts = jnp.cumsum(column_units) - column_units
    order = column_order[0]
    lat = jnp.zeros_like(order)
    for i in range(1, BAND_LATS):
        lat = lat + (order >= i * NLON).astype(jnp.int32)
    rows = jnp.pad(order + lat * (LON_PAD - NLON), (0, ORDER_PAD - BAND_COLS))
    own_units = column_units[lev].reshape(1)
    padded = jnp.pad(order, (0, SLOTS_PAD))
    own = lax.dynamic_slice(padded, (TUBE_COLS * starts[lev],), (SLOTS_PAD,))
    own_lat = jnp.zeros_like(own)
    for i in range(1, BAND_LATS):
        own_lat = own_lat + (own >= i * NLON).astype(jnp.int32)
    own_lon = own - own_lat * NLON
    own_rows = (own_lat * 6 + own_lon // 512) * LANES + own_lon % LANES
    own_sel = ((own_lon // LANES) % 4).reshape(SLOT_BLOCKS, LANES)
    zero = jnp.zeros((SPECIES, 1), f32)
    lower = jnp.concatenate([zero, eddy_coupling[:, 1:]], 1)
    upper = jnp.concatenate([eddy_coupling[:, 1:], zero], 1)
    inv = 1.0 / (1.0 + lower + upper)
    coefs = jnp.stack([lower * inv, upper * inv, inv]).reshape(3, SPECIES, 8, 8)
    table, own_weights, coefs = prepare(
        own_units,
        tube_owner[lev, :, 0],
        own_rows,
        own_sel,
        pair_weight.reshape(PAIRS * BAND_LATS, NLON),
        jnp.swapaxes(coefs, 2, 3).reshape(-1, 1),
    )

    halo = (south, north, below, above, north, above)
    density, bottom, top, first_row, last_row = transport_step(neutrals, winds, halo, False)
    halo = (up(last_row, "band"), down(first_row, "band"), up(top, "lev"), down(bottom, "lev"), north, above)
    (mine,) = transport_step(density, winds, halo, True)
    owners = lax.axis_size("lev")
    other = lax.ppermute(mine, "lev", [(i, i ^ 1) for i in range(owners)])

    core = (lev % 2).reshape(1)
    parity = [[2 * i + c for i in range(owners // 2)] for c in range(2)]
    outgoing = pack(core, starts, column_units, rows, mine, other)
    got = lax.all_to_all(
        outgoing.reshape(16, PEER_ROWS, LANES), "lev", 0, 0, axis_index_groups=parity, tiled=True
    ).reshape(16 * PEER_ROWS, LANES)
    column_state, items = solve(core, own_units, table, got, coefs, own_weights)

    items = lax.all_to_all(
        items.reshape(PEERS, ITEM_ROWS, LANES), ("band", "lev"), 0, 0, tiled=True
    ).reshape(PEERS * ITEM_ROWS, LANES)
    return column_state, lines(items, ion_yield, ion_spread, ion_loss)


def solution(mesh):
    placed = (
        P(None, "lev", "band", None),
        P("lev", "band", None),
        P("lev", "band", None),
        P("lev", "band", None),
        P(),
        P(None, "band", None),
        P(),
        P(),
        P(),
        P("band", None),
        P(),
        P(),
    )
    return jax.shard_map(
        on_device,
        mesh=mesh,
        in_specs=placed,
        out_specs=(P("band", "lev", None, None, None), P(("band", "lev"), None, None, None)),
        check_vma=False,
    )
```

```python
import functools

import jax
import jax.numpy as jnp
import numpy as np
from jax import lax
from jax.experimental import pallas as pl
from jax.experimental.pallas import tpu as pltpu
from jax.sharding import PartitionSpec as P

SPECIES = 5
IONS = 7
NLON = 2880
NLEV = 64
PAIRS = 32
BAND_LATS = 8
TSTEPS = 2
SWEEPS = 8
SECTIONS = 20
TUBE_COLS = 4
PEERS = 128
PEER_SLOTS = 3
COL_CAP = 1080
TUBE_CAP = 270
BAND_COLS = BAND_LATS * NLON
LINE_PTS = 512

LANES = 128
LON_BLOCKS = 23
LON_PAD = LON_BLOCKS * LANES
CHIP_LEVS = 4
PITCH = 9
LEVEL_PITCH = 257
PLANES = 12
GROUPS = 6
CHUNKS = 3
MSG_ROWS = 64
PEER_ROWS = CHUNKS * MSG_ROWS
CHUNK_BLOCKS = 3
CHUNK_SLOTS = GROUPS * MSG_ROWS
SLOT_BLOCKS = 9
SLOTS_PAD = SLOT_BLOCKS * LANES
ORDER_PAD = BAND_COLS + 2 * LANES
UNROLL = 64
ZERO_TUBE = SLOT_BLOCKS * 32
ITEM_ROWS = 16

f32 = jnp.float32
VMEM = pl.BlockSpec(memory_space=pltpu.VMEM)
HELD = pl.BlockSpec(memory_space=pltpu.VMEM)
SMEM = pl.BlockSpec(memory_space=pltpu.SMEM)
HBM = pl.BlockSpec(memory_space=pltpu.HBM)


def on_chip(shape, dtype=f32):
    return pltpu.VMEM(shape, dtype)


def call(kernel, out_shape, in_specs, out_specs, scratch=(), name=None, flops=0, vmem=16):
    run = pl.pallas_call(
        kernel,
        out_shape=out_shape,
        in_specs=in_specs,
        out_specs=out_specs,
        scratch_shapes=list(scratch),
        name=name,
        cost_estimate=pl.CostEstimate(flops=flops, bytes_accessed=1 << 20, transcendentals=0),
        compiler_params=pltpu.CompilerParams(vmem_limit_bytes=vmem * 1024 * 1024),
    )

    def place(x, spec):
        space = pltpu.VMEM if spec is HELD else pltpu.HBM if spec is HBM else None
        return x if space is None else pltpu.with_memory_space_constraint(x, space)

    def placed(*args):
        return run(*(place(x, spec) for x, spec in zip(args, in_specs)))

    return placed


def sds(shape, dtype=f32):
    return jax.ShapeDtypeStruct(shape, dtype)


def upwind(courant_plus, courant_minus, upstream, downstream):
    return courant_plus * upstream + courant_minus * downstream


def edges_kernel(
    side_ref, n_hbm, wlon_hbm, wlat_hbm, wlev_hbm,
    n_ref, wlon_ref, wlat_ref, wlev_ref, inner_ref, outer_ref, row_ref, far_row_ref, sems,
):
    fetches = [
        pltpu.make_async_copy(n_hbm.at[s], n_ref.at[s], sems.at[s]) for s in range(SPECIES)
    ]
    fetches.append(pltpu.make_async_copy(wlat_hbm, wlat_ref, sems.at[SPECIES]))
    fetches.append(pltpu.make_async_copy(wlev_hbm, wlev_ref, sems.at[SPECIES + 1]))
    fetches.append(pltpu.make_async_copy(wlon_hbm, wlon_ref, sems.at[SPECIES + 2]))
    for fetch in fetches:
        fetch.start()
    for fetch in fetches[:-1]:
        fetch.wait()
    core, odd = side_ref[0], side_ref[1] == 1
    inner_ref[SPECIES] = wlev_ref[0]
    outer_ref[SPECIES] = wlev_ref[0]
    for j in range(2):
        row_ref[SPECIES, j] = wlat_ref[j, :1]
        far_row_ref[SPECIES, j] = wlat_ref[j, :1]

    @pl.loop(0, SPECIES)
    def _(s):
        inner_ref[s] = n_ref[s, 1 - core]
        outer_ref[s] = n_ref[s, core]
        for j in range(2):
            first, last = n_ref[s, j, :1], n_ref[s, j, BAND_LATS - 1 :]
            row_ref[s, j] = jnp.where(odd, first, last)
            far_row_ref[s, j] = jnp.where(odd, last, first)

    fetches[-1].wait()


def edges(side, density, wind_lon, wind_lat, wind_lev):
    return call(
        edges_kernel,
        (
            on_chip(density.shape),
            on_chip(wind_lon.shape),
            on_chip(wind_lat.shape),
            on_chip(wind_lev.shape),
            on_chip((SPECIES + 1, BAND_LATS, NLON)),
            on_chip((SPECIES + 1, BAND_LATS, NLON)),
            on_chip((SPECIES + 1, 2, 1, NLON)),
            on_chip((SPECIES + 1, 2, 1, NLON)),
        ),
        [SMEM] + [HBM] * 4,
        (VMEM,) * 8,
        [pltpu.SemaphoreType.DMA((SPECIES + 3,))],
        name="edges",
        flops=1_000_000,
    )(side, density, wind_lon, wind_lat, wind_lev)


def transport_kernel(side_ref, n_ref, wlon_ref, wlat_ref, wlev_ref, *refs, last):
    inner_ref, outer_ref, row_ref, far_row_ref = refs[:4]
    inner_wind, outer_wind, row_wind, far_row_wind = refs[4:8]
    outs = refs[8:]
    core, odd = side_ref[0], side_ref[1] == 1
    south_core = core == 0

    def split(c):
        return jnp.maximum(c, 0.0), jnp.minimum(c, 0.0)

    def shift_west(x):
        return jnp.concatenate([x[:, NLON - 1 :], x[:, : NLON - 1]], axis=1)

    def shift_east(x):
        return jnp.concatenate([x[:, 1:], x[:, :1]], axis=1)

    for j in range(2):

        @pl.loop(0, SPECIES)
        def _(s):
            x = n_ref[s, j]
            flux = upwind(*split(wlon_ref[j]), shift_west(x), x)
            total = x + (flux - shift_east(flux))
            south = jnp.where(odd, row_ref[s, j], far_row_ref[s, j])
            north = jnp.where(odd, far_row_ref[s, j], row_ref[s, j])
            north_wind = jnp.where(odd, far_row_wind[SPECIES, j], row_wind[SPECIES, j])
            southern = jnp.concatenate([south, x[: BAND_LATS - 1]], axis=0)
            flux = upwind(*split(wlat_ref[j]), southern, x)
            edge = upwind(*split(north_wind), x[BAND_LATS - 1 :], north)
            total = total + (flux - jnp.concatenate([flux[1:], edge], axis=0))
            if j == 0:
                beneath = jnp.where(south_core, outer_ref[s], inner_ref[s])
                overhead, over_wind = n_ref[s, 1], wlev_ref[1]
            else:
                beneath = n_ref[s, 0]
                overhead = jnp.where(south_core, inner_ref[s], outer_ref[s])
                over_wind = jnp.where(south_core, inner_wind[SPECIES], outer_wind[SPECIES])
            flux = upwind(*split(wlev_ref[j]), beneath, x)
            total = total + (flux - upwind(*split(over_wind), x, overhead))
            if last:
                row = pl.multiple_of((j * SPECIES + s) * BAND_LATS, BAND_LATS)
                for blk in range(LON_BLOCKS):
                    wide = min(LANES, NLON - blk * LANES)
                    outs[0][blk, pl.ds(row, BAND_LATS), :wide] = total[:, blk * LANES : blk * LANES + wide]
            else:
                outs[0][s, j] = total

                @pl.when(core == 1 - j)
                def _():
                    outs[1][s] = total

                @pl.when(core == j)
                def _():
                    outs[2][s] = total

                outs[3][s, j] = jnp.where(odd, total[:1], total[BAND_LATS - 1 :])
                outs[4][s, j] = jnp.where(odd, total[BAND_LATS - 1 :], total[:1])


def transport_step(side, density, winds, halo, wind_halo, last):
    if last:
        out_shape = (on_chip((LON_BLOCKS, 2 * SPECIES * BAND_LATS, LANES)),)
    else:
        out_shape = (
            on_chip((SPECIES, 2, BAND_LATS, NLON)),
            on_chip((SPECIES, BAND_LATS, NLON)),
            on_chip((SPECIES, BAND_LATS, NLON)),
            on_chip((SPECIES, 2, 1, NLON)),
            on_chip((SPECIES, 2, 1, NLON)),
        )
    return call(
        functools.partial(transport_kernel, last=last),
        out_shape,
        [SMEM] + [HELD] * 12,
        (VMEM,) * len(out_shape),
        name="transport",
        flops=4_000_000,
    )(side, density, *winds, *halo, *wind_halo)


def prepare_kernel(
    units_ref, owner_ref, rows_ref, sel_ref, weight_ref, column_ref,
    table_ref, own_ref, coef_ref, count, blocks, table, picked,
):
    @pl.loop(0, PEERS * PEER_SLOTS // 8)
    def _(i):
        for k in range(8):
            table_ref[i * 8 + k] = ZERO_TUBE

    @pl.loop(0, PEERS // 8)
    def _(i):
        for k in range(8):
            count[i * 8 + k] = 0

    @pl.loop(0, units_ref[0])
    def _(u):
        dest = owner_ref[u]
        rank = count[dest]
        count[dest] = rank + 1
        table_ref[dest * PEER_SLOTS + rank] = u

    coef_ref[...] = jnp.broadcast_to(column_ref[...], coef_ref.shape)

    for blk in range(LON_BLOCKS):
        wide = min(LANES, NLON - blk * LANES)
        blocks[blk, :, :wide] = weight_ref[:, blk * LANES : blk * LANES + wide]

    @pl.loop(0, BAND_LATS)
    def _(lat):
        for g in range(6):
            parts = [
                blocks[min(4 * g + i, LON_BLOCKS - 1), pl.ds(lat + h * BAND_LATS, 8, stride=4 * BAND_LATS), :]
                for i in range(4)
                for h in range(4)
            ]
            start = pl.multiple_of((lat * 6 + g) * LANES, LANES)
            table[pl.ds(start, LANES), :] = jnp.concatenate(parts, axis=0).T

    @pl.loop(0, SLOTS_PAD // UNROLL)
    def _(step):
        base = pl.multiple_of(step * UNROLL, UNROLL)
        places = rows_ref.at[pl.ds(base, UNROLL)]
        for i in range(UNROLL):
            picked[pl.ds(base + i, 1), :] = table[pl.ds(places[i], 1), :]

    for blk in range(SLOT_BLOCKS):
        turned = picked[blk * LANES : (blk + 1) * LANES, :].T
        which = sel_ref[blk : blk + 1, :]
        kept = turned[:PAIRS]
        for i in range(1, 4):
            kept = jnp.where(which == i, turned[i * PAIRS : (i + 1) * PAIRS], kept)
        own_ref[blk] = kept


def prepare(units, owners, rows, sel, weights, column):
    return call(
        prepare_kernel,
        (
            sds((PEERS * PEER_SLOTS,), jnp.int32),
            on_chip((SLOT_BLOCKS, PAIRS, LANES)),
            on_chip((3 * SPECIES * NLEV, LANES)),
        ),
        [SMEM, SMEM, SMEM, VMEM, VMEM, VMEM],
        (SMEM, VMEM, VMEM),
        [
            pltpu.SMEM((PEERS,), jnp.int32),
            pltpu.VMEM((LON_BLOCKS, PAIRS * BAND_LATS, LANES), f32),
            pltpu.VMEM((BAND_LATS * 6 * LANES, LANES), f32),
            pltpu.VMEM((SLOTS_PAD, LANES), f32),
        ],
        name="prepare",
        flops=20_000_000,
    )(units, owners, rows, sel, weights, column)


def pack_kernel(
    core_ref, starts_ref, units_ref, order_ref, mine_ref, other_ref, out_hbm, planes, table_ref, msg_ref, sems
):
    @pl.loop(0, LON_BLOCKS)
    def _(blk):
        for side, source in enumerate((mine_ref, other_ref)):
            for j in range(2):
                for i in range(PLANES):
                    from_row = (j * SPECIES + i % SPECIES) * BAND_LATS
                    planes[blk, pl.ds(((2 * side + j) * PLANES + i) * PITCH, BAND_LATS), :] = source[
                        blk, from_row : from_row + BAND_LATS, :
                    ]

    @pl.loop(0, LON_BLOCKS)
    def _(blk):
        for lat in range(BAND_LATS):
            parts = [
                planes[blk, pl.ds((jj * PLANES + first) * PITCH + lat, 8, stride=PITCH), :]
                for jj in range(CHIP_LEVS)
                for first in (0, 3, 1, 4)
            ]
            start = pl.multiple_of((lat * LON_BLOCKS + blk) * LANES, LANES)
            table_ref[pl.ds(start, LANES), :] = jnp.concatenate(parts, axis=0).T

    core = core_ref[0]
    lane = lax.broadcasted_iota(jnp.int32, (1, LANES), 1)
    group_of = lax.div(lax.rem(lane, 32), SPECIES)

    def send(peer):
        rows = pl.ds(pl.multiple_of(peer * PEER_ROWS, PEER_ROWS), PEER_ROWS)
        return pltpu.make_async_copy(msg_ref.at[rows, :], out_hbm.at[rows, :], sems.at[peer])

    @pl.loop(0, 16)
    def _(peer):
        owner = 2 * peer + core
        live = TUBE_COLS * units_ref[owner]
        first = TUBE_COLS * starts_ref[owner]

        @pl.loop(0, lax.div(live + (MSG_ROWS - 1), MSG_ROWS))
        def _(piece):
            chunk = lax.div(piece, GROUPS)
            mask = group_of == piece - chunk * GROUPS
            row = pl.multiple_of(peer * PEER_ROWS + chunk * MSG_ROWS, MSG_ROWS)
            base = first + piece * MSG_ROWS
            for i in range(MSG_ROWS):
                place = order_ref.at[pl.ds(i, ORDER_PAD - MSG_ROWS)][base]
                value = table_ref[pl.ds(place, 1), :]
                pltpu.store(msg_ref.at[pl.ds(row + i, 1), :], value, mask=mask)

        send(peer).start()

    @pl.loop(0, 16)
    def _(peer):
        send(peer).wait()


def pack(core, starts, units, order, mine, other):
    return call(
        pack_kernel,
        sds((16 * PEER_ROWS, LANES)),
        [SMEM, SMEM, SMEM, SMEM, HELD, HELD],
        HBM,
        [
            pltpu.VMEM((LON_BLOCKS, CHIP_LEVS * PLANES * PITCH, LANES), f32),
            pltpu.VMEM((BAND_LATS * LON_PAD, LANES), f32),
            pltpu.VMEM((16 * PEER_ROWS, LANES), f32),
            pltpu.SemaphoreType.DMA((16,)),
        ],
        name="pack",
        flops=30_000_000,
        vmem=32,
    )(core, starts, units, order, mine, other)


def solve_kernel(
    core_ref, units_ref, table_ref, got_ref, coef_ref, weight_ref, state_hbm, items_ref,
    turned, natural, pairs, wide, tubes, state, sems,
):
    core = core_ref[0]
    live = TUBE_COLS * units_ref[0]
    lane = lax.broadcasted_iota(jnp.int32, (1, LANES), 1)
    low = lane < 64
    quarter = lax.div(lane, 32)

    @pl.loop(0, 8)
    def _(i):
        for side in range(2):
            out = i * LEVEL_PITCH + side * LANES
            for chunk in range(CHUNKS):
                row = pl.multiple_of((2 * i + side) * PEER_ROWS + chunk * MSG_ROWS, MSG_ROWS)
                flipped = jnp.concatenate([got_ref[pl.ds(row, MSG_ROWS), :]] * 2, axis=0).T
                turned[chunk, pl.ds(out + 64 * core, 64), :] = flipped[:64]
                turned[chunk, pl.ds(out + 64 - 64 * core, 64), :] = flipped[64:]

    def leave(s):
        return pltpu.make_async_copy(state.at[s], state_hbm.at[0, 0, s], sems.at[s])

    @pl.loop(0, SPECIES)
    def _(s):
        def coefs(which):
            row = pl.multiple_of((which * SPECIES + s) * NLEV, NLEV)
            return [coef_ref[pl.ds(row + 8 * v, 8), :] for v in range(8)]

        lower, upper, inv = coefs(0), coefs(1), coefs(2)
        for blk in range(SLOT_BLOCKS):
            chunk, i = divmod(blk, 3)

            def levels(group, v):
                return turned[chunk, pl.ds(32 * v + group * SPECIES + s, 8, stride=LEVEL_PITCH), :]

            rhs = [jnp.where(low, levels(2 * i, v), levels(2 * i + 1, v)) for v in range(8)]
            scaled = [rhs[v] * inv[v] for v in range(8)]
            x = rhs
            for _ in range(SWEEPS):
                beneath = [pltpu.roll(x[7], 1, axis=0)] + x[:7]
                overhead = x[1:] + [pltpu.roll(x[0], 7, axis=0)]
                x = [scaled[v] + lower[v] * beneath[v] + upper[v] * overhead[v] for v in range(8)]
            keep = lane + blk * LANES < live
            for v in range(8):
                natural[i, pl.ds(v, 8, stride=PITCH), :] = jnp.where(keep, x[v], 0.0)
            width = min(LANES, COL_CAP - blk * LANES)
            for g in range(8):
                state[s, g * 8 : g * 8 + 8, blk * LANES : blk * LANES + width] = natural[
                    i, g * PITCH : g * PITCH + 8, :width
                ]
            for h in range(4):
                weight = weight_ref[blk, 8 * h : 8 * h + 8, :]
                paired = weight * x[2 * h] + (1.0 - weight) * x[2 * h + 1]
                pairs[i, pl.ds(h, 8, stride=4), :] = paired
            wide[i] = jnp.concatenate([pairs[i]] * 4, axis=0).T
            item = wide[i, pl.ds(0, 32, stride=TUBE_COLS), :]
            for c in range(1, TUBE_COLS):
                item = jnp.where(quarter == c, wide[i, pl.ds(c, 32, stride=TUBE_COLS), :], item)
            tubes[pl.ds(blk * 256 + s, 32, stride=8), :] = item
        leave(s).start()

    tubes[ZERO_TUBE * 8 :, :] = jnp.zeros((8, LANES), f32)
    sub = lax.broadcasted_iota(jnp.int32, (8, LANES), 0)

    @pl.loop(0, PEERS // 4)
    def _(step):
        for i in range(4):
            d = step * 4 + i
            tiles = [
                tubes[pl.ds(pl.multiple_of(table_ref[d * PEER_SLOTS + r] * 8, 8), 8), :] for r in range(PEER_SLOTS)
            ]
            mid = pltpu.roll(tiles[1], 5, axis=0)
            top = pltpu.roll(tiles[2], 2, axis=0)
            row = pl.multiple_of(d * ITEM_ROWS, ITEM_ROWS)
            items_ref[pl.ds(row, 8), :] = jnp.where(sub < 5, tiles[0], mid)
            items_ref[pl.ds(row + 8, 8), :] = jnp.where(sub < 2, mid, jnp.where(sub < 7, top, 0.0))

    for s in range(SPECIES):
        leave(s).wait()


def solve(core, units, table, got, coefs, weights):
    return call(
        solve_kernel,
        (sds((1, 1, SPECIES, NLEV, COL_CAP)), sds((PEERS * ITEM_ROWS, LANES))),
        [SMEM, SMEM, SMEM] + [HELD] * 3,
        (HBM, VMEM),
        [
            pltpu.VMEM((CHUNKS, 8 * LEVEL_PITCH, LANES), f32),
            pltpu.VMEM((3, 8 * PITCH, LANES), f32),
            pltpu.VMEM((3, PAIRS, LANES), f32),
            pltpu.VMEM((3, LANES, LANES), f32),
            pltpu.VMEM((ZERO_TUBE * 8 + 8, LANES), f32),
            pltpu.VMEM((SPECIES, NLEV, COL_CAP), f32),
            pltpu.SemaphoreType.DMA((SPECIES,)),
        ],
        name="solve",
        flops=40_000_000,
    )(core, units, table, got, coefs, weights)


def halves(x):
    high = x.astype(jnp.bfloat16)
    return high, (x - high.astype(f32)).astype(jnp.bfloat16)


def product(x, high, low):
    x_high, x_low = halves(x)
    dot = functools.partial(jnp.dot, preferred_element_type=f32)
    return dot(x_high, high) + (dot(x_low, high) + dot(x_high, low))


def lines_kernel(
    items_ref, yield_ref, rates_ref, waves_ref, fwd_high, fwd_low, inv_high, inv_low, out_hbm,
    spec_in, spec, mixed, done, sems,
):
    tubes = 32 * PEER_SLOTS
    for b in range(4):
        for s in range(SPECIES):
            for r in range(PEER_SLOTS):
                rows = items_ref[pl.ds(b * 32 * ITEM_ROWS + r * SPECIES + s, 32, stride=ITEM_ROWS), :]
                spec_in[b, pl.ds(s * tubes + r, 32, stride=PEER_SLOTS), :] = rows

    half = SPECIES * tubes // 2

    @pl.loop(0, 2)
    def _(step):
        row = pl.multiple_of(step * half, half)
        x = jnp.concatenate([spec_in[b, pl.ds(row, half), :] for b in range(4)], axis=1)
        spec[pl.ds(row, half), :] = product(x, fwd_high[...], fwd_low[...])

    waves = waves_ref[...]
    for i in range(IONS):
        keep = (1.0 - rates_ref[IONS + i]) + rates_ref[i] * waves
        gain = jnp.ones_like(waves)
        for _ in range(SECTIONS - 1):
            gain = gain * keep + 1.0
        total = (yield_ref[i * SPECIES] * gain) * spec[:tubes, :]
        for s in range(1, SPECIES):
            total = total + (yield_ref[i * SPECIES + s] * gain) * spec[s * tubes : (s + 1) * tubes, :]
        mixed[i] = total

    def leave(i):
        return pltpu.make_async_copy(done.at[i], out_hbm.at[0, i], sems.at[i])

    @pl.loop(0, IONS)
    def _(i):
        done[i] = product(mixed[i], inv_high[...], inv_low[...])
        leave(i).start()

    for i in range(IONS):
        leave(i).wait()


def cosine_basis():
    k = np.arange(LINE_PTS)[:, None]
    n = np.arange(LINE_PTS)[None, :]
    basis = np.cos(np.pi * k * (n + 0.5) / LINE_PTS) * np.sqrt(2.0 / LINE_PTS)
    basis[0] *= np.sqrt(0.5)
    waves = 2.0 * np.cos(np.pi * np.arange(LINE_PTS) / LINE_PTS) - 2.0
    return basis, waves


def lines(items, ion_yield, ion_spread, ion_loss):
    basis, waves = cosine_basis()

    def parts(matrix):
        matrix = matrix.astype(np.float32)
        high = matrix.astype(jnp.bfloat16)
        low = (matrix - high.astype(np.float32)).astype(jnp.bfloat16)
        return jnp.asarray(high), jnp.asarray(low)

    waves = jnp.asarray(waves.astype(np.float32))[None]
    tubes = 32 * PEER_SLOTS
    by_ion = call(
        lines_kernel,
        sds((1, IONS, tubes, LINE_PTS)),
        [HELD, SMEM, SMEM] + [HELD] * 5,
        HBM,
        [
            pltpu.VMEM((4, SPECIES * tubes, LANES), f32),
            pltpu.VMEM((SPECIES * tubes, LINE_PTS), f32),
            pltpu.VMEM((IONS, tubes, LINE_PTS), f32),
            pltpu.VMEM((IONS, tubes, LINE_PTS), f32),
            pltpu.SemaphoreType.DMA((IONS,)),
        ],
        name="lines",
        flops=2_000_000_000,
    )(items, ion_yield.reshape(-1), jnp.concatenate([ion_spread, ion_loss]), waves, *parts(basis.T), *parts(basis))
    return jnp.swapaxes(by_ion, 1, 2)


def swap(x, axis, offset):
    count = lax.axis_size(axis)
    lows = range(offset, count - 1, 2)
    return lax.ppermute(x, axis, [(i, i + 1) for i in lows] + [(i + 1, i) for i in lows])


def exchange(inner, outer, row, far_row):
    outer = swap(outer, "lev", 1)
    row = swap(row, "band", 0)
    far_row = swap(far_row, "band", 1)
    return swap(inner, "lev", 0), outer, row, far_row


def on_device(
    neutrals,
    wind_lon,
    wind_lat,
    wind_lev,
    eddy_coupling,
    pair_weight,
    ion_yield,
    ion_spread,
    ion_loss,
    column_order,
    column_units,
    tube_owner,
):
    lev = lax.axis_index("lev")

    side = jnp.stack([lev % 2, lax.axis_index("band") % 2]).astype(jnp.int32)
    neutrals, *rest = edges(side, neutrals, wind_lon, wind_lat, wind_lev)
    winds, first_halo = rest[:3], exchange(*rest[3:])

    starts = jnp.cumsum(column_units) - column_units
    order = column_order[0]
    lat = jnp.zeros_like(order)
    for i in range(1, BAND_LATS):
        lat = lat + (order >= i * NLON).astype(jnp.int32)
    rows = jnp.pad(order + lat * (LON_PAD - NLON), (0, ORDER_PAD - BAND_COLS))
    own_units = column_units[lev].reshape(1)
    padded = jnp.pad(order, (0, SLOTS_PAD))
    own = lax.dynamic_slice(padded, (TUBE_COLS * starts[lev],), (SLOTS_PAD,))
    own_lat = jnp.zeros_like(own)
    for i in range(1, BAND_LATS):
        own_lat = own_lat + (own >= i * NLON).astype(jnp.int32)
    own_lon = own - own_lat * NLON
    own_rows = (own_lat * 6 + own_lon // 512) * LANES + own_lon % LANES
    own_sel = ((own_lon // LANES) % 4).reshape(SLOT_BLOCKS, LANES)
    zero = jnp.zeros((SPECIES, 1), f32)
    lower = jnp.concatenate([zero, eddy_coupling[:, 1:]], 1)
    upper = jnp.concatenate([eddy_coupling[:, 1:], zero], 1)
    inv = 1.0 / (1.0 + lower + upper)
    coefs = jnp.stack([lower * inv, upper * inv, inv]).reshape(3, SPECIES, 8, 8)
    table, own_weights, coefs = prepare(
        own_units,
        tube_owner[lev, :, 0],
        own_rows,
        own_sel,
        pair_weight.reshape(PAIRS * BAND_LATS, NLON),
        jnp.swapaxes(coefs, 2, 3).reshape(-1, 1),
    )

    density, *halo = transport_step(side, neutrals, winds, first_halo, first_halo, False)
    (mine,) = transport_step(side, density, winds, exchange(*halo), first_halo, True)
    owners = lax.axis_size("lev")
    other = swap(mine, "lev", 0)

    core = (lev % 2).reshape(1)
    parity = [[2 * i + c for i in range(owners // 2)] for c in range(2)]
    outgoing = pack(core, starts, column_units, rows, mine, other)
    got = lax.all_to_all(
        outgoing.reshape(16, PEER_ROWS, LANES), "lev", 0, 0, axis_index_groups=parity, tiled=True
    ).reshape(16 * PEER_ROWS, LANES)
    column_state, items = solve(core, own_units, table, got, coefs, own_weights)

    items = lax.all_to_all(
        items.reshape(PEERS, ITEM_ROWS, LANES), ("band", "lev"), 0, 0, tiled=True
    ).reshape(PEERS * ITEM_ROWS, LANES)
    return column_state, lines(items, ion_yield, ion_spread, ion_loss)


def solution(mesh):
    placed = (
        P(None, "lev", "band", None),
        P("lev", "band", None),
        P("lev", "band", None),
        P("lev", "band", None),
        P(),
        P(None, "band", None),
        P(),
        P(),
        P(),
        P("band", None),
        P(),
        P(),
    )
    return jax.shard_map(
        on_device,
        mesh=mesh,
        in_specs=placed,
        out_specs=(P("band", "lev", None, None, None), P(("band", "lev"), None, None, None)),
        check_vma=False,
    )
```

```python
import functools

import jax
import jax.numpy as jnp
import numpy as np
from jax import lax
from jax.experimental import pallas as pl
from jax.experimental.pallas import tpu as pltpu
from jax.sharding import PartitionSpec as P

SPECIES = 5
IONS = 7
NLON = 2880
NLEV = 64
PAIRS = 32
BAND_LATS = 8
TSTEPS = 2
SWEEPS = 8
SECTIONS = 20
TUBE_COLS = 4
PEERS = 128
PEER_SLOTS = 3
COL_CAP = 1080
TUBE_CAP = 270
BAND_COLS = BAND_LATS * NLON
LINE_PTS = 512

LANES = 128
LON_BLOCKS = 23
LON_PAD = LON_BLOCKS * LANES
CHIP_LEVS = 4
PITCH = 9
LEVEL_PITCH = 257
PLANES = 12
GROUPS = 6
CHUNKS = 3
MSG_ROWS = 64
PEER_ROWS = CHUNKS * MSG_ROWS
CHUNK_BLOCKS = 3
CHUNK_SLOTS = GROUPS * MSG_ROWS
SLOT_BLOCKS = 9
SLOTS_PAD = SLOT_BLOCKS * LANES
ORDER_PAD = BAND_COLS + 2 * LANES
UNROLL = 64
ZERO_TUBE = SLOT_BLOCKS * 32
ITEM_ROWS = 16

f32 = jnp.float32
VMEM = pl.BlockSpec(memory_space=pltpu.VMEM)
HELD = pl.BlockSpec(memory_space=pltpu.VMEM)
SMEM = pl.BlockSpec(memory_space=pltpu.SMEM)
HBM = pl.BlockSpec(memory_space=pltpu.HBM)


def on_chip(shape, dtype=f32):
    return pltpu.VMEM(shape, dtype)


def call(kernel, out_shape, in_specs, out_specs, scratch=(), name=None, flops=0, vmem=16):
    run = pl.pallas_call(
        kernel,
        out_shape=out_shape,
        in_specs=in_specs,
        out_specs=out_specs,
        scratch_shapes=list(scratch),
        name=name,
        cost_estimate=pl.CostEstimate(flops=flops, bytes_accessed=1 << 20, transcendentals=0),
        compiler_params=pltpu.CompilerParams(vmem_limit_bytes=vmem * 1024 * 1024),
    )

    def place(x, spec):
        space = pltpu.VMEM if spec is HELD else pltpu.HBM if spec is HBM else None
        return x if space is None else pltpu.with_memory_space_constraint(x, space)

    def placed(*args):
        return run(*(place(x, spec) for x, spec in zip(args, in_specs)))

    return placed


def sds(shape, dtype=f32):
    return jax.ShapeDtypeStruct(shape, dtype)


def upwind(courant_plus, courant_minus, upstream, downstream):
    return courant_plus * upstream + courant_minus * downstream


def outer_slab_kernel(side_ref, n_hbm, wlev_hbm, slab_ref, sems):
    core = side_ref[0]
    fetches = [
        pltpu.make_async_copy(n_hbm.at[s, core], slab_ref.at[s], sems.at[s]) for s in range(SPECIES)
    ]
    fetches.append(pltpu.make_async_copy(wlev_hbm.at[0], slab_ref.at[SPECIES], sems.at[SPECIES]))
    for fetch in fetches:
        fetch.start()
    for fetch in fetches:
        fetch.wait()


def outer_slab(side, density, wind_lev):
    return call(
        outer_slab_kernel,
        on_chip((SPECIES + 1, BAND_LATS, NLON)),
        [SMEM, HBM, HBM],
        VMEM,
        [pltpu.SemaphoreType.DMA((SPECIES + 1,))],
        name="outer_slab",
        flops=100_000,
    )(side, density, wind_lev)


def edges_kernel(
    side_ref, n_hbm, wlon_hbm, wlat_hbm, wlev_hbm, _,
    n_ref, wlon_ref, wlat_ref, wlev_ref, inner_ref, row_ref, far_row_ref, sems,
):
    fetches = [
        pltpu.make_async_copy(n_hbm.at[s], n_ref.at[s], sems.at[s]) for s in range(SPECIES)
    ]
    fetches.append(pltpu.make_async_copy(wlat_hbm, wlat_ref, sems.at[SPECIES]))
    fetches.append(pltpu.make_async_copy(wlev_hbm, wlev_ref, sems.at[SPECIES + 1]))
    fetches.append(pltpu.make_async_copy(wlon_hbm, wlon_ref, sems.at[SPECIES + 2]))
    for fetch in fetches:
        fetch.start()
    for fetch in fetches[:-1]:
        fetch.wait()
    core, odd = side_ref[0], side_ref[1] == 1
    inner_ref[SPECIES] = wlev_ref[0]
    for j in range(2):
        row_ref[SPECIES, j] = wlat_ref[j, :1]
        far_row_ref[SPECIES, j] = wlat_ref[j, :1]

    @pl.loop(0, SPECIES)
    def _(s):
        inner_ref[s] = n_ref[s, 1 - core]
        for j in range(2):
            first, last = n_ref[s, j, :1], n_ref[s, j, BAND_LATS - 1 :]
            row_ref[s, j] = jnp.where(odd, first, last)
            far_row_ref[s, j] = jnp.where(odd, last, first)

    fetches[-1].wait()


def edges(side, density, wind_lon, wind_lat, wind_lev, slab):
    return call(
        edges_kernel,
        (
            on_chip(density.shape),
            on_chip(wind_lon.shape),
            on_chip(wind_lat.shape),
            on_chip(wind_lev.shape),
            on_chip((SPECIES + 1, BAND_LATS, NLON)),
            on_chip((SPECIES + 1, 2, 1, NLON)),
            on_chip((SPECIES + 1, 2, 1, NLON)),
        ),
        [SMEM] + [HBM] * 4 + [HELD],
        (VMEM,) * 7,
        [pltpu.SemaphoreType.DMA((SPECIES + 3,))],
        name="edges",
        flops=1_000_000,
    )(side, density, wind_lon, wind_lat, wind_lev, slab)


def level_kernel(side_ref, wlon_ref, wlat_ref, wlev_ref, *refs, outer, last, whole):
    row_ref, far_row_ref, row_wind, far_row_wind, cross_ref, cross_wind = refs[:6]
    odd = side_ref[1] == 1

    def split(c):
        return jnp.maximum(c, 0.0), jnp.minimum(c, 0.0)

    def shift_west(x):
        return jnp.concatenate([x[:, NLON - 1 :], x[:, : NLON - 1]], axis=1)

    def shift_east(x):
        return jnp.concatenate([x[:, 1:], x[:, :1]], axis=1)

    def advance(core):
        j = core if outer else 1 - core
        if whole:
            n_ref, outs = refs[6], refs[7:]
            level = lambda which, s: n_ref[s, which]
        else:
            outer_ref, inner_ref, outs = refs[6], refs[7], refs[8:]
            level = lambda which, s: (outer_ref if which == core else inner_ref)[s]
        if outer:
            sent_ref, outs = outs[0], outs[1:]
        if not last:
            outs[1][0] = cross_wind[SPECIES]

        @pl.loop(0, SPECIES)
        def _(s):
            x = level(j, s)
            flux = upwind(*split(wlon_ref[j]), shift_west(x), x)
            total = x + (flux - shift_east(flux))
            south = jnp.where(odd, row_ref[s, j], far_row_ref[s, j])
            north = jnp.where(odd, far_row_ref[s, j], row_ref[s, j])
            north_wind = jnp.where(odd, far_row_wind[SPECIES, j], row_wind[SPECIES, j])
            southern = jnp.concatenate([south, x[: BAND_LATS - 1]], axis=0)
            flux = upwind(*split(wlat_ref[j]), southern, x)
            edge = upwind(*split(north_wind), x[BAND_LATS - 1 :], north)
            total = total + (flux - jnp.concatenate([flux[1:], edge], axis=0))
            if j == 0:
                beneath, overhead, over_wind = cross_ref[s], level(1, s), wlev_ref[1]
            else:
                beneath, overhead, over_wind = level(0, s), cross_ref[s], cross_wind[0 if last else SPECIES]
            flux = upwind(*split(wlev_ref[j]), beneath, x)
            total = total + (flux - upwind(*split(over_wind), x, overhead))
            if last:
                row = pl.multiple_of(s * BAND_LATS, BAND_LATS)
                for blk in range(LON_BLOCKS):
                    wide = min(LANES, NLON - blk * LANES)
                    outs[0][blk, pl.ds(row, BAND_LATS), :wide] = total[:, blk * LANES : blk * LANES + wide]
                return
            outs[0][s] = total
            if outer:
                for which, values in ((j, total), (1 - j, sent_ref[s])):
                    first, final = values[:1], values[BAND_LATS - 1 :]
                    outs[2][s, which] = jnp.where(odd, first, final)
                    outs[3][s, which] = jnp.where(odd, final, first)

    for core in range(2):
        pl.when(side_ref[0] == core)(functools.partial(advance, core))


def advance_level(side, winds, rows, wind_rows, cross, cross_wind, density, outer, last, sent=()):
    if last:
        out_shape = (on_chip((LON_BLOCKS, SPECIES * BAND_LATS, LANES)),)
    else:
        out_shape = on_chip((SPECIES, BAND_LATS, NLON)), on_chip((1, BAND_LATS, NLON))
        if outer:
            out_shape += (on_chip((SPECIES, 2, 1, NLON)),) * 2
    args = (side, *winds, *rows, *wind_rows, cross, cross_wind, *density, *sent)
    return call(
        functools.partial(level_kernel, outer=outer, last=last, whole=len(density) == 1),
        out_shape,
        [SMEM] + [HELD] * (len(args) - 1),
        (VMEM,) * len(out_shape),
        name="outer_level" if outer else "inner_level",
        flops=2_000_000,
    )(*args)


def prepare_kernel(
    units_ref, owner_ref, rows_ref, sel_ref, weight_ref, column_ref,
    table_ref, own_ref, coef_ref, count, blocks, table, picked,
):
    @pl.loop(0, PEERS * PEER_SLOTS // 8)
    def _(i):
        for k in range(8):
            table_ref[i * 8 + k] = ZERO_TUBE

    @pl.loop(0, PEERS // 8)
    def _(i):
        for k in range(8):
            count[i * 8 + k] = 0

    @pl.loop(0, units_ref[0])
    def _(u):
        dest = owner_ref[u]
        rank = count[dest]
        count[dest] = rank + 1
        table_ref[dest * PEER_SLOTS + rank] = u

    coef_ref[...] = jnp.broadcast_to(column_ref[...], coef_ref.shape)

    for blk in range(LON_BLOCKS):
        wide = min(LANES, NLON - blk * LANES)
        blocks[blk, :, :wide] = weight_ref[:, blk * LANES : blk * LANES + wide]

    @pl.loop(0, BAND_LATS)
    def _(lat):
        for g in range(6):
            parts = [
                blocks[min(4 * g + i, LON_BLOCKS - 1), pl.ds(lat + h * BAND_LATS, 8, stride=4 * BAND_LATS), :]
                for i in range(4)
                for h in range(4)
            ]
            start = pl.multiple_of((lat * 6 + g) * LANES, LANES)
            table[pl.ds(start, LANES), :] = jnp.concatenate(parts, axis=0).T

    @pl.loop(0, SLOTS_PAD // UNROLL)
    def _(step):
        base = pl.multiple_of(step * UNROLL, UNROLL)
        places = rows_ref.at[pl.ds(base, UNROLL)]
        for i in range(UNROLL):
            picked[pl.ds(base + i, 1), :] = table[pl.ds(places[i], 1), :]

    for blk in range(SLOT_BLOCKS):
        turned = picked[blk * LANES : (blk + 1) * LANES, :].T
        which = sel_ref[blk : blk + 1, :]
        kept = turned[:PAIRS]
        for i in range(1, 4):
            kept = jnp.where(which == i, turned[i * PAIRS : (i + 1) * PAIRS], kept)
        own_ref[blk] = kept


def prepare(units, owners, rows, sel, weights, column):
    return call(
        prepare_kernel,
        (
            sds((PEERS * PEER_SLOTS,), jnp.int32),
            on_chip((SLOT_BLOCKS, PAIRS, LANES)),
            on_chip((3 * SPECIES * NLEV, LANES)),
        ),
        [SMEM, SMEM, SMEM, VMEM, VMEM, VMEM],
        (SMEM, VMEM, VMEM),
        [
            pltpu.SMEM((PEERS,), jnp.int32),
            pltpu.VMEM((LON_BLOCKS, PAIRS * BAND_LATS, LANES), f32),
            pltpu.VMEM((BAND_LATS * 6 * LANES, LANES), f32),
            pltpu.VMEM((SLOTS_PAD, LANES), f32),
        ],
        name="prepare",
        flops=20_000_000,
    )(units, owners, rows, sel, weights, column)


def pack_kernel(
    core_ref, starts_ref, units_ref, order_ref, *refs
):
    sources, (out_hbm, planes, table_ref, msg_ref, sems) = refs[:CHIP_LEVS], refs[CHIP_LEVS:]

    @pl.loop(0, LON_BLOCKS)
    def _(blk):
        for jj, source in enumerate(sources):
            for i in range(PLANES):
                from_row = i % SPECIES * BAND_LATS
                planes[blk, pl.ds((jj * PLANES + i) * PITCH, BAND_LATS), :] = source[
                    blk, from_row : from_row + BAND_LATS, :
                ]

    @pl.loop(0, LON_BLOCKS)
    def _(blk):
        for lat in range(BAND_LATS):
            parts = [
                planes[blk, pl.ds((jj * PLANES + first) * PITCH + lat, 8, stride=PITCH), :]
                for jj in range(CHIP_LEVS)
                for first in (0, 3, 1, 4)
            ]
            start = pl.multiple_of((lat * LON_BLOCKS + blk) * LANES, LANES)
            table_ref[pl.ds(start, LANES), :] = jnp.concatenate(parts, axis=0).T

    core = core_ref[0]
    lane = lax.broadcasted_iota(jnp.int32, (1, LANES), 1)
    group_of = lax.div(lax.rem(lane, 32), SPECIES)

    def send(peer):
        rows = pl.ds(pl.multiple_of(peer * PEER_ROWS, PEER_ROWS), PEER_ROWS)
        return pltpu.make_async_copy(msg_ref.at[rows, :], out_hbm.at[rows, :], sems.at[peer])

    @pl.loop(0, 16)
    def _(peer):
        owner = 2 * peer + core
        live = TUBE_COLS * units_ref[owner]
        first = TUBE_COLS * starts_ref[owner]

        @pl.loop(0, lax.div(live + (MSG_ROWS - 1), MSG_ROWS))
        def _(piece):
            chunk = lax.div(piece, GROUPS)
            mask = group_of == piece - chunk * GROUPS
            row = pl.multiple_of(peer * PEER_ROWS + chunk * MSG_ROWS, MSG_ROWS)
            base = first + piece * MSG_ROWS
            for i in range(MSG_ROWS):
                place = order_ref.at[pl.ds(i, ORDER_PAD - MSG_ROWS)][base]
                value = table_ref[pl.ds(place, 1), :]
                pltpu.store(msg_ref.at[pl.ds(row + i, 1), :], value, mask=mask)

        send(peer).start()

    @pl.loop(0, 16)
    def _(peer):
        send(peer).wait()


def pack(core, starts, units, order, blocks):
    return call(
        pack_kernel,
        sds((16 * PEER_ROWS, LANES)),
        [SMEM] * 4 + [HELD] * CHIP_LEVS,
        HBM,
        [
            pltpu.VMEM((LON_BLOCKS, CHIP_LEVS * PLANES * PITCH, LANES), f32),
            pltpu.VMEM((BAND_LATS * LON_PAD, LANES), f32),
            pltpu.VMEM((16 * PEER_ROWS, LANES), f32),
            pltpu.SemaphoreType.DMA((16,)),
        ],
        name="pack",
        flops=30_000_000,
        vmem=32,
    )(core, starts, units, order, *blocks)


def solve_kernel(
    core_ref, units_ref, table_ref, got_ref, coef_ref, weight_ref, state_hbm, items_ref,
    turned, natural, pairs, wide, tubes, state, sems,
):
    core = core_ref[0]
    live = TUBE_COLS * units_ref[0]
    lane = lax.broadcasted_iota(jnp.int32, (1, LANES), 1)
    low = lane < 64
    quarter = lax.div(lane, 32)

    @pl.loop(0, 8)
    def _(i):
        for side in range(2):
            out = i * LEVEL_PITCH + side * LANES
            for chunk in range(CHUNKS):
                row = pl.multiple_of((2 * i + side) * PEER_ROWS + chunk * MSG_ROWS, MSG_ROWS)
                flipped = jnp.concatenate([got_ref[pl.ds(row, MSG_ROWS), :]] * 2, axis=0).T
                for part, level in enumerate((1 + core, 3 * core, 2 - core, 3 - 3 * core)):
                    turned[chunk, pl.ds(out + 32 * level, 32), :] = flipped[32 * part : 32 * part + 32]

    def leave(s):
        return pltpu.make_async_copy(state.at[s], state_hbm.at[0, 0, s], sems.at[s])

    @pl.loop(0, SPECIES)
    def _(s):
        def coefs(which):
            row = pl.multiple_of((which * SPECIES + s) * NLEV, NLEV)
            return [coef_ref[pl.ds(row + 8 * v, 8), :] for v in range(8)]

        lower, upper, inv = coefs(0), coefs(1), coefs(2)
        for blk in range(SLOT_BLOCKS):
            chunk, i = divmod(blk, 3)

            def levels(group, v):
                return turned[chunk, pl.ds(32 * v + group * SPECIES + s, 8, stride=LEVEL_PITCH), :]

            rhs = [jnp.where(low, levels(2 * i, v), levels(2 * i + 1, v)) for v in range(8)]
            scaled = [rhs[v] * inv[v] for v in range(8)]
            x = rhs
            for _ in range(SWEEPS):
                beneath = [pltpu.roll(x[7], 1, axis=0)] + x[:7]
                overhead = x[1:] + [pltpu.roll(x[0], 7, axis=0)]
                x = [scaled[v] + lower[v] * beneath[v] + upper[v] * overhead[v] for v in range(8)]
            keep = lane + blk * LANES < live
            for v in range(8):
                natural[i, pl.ds(v, 8, stride=PITCH), :] = jnp.where(keep, x[v], 0.0)
            width = min(LANES, COL_CAP - blk * LANES)
            for g in range(8):
                state[s, g * 8 : g * 8 + 8, blk * LANES : blk * LANES + width] = natural[
                    i, g * PITCH : g * PITCH + 8, :width
                ]
            for h in range(4):
                weight = weight_ref[blk, 8 * h : 8 * h + 8, :]
                paired = weight * x[2 * h] + (1.0 - weight) * x[2 * h + 1]
                pairs[i, pl.ds(h, 8, stride=4), :] = paired
            wide[i] = jnp.concatenate([pairs[i]] * 4, axis=0).T
            item = wide[i, pl.ds(0, 32, stride=TUBE_COLS), :]
            for c in range(1, TUBE_COLS):
                item = jnp.where(quarter == c, wide[i, pl.ds(c, 32, stride=TUBE_COLS), :], item)
            tubes[pl.ds(blk * 256 + s, 32, stride=8), :] = item
        leave(s).start()

    tubes[ZERO_TUBE * 8 :, :] = jnp.zeros((8, LANES), f32)
    sub = lax.broadcasted_iota(jnp.int32, (8, LANES), 0)

    @pl.loop(0, PEERS // 4)
    def _(step):
        for i in range(4):
            d = step * 4 + i
            tiles = [
                tubes[pl.ds(pl.multiple_of(table_ref[d * PEER_SLOTS + r] * 8, 8), 8), :] for r in range(PEER_SLOTS)
            ]
            mid = pltpu.roll(tiles[1], 5, axis=0)
            top = pltpu.roll(tiles[2], 2, axis=0)
            row = pl.multiple_of(d * ITEM_ROWS, ITEM_ROWS)
            items_ref[pl.ds(row, 8), :] = jnp.where(sub < 5, tiles[0], mid)
            items_ref[pl.ds(row + 8, 8), :] = jnp.where(sub < 2, mid, jnp.where(sub < 7, top, 0.0))

    for s in range(SPECIES):
        leave(s).wait()


def solve(core, units, table, got, coefs, weights):
    return call(
        solve_kernel,
        (sds((1, 1, SPECIES, NLEV, COL_CAP)), sds((PEERS * ITEM_ROWS, LANES))),
        [SMEM, SMEM, SMEM] + [HELD] * 3,
        (HBM, VMEM),
        [
            pltpu.VMEM((CHUNKS, 8 * LEVEL_PITCH, LANES), f32),
            pltpu.VMEM((3, 8 * PITCH, LANES), f32),
            pltpu.VMEM((3, PAIRS, LANES), f32),
            pltpu.VMEM((3, LANES, LANES), f32),
            pltpu.VMEM((ZERO_TUBE * 8 + 8, LANES), f32),
            pltpu.VMEM((SPECIES, NLEV, COL_CAP), f32),
            pltpu.SemaphoreType.DMA((SPECIES,)),
        ],
        name="solve",
        flops=40_000_000,
    )(core, units, table, got, coefs, weights)


def halves(x):
    high = x.astype(jnp.bfloat16)
    return high, (x - high.astype(f32)).astype(jnp.bfloat16)


def product(x, high, low):
    x_high, x_low = halves(x)
    dot = functools.partial(jnp.dot, preferred_element_type=f32)
    return dot(x_high, high) + (dot(x_low, high) + dot(x_high, low))


def lines_kernel(
    items_ref, yield_ref, rates_ref, waves_ref, fwd_high, fwd_low, inv_high, inv_low, out_hbm,
    spec_in, spec, mixed, done, sems,
):
    tubes = 32 * PEER_SLOTS
    for b in range(4):
        for s in range(SPECIES):
            for r in range(PEER_SLOTS):
                rows = items_ref[pl.ds(b * 32 * ITEM_ROWS + r * SPECIES + s, 32, stride=ITEM_ROWS), :]
                spec_in[b, pl.ds(s * tubes + r, 32, stride=PEER_SLOTS), :] = rows

    half = SPECIES * tubes // 2

    @pl.loop(0, 2)
    def _(step):
        row = pl.multiple_of(step * half, half)
        x = jnp.concatenate([spec_in[b, pl.ds(row, half), :] for b in range(4)], axis=1)
        spec[pl.ds(row, half), :] = product(x, fwd_high[...], fwd_low[...])

    waves = waves_ref[...]
    for i in range(IONS):
        keep = (1.0 - rates_ref[IONS + i]) + rates_ref[i] * waves
        gain = jnp.ones_like(waves)
        for _ in range(SECTIONS - 1):
            gain = gain * keep + 1.0
        total = (yield_ref[i * SPECIES] * gain) * spec[:tubes, :]
        for s in range(1, SPECIES):
            total = total + (yield_ref[i * SPECIES + s] * gain) * spec[s * tubes : (s + 1) * tubes, :]
        mixed[i] = total

    def leave(i):
        return pltpu.make_async_copy(done.at[i], out_hbm.at[0, i], sems.at[i])

    @pl.loop(0, IONS)
    def _(i):
        done[i] = product(mixed[i], inv_high[...], inv_low[...])
        leave(i).start()

    for i in range(IONS):
        leave(i).wait()


def cosine_basis():
    k = np.arange(LINE_PTS)[:, None]
    n = np.arange(LINE_PTS)[None, :]
    basis = np.cos(np.pi * k * (n + 0.5) / LINE_PTS) * np.sqrt(2.0 / LINE_PTS)
    basis[0] *= np.sqrt(0.5)
    waves = 2.0 * np.cos(np.pi * np.arange(LINE_PTS) / LINE_PTS) - 2.0
    return basis, waves


def lines(items, ion_yield, ion_spread, ion_loss):
    basis, waves = cosine_basis()

    def parts(matrix):
        matrix = matrix.astype(np.float32)
        high = matrix.astype(jnp.bfloat16)
        low = (matrix - high.astype(np.float32)).astype(jnp.bfloat16)
        return jnp.asarray(high), jnp.asarray(low)

    waves = jnp.asarray(waves.astype(np.float32))[None]
    tubes = 32 * PEER_SLOTS
    by_ion = call(
        lines_kernel,
        sds((1, IONS, tubes, LINE_PTS)),
        [HELD, SMEM, SMEM] + [HELD] * 5,
        HBM,
        [
            pltpu.VMEM((4, SPECIES * tubes, LANES), f32),
            pltpu.VMEM((SPECIES * tubes, LINE_PTS), f32),
            pltpu.VMEM((IONS, tubes, LINE_PTS), f32),
            pltpu.VMEM((IONS, tubes, LINE_PTS), f32),
            pltpu.SemaphoreType.DMA((IONS,)),
        ],
        name="lines",
        flops=2_000_000_000,
    )(items, ion_yield.reshape(-1), jnp.concatenate([ion_spread, ion_loss]), waves, *parts(basis.T), *parts(basis))
    return jnp.swapaxes(by_ion, 1, 2)


def swap(x, axis, offset):
    count = lax.axis_size(axis)
    lows = range(offset, count - 1, 2)
    return lax.ppermute(x, axis, [(i, i + 1) for i in lows] + [(i + 1, i) for i in lows])


def on_device(
    neutrals,
    wind_lon,
    wind_lat,
    wind_lev,
    eddy_coupling,
    pair_weight,
    ion_yield,
    ion_spread,
    ion_loss,
    column_order,
    column_units,
    tube_owner,
):
    lev = lax.axis_index("lev")

    side = jnp.stack([lev % 2, lax.axis_index("band") % 2]).astype(jnp.int32)
    slab = outer_slab(side, neutrals, wind_lev)
    outer_wind = outer_halo = swap(slab, "lev", 1)
    neutrals, *winds, inner, row, far_row = edges(side, neutrals, wind_lon, wind_lat, wind_lev, slab)
    wind_rows = rows = swap(row, "band", 0), swap(far_row, "band", 1)
    inner_wind = inner_halo = swap(inner, "lev", 0)

    starts = jnp.cumsum(column_units) - column_units
    order = column_order[0]
    lat = jnp.zeros_like(order)
    for i in range(1, BAND_LATS):
        lat = lat + (order >= i * NLON).astype(jnp.int32)
    places = jnp.pad(order + lat * (LON_PAD - NLON), (0, ORDER_PAD - BAND_COLS))
    own_units = column_units[lev].reshape(1)
    padded = jnp.pad(order, (0, SLOTS_PAD))
    own = lax.dynamic_slice(padded, (TUBE_COLS * starts[lev],), (SLOTS_PAD,))
    own_lat = jnp.zeros_like(own)
    for i in range(1, BAND_LATS):
        own_lat = own_lat + (own >= i * NLON).astype(jnp.int32)
    own_lon = own - own_lat * NLON
    own_rows = (own_lat * 6 + own_lon // 512) * LANES + own_lon % LANES
    own_sel = ((own_lon // LANES) % 4).reshape(SLOT_BLOCKS, LANES)
    zero = jnp.zeros((SPECIES, 1), f32)
    lower = jnp.concatenate([zero, eddy_coupling[:, 1:]], 1)
    upper = jnp.concatenate([eddy_coupling[:, 1:], zero], 1)
    inv = 1.0 / (1.0 + lower + upper)
    coefs = jnp.stack([lower * inv, upper * inv, inv]).reshape(3, SPECIES, 8, 8)
    table, own_weights, coefs = prepare(
        own_units,
        tube_owner[lev, :, 0],
        own_rows,
        own_sel,
        pair_weight.reshape(PAIRS * BAND_LATS, NLON),
        jnp.swapaxes(coefs, 2, 3).reshape(-1, 1),
    )

    owners = lax.axis_size("lev")
    step = functools.partial(advance_level, side, winds)
    inner, inner_wind = step(rows, wind_rows, inner_halo, inner_wind, (neutrals,), False, False)
    inner_halo = swap(inner, "lev", 0)
    outer, outer_wind, row, far_row = step(rows, wind_rows, outer_halo, outer_wind, (neutrals,), True, False, (inner,))
    outer_halo = swap(outer, "lev", 1)
    rows = swap(row, "band", 0), swap(far_row, "band", 1)
    (inner_mine,) = step(rows, wind_rows, inner_halo, inner_wind, (outer, inner), False, True)
    inner_other = swap(inner_mine, "lev", 0)
    (outer_mine,) = step(rows, wind_rows, outer_halo, outer_wind, (outer, inner), True, True, (inner_mine,))
    blocks = (inner_mine, outer_mine, inner_other, swap(outer_mine, "lev", 0))

    core = (lev % 2).reshape(1)
    parity = [[2 * i + c for i in range(owners // 2)] for c in range(2)]
    outgoing = pack(core, starts, column_units, places, blocks)
    got = lax.all_to_all(
        outgoing.reshape(16, PEER_ROWS, LANES), "lev", 0, 0, axis_index_groups=parity, tiled=True
    ).reshape(16 * PEER_ROWS, LANES)
    column_state, items = solve(core, own_units, table, got, coefs, own_weights)

    items = lax.all_to_all(
        items.reshape(PEERS, ITEM_ROWS, LANES), ("band", "lev"), 0, 0, tiled=True
    ).reshape(PEERS * ITEM_ROWS, LANES)
    return column_state, lines(items, ion_yield, ion_spread, ion_loss)


def solution(mesh):
    placed = (
        P(None, "lev", "band", None),
        P("lev", "band", None),
        P("lev", "band", None),
        P("lev", "band", None),
        P(),
        P(None, "band", None),
        P(),
        P(),
        P(),
        P("band", None),
        P(),
        P(),
    )
    return jax.shard_map(
        on_device,
        mesh=mesh,
        in_specs=placed,
        out_specs=(P("band", "lev", None, None, None), P(("band", "lev"), None, None, None)),
        check_vma=False,
    )
```

```python
import functools

import jax
import jax.numpy as jnp
import numpy as np
from jax import lax
from jax.experimental import pallas as pl
from jax.experimental.pallas import tpu as pltpu
from jax.sharding import PartitionSpec as P


SPECIES = 5
IONS = 7
NLON = 2880
NLEV = 64
PAIRS = 32
BAND_LATS = 8
SWEEPS = 8
SECTIONS = 20
TUBE_COLS = 4
PEERS = 128
PEER_SLOTS = 3
COL_CAP = 1080
BAND_COLS = BAND_LATS * NLON
LINE_PTS = 512

LANES = 128
LON_BLOCKS = 23
LON_PAD = LON_BLOCKS * LANES
CHIP_LEVS = 4
PITCH = 9
LEVEL_PITCH = 257
PLANES = 12
GROUPS = 6
CHUNKS = 3
MSG_ROWS = 64
PEER_ROWS = CHUNKS * MSG_ROWS
SLOT_BLOCKS = 9
SLOTS_PAD = SLOT_BLOCKS * LANES
ORDER_PAD = BAND_COLS + 2 * LANES
UNROLL = 64
ZERO_TUBE = SLOT_BLOCKS * 32
ITEM_ROWS = 16

f32 = jnp.float32
VMEM = pl.BlockSpec(memory_space=pltpu.VMEM)
HELD = pl.BlockSpec(memory_space=pltpu.VMEM)
SMEM = pl.BlockSpec(memory_space=pltpu.SMEM)
HBM = pl.BlockSpec(memory_space=pltpu.HBM)


def on_chip(shape, dtype=f32):
    return pltpu.VMEM(shape, dtype)


def call(kernel, out_shape, in_specs, out_specs, scratch=(), flops=0, vmem=16):
    run = pl.pallas_call(
        kernel,
        out_shape=out_shape,
        in_specs=in_specs,
        out_specs=out_specs,
        scratch_shapes=list(scratch),
        cost_estimate=pl.CostEstimate(flops=flops, bytes_accessed=1 << 20, transcendentals=0),
        compiler_params=pltpu.CompilerParams(vmem_limit_bytes=vmem * 1024 * 1024),
    )

    def place(x, spec):
        space = pltpu.VMEM if spec is HELD else pltpu.HBM if spec is HBM else None
        return x if space is None else pltpu.with_memory_space_constraint(x, space)

    def placed(*args):
        return run(*(place(x, spec) for x, spec in zip(args, in_specs)))

    return placed


def sds(shape, dtype=f32):
    return jax.ShapeDtypeStruct(shape, dtype)


def upwind(courant_plus, courant_minus, upstream, downstream):
    return courant_plus * upstream + courant_minus * downstream


def edges_kernel(
    side_ref, n_hbm, wlon_hbm, wlat_hbm, wlev_hbm,
    n_ref, wlon_ref, wlat_ref, wlev_ref, inner_ref, outer_ref, row_ref, far_row_ref, sems,
):
    fetches = [
        pltpu.make_async_copy(n_hbm.at[s], n_ref.at[s], sems.at[s]) for s in range(SPECIES)
    ]
    fetches.append(pltpu.make_async_copy(wlat_hbm, wlat_ref, sems.at[SPECIES]))
    fetches.append(pltpu.make_async_copy(wlev_hbm, wlev_ref, sems.at[SPECIES + 1]))
    fetches.append(pltpu.make_async_copy(wlon_hbm, wlon_ref, sems.at[SPECIES + 2]))
    for fetch in fetches:
        fetch.start()
    for fetch in fetches[:-1]:
        fetch.wait()
    core, odd = side_ref[0], side_ref[1] == 1
    inner_ref[SPECIES] = wlev_ref[0]
    outer_ref[SPECIES] = wlev_ref[0]
    for j in range(2):
        row_ref[SPECIES, j] = wlat_ref[j, :1]
        far_row_ref[SPECIES, j] = wlat_ref[j, :1]

    @pl.loop(0, SPECIES)
    def _(s):
        inner_ref[s] = n_ref[s, 1 - core]
        outer_ref[s] = n_ref[s, core]
        for j in range(2):
            first, last = n_ref[s, j, :1], n_ref[s, j, BAND_LATS - 1 :]
            row_ref[s, j] = jnp.where(odd, first, last)
            far_row_ref[s, j] = jnp.where(odd, last, first)

    fetches[-1].wait()


def edges(side, density, wind_lon, wind_lat, wind_lev):
    return call(
        edges_kernel,
        (
            on_chip(density.shape),
            on_chip(wind_lon.shape),
            on_chip(wind_lat.shape),
            on_chip(wind_lev.shape),
            on_chip((SPECIES + 1, BAND_LATS, NLON)),
            on_chip((SPECIES + 1, BAND_LATS, NLON)),
            on_chip((SPECIES + 1, 2, 1, NLON)),
            on_chip((SPECIES + 1, 2, 1, NLON)),
        ),
        [SMEM] + [HBM] * 4,
        (VMEM,) * 8,
        [pltpu.SemaphoreType.DMA((SPECIES + 3,))],
        flops=1_000_000,
    )(side, density, wind_lon, wind_lat, wind_lev)


def transport_kernel(side_ref, n_ref, wlon_ref, wlat_ref, wlev_ref, *refs, last):
    inner_ref, outer_ref, row_ref, far_row_ref = refs[:4]
    inner_wind, outer_wind, row_wind, far_row_wind = refs[4:8]
    outs = refs[8:]
    odd = side_ref[1] == 1

    def split(c):
        return jnp.maximum(c, 0.0), jnp.minimum(c, 0.0)

    def shift_west(x):
        return jnp.concatenate([x[:, NLON - 1 :], x[:, : NLON - 1]], axis=1)

    def shift_east(x):
        return jnp.concatenate([x[:, 1:], x[:, :1]], axis=1)

    def advance(core):
        below_ref, above_ref, above_wind = (
            (outer_ref, inner_ref, inner_wind) if core == 0 else (inner_ref, outer_ref, outer_wind)
        )
        for j in range(2):

            @pl.loop(0, SPECIES)
            def _(s):
                x = n_ref[s, j]
                flux = upwind(*split(wlon_ref[j]), shift_west(x), x)
                total = x + (flux - shift_east(flux))
                south = jnp.where(odd, row_ref[s, j], far_row_ref[s, j])
                north = jnp.where(odd, far_row_ref[s, j], row_ref[s, j])
                north_wind = jnp.where(odd, far_row_wind[SPECIES, j], row_wind[SPECIES, j])
                southern = jnp.concatenate([south, x[: BAND_LATS - 1]], axis=0)
                flux = upwind(*split(wlat_ref[j]), southern, x)
                edge = upwind(*split(north_wind), x[BAND_LATS - 1 :], north)
                total = total + (flux - jnp.concatenate([flux[1:], edge], axis=0))
                if j == 0:
                    beneath, overhead, over_wind = below_ref[s], n_ref[s, 1], wlev_ref[1]
                else:
                    beneath, overhead, over_wind = n_ref[s, 0], above_ref[s], above_wind[SPECIES]
                flux = upwind(*split(wlev_ref[j]), beneath, x)
                total = total + (flux - upwind(*split(over_wind), x, overhead))
                if last:
                    row = pl.multiple_of((j * SPECIES + s) * BAND_LATS, BAND_LATS)
                    for blk in range(LON_BLOCKS):
                        wide = min(LANES, NLON - blk * LANES)
                        outs[0][blk, pl.ds(row, BAND_LATS), :wide] = total[:, blk * LANES : blk * LANES + wide]
                    return
                outs[0][s, j] = total
                outs[2 if j == core else 1][s] = total
                first, final = total[:1], total[BAND_LATS - 1 :]
                outs[3][s, j] = jnp.where(odd, first, final)
                outs[4][s, j] = jnp.where(odd, final, first)

    for core in range(2):
        pl.when(side_ref[0] == core)(functools.partial(advance, core))


def transport_step(side, density, winds, halo, wind_halo, last):
    if last:
        out_shape = (on_chip((LON_BLOCKS, 2 * SPECIES * BAND_LATS, LANES)),)
    else:
        out_shape = (
            on_chip((SPECIES, 2, BAND_LATS, NLON)),
            on_chip((SPECIES, BAND_LATS, NLON)),
            on_chip((SPECIES, BAND_LATS, NLON)),
            on_chip((SPECIES, 2, 1, NLON)),
            on_chip((SPECIES, 2, 1, NLON)),
        )
    return call(
        functools.partial(transport_kernel, last=last),
        out_shape,
        [SMEM] + [HELD] * 12,
        (VMEM,) * len(out_shape),
        flops=4_000_000,
    )(side, density, *winds, *halo, *wind_halo)


def prepare_kernel(
    units_ref, owner_ref, rows_ref, sel_ref, weight_ref, column_ref,
    table_ref, own_ref, coef_ref, count, blocks, table, picked,
):
    @pl.loop(0, PEERS * PEER_SLOTS // 8)
    def _(i):
        for k in range(8):
            table_ref[i * 8 + k] = ZERO_TUBE

    @pl.loop(0, PEERS // 8)
    def _(i):
        for k in range(8):
            count[i * 8 + k] = 0

    @pl.loop(0, units_ref[0])
    def _(u):
        dest = owner_ref[u]
        rank = count[dest]
        count[dest] = rank + 1
        table_ref[dest * PEER_SLOTS + rank] = u

    coef_ref[...] = jnp.broadcast_to(column_ref[...], coef_ref.shape)

    for blk in range(LON_BLOCKS):
        wide = min(LANES, NLON - blk * LANES)
        blocks[blk, :, :wide] = weight_ref[:, blk * LANES : blk * LANES + wide]

    @pl.loop(0, BAND_LATS)
    def _(lat):
        for g in range(6):
            parts = [
                blocks[min(4 * g + i, LON_BLOCKS - 1), pl.ds(lat + h * BAND_LATS, 8, stride=4 * BAND_LATS), :]
                for i in range(4)
                for h in range(4)
            ]
            start = pl.multiple_of((lat * 6 + g) * LANES, LANES)
            table[pl.ds(start, LANES), :] = jnp.concatenate(parts, axis=0).T

    @pl.loop(0, SLOTS_PAD // UNROLL)
    def _(step):
        base = pl.multiple_of(step * UNROLL, UNROLL)
        places = rows_ref.at[pl.ds(base, UNROLL)]
        for i in range(UNROLL):
            picked[pl.ds(base + i, 1), :] = table[pl.ds(places[i], 1), :]

    for blk in range(SLOT_BLOCKS):
        turned = picked[blk * LANES : (blk + 1) * LANES, :].T
        which = sel_ref[blk : blk + 1, :]
        kept = turned[:PAIRS]
        for i in range(1, 4):
            kept = jnp.where(which == i, turned[i * PAIRS : (i + 1) * PAIRS], kept)
        own_ref[blk] = kept


def prepare(units, owners, rows, sel, weights, column):
    return call(
        prepare_kernel,
        (
            sds((PEERS * PEER_SLOTS,), jnp.int32),
            on_chip((SLOT_BLOCKS, PAIRS, LANES)),
            on_chip((3 * SPECIES * NLEV, LANES)),
        ),
        [SMEM, SMEM, SMEM, VMEM, VMEM, VMEM],
        (SMEM, VMEM, VMEM),
        [
            pltpu.SMEM((PEERS,), jnp.int32),
            pltpu.VMEM((LON_BLOCKS, PAIRS * BAND_LATS, LANES), f32),
            pltpu.VMEM((BAND_LATS * 6 * LANES, LANES), f32),
            pltpu.VMEM((SLOTS_PAD, LANES), f32),
        ],
        flops=20_000_000,
    )(units, owners, rows, sel, weights, column)


def pack_kernel(
    core_ref, starts_ref, units_ref, order_ref, mine_ref, other_ref, out_hbm, planes, table_ref, msg_ref, sems
):
    @pl.loop(0, LON_BLOCKS)
    def _(blk):
        for side, source in enumerate((mine_ref, other_ref)):
            for j in range(2):
                for i in range(PLANES):
                    from_row = (j * SPECIES + i % SPECIES) * BAND_LATS
                    planes[blk, pl.ds(((2 * side + j) * PLANES + i) * PITCH, BAND_LATS), :] = source[
                        blk, from_row : from_row + BAND_LATS, :
                    ]

    @pl.loop(0, LON_BLOCKS)
    def _(blk):
        for lat in range(BAND_LATS):
            parts = [
                planes[blk, pl.ds((jj * PLANES + first) * PITCH + lat, 8, stride=PITCH), :]
                for jj in range(CHIP_LEVS)
                for first in (0, 3, 1, 4)
            ]
            start = pl.multiple_of((lat * LON_BLOCKS + blk) * LANES, LANES)
            table_ref[pl.ds(start, LANES), :] = jnp.concatenate(parts, axis=0).T

    core = core_ref[0]
    lane = lax.broadcasted_iota(jnp.int32, (1, LANES), 1)
    group_of = lax.div(lax.rem(lane, 32), SPECIES)

    def send(peer):
        rows = pl.ds(pl.multiple_of(peer * PEER_ROWS, PEER_ROWS), PEER_ROWS)
        return pltpu.make_async_copy(msg_ref.at[rows, :], out_hbm.at[rows, :], sems.at[peer])

    @pl.loop(0, 16)
    def _(peer):
        owner = 2 * peer + core
        live = TUBE_COLS * units_ref[owner]
        first = TUBE_COLS * starts_ref[owner]

        @pl.loop(0, lax.div(live + (MSG_ROWS - 1), MSG_ROWS))
        def _(piece):
            chunk = lax.div(piece, GROUPS)
            mask = group_of == piece - chunk * GROUPS
            row = pl.multiple_of(peer * PEER_ROWS + chunk * MSG_ROWS, MSG_ROWS)
            base = first + piece * MSG_ROWS
            for i in range(MSG_ROWS):
                place = order_ref.at[pl.ds(i, ORDER_PAD - MSG_ROWS)][base]
                value = table_ref[pl.ds(place, 1), :]
                pltpu.store(msg_ref.at[pl.ds(row + i, 1), :], value, mask=mask)

        send(peer).start()

    @pl.loop(0, 16)
    def _(peer):
        send(peer).wait()


def pack(core, starts, units, order, mine, other):
    return call(
        pack_kernel,
        sds((16 * PEER_ROWS, LANES)),
        [SMEM, SMEM, SMEM, SMEM, HELD, HELD],
        HBM,
        [
            pltpu.VMEM((LON_BLOCKS, CHIP_LEVS * PLANES * PITCH, LANES), f32),
            pltpu.VMEM((BAND_LATS * LON_PAD, LANES), f32),
            pltpu.VMEM((16 * PEER_ROWS, LANES), f32),
            pltpu.SemaphoreType.DMA((16,)),
        ],
        flops=30_000_000,
        vmem=32,
    )(core, starts, units, order, mine, other)


def solve_kernel(
    core_ref, units_ref, table_ref, got_ref, coef_ref, weight_ref, state_hbm, items_ref,
    turned, natural, pairs, wide, tubes, state, sems,
):
    core = core_ref[0]
    live = TUBE_COLS * units_ref[0]
    lane = lax.broadcasted_iota(jnp.int32, (1, LANES), 1)
    low = lane < 64
    quarter = lax.div(lane, 32)

    @pl.loop(0, 8)
    def _(i):
        for side in range(2):
            out = i * LEVEL_PITCH + side * LANES
            for chunk in range(CHUNKS):
                row = pl.multiple_of((2 * i + side) * PEER_ROWS + chunk * MSG_ROWS, MSG_ROWS)
                flipped = jnp.concatenate([got_ref[pl.ds(row, MSG_ROWS), :]] * 2, axis=0).T
                turned[chunk, pl.ds(out + 64 * core, 64), :] = flipped[:64]
                turned[chunk, pl.ds(out + 64 - 64 * core, 64), :] = flipped[64:]

    def leave(s):
        return pltpu.make_async_copy(state.at[s], state_hbm.at[0, 0, s], sems.at[s])

    @pl.loop(0, SPECIES)
    def _(s):
        def coefs(which):
            row = pl.multiple_of((which * SPECIES + s) * NLEV, NLEV)
            return [coef_ref[pl.ds(row + 8 * v, 8), :] for v in range(8)]

        lower, upper, inv = coefs(0), coefs(1), coefs(2)
        for blk in range(SLOT_BLOCKS):
            chunk, i = divmod(blk, 3)

            def levels(group, v):
                return turned[chunk, pl.ds(32 * v + group * SPECIES + s, 8, stride=LEVEL_PITCH), :]

            rhs = [jnp.where(low, levels(2 * i, v), levels(2 * i + 1, v)) for v in range(8)]
            scaled = [rhs[v] * inv[v] for v in range(8)]
            x = rhs
            for _ in range(SWEEPS):
                beneath = [pltpu.roll(x[7], 1, axis=0)] + x[:7]
                overhead = x[1:] + [pltpu.roll(x[0], 7, axis=0)]
                x = [scaled[v] + lower[v] * beneath[v] + upper[v] * overhead[v] for v in range(8)]
            keep = lane + blk * LANES < live
            for v in range(8):
                natural[i, pl.ds(v, 8, stride=PITCH), :] = jnp.where(keep, x[v], 0.0)
            width = min(LANES, COL_CAP - blk * LANES)
            for g in range(8):
                state[s, g * 8 : g * 8 + 8, blk * LANES : blk * LANES + width] = natural[
                    i, g * PITCH : g * PITCH + 8, :width
                ]
            for h in range(4):
                weight = weight_ref[blk, 8 * h : 8 * h + 8, :]
                paired = weight * x[2 * h] + (1.0 - weight) * x[2 * h + 1]
                pairs[i, pl.ds(h, 8, stride=4), :] = paired
            wide[i] = jnp.concatenate([pairs[i]] * 4, axis=0).T
            item = wide[i, pl.ds(0, 32, stride=TUBE_COLS), :]
            for c in range(1, TUBE_COLS):
                item = jnp.where(quarter == c, wide[i, pl.ds(c, 32, stride=TUBE_COLS), :], item)
            tubes[pl.ds(blk * 256 + s, 32, stride=8), :] = item
        leave(s).start()

    tubes[ZERO_TUBE * 8 :, :] = jnp.zeros((8, LANES), f32)
    sub = lax.broadcasted_iota(jnp.int32, (8, LANES), 0)

    @pl.loop(0, PEERS // 4)
    def _(step):
        for i in range(4):
            d = step * 4 + i
            tiles = [
                tubes[pl.ds(pl.multiple_of(table_ref[d * PEER_SLOTS + r] * 8, 8), 8), :] for r in range(PEER_SLOTS)
            ]
            mid = pltpu.roll(tiles[1], 5, axis=0)
            top = pltpu.roll(tiles[2], 2, axis=0)
            row = pl.multiple_of(d * ITEM_ROWS, ITEM_ROWS)
            items_ref[pl.ds(row, 8), :] = jnp.where(sub < 5, tiles[0], mid)
            items_ref[pl.ds(row + 8, 8), :] = jnp.where(sub < 2, mid, jnp.where(sub < 7, top, 0.0))

    for s in range(SPECIES):
        leave(s).wait()


def solve(core, units, table, got, coefs, weights):
    return call(
        solve_kernel,
        (sds((1, 1, SPECIES, NLEV, COL_CAP)), sds((PEERS * ITEM_ROWS, LANES))),
        [SMEM, SMEM, SMEM] + [HELD] * 3,
        (HBM, VMEM),
        [
            pltpu.VMEM((CHUNKS, 8 * LEVEL_PITCH, LANES), f32),
            pltpu.VMEM((3, 8 * PITCH, LANES), f32),
            pltpu.VMEM((3, PAIRS, LANES), f32),
            pltpu.VMEM((3, LANES, LANES), f32),
            pltpu.VMEM((ZERO_TUBE * 8 + 8, LANES), f32),
            pltpu.VMEM((SPECIES, NLEV, COL_CAP), f32),
            pltpu.SemaphoreType.DMA((SPECIES,)),
        ],
        flops=40_000_000,
    )(core, units, table, got, coefs, weights)


def halves(x):
    high = x.astype(jnp.bfloat16)
    return high, (x - high.astype(f32)).astype(jnp.bfloat16)


def product(x, high, low):
    x_high, x_low = halves(x)
    dot = functools.partial(jnp.dot, preferred_element_type=f32)
    return dot(x_high, high) + (dot(x_low, high) + dot(x_high, low))


def lines_kernel(
    items_ref, yield_ref, rates_ref, waves_ref, fwd_high, fwd_low, inv_high, inv_low, out_hbm,
    spec_in, spec, mixed, done, sems,
):
    tubes = 32 * PEER_SLOTS
    for b in range(4):
        for s in range(SPECIES):
            for r in range(PEER_SLOTS):
                rows = items_ref[pl.ds(b * 32 * ITEM_ROWS + r * SPECIES + s, 32, stride=ITEM_ROWS), :]
                spec_in[b, pl.ds(s * tubes + r, 32, stride=PEER_SLOTS), :] = rows

    half = SPECIES * tubes // 2

    @pl.loop(0, 2)
    def _(step):
        row = pl.multiple_of(step * half, half)
        x = jnp.concatenate([spec_in[b, pl.ds(row, half), :] for b in range(4)], axis=1)
        spec[pl.ds(row, half), :] = product(x, fwd_high[...], fwd_low[...])

    waves = waves_ref[...]
    for i in range(IONS):
        keep = (1.0 - rates_ref[IONS + i]) + rates_ref[i] * waves
        gain = jnp.ones_like(waves)
        for _ in range(SECTIONS - 1):
            gain = gain * keep + 1.0
        total = (yield_ref[i * SPECIES] * gain) * spec[:tubes, :]
        for s in range(1, SPECIES):
            total = total + (yield_ref[i * SPECIES + s] * gain) * spec[s * tubes : (s + 1) * tubes, :]
        mixed[i] = total

    def leave(i):
        return pltpu.make_async_copy(done.at[i], out_hbm.at[0, i], sems.at[i])

    @pl.loop(0, IONS)
    def _(i):
        done[i] = product(mixed[i], inv_high[...], inv_low[...])
        leave(i).start()

    for i in range(IONS):
        leave(i).wait()


def cosine_basis():
    k = np.arange(LINE_PTS)[:, None]
    n = np.arange(LINE_PTS)[None, :]
    basis = np.cos(np.pi * k * (n + 0.5) / LINE_PTS) * np.sqrt(2.0 / LINE_PTS)
    basis[0] *= np.sqrt(0.5)
    waves = 2.0 * np.cos(np.pi * np.arange(LINE_PTS) / LINE_PTS) - 2.0
    return basis, waves


def lines(items, ion_yield, ion_spread, ion_loss):
    basis, waves = cosine_basis()

    def parts(matrix):
        matrix = matrix.astype(np.float32)
        high = matrix.astype(jnp.bfloat16)
        low = (matrix - high.astype(np.float32)).astype(jnp.bfloat16)
        return jnp.asarray(high), jnp.asarray(low)

    waves = jnp.asarray(waves.astype(np.float32))[None]
    tubes = 32 * PEER_SLOTS
    by_ion = call(
        lines_kernel,
        sds((1, IONS, tubes, LINE_PTS)),
        [HELD, SMEM, SMEM] + [HELD] * 5,
        HBM,
        [
            pltpu.VMEM((4, SPECIES * tubes, LANES), f32),
            pltpu.VMEM((SPECIES * tubes, LINE_PTS), f32),
            pltpu.VMEM((IONS, tubes, LINE_PTS), f32),
            pltpu.VMEM((IONS, tubes, LINE_PTS), f32),
            pltpu.SemaphoreType.DMA((IONS,)),
        ],
        flops=2_000_000_000,
    )(items, ion_yield.reshape(-1), jnp.concatenate([ion_spread, ion_loss]), waves, *parts(basis.T), *parts(basis))
    return jnp.swapaxes(by_ion, 1, 2)


def swap(x, axis, offset):
    count = lax.axis_size(axis)
    lows = range(offset, count - 1, 2)
    return lax.ppermute(x, axis, [(i, i + 1) for i in lows] + [(i + 1, i) for i in lows])


def exchange(inner, outer, row, far_row):
    outer = swap(outer, "lev", 1)
    row = swap(row, "band", 0)
    far_row = swap(far_row, "band", 1)
    inner = swap(inner, "lev", 0)
    return inner, outer, row, far_row


def on_device(
    neutrals,
    wind_lon,
    wind_lat,
    wind_lev,
    eddy_coupling,
    pair_weight,
    ion_yield,
    ion_spread,
    ion_loss,
    column_order,
    column_units,
    tube_owner,
):
    lev = lax.axis_index("lev")

    side = jnp.stack([lev % 2, lax.axis_index("band") % 2]).astype(jnp.int32)
    neutrals, *rest = edges(side, neutrals, wind_lon, wind_lat, wind_lev)
    winds, first_halo = rest[:3], exchange(*rest[3:])

    starts = jnp.cumsum(column_units) - column_units
    order = column_order[0]
    lat = jnp.zeros_like(order)
    for i in range(1, BAND_LATS):
        lat = lat + (order >= i * NLON).astype(jnp.int32)
    rows = jnp.pad(order + lat * (LON_PAD - NLON), (0, ORDER_PAD - BAND_COLS))
    own_units = column_units[lev].reshape(1)
    padded = jnp.pad(order, (0, SLOTS_PAD))
    own = lax.dynamic_slice(padded, (TUBE_COLS * starts[lev],), (SLOTS_PAD,))
    own_lat = jnp.zeros_like(own)
    for i in range(1, BAND_LATS):
        own_lat = own_lat + (own >= i * NLON).astype(jnp.int32)
    own_lon = own - own_lat * NLON
    own_rows = (own_lat * 6 + own_lon // 512) * LANES + own_lon % LANES
    own_sel = ((own_lon // LANES) % 4).reshape(SLOT_BLOCKS, LANES)
    zero = jnp.zeros((SPECIES, 1), f32)
    lower = jnp.concatenate([zero, eddy_coupling[:, 1:]], 1)
    upper = jnp.concatenate([eddy_coupling[:, 1:], zero], 1)
    inv = 1.0 / (1.0 + lower + upper)
    coefs = jnp.stack([lower * inv, upper * inv, inv]).reshape(3, SPECIES, 8, 8)
    table, own_weights, coefs = prepare(
        own_units,
        tube_owner[lev, :, 0],
        own_rows,
        own_sel,
        pair_weight.reshape(PAIRS * BAND_LATS, NLON),
        jnp.swapaxes(coefs, 2, 3).reshape(-1, 1),
    )

    density, *halo = transport_step(side, neutrals, winds, first_halo, first_halo, False)
    (mine,) = transport_step(side, density, winds, exchange(*halo), first_halo, True)
    owners = lax.axis_size("lev")
    other = swap(mine, "lev", 0)

    core = (lev % 2).reshape(1)
    parity = [[2 * i + c for i in range(owners // 2)] for c in range(2)]
    outgoing = pack(core, starts, column_units, rows, mine, other)
    got = lax.all_to_all(
        outgoing.reshape(16, PEER_ROWS, LANES), "lev", 0, 0, axis_index_groups=parity, tiled=True
    ).reshape(16 * PEER_ROWS, LANES)
    column_state, items = solve(core, own_units, table, got, coefs, own_weights)

    items = lax.all_to_all(
        items.reshape(PEERS, ITEM_ROWS, LANES), ("band", "lev"), 0, 0, tiled=True
    ).reshape(PEERS * ITEM_ROWS, LANES)
    return column_state, lines(items, ion_yield, ion_spread, ion_loss)


def solution(mesh):
    placed = (
        P(None, "lev", "band", None),
        P("lev", "band", None),
        P("lev", "band", None),
        P("lev", "band", None),
        P(),
        P(None, "band", None),
        P(),
        P(),
        P(),
        P("band", None),
        P(),
        P(),
    )

    return jax.shard_map(
        on_device,
        mesh=mesh,
        in_specs=placed,
        out_specs=(P("band", "lev", None, None, None), P(("band", "lev"), None, None, None)),
        check_vma=False,
    )
```

```python
import functools

import jax
import jax.numpy as jnp
import numpy as np
from jax import lax
from jax.experimental import pallas as pl
from jax.experimental.pallas import tpu as pltpu
from jax.sharding import PartitionSpec as P


SPECIES = 5
IONS = 7
NLON = 2880
NLEV = 64
PAIRS = 32
BAND_LATS = 8
SWEEPS = 8
SECTIONS = 20
TUBE_COLS = 4
PEERS = 128
PEER_SLOTS = 3
COL_CAP = 1080
BAND_COLS = BAND_LATS * NLON
LINE_PTS = 512

LANES = 128
LON_BLOCKS = 23
LON_PAD = LON_BLOCKS * LANES
CHIP_LEVS = 4
PITCH = 9
LEVEL_PITCH = 257
PLANES = 12
GROUPS = 6
CHUNKS = 3
MSG_ROWS = 64
PEER_ROWS = CHUNKS * MSG_ROWS
SLOT_BLOCKS = 9
SLOTS_PAD = SLOT_BLOCKS * LANES
ORDER_PAD = BAND_COLS + 3 * LANES
UNROLL = 64
ZERO_TUBE = SLOT_BLOCKS * 32
ITEM_ROWS = 16

f32 = jnp.float32
VMEM = pl.BlockSpec(memory_space=pltpu.VMEM)
HELD = pl.BlockSpec(memory_space=pltpu.VMEM)
SMEM = pl.BlockSpec(memory_space=pltpu.SMEM)
HBM = pl.BlockSpec(memory_space=pltpu.HBM)


def on_chip(shape, dtype=f32):
    return pltpu.VMEM(shape, dtype)


def call(kernel, out_shape, in_specs, out_specs, scratch=(), flops=0, vmem=16):
    run = pl.pallas_call(
        kernel,
        out_shape=out_shape,
        in_specs=in_specs,
        out_specs=out_specs,
        scratch_shapes=list(scratch),
        cost_estimate=pl.CostEstimate(flops=flops, bytes_accessed=1 << 20, transcendentals=0),
        compiler_params=pltpu.CompilerParams(vmem_limit_bytes=vmem * 1024 * 1024),
    )

    def place(x, spec):
        space = pltpu.VMEM if spec is HELD else pltpu.HBM if spec is HBM else None
        return x if space is None else pltpu.with_memory_space_constraint(x, space)

    def placed(*args):
        return run(*(place(x, spec) for x, spec in zip(args, in_specs)))

    return placed


def sds(shape, dtype=f32):
    return jax.ShapeDtypeStruct(shape, dtype)


def upwind(courant_plus, courant_minus, upstream, downstream):
    return courant_plus * upstream + courant_minus * downstream


def edges_kernel(
    side_ref, n_hbm, wlon_hbm, wlat_hbm, wlev_hbm,
    n_ref, wlon_ref, wlat_ref, wlev_ref, inner_ref, outer_ref, row_ref, far_row_ref, sems,
):
    fetches = [
        pltpu.make_async_copy(n_hbm.at[s], n_ref.at[s], sems.at[s]) for s in range(SPECIES)
    ]
    fetches.append(pltpu.make_async_copy(wlat_hbm, wlat_ref, sems.at[SPECIES]))
    fetches.append(pltpu.make_async_copy(wlev_hbm, wlev_ref, sems.at[SPECIES + 1]))
    fetches.append(pltpu.make_async_copy(wlon_hbm, wlon_ref, sems.at[SPECIES + 2]))
    for fetch in fetches:
        fetch.start()
    for fetch in fetches[:-1]:
        fetch.wait()
    core, odd = side_ref[0], side_ref[1] == 1
    inner_ref[SPECIES] = wlev_ref[0]
    outer_ref[SPECIES] = wlev_ref[0]
    for j in range(2):
        row_ref[SPECIES, j] = wlat_ref[j, :1]
        far_row_ref[SPECIES, j] = wlat_ref[j, :1]

    @pl.loop(0, SPECIES)
    def _(s):
        inner_ref[s] = n_ref[s, 1 - core]
        outer_ref[s] = n_ref[s, core]
        for j in range(2):
            first, last = n_ref[s, j, :1], n_ref[s, j, BAND_LATS - 1 :]
            row_ref[s, j] = jnp.where(odd, first, last)
            far_row_ref[s, j] = jnp.where(odd, last, first)

    fetches[-1].wait()


def edges(side, density, wind_lon, wind_lat, wind_lev):
    return call(
        edges_kernel,
        (
            on_chip(density.shape),
            on_chip(wind_lon.shape),
            on_chip(wind_lat.shape),
            on_chip(wind_lev.shape),
            on_chip((SPECIES + 1, BAND_LATS, NLON)),
            on_chip((SPECIES + 1, BAND_LATS, NLON)),
            on_chip((SPECIES + 1, 2, 1, NLON)),
            on_chip((SPECIES + 1, 2, 1, NLON)),
        ),
        [SMEM] + [HBM] * 4,
        (VMEM,) * 8,
        [pltpu.SemaphoreType.DMA((SPECIES + 3,))],
        flops=1_000_000,
    )(side, density, wind_lon, wind_lat, wind_lev)


def transport_kernel(side_ref, n_ref, wlon_ref, wlat_ref, wlev_ref, *refs, last):
    inner_ref, outer_ref, row_ref, far_row_ref = refs[:4]
    inner_wind, outer_wind, row_wind, far_row_wind = refs[4:8]
    outs = refs[8:]
    odd = side_ref[1] == 1

    def split(c):
        return jnp.maximum(c, 0.0), jnp.minimum(c, 0.0)

    def shift_west(x):
        return jnp.concatenate([x[:, NLON - 1 :], x[:, : NLON - 1]], axis=1)

    def shift_east(x):
        return jnp.concatenate([x[:, 1:], x[:, :1]], axis=1)

    def advance(core):
        below_ref, above_ref, above_wind = (
            (outer_ref, inner_ref, inner_wind) if core == 0 else (inner_ref, outer_ref, outer_wind)
        )
        for j in range(2):

            @pl.loop(0, SPECIES)
            def _(s):
                x = n_ref[s, j]
                flux = upwind(*split(wlon_ref[j]), shift_west(x), x)
                total = x + (flux - shift_east(flux))
                south = jnp.where(odd, row_ref[s, j], far_row_ref[s, j])
                north = jnp.where(odd, far_row_ref[s, j], row_ref[s, j])
                north_wind = jnp.where(odd, far_row_wind[SPECIES, j], row_wind[SPECIES, j])
                southern = jnp.concatenate([south, x[: BAND_LATS - 1]], axis=0)
                flux = upwind(*split(wlat_ref[j]), southern, x)
                edge = upwind(*split(north_wind), x[BAND_LATS - 1 :], north)
                total = total + (flux - jnp.concatenate([flux[1:], edge], axis=0))
                if j == 0:
                    beneath, overhead, over_wind = below_ref[s], n_ref[s, 1], wlev_ref[1]
                else:
                    beneath, overhead, over_wind = n_ref[s, 0], above_ref[s], above_wind[SPECIES]
                flux = upwind(*split(wlev_ref[j]), beneath, x)
                total = total + (flux - upwind(*split(over_wind), x, overhead))
                if last:
                    row = pl.multiple_of((j * SPECIES + s) * BAND_LATS, BAND_LATS)
                    for blk in range(LON_BLOCKS):
                        wide = min(LANES, NLON - blk * LANES)
                        outs[0][blk, pl.ds(row, BAND_LATS), :wide] = total[:, blk * LANES : blk * LANES + wide]
                    return
                outs[0][s, j] = total
                outs[2 if j == core else 1][s] = total
                first, final = total[:1], total[BAND_LATS - 1 :]
                outs[3][s, j] = jnp.where(odd, first, final)
                outs[4][s, j] = jnp.where(odd, final, first)

    for core in range(2):
        pl.when(side_ref[0] == core)(functools.partial(advance, core))


def transport_step(side, density, winds, halo, wind_halo, last):
    if last:
        out_shape = (on_chip((LON_BLOCKS, 2 * SPECIES * BAND_LATS, LANES)),)
    else:
        out_shape = (
            on_chip((SPECIES, 2, BAND_LATS, NLON)),
            on_chip((SPECIES, BAND_LATS, NLON)),
            on_chip((SPECIES, BAND_LATS, NLON)),
            on_chip((SPECIES, 2, 1, NLON)),
            on_chip((SPECIES, 2, 1, NLON)),
        )
    return call(
        functools.partial(transport_kernel, last=last),
        out_shape,
        [SMEM] + [HELD] * 12,
        (VMEM,) * len(out_shape),
        flops=4_000_000,
    )(side, density, *winds, *halo, *wind_halo)


def prepare_kernel(
    units_ref, owner_ref, rows_ref, sel_ref, weight_ref, column_ref,
    table_ref, own_ref, coef_ref, count, blocks, table, picked,
):
    @pl.loop(0, PEERS * PEER_SLOTS // 8)
    def _(i):
        for k in range(8):
            table_ref[i * 8 + k] = ZERO_TUBE

    @pl.loop(0, PEERS // 8)
    def _(i):
        for k in range(8):
            count[i * 8 + k] = 0

    @pl.loop(0, units_ref[0])
    def _(u):
        dest = owner_ref[u]
        rank = count[dest]
        count[dest] = rank + 1
        table_ref[dest * PEER_SLOTS + rank] = u

    coef_ref[...] = jnp.broadcast_to(column_ref[...], coef_ref.shape)

    for blk in range(LON_BLOCKS):
        wide = min(LANES, NLON - blk * LANES)
        blocks[blk, :, :wide] = weight_ref[:, blk * LANES : blk * LANES + wide]

    @pl.loop(0, BAND_LATS)
    def _(lat):
        for g in range(6):
            parts = [
                blocks[min(4 * g + i, LON_BLOCKS - 1), pl.ds(lat + h * BAND_LATS, 8, stride=4 * BAND_LATS), :]
                for i in range(4)
                for h in range(4)
            ]
            start = pl.multiple_of((lat * 6 + g) * LANES, LANES)
            table[pl.ds(start, LANES), :] = jnp.concatenate(parts, axis=0).T

    @pl.loop(0, SLOTS_PAD // UNROLL)
    def _(step):
        base = pl.multiple_of(step * UNROLL, UNROLL)
        places = rows_ref.at[pl.ds(base, UNROLL)]
        for i in range(UNROLL):
            picked[pl.ds(base + i, 1), :] = table[pl.ds(places[i], 1), :]

    for blk in range(SLOT_BLOCKS):
        turned = picked[blk * LANES : (blk + 1) * LANES, :].T
        which = sel_ref[blk : blk + 1, :]
        kept = turned[:PAIRS]
        for i in range(1, 4):
            kept = jnp.where(which == i, turned[i * PAIRS : (i + 1) * PAIRS], kept)
        own_ref[blk] = kept


def prepare(units, owners, rows, sel, weights, column):
    return call(
        prepare_kernel,
        (
            sds((PEERS * PEER_SLOTS,), jnp.int32),
            on_chip((SLOT_BLOCKS, PAIRS, LANES)),
            on_chip((3 * SPECIES * NLEV, LANES)),
        ),
        [SMEM, SMEM, SMEM, VMEM, VMEM, VMEM],
        (SMEM, VMEM, VMEM),
        [
            pltpu.SMEM((PEERS,), jnp.int32),
            pltpu.VMEM((LON_BLOCKS, PAIRS * BAND_LATS, LANES), f32),
            pltpu.VMEM((BAND_LATS * 6 * LANES, LANES), f32),
            pltpu.VMEM((SLOTS_PAD, LANES), f32),
        ],
        flops=20_000_000,
    )(units, owners, rows, sel, weights, column)


def pack_kernel(
    core_ref, starts_ref, units_ref, order_hbm, mine_ref, other_ref,
    out_hbm, order_ref, planes, table_ref, msg_ref, sems, order_sem,
):
    core = core_ref[0]

    fetch = pltpu.make_async_copy(order_hbm, order_ref, order_sem)
    fetch.start()

    @pl.loop(0, LON_BLOCKS)
    def _(blk):
        for side, source in enumerate((mine_ref, other_ref)):
            for j in range(2):
                for i in range(PLANES):
                    from_row = (j * SPECIES + i % SPECIES) * BAND_LATS
                    planes[blk, pl.ds(((2 * side + j) * PLANES + i) * PITCH, BAND_LATS), :] = source[
                        blk, from_row : from_row + BAND_LATS, :
                    ]

    @pl.loop(0, LON_BLOCKS)
    def _(blk):
        for lat in range(BAND_LATS):
            parts = [
                planes[blk, pl.ds((jj * PLANES + first) * PITCH + lat, 8, stride=PITCH), :]
                for jj in range(CHIP_LEVS)
                for first in (0, 3, 1, 4)
            ]
            start = pl.multiple_of((lat * LON_BLOCKS + blk) * LANES, LANES)
            table_ref[pl.ds(start, LANES), :] = jnp.concatenate(parts, axis=0).T

    lane = lax.broadcasted_iota(jnp.int32, (1, LANES), 1)
    group_of = lax.div(lax.rem(lane, 32), SPECIES)

    def send(peer):
        rows = pl.ds(pl.multiple_of(peer * PEER_ROWS, PEER_ROWS), PEER_ROWS)
        return pltpu.make_async_copy(msg_ref.at[rows, :], out_hbm.at[rows, :], sems.at[peer])

    fetch.wait()

    @pl.loop(0, 16)
    def _(peer):
        owner = 2 * peer + core
        first = TUBE_COLS * starts_ref[owner]
        pieces = lax.div(TUBE_COLS * units_ref[owner] + (MSG_ROWS - 1), MSG_ROWS)

        def copy(start, number):
            places = []
            for k in range(number):
                piece = start + k
                chunk = lax.div(piece, GROUPS)
                mask = group_of == piece - chunk * GROUPS
                places.append((pl.multiple_of(peer * PEER_ROWS + chunk * MSG_ROWS, MSG_ROWS), mask))
            base = first + start * MSG_ROWS
            for i in range(number * MSG_ROWS):
                place = order_ref.at[pl.ds(i, ORDER_PAD - 2 * MSG_ROWS)][base]
                row, mask = places[i // MSG_ROWS]
                value = table_ref[pl.ds(place, 1), :]
                pltpu.store(msg_ref.at[pl.ds(row + i % MSG_ROWS, 1), :], value, mask=mask)

        @pl.loop(0, lax.div(pieces, 2))
        def _(pair):
            copy(2 * pair, 2)

        pl.when(lax.rem(pieces, 2) == 1)(functools.partial(copy, pieces - 1, 1))
        send(peer).start()

    @pl.loop(0, 16)
    def _(peer):
        send(peer).wait()


def pack(core, starts, units, order, mine, other):
    return call(
        pack_kernel,
        sds((16 * PEER_ROWS, LANES)),
        [SMEM, SMEM, SMEM, HBM, HELD, HELD],
        HBM,
        [
            pltpu.SMEM((ORDER_PAD,), jnp.int32),
            pltpu.VMEM((LON_BLOCKS, CHIP_LEVS * PLANES * PITCH, LANES), f32),
            pltpu.VMEM((BAND_LATS * LON_PAD, LANES), f32),
            pltpu.VMEM((16 * PEER_ROWS, LANES), f32),
            pltpu.SemaphoreType.DMA((16,)),
            pltpu.SemaphoreType.DMA,
        ],
        flops=30_000_000,
        vmem=32,
    )(core, starts, units, order, mine, other)


def solve_kernel(
    core_ref, units_ref, table_ref, got_ref, coef_ref, weight_ref, state_hbm, items_ref,
    turned, natural, pairs, wide, tubes, state, sems,
):
    core = core_ref[0]
    live = TUBE_COLS * units_ref[0]
    lane = lax.broadcasted_iota(jnp.int32, (1, LANES), 1)
    low = lane < 64
    quarter = lax.div(lane, 32)

    @pl.loop(0, 8)
    def _(i):
        for side in range(2):
            out = i * LEVEL_PITCH + side * LANES
            for chunk in range(CHUNKS):
                row = pl.multiple_of((2 * i + side) * PEER_ROWS + chunk * MSG_ROWS, MSG_ROWS)
                flipped = jnp.concatenate([got_ref[pl.ds(row, MSG_ROWS), :]] * 2, axis=0).T
                turned[chunk, pl.ds(out + 64 * core, 64), :] = flipped[:64]
                turned[chunk, pl.ds(out + 64 - 64 * core, 64), :] = flipped[64:]

    def leave(s):
        return pltpu.make_async_copy(state.at[s], state_hbm.at[0, 0, s], sems.at[s])

    @pl.loop(0, SPECIES)
    def _(s):
        def coefs(which):
            row = pl.multiple_of((which * SPECIES + s) * NLEV, NLEV)
            return [coef_ref[pl.ds(row + 8 * v, 8), :] for v in range(8)]

        lower, upper, inv = coefs(0), coefs(1), coefs(2)
        for blk in range(SLOT_BLOCKS):
            chunk, i = divmod(blk, 3)

            def levels(group, v):
                return turned[chunk, pl.ds(32 * v + group * SPECIES + s, 8, stride=LEVEL_PITCH), :]

            rhs = [jnp.where(low, levels(2 * i, v), levels(2 * i + 1, v)) for v in range(8)]
            scaled = [rhs[v] * inv[v] for v in range(8)]
            x = rhs
            for _ in range(SWEEPS):
                beneath = [pltpu.roll(x[7], 1, axis=0)] + x[:7]
                overhead = x[1:] + [pltpu.roll(x[0], 7, axis=0)]
                x = [scaled[v] + lower[v] * beneath[v] + upper[v] * overhead[v] for v in range(8)]
            keep = lane + blk * LANES < live
            for v in range(8):
                natural[i, pl.ds(v, 8, stride=PITCH), :] = jnp.where(keep, x[v], 0.0)
            width = min(LANES, COL_CAP - blk * LANES)
            for g in range(8):
                state[s, g * 8 : g * 8 + 8, blk * LANES : blk * LANES + width] = natural[
                    i, g * PITCH : g * PITCH + 8, :width
                ]
            for h in range(4):
                weight = weight_ref[blk, 8 * h : 8 * h + 8, :]
                paired = weight * x[2 * h] + (1.0 - weight) * x[2 * h + 1]
                pairs[i, pl.ds(h, 8, stride=4), :] = paired
            wide[i] = jnp.concatenate([pairs[i]] * 4, axis=0).T
            item = wide[i, pl.ds(0, 32, stride=TUBE_COLS), :]
            for c in range(1, TUBE_COLS):
                item = jnp.where(quarter == c, wide[i, pl.ds(c, 32, stride=TUBE_COLS), :], item)
            tubes[pl.ds(blk * 256 + s, 32, stride=8), :] = item
        leave(s).start()

    tubes[ZERO_TUBE * 8 :, :] = jnp.zeros((8, LANES), f32)
    sub = lax.broadcasted_iota(jnp.int32, (8, LANES), 0)

    @pl.loop(0, PEERS // 4)
    def _(step):
        for i in range(4):
            d = step * 4 + i
            tiles = [
                tubes[pl.ds(pl.multiple_of(table_ref[d * PEER_SLOTS + r] * 8, 8), 8), :] for r in range(PEER_SLOTS)
            ]
            mid = pltpu.roll(tiles[1], 5, axis=0)
            top = pltpu.roll(tiles[2], 2, axis=0)
            row = pl.multiple_of(d * ITEM_ROWS, ITEM_ROWS)
            items_ref[pl.ds(row, 8), :] = jnp.where(sub < 5, tiles[0], mid)
            items_ref[pl.ds(row + 8, 8), :] = jnp.where(sub < 2, mid, jnp.where(sub < 7, top, 0.0))

    for s in range(SPECIES):
        leave(s).wait()


def solve(core, units, table, got, coefs, weights):
    return call(
        solve_kernel,
        (sds((1, 1, SPECIES, NLEV, COL_CAP)), sds((PEERS * ITEM_ROWS, LANES))),
        [SMEM, SMEM, SMEM] + [HELD] * 3,
        (HBM, VMEM),
        [
            pltpu.VMEM((CHUNKS, 8 * LEVEL_PITCH, LANES), f32),
            pltpu.VMEM((3, 8 * PITCH, LANES), f32),
            pltpu.VMEM((3, PAIRS, LANES), f32),
            pltpu.VMEM((3, LANES, LANES), f32),
            pltpu.VMEM((ZERO_TUBE * 8 + 8, LANES), f32),
            pltpu.VMEM((SPECIES, NLEV, COL_CAP), f32),
            pltpu.SemaphoreType.DMA((SPECIES,)),
        ],
        flops=40_000_000,
    )(core, units, table, got, coefs, weights)


def halves(x):
    high = x.astype(jnp.bfloat16)
    return high, (x - high.astype(f32)).astype(jnp.bfloat16)


def product(x, high, low):
    x_high, x_low = halves(x)
    dot = functools.partial(jnp.dot, preferred_element_type=f32)
    return dot(x_high, high) + (dot(x_low, high) + dot(x_high, low))


def lines_kernel(
    items_ref, yield_ref, rates_ref, waves_ref, fwd_high, fwd_low, inv_high, inv_low, out_hbm,
    spec_in, spec, mixed, done, sems,
):
    tubes = 32 * PEER_SLOTS
    for b in range(4):
        for s in range(SPECIES):
            for r in range(PEER_SLOTS):
                rows = items_ref[pl.ds(b * 32 * ITEM_ROWS + r * SPECIES + s, 32, stride=ITEM_ROWS), :]
                spec_in[b, pl.ds(s * tubes + r, 32, stride=PEER_SLOTS), :] = rows

    half = SPECIES * tubes // 2
    for step in range(2):
        row = step * half
        x = jnp.concatenate([spec_in[b, pl.ds(row, half), :] for b in range(4)], axis=1)
        spec[pl.ds(row, half), :] = product(x, fwd_high[...], fwd_low[...])

    waves = waves_ref[...]
    for i in range(IONS):
        keep = (1.0 - rates_ref[IONS + i]) + rates_ref[i] * waves
        gain = jnp.ones_like(waves)
        for _ in range(SECTIONS - 1):
            gain = gain * keep + 1.0
        total = (yield_ref[i * SPECIES] * gain) * spec[:tubes, :]
        for s in range(1, SPECIES):
            total = total + (yield_ref[i * SPECIES + s] * gain) * spec[s * tubes : (s + 1) * tubes, :]
        mixed[i] = total

    def leave(i):
        return pltpu.make_async_copy(done.at[i], out_hbm.at[0, i], sems.at[i])

    for i in range(0, IONS, 2):
        j = min(i + 2, IONS)
        back = product(mixed[i:j].reshape((j - i) * tubes, LINE_PTS), inv_high[...], inv_low[...])
        done[i:j] = back.reshape(j - i, tubes, LINE_PTS)
        for k in range(i, j):
            leave(k).start()

    for i in range(IONS):
        leave(i).wait()


def cosine_basis():
    k = np.arange(LINE_PTS)[:, None]
    n = np.arange(LINE_PTS)[None, :]
    basis = np.cos(np.pi * k * (n + 0.5) / LINE_PTS) * np.sqrt(2.0 / LINE_PTS)
    basis[0] *= np.sqrt(0.5)
    waves = 2.0 * np.cos(np.pi * np.arange(LINE_PTS) / LINE_PTS) - 2.0
    return basis, waves


def lines(items, ion_yield, ion_spread, ion_loss):
    basis, waves = cosine_basis()

    def parts(matrix):
        matrix = matrix.astype(np.float32)
        high = matrix.astype(jnp.bfloat16)
        low = (matrix - high.astype(np.float32)).astype(jnp.bfloat16)
        return jnp.asarray(high), jnp.asarray(low)

    waves = jnp.asarray(waves.astype(np.float32))[None]
    tubes = 32 * PEER_SLOTS
    by_ion = call(
        lines_kernel,
        sds((1, IONS, tubes, LINE_PTS)),
        [HELD, SMEM, SMEM] + [HELD] * 5,
        HBM,
        [
            pltpu.VMEM((4, SPECIES * tubes, LANES), f32),
            pltpu.VMEM((SPECIES * tubes, LINE_PTS), f32),
            pltpu.VMEM((IONS, tubes, LINE_PTS), f32),
            pltpu.VMEM((IONS, tubes, LINE_PTS), f32),
            pltpu.SemaphoreType.DMA((IONS,)),
        ],
        flops=2_000_000_000,
    )(items, ion_yield.reshape(-1), jnp.concatenate([ion_spread, ion_loss]), waves, *parts(basis.T), *parts(basis))
    return jnp.swapaxes(by_ion, 1, 2)


def swap(x, axis, offset):
    count = lax.axis_size(axis)
    lows = range(offset, count - 1, 2)
    return lax.ppermute(x, axis, [(i, i + 1) for i in lows] + [(i + 1, i) for i in lows])


def exchange(inner, outer, row, far_row):
    outer = swap(outer, "lev", 1)
    row = swap(row, "band", 0)
    far_row = swap(far_row, "band", 1)
    inner = swap(inner, "lev", 0)
    return inner, outer, row, far_row


def on_device(
    neutrals,
    wind_lon,
    wind_lat,
    wind_lev,
    eddy_coupling,
    pair_weight,
    ion_yield,
    ion_spread,
    ion_loss,
    column_order,
    column_units,
    tube_owner,
):
    lev = lax.axis_index("lev")

    side = jnp.stack([lev % 2, lax.axis_index("band") % 2]).astype(jnp.int32)
    neutrals, *rest = edges(side, neutrals, wind_lon, wind_lat, wind_lev)
    winds, first_halo = rest[:3], exchange(*rest[3:])

    starts = jnp.cumsum(column_units) - column_units
    order = column_order[0]
    lat = jnp.zeros_like(order)
    for i in range(1, BAND_LATS):
        lat = lat + (order >= i * NLON).astype(jnp.int32)
    rows = jnp.pad(order + lat * (LON_PAD - NLON), (0, ORDER_PAD - BAND_COLS))
    own_units = column_units[lev].reshape(1)
    padded = jnp.pad(order, (0, SLOTS_PAD))
    own = lax.dynamic_slice(padded, (TUBE_COLS * starts[lev],), (SLOTS_PAD,))
    own_lat = jnp.zeros_like(own)
    for i in range(1, BAND_LATS):
        own_lat = own_lat + (own >= i * NLON).astype(jnp.int32)
    own_lon = own - own_lat * NLON
    own_rows = (own_lat * 6 + own_lon // 512) * LANES + own_lon % LANES
    own_sel = ((own_lon // LANES) % 4).reshape(SLOT_BLOCKS, LANES)
    zero = jnp.zeros((SPECIES, 1), f32)
    lower = jnp.concatenate([zero, eddy_coupling[:, 1:]], 1)
    upper = jnp.concatenate([eddy_coupling[:, 1:], zero], 1)
    inv = 1.0 / (1.0 + lower + upper)
    coefs = jnp.stack([lower * inv, upper * inv, inv]).reshape(3, SPECIES, 8, 8)
    table, own_weights, coefs = prepare(
        own_units,
        tube_owner[lev, :, 0],
        own_rows,
        own_sel,
        pair_weight.reshape(PAIRS * BAND_LATS, NLON),
        jnp.swapaxes(coefs, 2, 3).reshape(-1, 1),
    )

    density, *halo = transport_step(side, neutrals, winds, first_halo, first_halo, False)
    (mine,) = transport_step(side, density, winds, exchange(*halo), first_halo, True)
    owners = lax.axis_size("lev")
    other = swap(mine, "lev", 0)

    core = (lev % 2).reshape(1)
    parity = [[2 * i + c for i in range(owners // 2)] for c in range(2)]
    outgoing = pack(core, starts, column_units, rows, mine, other)
    got = lax.all_to_all(
        outgoing.reshape(16, PEER_ROWS, LANES), "lev", 0, 0, axis_index_groups=parity, tiled=True
    ).reshape(16 * PEER_ROWS, LANES)
    column_state, items = solve(core, own_units, table, got, coefs, own_weights)

    items = lax.all_to_all(
        items.reshape(PEERS, ITEM_ROWS, LANES), ("band", "lev"), 0, 0, tiled=True
    ).reshape(PEERS * ITEM_ROWS, LANES)
    return column_state, lines(items, ion_yield, ion_spread, ion_loss)


def solution(mesh):
    placed = (
        P(None, "lev", "band", None),
        P("lev", "band", None),
        P("lev", "band", None),
        P("lev", "band", None),
        P(),
        P(None, "band", None),
        P(),
        P(),
        P(),
        P("band", None),
        P(),
        P(),
    )

    return jax.shard_map(
        on_device,
        mesh=mesh,
        in_specs=placed,
        out_specs=(P("band", "lev", None, None, None), P(("band", "lev"), None, None, None)),
        check_vma=False,
    )
```

```python
import functools

import jax
import jax.numpy as jnp
import numpy as np
from jax import lax
from jax.experimental import pallas as pl
from jax.experimental.pallas import tpu as pltpu
from jax.sharding import PartitionSpec as P


SPECIES = 5
IONS = 7
NLON = 2880
NLEV = 64
PAIRS = 32
BAND_LATS = 8
SWEEPS = 8
SECTIONS = 20
TUBE_COLS = 4
PEERS = 128
PEER_SLOTS = 3
COL_CAP = 1080
BAND_COLS = BAND_LATS * NLON
LINE_PTS = 512

LANES = 128
LON_BLOCKS = 23
LON_PAD = LON_BLOCKS * LANES
CHIP_LEVS = 4
PITCH = 9
LEVEL_PITCH = 257
PLANES = 12
GROUPS = 6
CHUNKS = 3
MSG_ROWS = 64
PEER_ROWS = CHUNKS * MSG_ROWS
SLOT_BLOCKS = 9
SLOTS_PAD = SLOT_BLOCKS * LANES
ORDER_PAD = BAND_COLS + 3 * LANES
UNROLL = 64
ZERO_TUBE = SLOT_BLOCKS * 32
ITEM_ROWS = 16

f32 = jnp.float32
VMEM = pl.BlockSpec(memory_space=pltpu.VMEM)
HELD = pl.BlockSpec(memory_space=pltpu.VMEM)
SMEM = pl.BlockSpec(memory_space=pltpu.SMEM)
HBM = pl.BlockSpec(memory_space=pltpu.HBM)


def on_chip(shape, dtype=f32):
    return pltpu.VMEM(shape, dtype)


def call(kernel, out_shape, in_specs, out_specs, scratch=(), flops=0, vmem=16):
    run = pl.pallas_call(
        kernel,
        out_shape=out_shape,
        in_specs=in_specs,
        out_specs=out_specs,
        scratch_shapes=list(scratch),
        cost_estimate=pl.CostEstimate(flops=flops, bytes_accessed=1 << 20, transcendentals=0),
        compiler_params=pltpu.CompilerParams(vmem_limit_bytes=vmem * 1024 * 1024),
    )

    def place(x, spec):
        space = pltpu.VMEM if spec is HELD else pltpu.HBM if spec is HBM else None
        return x if space is None else pltpu.with_memory_space_constraint(x, space)

    def placed(*args):
        return run(*(place(x, spec) for x, spec in zip(args, in_specs)))

    return placed


def sds(shape, dtype=f32):
    return jax.ShapeDtypeStruct(shape, dtype)


def upwind(courant, upstream, downstream):
    return courant * jnp.where(courant > 0.0, upstream, downstream)


def edges_kernel(
    side_ref, n_hbm, wlon_hbm, wlat_hbm, wlev_hbm,
    n_ref, wlon_ref, wlat_ref, wlev_ref, inner_ref, outer_ref, row_ref, far_row_ref, sems,
):
    fetches = [
        pltpu.make_async_copy(n_hbm.at[s], n_ref.at[s], sems.at[s]) for s in range(SPECIES)
    ]
    fetches.append(pltpu.make_async_copy(wlat_hbm, wlat_ref, sems.at[SPECIES]))
    fetches.append(pltpu.make_async_copy(wlev_hbm, wlev_ref, sems.at[SPECIES + 1]))
    fetches.append(pltpu.make_async_copy(wlon_hbm, wlon_ref, sems.at[SPECIES + 2]))
    for fetch in fetches:
        fetch.start()
    for fetch in fetches[:-1]:
        fetch.wait()
    core, odd = side_ref[0], side_ref[1] == 1
    inner_ref[SPECIES] = wlev_ref[0]
    outer_ref[SPECIES] = wlev_ref[0]
    for j in range(2):
        row_ref[SPECIES, j] = wlat_ref[j, :1]
        far_row_ref[SPECIES, j] = wlat_ref[j, :1]

    @pl.loop(0, SPECIES)
    def _(s):
        inner_ref[s] = n_ref[s, 1 - core]
        outer_ref[s] = n_ref[s, core]
        for j in range(2):
            first, last = n_ref[s, j, :1], n_ref[s, j, BAND_LATS - 1 :]
            row_ref[s, j] = jnp.where(odd, first, last)
            far_row_ref[s, j] = jnp.where(odd, last, first)

    fetches[-1].wait()


def edges(side, density, wind_lon, wind_lat, wind_lev):
    return call(
        edges_kernel,
        (
            on_chip(density.shape),
            on_chip(wind_lon.shape),
            on_chip(wind_lat.shape),
            on_chip(wind_lev.shape),
            on_chip((SPECIES + 1, BAND_LATS, NLON)),
            on_chip((SPECIES + 1, BAND_LATS, NLON)),
            on_chip((SPECIES + 1, 2, 1, NLON)),
            on_chip((SPECIES + 1, 2, 1, NLON)),
        ),
        [SMEM] + [HBM] * 4,
        (VMEM,) * 8,
        [pltpu.SemaphoreType.DMA((SPECIES + 3,))],
        flops=1_000_000,
    )(side, density, wind_lon, wind_lat, wind_lev)


def interior_kernel(n_ref, wlon_ref, wlat_ref, wlev_ref, out_ref):
    row = lax.broadcasted_iota(jnp.int32, (BAND_LATS, NLON), 0)

    @pl.loop(0, SPECIES)
    def _(s):
        for j in range(2):
            x = n_ref[s, j]
            west = jnp.concatenate([x[:, NLON - 1 :], x[:, : NLON - 1]], axis=1)
            flux = upwind(wlon_ref[j], west, x)
            total = x + (flux - jnp.concatenate([flux[:, 1:], flux[:, :1]], axis=1))
            flux = upwind(wlat_ref[j], pltpu.roll(x, 1, axis=0), x)
            flux = jnp.where(row == 0, 0.0, flux)
            total = total + (flux - pltpu.roll(flux, BAND_LATS - 1, axis=0))
            flux = upwind(wlev_ref[1], n_ref[s, 0], n_ref[s, 1])
            out_ref[s, j] = total + flux if j else total - flux


def interior(density, winds):
    return call(
        interior_kernel, on_chip((SPECIES, 2, BAND_LATS, NLON)), [HELD] * 4, VMEM, flops=8_000_000
    )(density, *winds)


def faces_kernel(side_ref, n_ref, inside_ref, wlat_ref, wlev_ref, *refs, last):
    inner_ref, outer_ref, row_ref, far_row_ref = refs[:4]
    inner_wind, outer_wind, row_wind, far_row_wind = refs[4:8]
    outs = refs[8:]
    odd = side_ref[1] == 1
    row = lax.broadcasted_iota(jnp.int32, (BAND_LATS, NLON), 0)

    def advance(core):
        below_ref, above_ref, above_wind = (
            (outer_ref, inner_ref, inner_wind) if core == 0 else (inner_ref, outer_ref, outer_wind)
        )

        @pl.loop(0, SPECIES)
        def _(s):
            for j in range(2):
                x = n_ref[s, j]
                total = inside_ref[s, j]
                south = jnp.where(odd, row_ref[s, j], far_row_ref[s, j])
                north = jnp.where(odd, far_row_ref[s, j], row_ref[s, j])
                north_wind = jnp.where(odd, far_row_wind[SPECIES, j], row_wind[SPECIES, j])
                into = upwind(wlat_ref[j, :1], south, x[:1])
                out_of = upwind(north_wind, x[BAND_LATS - 1 :], north)
                total = total + jnp.where(row == 0, into, 0.0) - jnp.where(row == BAND_LATS - 1, out_of, 0.0)
                if j == 0:
                    total = total + upwind(wlev_ref[0], below_ref[s], x)
                else:
                    total = total - upwind(above_wind[SPECIES], x, above_ref[s])
                if last:
                    start = pl.multiple_of((j * SPECIES + s) * BAND_LATS, BAND_LATS)
                    for blk in range(LON_BLOCKS):
                        wide = min(LANES, NLON - blk * LANES)
                        outs[0][blk, pl.ds(start, BAND_LATS), :wide] = total[:, blk * LANES : blk * LANES + wide]
                    continue
                outs[0][s, j] = total
                outs[2 if j == core else 1][s] = total
                first, final = total[:1], total[BAND_LATS - 1 :]
                outs[3][s, j] = jnp.where(odd, first, final)
                outs[4][s, j] = jnp.where(odd, final, first)

    for core in range(2):
        pl.when(side_ref[0] == core)(functools.partial(advance, core))


def faces(side, density, inside, winds, halo, wind_halo, last):
    if last:
        out_shape = (on_chip((LON_BLOCKS, 2 * SPECIES * BAND_LATS, LANES)),)
    else:
        out_shape = (
            on_chip((SPECIES, 2, BAND_LATS, NLON)),
            on_chip((SPECIES, BAND_LATS, NLON)),
            on_chip((SPECIES, BAND_LATS, NLON)),
            on_chip((SPECIES, 2, 1, NLON)),
            on_chip((SPECIES, 2, 1, NLON)),
        )
    return call(
        functools.partial(faces_kernel, last=last),
        out_shape,
        [SMEM] + [HELD] * 12,
        (VMEM,) * len(out_shape),
        flops=2_000_000,
    )(side, density, inside, *winds[1:], *halo, *wind_halo)


def prepare_kernel(
    units_ref, owner_ref, rows_ref, sel_ref, weight_ref, column_ref,
    table_ref, own_ref, coef_ref, count, blocks, table, picked,
):
    @pl.loop(0, PEERS * PEER_SLOTS // 8)
    def _(i):
        for k in range(8):
            table_ref[i * 8 + k] = ZERO_TUBE

    @pl.loop(0, PEERS // 8)
    def _(i):
        for k in range(8):
            count[i * 8 + k] = 0

    @pl.loop(0, units_ref[0])
    def _(u):
        dest = owner_ref[u]
        rank = count[dest]
        count[dest] = rank + 1
        table_ref[dest * PEER_SLOTS + rank] = u

    coef_ref[...] = jnp.broadcast_to(column_ref[...], coef_ref.shape)

    for blk in range(LON_BLOCKS):
        wide = min(LANES, NLON - blk * LANES)
        blocks[blk, :, :wide] = weight_ref[:, blk * LANES : blk * LANES + wide]

    @pl.loop(0, BAND_LATS)
    def _(lat):
        for g in range(6):
            parts = [
                blocks[min(4 * g + i, LON_BLOCKS - 1), pl.ds(lat + h * BAND_LATS, 8, stride=4 * BAND_LATS), :]
                for i in range(4)
                for h in range(4)
            ]
            start = pl.multiple_of((lat * 6 + g) * LANES, LANES)
            table[pl.ds(start, LANES), :] = jnp.concatenate(parts, axis=0).T

    @pl.loop(0, SLOTS_PAD // UNROLL)
    def _(step):
        base = pl.multiple_of(step * UNROLL, UNROLL)
        places = rows_ref.at[pl.ds(base, UNROLL)]
        for i in range(UNROLL):
            picked[pl.ds(base + i, 1), :] = table[pl.ds(places[i], 1), :]

    for blk in range(SLOT_BLOCKS):
        turned = picked[blk * LANES : (blk + 1) * LANES, :].T
        which = sel_ref[blk : blk + 1, :]
        kept = turned[:PAIRS]
        for i in range(1, 4):
            kept = jnp.where(which == i, turned[i * PAIRS : (i + 1) * PAIRS], kept)
        own_ref[blk] = kept


def prepare(units, owners, rows, sel, weights, column):
    return call(
        prepare_kernel,
        (
            sds((PEERS * PEER_SLOTS,), jnp.int32),
            on_chip((SLOT_BLOCKS, PAIRS, LANES)),
            on_chip((3 * SPECIES * NLEV, LANES)),
        ),
        [SMEM, SMEM, SMEM, VMEM, VMEM, VMEM],
        (SMEM, VMEM, VMEM),
        [
            pltpu.SMEM((PEERS,), jnp.int32),
            pltpu.VMEM((LON_BLOCKS, PAIRS * BAND_LATS, LANES), f32),
            pltpu.VMEM((BAND_LATS * 6 * LANES, LANES), f32),
            pltpu.VMEM((SLOTS_PAD, LANES), f32),
        ],
        flops=20_000_000,
    )(units, owners, rows, sel, weights, column)


def pack_kernel(
    core_ref, starts_ref, units_ref, order_hbm, mine_ref, other_ref,
    out_hbm, order_ref, planes, table_ref, msg_ref, sems, order_sem,
):
    core = core_ref[0]

    fetch = pltpu.make_async_copy(order_hbm, order_ref, order_sem)
    fetch.start()

    @pl.loop(0, LON_BLOCKS)
    def _(blk):
        for side, source in enumerate((mine_ref, other_ref)):
            for j in range(2):
                for i in range(PLANES):
                    from_row = (j * SPECIES + i % SPECIES) * BAND_LATS
                    planes[blk, pl.ds(((2 * side + j) * PLANES + i) * PITCH, BAND_LATS), :] = source[
                        blk, from_row : from_row + BAND_LATS, :
                    ]

    @pl.loop(0, LON_BLOCKS)
    def _(blk):
        for lat in range(BAND_LATS):
            parts = [
                planes[blk, pl.ds((jj * PLANES + first) * PITCH + lat, 8, stride=PITCH), :]
                for jj in range(CHIP_LEVS)
                for first in (0, 3, 1, 4)
            ]
            start = pl.multiple_of((lat * LON_BLOCKS + blk) * LANES, LANES)
            table_ref[pl.ds(start, LANES), :] = jnp.concatenate(parts, axis=0).T

    lane = lax.broadcasted_iota(jnp.int32, (1, LANES), 1)
    group_of = lax.div(lax.rem(lane, 32), SPECIES)

    def send(peer):
        rows = pl.ds(pl.multiple_of(peer * PEER_ROWS, PEER_ROWS), PEER_ROWS)
        return pltpu.make_async_copy(msg_ref.at[rows, :], out_hbm.at[rows, :], sems.at[peer])

    fetch.wait()

    @pl.loop(0, 16)
    def _(peer):
        owner = 2 * peer + core
        first = TUBE_COLS * starts_ref[owner]
        pieces = lax.div(TUBE_COLS * units_ref[owner] + (MSG_ROWS - 1), MSG_ROWS)

        def copy(start, number):
            places = []
            for k in range(number):
                piece = start + k
                chunk = lax.div(piece, GROUPS)
                mask = group_of == piece - chunk * GROUPS
                places.append((pl.multiple_of(peer * PEER_ROWS + chunk * MSG_ROWS, MSG_ROWS), mask))
            base = first + start * MSG_ROWS
            for i in range(number * MSG_ROWS):
                place = order_ref.at[pl.ds(i, ORDER_PAD - 2 * MSG_ROWS)][base]
                row, mask = places[i // MSG_ROWS]
                value = table_ref[pl.ds(place, 1), :]
                pltpu.store(msg_ref.at[pl.ds(row + i % MSG_ROWS, 1), :], value, mask=mask)

        @pl.loop(0, lax.div(pieces, 2))
        def _(pair):
            copy(2 * pair, 2)

        pl.when(lax.rem(pieces, 2) == 1)(functools.partial(copy, pieces - 1, 1))
        send(peer).start()

    @pl.loop(0, 16)
    def _(peer):
        send(peer).wait()


def pack(core, starts, units, order, mine, other):
    return call(
        pack_kernel,
        sds((16 * PEER_ROWS, LANES)),
        [SMEM, SMEM, SMEM, HBM, HELD, HELD],
        HBM,
        [
            pltpu.SMEM((ORDER_PAD,), jnp.int32),
            pltpu.VMEM((LON_BLOCKS, CHIP_LEVS * PLANES * PITCH, LANES), f32),
            pltpu.VMEM((BAND_LATS * LON_PAD, LANES), f32),
            pltpu.VMEM((16 * PEER_ROWS, LANES), f32),
            pltpu.SemaphoreType.DMA((16,)),
            pltpu.SemaphoreType.DMA,
        ],
        flops=30_000_000,
        vmem=32,
    )(core, starts, units, order, mine, other)


def solve_kernel(
    core_ref, units_ref, table_ref, got_ref, coef_ref, weight_ref, state_hbm, items_ref,
    turned, natural, pairs, wide, tubes, state, sems,
):
    core = core_ref[0]
    live = TUBE_COLS * units_ref[0]
    lane = lax.broadcasted_iota(jnp.int32, (1, LANES), 1)
    low = lane < 64
    quarter = lax.div(lane, 32)

    @pl.loop(0, 8)
    def _(i):
        for side in range(2):
            out = i * LEVEL_PITCH + side * LANES
            for chunk in range(CHUNKS):
                row = pl.multiple_of((2 * i + side) * PEER_ROWS + chunk * MSG_ROWS, MSG_ROWS)
                flipped = jnp.concatenate([got_ref[pl.ds(row, MSG_ROWS), :]] * 2, axis=0).T
                turned[chunk, pl.ds(out + 64 * core, 64), :] = flipped[:64]
                turned[chunk, pl.ds(out + 64 - 64 * core, 64), :] = flipped[64:]

    def leave(s):
        return pltpu.make_async_copy(state.at[s], state_hbm.at[0, 0, s], sems.at[s])

    @pl.loop(0, SPECIES)
    def _(s):
        def coefs(which):
            row = pl.multiple_of((which * SPECIES + s) * NLEV, NLEV)
            return [coef_ref[pl.ds(row + 8 * v, 8), :] for v in range(8)]

        lower, upper, inv = coefs(0), coefs(1), coefs(2)
        for blk in range(SLOT_BLOCKS):
            chunk, i = divmod(blk, 3)

            def levels(group, v):
                return turned[chunk, pl.ds(32 * v + group * SPECIES + s, 8, stride=LEVEL_PITCH), :]

            rhs = [jnp.where(low, levels(2 * i, v), levels(2 * i + 1, v)) for v in range(8)]
            scaled = [rhs[v] * inv[v] for v in range(8)]
            x = rhs
            for _ in range(SWEEPS):
                beneath = [pltpu.roll(x[7], 1, axis=0)] + x[:7]
                overhead = x[1:] + [pltpu.roll(x[0], 7, axis=0)]
                x = [scaled[v] + lower[v] * beneath[v] + upper[v] * overhead[v] for v in range(8)]
            keep = lane + blk * LANES < live
            for v in range(8):
                natural[i, pl.ds(v, 8, stride=PITCH), :] = jnp.where(keep, x[v], 0.0)
            width = min(LANES, COL_CAP - blk * LANES)
            for g in range(8):
                state[s, g * 8 : g * 8 + 8, blk * LANES : blk * LANES + width] = natural[
                    i, g * PITCH : g * PITCH + 8, :width
                ]
            for h in range(4):
                weight = weight_ref[blk, 8 * h : 8 * h + 8, :]
                paired = weight * x[2 * h] + (1.0 - weight) * x[2 * h + 1]
                pairs[i, pl.ds(h, 8, stride=4), :] = paired
            wide[i] = jnp.concatenate([pairs[i]] * 4, axis=0).T
            item = wide[i, pl.ds(0, 32, stride=TUBE_COLS), :]
            for c in range(1, TUBE_COLS):
                item = jnp.where(quarter == c, wide[i, pl.ds(c, 32, stride=TUBE_COLS), :], item)
            tubes[pl.ds(blk * 256 + s, 32, stride=8), :] = item
        leave(s).start()

    tubes[ZERO_TUBE * 8 :, :] = jnp.zeros((8, LANES), f32)
    sub = lax.broadcasted_iota(jnp.int32, (8, LANES), 0)

    @pl.loop(0, PEERS // 4)
    def _(step):
        for i in range(4):
            d = step * 4 + i
            tiles = [
                tubes[pl.ds(pl.multiple_of(table_ref[d * PEER_SLOTS + r] * 8, 8), 8), :] for r in range(PEER_SLOTS)
            ]
            mid = pltpu.roll(tiles[1], 5, axis=0)
            top = pltpu.roll(tiles[2], 2, axis=0)
            row = pl.multiple_of(d * ITEM_ROWS, ITEM_ROWS)
            items_ref[pl.ds(row, 8), :] = jnp.where(sub < 5, tiles[0], mid)
            items_ref[pl.ds(row + 8, 8), :] = jnp.where(sub < 2, mid, jnp.where(sub < 7, top, 0.0))

    for s in range(SPECIES):
        leave(s).wait()


def solve(core, units, table, got, coefs, weights):
    return call(
        solve_kernel,
        (sds((1, 1, SPECIES, NLEV, COL_CAP)), sds((PEERS * ITEM_ROWS, LANES))),
        [SMEM, SMEM, SMEM] + [HELD] * 3,
        (HBM, VMEM),
        [
            pltpu.VMEM((CHUNKS, 8 * LEVEL_PITCH, LANES), f32),
            pltpu.VMEM((3, 8 * PITCH, LANES), f32),
            pltpu.VMEM((3, PAIRS, LANES), f32),
            pltpu.VMEM((3, LANES, LANES), f32),
            pltpu.VMEM((ZERO_TUBE * 8 + 8, LANES), f32),
            pltpu.VMEM((SPECIES, NLEV, COL_CAP), f32),
            pltpu.SemaphoreType.DMA((SPECIES,)),
        ],
        flops=40_000_000,
    )(core, units, table, got, coefs, weights)


def halves(x):
    high = x.astype(jnp.bfloat16)
    return high, (x - high.astype(f32)).astype(jnp.bfloat16)


def product(x, high, low):
    x_high, x_low = halves(x)
    dot = functools.partial(jnp.dot, preferred_element_type=f32)
    return dot(x_high, high) + (dot(x_low, high) + dot(x_high, low))


def lines_kernel(
    items_ref, yield_ref, rates_ref, waves_ref, fwd_high, fwd_low, inv_high, inv_low, out_hbm,
    spec_in, spec, mixed, done, sems,
):
    tubes = 32 * PEER_SLOTS
    for b in range(4):
        for s in range(SPECIES):
            for r in range(PEER_SLOTS):
                rows = items_ref[pl.ds(b * 32 * ITEM_ROWS + r * SPECIES + s, 32, stride=ITEM_ROWS), :]
                spec_in[b, pl.ds(s * tubes + r, 32, stride=PEER_SLOTS), :] = rows

    half = SPECIES * tubes // 2
    for step in range(2):
        row = step * half
        x = jnp.concatenate([spec_in[b, pl.ds(row, half), :] for b in range(4)], axis=1)
        spec[pl.ds(row, half), :] = product(x, fwd_high[...], fwd_low[...])

    waves = waves_ref[...]
    for i in range(IONS):
        keep = (1.0 - rates_ref[IONS + i]) + rates_ref[i] * waves
        gain = jnp.ones_like(waves)
        for _ in range(SECTIONS - 1):
            gain = gain * keep + 1.0
        total = (yield_ref[i * SPECIES] * gain) * spec[:tubes, :]
        for s in range(1, SPECIES):
            total = total + (yield_ref[i * SPECIES + s] * gain) * spec[s * tubes : (s + 1) * tubes, :]
        mixed[i] = total

    def leave(i):
        return pltpu.make_async_copy(done.at[i], out_hbm.at[0, i], sems.at[i])

    for i in range(0, IONS, 2):
        j = min(i + 2, IONS)
        back = product(mixed[i:j].reshape((j - i) * tubes, LINE_PTS), inv_high[...], inv_low[...])
        done[i:j] = back.reshape(j - i, tubes, LINE_PTS)
        for k in range(i, j):
            leave(k).start()

    for i in range(IONS):
        leave(i).wait()


def cosine_basis():
    k = np.arange(LINE_PTS)[:, None]
    n = np.arange(LINE_PTS)[None, :]
    basis = np.cos(np.pi * k * (n + 0.5) / LINE_PTS) * np.sqrt(2.0 / LINE_PTS)
    basis[0] *= np.sqrt(0.5)
    waves = 2.0 * np.cos(np.pi * np.arange(LINE_PTS) / LINE_PTS) - 2.0
    return basis, waves


def lines(items, ion_yield, ion_spread, ion_loss):
    basis, waves = cosine_basis()

    def parts(matrix):
        matrix = matrix.astype(np.float32)
        high = matrix.astype(jnp.bfloat16)
        low = (matrix - high.astype(np.float32)).astype(jnp.bfloat16)
        return jnp.asarray(high), jnp.asarray(low)

    waves = jnp.asarray(waves.astype(np.float32))[None]
    tubes = 32 * PEER_SLOTS
    by_ion = call(
        lines_kernel,
        sds((1, IONS, tubes, LINE_PTS)),
        [HELD, SMEM, SMEM] + [HELD] * 5,
        HBM,
        [
            pltpu.VMEM((4, SPECIES * tubes, LANES), f32),
            pltpu.VMEM((SPECIES * tubes, LINE_PTS), f32),
            pltpu.VMEM((IONS, tubes, LINE_PTS), f32),
            pltpu.VMEM((IONS, tubes, LINE_PTS), f32),
            pltpu.SemaphoreType.DMA((IONS,)),
        ],
        flops=2_000_000_000,
    )(items, ion_yield.reshape(-1), jnp.concatenate([ion_spread, ion_loss]), waves, *parts(basis.T), *parts(basis))
    return jnp.swapaxes(by_ion, 1, 2)


def swap(x, axis, offset):
    count = lax.axis_size(axis)
    lows = range(offset, count - 1, 2)
    return lax.ppermute(x, axis, [(i, i + 1) for i in lows] + [(i + 1, i) for i in lows])


def exchange(inner, outer, row, far_row):
    outer = swap(outer, "lev", 1)
    row = swap(row, "band", 0)
    far_row = swap(far_row, "band", 1)
    inner = swap(inner, "lev", 0)
    return inner, outer, row, far_row


def on_device(
    neutrals,
    wind_lon,
    wind_lat,
    wind_lev,
    eddy_coupling,
    pair_weight,
    ion_yield,
    ion_spread,
    ion_loss,
    column_order,
    column_units,
    tube_owner,
):
    lev = lax.axis_index("lev")

    side = jnp.stack([lev % 2, lax.axis_index("band") % 2]).astype(jnp.int32)
    neutrals, *rest = edges(side, neutrals, wind_lon, wind_lat, wind_lev)
    winds, first_halo = rest[:3], exchange(*rest[3:])

    starts = jnp.cumsum(column_units) - column_units
    order = column_order[0]
    lat = jnp.zeros_like(order)
    for i in range(1, BAND_LATS):
        lat = lat + (order >= i * NLON).astype(jnp.int32)
    rows = jnp.pad(order + lat * (LON_PAD - NLON), (0, ORDER_PAD - BAND_COLS))
    own_units = column_units[lev].reshape(1)
    padded = jnp.pad(order, (0, SLOTS_PAD))
    own = lax.dynamic_slice(padded, (TUBE_COLS * starts[lev],), (SLOTS_PAD,))
    own_lat = jnp.zeros_like(own)
    for i in range(1, BAND_LATS):
        own_lat = own_lat + (own >= i * NLON).astype(jnp.int32)
    own_lon = own - own_lat * NLON
    own_rows = (own_lat * 6 + own_lon // 512) * LANES + own_lon % LANES
    own_sel = ((own_lon // LANES) % 4).reshape(SLOT_BLOCKS, LANES)
    zero = jnp.zeros((SPECIES, 1), f32)
    lower = jnp.concatenate([zero, eddy_coupling[:, 1:]], 1)
    upper = jnp.concatenate([eddy_coupling[:, 1:], zero], 1)
    inv = 1.0 / (1.0 + lower + upper)
    coefs = jnp.stack([lower * inv, upper * inv, inv]).reshape(3, SPECIES, 8, 8)
    table, own_weights, coefs = prepare(
        own_units,
        tube_owner[lev, :, 0],
        own_rows,
        own_sel,
        pair_weight.reshape(PAIRS * BAND_LATS, NLON),
        jnp.swapaxes(coefs, 2, 3).reshape(-1, 1),
    )

    inside = interior(neutrals, winds)
    density, *halo = faces(side, neutrals, inside, winds, first_halo, first_halo, False)
    inside = interior(density, winds)
    (mine,) = faces(side, density, inside, winds, exchange(*halo), first_halo, True)
    owners = lax.axis_size("lev")
    other = swap(mine, "lev", 0)

    core = (lev % 2).reshape(1)
    parity = [[2 * i + c for i in range(owners // 2)] for c in range(2)]
    outgoing = pack(core, starts, column_units, rows, mine, other)
    got = lax.all_to_all(
        outgoing.reshape(16, PEER_ROWS, LANES), "lev", 0, 0, axis_index_groups=parity, tiled=True
    ).reshape(16 * PEER_ROWS, LANES)
    column_state, items = solve(core, own_units, table, got, coefs, own_weights)

    items = lax.all_to_all(
        items.reshape(PEERS, ITEM_ROWS, LANES), ("band", "lev"), 0, 0, tiled=True
    ).reshape(PEERS * ITEM_ROWS, LANES)
    return column_state, lines(items, ion_yield, ion_spread, ion_loss)


def solution(mesh):
    placed = (
        P(None, "lev", "band", None),
        P("lev", "band", None),
        P("lev", "band", None),
        P("lev", "band", None),
        P(),
        P(None, "band", None),
        P(),
        P(),
        P(),
        P("band", None),
        P(),
        P(),
    )

    return jax.shard_map(
        on_device,
        mesh=mesh,
        in_specs=placed,
        out_specs=(P("band", "lev", None, None, None), P(("band", "lev"), None, None, None)),
        check_vma=False,
    )
```

```python
import functools

import jax
import jax.numpy as jnp
import numpy as np
from jax import lax
from jax.experimental import pallas as pl
from jax.experimental.pallas import tpu as pltpu
from jax.sharding import PartitionSpec as P


SPECIES = 5
IONS = 7
NLON = 2880
NLEV = 64
PAIRS = 32
BAND_LATS = 8
SWEEPS = 8
SECTIONS = 20
TUBE_COLS = 4
PEERS = 128
PEER_SLOTS = 3
COL_CAP = 1080
BAND_COLS = BAND_LATS * NLON
LINE_PTS = 512

LANES = 128
LON_BLOCKS = 23
LON_PAD = LON_BLOCKS * LANES
PITCH = 9
LEVEL_PITCH = 257
PLANES = 12
GROUPS = 6
PIECE = 64
PEER_ROWS = 3 * PIECE
SLOT_BLOCKS = 9
SLOTS_PAD = SLOT_BLOCKS * LANES
ORDER_PAD = BAND_COLS + 3 * LANES
UNROLL = 64
ZERO_TUBE = SLOT_BLOCKS * 32
ITEM_ROWS = 16

f32 = jnp.float32
VMEM = pl.BlockSpec(memory_space=pltpu.VMEM)
HELD = pl.BlockSpec(memory_space=pltpu.VMEM)
SMEM = pl.BlockSpec(memory_space=pltpu.SMEM)
HBM = pl.BlockSpec(memory_space=pltpu.HBM)


def on_chip(shape, dtype=f32):
    return pltpu.VMEM(shape, dtype)


def call(kernel, out_shape, in_specs, out_specs, scratch=(), flops=0, vmem=16, aliases=()):
    run = pl.pallas_call(
        kernel,
        out_shape=out_shape,
        in_specs=in_specs,
        out_specs=out_specs,
        scratch_shapes=list(scratch),
        input_output_aliases=dict(aliases),
        cost_estimate=pl.CostEstimate(flops=flops, bytes_accessed=1 << 20, transcendentals=0),
        compiler_params=pltpu.CompilerParams(vmem_limit_bytes=vmem * 1024 * 1024),
    )

    def place(x, spec):
        space = pltpu.VMEM if spec is HELD else pltpu.HBM if spec is HBM else None
        return x if space is None else pltpu.with_memory_space_constraint(x, space)

    def placed(*args):
        return run(*(place(x, spec) for x, spec in zip(args, in_specs)))

    return placed


def sds(shape, dtype=f32):
    return jax.ShapeDtypeStruct(shape, dtype)


def upwind(courant, upstream, downstream):
    return courant * jnp.where(courant > 0.0, upstream, downstream)


def edges_kernel(
    side_ref, n_hbm, wlon_hbm, wlat_hbm, wlev_hbm,
    n_ref, wlon_ref, wlat_ref, wlev_ref, inner_ref, outer_ref, row_ref, far_row_ref, sems,
):
    fetches = [
        pltpu.make_async_copy(n_hbm.at[s], n_ref.at[s], sems.at[s]) for s in range(SPECIES)
    ]
    fetches.append(pltpu.make_async_copy(wlat_hbm, wlat_ref, sems.at[SPECIES]))
    fetches.append(pltpu.make_async_copy(wlev_hbm, wlev_ref, sems.at[SPECIES + 1]))
    fetches.append(pltpu.make_async_copy(wlon_hbm, wlon_ref, sems.at[SPECIES + 2]))
    for fetch in fetches:
        fetch.start()
    for fetch in fetches[:-1]:
        fetch.wait()
    core, odd = side_ref[0], side_ref[1] == 1
    inner_ref[SPECIES] = wlev_ref[0]
    outer_ref[SPECIES] = wlev_ref[0]
    for j in range(2):
        row_ref[SPECIES, j] = wlat_ref[j, :1]
        far_row_ref[SPECIES, j] = wlat_ref[j, :1]

    @pl.loop(0, SPECIES)
    def _(s):
        inner_ref[s] = n_ref[s, 1 - core]
        outer_ref[s] = n_ref[s, core]
        for j in range(2):
            first, last = n_ref[s, j, :1], n_ref[s, j, BAND_LATS - 1 :]
            row_ref[s, j] = jnp.where(odd, first, last)
            far_row_ref[s, j] = jnp.where(odd, last, first)

    fetches[-1].wait()


def edges(side, density, wind_lon, wind_lat, wind_lev):
    return call(
        edges_kernel,
        (
            on_chip(density.shape),
            on_chip(wind_lon.shape),
            on_chip(wind_lat.shape),
            on_chip(wind_lev.shape),
            on_chip((SPECIES + 1, BAND_LATS, NLON)),
            on_chip((SPECIES + 1, BAND_LATS, NLON)),
            on_chip((SPECIES + 1, 2, 1, NLON)),
            on_chip((SPECIES + 1, 2, 1, NLON)),
        ),
        [SMEM] + [HBM] * 4,
        (VMEM,) * 8,
        [pltpu.SemaphoreType.DMA((SPECIES + 3,))],
        flops=1_000_000,
    )(side, density, wind_lon, wind_lat, wind_lev)


def interior_kernel(n_ref, wlon_ref, wlat_ref, wlev_ref, out_ref):
    row = lax.broadcasted_iota(jnp.int32, (BAND_LATS, NLON), 0)

    @pl.loop(0, SPECIES)
    def _(s):
        for j in range(2):
            x = n_ref[s, j]
            west = jnp.concatenate([x[:, NLON - 1 :], x[:, : NLON - 1]], axis=1)
            flux = upwind(wlon_ref[j], west, x)
            total = x + (flux - jnp.concatenate([flux[:, 1:], flux[:, :1]], axis=1))
            flux = upwind(wlat_ref[j], pltpu.roll(x, 1, axis=0), x)
            flux = jnp.where(row == 0, 0.0, flux)
            total = total + (flux - pltpu.roll(flux, BAND_LATS - 1, axis=0))
            flux = upwind(wlev_ref[1], n_ref[s, 0], n_ref[s, 1])
            out_ref[s, j] = total + flux if j else total - flux


def interior(density, winds):
    return call(
        interior_kernel, on_chip((SPECIES, 2, BAND_LATS, NLON)), [HELD] * 4, VMEM, flops=8_000_000
    )(density, *winds)


def faces_kernel(side_ref, n_ref, inside_ref, wlat_ref, wlev_ref, *refs, last):
    inner_ref, outer_ref, row_ref, far_row_ref = refs[:4]
    inner_wind, outer_wind, row_wind, far_row_wind = refs[4:8]
    outs = refs[8:]
    odd = side_ref[1] == 1
    row = lax.broadcasted_iota(jnp.int32, (BAND_LATS, NLON), 0)

    def advance(core):
        below_ref, above_ref, above_wind = (
            (outer_ref, inner_ref, inner_wind) if core == 0 else (inner_ref, outer_ref, outer_wind)
        )

        @pl.loop(0, SPECIES)
        def _(s):
            for j in range(2):
                x = n_ref[s, j]
                total = inside_ref[s, j]
                south = jnp.where(odd, row_ref[s, j], far_row_ref[s, j])
                north = jnp.where(odd, far_row_ref[s, j], row_ref[s, j])
                north_wind = jnp.where(odd, far_row_wind[SPECIES, j], row_wind[SPECIES, j])
                into = upwind(wlat_ref[j, :1], south, x[:1])
                out_of = upwind(north_wind, x[BAND_LATS - 1 :], north)
                total = total + jnp.where(row == 0, into, 0.0) - jnp.where(row == BAND_LATS - 1, out_of, 0.0)
                if j == 0:
                    total = total + upwind(wlev_ref[0], below_ref[s], x)
                else:
                    total = total - upwind(above_wind[SPECIES], x, above_ref[s])
                if last:
                    start = pl.multiple_of((j * SPECIES + s) * BAND_LATS, BAND_LATS)
                    for blk in range(LON_BLOCKS):
                        wide = min(LANES, NLON - blk * LANES)
                        outs[0][blk, pl.ds(start, BAND_LATS), :wide] = total[:, blk * LANES : blk * LANES + wide]
                    continue
                outs[0][s, j] = total
                outs[2 if j == core else 1][s] = total
                first, final = total[:1], total[BAND_LATS - 1 :]
                outs[3][s, j] = jnp.where(odd, first, final)
                outs[4][s, j] = jnp.where(odd, final, first)

    for core in range(2):
        pl.when(side_ref[0] == core)(functools.partial(advance, core))


def faces(side, density, inside, winds, halo, wind_halo, last):
    if last:
        out_shape = (on_chip((LON_BLOCKS, 2 * SPECIES * BAND_LATS, LANES)),)
    else:
        out_shape = (
            on_chip((SPECIES, 2, BAND_LATS, NLON)),
            on_chip((SPECIES, BAND_LATS, NLON)),
            on_chip((SPECIES, BAND_LATS, NLON)),
            on_chip((SPECIES, 2, 1, NLON)),
            on_chip((SPECIES, 2, 1, NLON)),
        )
    return call(
        functools.partial(faces_kernel, last=last),
        out_shape,
        [SMEM] + [HELD] * 12,
        (VMEM,) * len(out_shape),
        flops=2_000_000,
    )(side, density, inside, *winds[1:], *halo, *wind_halo)


def prepare_kernel(
    units_ref, owner_ref, rows_ref, sel_ref, weight_ref, column_ref,
    table_ref, own_ref, coef_ref, count, blocks, table, picked,
):
    @pl.loop(0, PEERS * PEER_SLOTS // 8)
    def _(i):
        for k in range(8):
            table_ref[i * 8 + k] = ZERO_TUBE

    @pl.loop(0, PEERS // 8)
    def _(i):
        for k in range(8):
            count[i * 8 + k] = 0

    @pl.loop(0, units_ref[0])
    def _(u):
        dest = owner_ref[u]
        rank = count[dest]
        count[dest] = rank + 1
        table_ref[dest * PEER_SLOTS + rank] = u

    coef_ref[...] = jnp.broadcast_to(column_ref[...], coef_ref.shape)

    for blk in range(LON_BLOCKS):
        wide = min(LANES, NLON - blk * LANES)
        blocks[blk, :, :wide] = weight_ref[:, blk * LANES : blk * LANES + wide]

    @pl.loop(0, BAND_LATS)
    def _(lat):
        for g in range(6):
            parts = [
                blocks[min(4 * g + i, LON_BLOCKS - 1), pl.ds(lat + h * BAND_LATS, 8, stride=4 * BAND_LATS), :]
                for i in range(4)
                for h in range(4)
            ]
            start = pl.multiple_of((lat * 6 + g) * LANES, LANES)
            table[pl.ds(start, LANES), :] = jnp.concatenate(parts, axis=0).T

    @pl.loop(0, SLOTS_PAD // UNROLL)
    def _(step):
        base = pl.multiple_of(step * UNROLL, UNROLL)
        places = rows_ref.at[pl.ds(base, UNROLL)]
        for i in range(UNROLL):
            picked[pl.ds(base + i, 1), :] = table[pl.ds(places[i], 1), :]

    for blk in range(SLOT_BLOCKS):
        turned = picked[blk * LANES : (blk + 1) * LANES, :].T
        which = sel_ref[blk : blk + 1, :]
        kept = turned[:PAIRS]
        for i in range(1, 4):
            kept = jnp.where(which == i, turned[i * PAIRS : (i + 1) * PAIRS], kept)
        own_ref[blk] = kept


def prepare(units, owners, rows, sel, weights, column):
    return call(
        prepare_kernel,
        (
            sds((PEERS * PEER_SLOTS,), jnp.int32),
            on_chip((SLOT_BLOCKS, PAIRS, LANES)),
            on_chip((3 * SPECIES * NLEV, LANES)),
        ),
        [SMEM, SMEM, SMEM, VMEM, VMEM, VMEM],
        (SMEM, VMEM, VMEM),
        [
            pltpu.SMEM((PEERS,), jnp.int32),
            pltpu.VMEM((LON_BLOCKS, PAIRS * BAND_LATS, LANES), f32),
            pltpu.VMEM((BAND_LATS * 6 * LANES, LANES), f32),
            pltpu.VMEM((SLOTS_PAD, LANES), f32),
        ],
        flops=20_000_000,
    )(units, owners, rows, sel, weights, column)


def fill_planes(planes, source_ref):
    @pl.loop(0, LON_BLOCKS)
    def _(blk):
        for j in range(2):
            for i in range(PLANES):
                from_row = (j * SPECIES + i % SPECIES) * BAND_LATS
                planes[blk, pl.ds((j * PLANES + i) * PITCH, BAND_LATS), :] = source_ref[
                    blk, from_row : from_row + BAND_LATS, :
                ]


def fill_table(planes, table_ref, lats):
    half = LANES // 2

    @pl.loop(0, LON_BLOCKS)
    def _(blk):
        for a in range(BAND_LATS // 2):
            parts = [
                planes[blk, pl.ds((j * PLANES + first) * PITCH + lat, 8, stride=PITCH), :]
                for lat in lats(a)
                for j in range(2)
                for first in (0, 3, 1, 4)
            ]
            rows = jnp.concatenate(parts, axis=0).T
            for side, lat in enumerate(lats(a)):
                start = pl.multiple_of((lat * LON_BLOCKS + blk) * LANES, LANES)
                lanes = slice(side * half, (side + 1) * half)
                table_ref[pl.ds(start, LANES), lanes] = rows[:, lanes]


def own_table_kernel(mine_ref, table_ref, planes):
    fill_planes(planes, mine_ref)
    fill_table(planes, table_ref, lambda a: (a, a + BAND_LATS // 2))


def own_table(mine):
    return call(
        own_table_kernel,
        on_chip((BAND_LATS * LON_PAD, LANES)),
        [HELD],
        VMEM,
        [pltpu.VMEM((LON_BLOCKS, 2 * PLANES * PITCH, LANES), f32)],
        flops=8_000_000,
    )(mine)


def pack_kernel(
    core_ref, starts_ref, units_ref, order_hbm, other_ref, _,
    out_hbm, table_ref, order_ref, planes, msg_ref, sems, order_sem,
):
    fetch = pltpu.make_async_copy(order_hbm, order_ref, order_sem)
    fetch.start()
    core = core_ref[0]
    fill_planes(planes, other_ref)
    fill_table(planes, table_ref, lambda a: (a + BAND_LATS // 2, a))

    lane = lax.broadcasted_iota(jnp.int32, (1, LANES), 1)
    group_of = lax.div(lax.rem(lane, 32), SPECIES)

    def send(peer):
        rows = pl.ds(pl.multiple_of(peer * PEER_ROWS, PEER_ROWS), PEER_ROWS)
        return pltpu.make_async_copy(msg_ref.at[rows, :], out_hbm.at[rows, :], sems.at[peer])

    fetch.wait()

    @pl.loop(0, 16)
    def _(peer):
        owner = 2 * peer + core
        first = TUBE_COLS * starts_ref[owner]
        pieces = lax.div(TUBE_COLS * units_ref[owner] + (PIECE - 1), PIECE)

        def copy(start, number):
            places = []
            for k in range(number):
                piece = start + k
                tail = piece >= 2 * GROUPS
                group = jnp.where(tail, piece - 2 * GROUPS, lax.div(piece, 2))
                row = peer * PEER_ROWS + jnp.where(tail, 2 * PIECE, PIECE * lax.rem(piece, 2))
                places.append((pl.multiple_of(row, PIECE), group_of == group))
            base = first + start * PIECE
            for i in range(number * PIECE):
                place = order_ref.at[pl.ds(i, ORDER_PAD - 2 * PIECE)][base]
                row, mask = places[i // PIECE]
                value = table_ref[pl.ds(place, 1), :]
                pltpu.store(msg_ref.at[pl.ds(row + i % PIECE, 1), :], value, mask=mask)

        @pl.loop(0, lax.div(pieces, 2))
        def _(pair):
            copy(2 * pair, 2)

        pl.when(lax.rem(pieces, 2) == 1)(functools.partial(copy, pieces - 1, 1))
        send(peer).start()

    @pl.loop(0, 16)
    def _(peer):
        send(peer).wait()


def pack(core, starts, units, order, other, table):
    outgoing, _ = call(
        pack_kernel,
        (sds((16 * PEER_ROWS, LANES)), on_chip((BAND_LATS * LON_PAD, LANES))),
        [SMEM, SMEM, SMEM, HBM, HELD, HELD],
        (HBM, VMEM),
        [
            pltpu.SMEM((ORDER_PAD,), jnp.int32),
            pltpu.VMEM((LON_BLOCKS, 2 * PLANES * PITCH, LANES), f32),
            pltpu.VMEM((16 * PEER_ROWS, LANES), f32),
            pltpu.SemaphoreType.DMA((16,)),
            pltpu.SemaphoreType.DMA,
        ],
        flops=30_000_000,
        aliases={5: 1},
    )(core, starts, units, order, other, table)
    return outgoing


def solve_kernel(
    core_ref, units_ref, table_ref, got_ref, coef_ref, weight_ref, north_ref, state_hbm, items_ref,
    turned, natural, pairs, wide, tubes, state, sems,
):
    core = core_ref[0]
    live = TUBE_COLS * units_ref[0]
    lane = lax.broadcasted_iota(jnp.int32, (1, LANES), 1)
    low = lane < 64
    quarter = lax.div(lane, 32)

    @pl.loop(0, 8)
    def _(i):
        for side in range(2):
            out = i * LEVEL_PITCH + side * LANES
            row = pl.multiple_of((2 * i + side) * PEER_ROWS, PIECE)
            tail = got_ref[pl.ds(row + LANES, PIECE), :]
            for part, rows in enumerate((got_ref[pl.ds(row, LANES), :], jnp.concatenate([tail] * 2, axis=0))):
                flipped = rows.T
                turned[part, pl.ds(out + 64 * core, 64), :] = flipped[:64]
                turned[part, pl.ds(out + 64 - 64 * core, 64), :] = flipped[64:]

    def leave(s):
        return pltpu.make_async_copy(state.at[s], state_hbm.at[0, 0, s], sems.at[s])

    @pl.loop(0, SPECIES)
    def _(s):
        def coefs(which):
            row = pl.multiple_of((which * SPECIES + s) * NLEV, NLEV)
            return [coef_ref[pl.ds(row + 8 * v, 8), :] for v in range(8)]

        lower, upper, inv = coefs(0), coefs(1), coefs(2)
        for blk in range(SLOT_BLOCKS):
            i = blk % 3

            def levels(part, group, v):
                return turned[part, pl.ds(32 * v + group * SPECIES + s, 8, stride=LEVEL_PITCH), :]

            if blk < GROUPS:
                raw = [levels(0, blk, v) for v in range(8)]
            else:
                raw = [jnp.where(low, levels(1, 2 * i, v), levels(1, 2 * i + 1, v)) for v in range(8)]
            north = north_ref[blk : blk + 1, :] == 1
            rhs = [jnp.where(north, raw[v ^ 2], raw[v]) for v in range(8)]
            scaled = [rhs[v] * inv[v] for v in range(8)]
            x = rhs
            for _ in range(SWEEPS):
                beneath = [pltpu.roll(x[7], 1, axis=0)] + x[:7]
                overhead = x[1:] + [pltpu.roll(x[0], 7, axis=0)]
                x = [scaled[v] + lower[v] * beneath[v] + upper[v] * overhead[v] for v in range(8)]
            keep = lane + blk * LANES < live
            for v in range(8):
                natural[i, pl.ds(v, 8, stride=PITCH), :] = jnp.where(keep, x[v], 0.0)
            width = min(LANES, COL_CAP - blk * LANES)
            for g in range(8):
                state[s, g * 8 : g * 8 + 8, blk * LANES : blk * LANES + width] = natural[
                    i, g * PITCH : g * PITCH + 8, :width
                ]
            for h in range(4):
                weight = weight_ref[blk, 8 * h : 8 * h + 8, :]
                paired = weight * x[2 * h] + (1.0 - weight) * x[2 * h + 1]
                pairs[i, pl.ds(h, 8, stride=4), :] = paired
            wide[i] = jnp.concatenate([pairs[i]] * 4, axis=0).T
            item = wide[i, pl.ds(0, 32, stride=TUBE_COLS), :]
            for c in range(1, TUBE_COLS):
                item = jnp.where(quarter == c, wide[i, pl.ds(c, 32, stride=TUBE_COLS), :], item)
            tubes[pl.ds(blk * 256 + s, 32, stride=8), :] = item
        leave(s).start()

    tubes[ZERO_TUBE * 8 :, :] = jnp.zeros((8, LANES), f32)
    sub = lax.broadcasted_iota(jnp.int32, (8, LANES), 0)

    @pl.loop(0, PEERS // 4)
    def _(step):
        for i in range(4):
            d = step * 4 + i
            tiles = [
                tubes[pl.ds(pl.multiple_of(table_ref[d * PEER_SLOTS + r] * 8, 8), 8), :] for r in range(PEER_SLOTS)
            ]
            mid = pltpu.roll(tiles[1], 5, axis=0)
            top = pltpu.roll(tiles[2], 2, axis=0)
            row = pl.multiple_of(d * ITEM_ROWS, ITEM_ROWS)
            items_ref[pl.ds(row, 8), :] = jnp.where(sub < 5, tiles[0], mid)
            items_ref[pl.ds(row + 8, 8), :] = jnp.where(sub < 2, mid, jnp.where(sub < 7, top, 0.0))

    for s in range(SPECIES):
        leave(s).wait()


def solve(core, units, table, got, coefs, weights, north):
    return call(
        solve_kernel,
        (sds((1, 1, SPECIES, NLEV, COL_CAP)), sds((PEERS * ITEM_ROWS, LANES))),
        [SMEM, SMEM, SMEM] + [HELD] * 4,
        (HBM, VMEM),
        [
            pltpu.VMEM((2, 8 * LEVEL_PITCH, LANES), f32),
            pltpu.VMEM((3, 8 * PITCH, LANES), f32),
            pltpu.VMEM((3, PAIRS, LANES), f32),
            pltpu.VMEM((3, LANES, LANES), f32),
            pltpu.VMEM((ZERO_TUBE * 8 + 8, LANES), f32),
            pltpu.VMEM((SPECIES, NLEV, COL_CAP), f32),
            pltpu.SemaphoreType.DMA((SPECIES,)),
        ],
        flops=40_000_000,
    )(core, units, table, got, coefs, weights, north)


def halves(x):
    high = x.astype(jnp.bfloat16)
    return high, (x - high.astype(f32)).astype(jnp.bfloat16)


def product(x, high, low):
    x_high, x_low = halves(x)
    dot = functools.partial(jnp.dot, preferred_element_type=f32)
    return dot(x_high, high) + (dot(x_low, high) + dot(x_high, low))


def lines_kernel(
    items_ref, yield_ref, rates_ref, waves_ref, fwd_high, fwd_low, inv_high, inv_low, out_hbm,
    spec_in, spec, mixed, done, sems,
):
    tubes = 32 * PEER_SLOTS
    for b in range(4):
        for s in range(SPECIES):
            for r in range(PEER_SLOTS):
                rows = items_ref[pl.ds(b * 32 * ITEM_ROWS + r * SPECIES + s, 32, stride=ITEM_ROWS), :]
                spec_in[b, pl.ds(s * tubes + r, 32, stride=PEER_SLOTS), :] = rows

    half = SPECIES * tubes // 2
    for step in range(2):
        row = step * half
        x = jnp.concatenate([spec_in[b, pl.ds(row, half), :] for b in range(4)], axis=1)
        spec[pl.ds(row, half), :] = product(x, fwd_high[...], fwd_low[...])

    waves = waves_ref[...]
    for i in range(IONS):
        keep = (1.0 - rates_ref[IONS + i]) + rates_ref[i] * waves
        gain = jnp.ones_like(waves)
        for _ in range(SECTIONS - 1):
            gain = gain * keep + 1.0
        total = (yield_ref[i * SPECIES] * gain) * spec[:tubes, :]
        for s in range(1, SPECIES):
            total = total + (yield_ref[i * SPECIES + s] * gain) * spec[s * tubes : (s + 1) * tubes, :]
        mixed[i] = total

    def leave(i):
        return pltpu.make_async_copy(done.at[i], out_hbm.at[0, i], sems.at[i])

    for i in range(0, IONS, 2):
        j = min(i + 2, IONS)
        back = product(mixed[i:j].reshape((j - i) * tubes, LINE_PTS), inv_high[...], inv_low[...])
        done[i:j] = back.reshape(j - i, tubes, LINE_PTS)
        for k in range(i, j):
            leave(k).start()

    for i in range(IONS):
        leave(i).wait()


def cosine_basis():
    k = np.arange(LINE_PTS)[:, None]
    n = np.arange(LINE_PTS)[None, :]
    basis = np.cos(np.pi * k * (n + 0.5) / LINE_PTS) * np.sqrt(2.0 / LINE_PTS)
    basis[0] *= np.sqrt(0.5)
    waves = 2.0 * np.cos(np.pi * np.arange(LINE_PTS) / LINE_PTS) - 2.0
    return basis, waves


def lines(items, ion_yield, ion_spread, ion_loss):
    basis, waves = cosine_basis()

    def parts(matrix):
        matrix = matrix.astype(np.float32)
        high = matrix.astype(jnp.bfloat16)
        low = (matrix - high.astype(np.float32)).astype(jnp.bfloat16)
        return jnp.asarray(high), jnp.asarray(low)

    waves = jnp.asarray(waves.astype(np.float32))[None]
    tubes = 32 * PEER_SLOTS
    by_ion = call(
        lines_kernel,
        sds((1, IONS, tubes, LINE_PTS)),
        [HELD, SMEM, SMEM] + [HELD] * 5,
        HBM,
        [
            pltpu.VMEM((4, SPECIES * tubes, LANES), f32),
            pltpu.VMEM((SPECIES * tubes, LINE_PTS), f32),
            pltpu.VMEM((IONS, tubes, LINE_PTS), f32),
            pltpu.VMEM((IONS, tubes, LINE_PTS), f32),
            pltpu.SemaphoreType.DMA((IONS,)),
        ],
        flops=2_000_000_000,
    )(items, ion_yield.reshape(-1), jnp.concatenate([ion_spread, ion_loss]), waves, *parts(basis.T), *parts(basis))
    return jnp.swapaxes(by_ion, 1, 2)


def swap(x, axis, offset):
    count = lax.axis_size(axis)
    lows = range(offset, count - 1, 2)
    return lax.ppermute(x, axis, [(i, i + 1) for i in lows] + [(i + 1, i) for i in lows])


def exchange(inner, outer, row, far_row):
    outer = swap(outer, "lev", 1)
    row = swap(row, "band", 0)
    far_row = swap(far_row, "band", 1)
    inner = swap(inner, "lev", 0)
    return inner, outer, row, far_row


def on_device(
    neutrals,
    wind_lon,
    wind_lat,
    wind_lev,
    eddy_coupling,
    pair_weight,
    ion_yield,
    ion_spread,
    ion_loss,
    column_order,
    column_units,
    tube_owner,
):
    lev = lax.axis_index("lev")

    side = jnp.stack([lev % 2, lax.axis_index("band") % 2]).astype(jnp.int32)
    neutrals, *rest = edges(side, neutrals, wind_lon, wind_lat, wind_lev)
    winds, first_halo = rest[:3], exchange(*rest[3:])

    starts = jnp.cumsum(column_units) - column_units
    order = column_order[0]
    lat = jnp.zeros_like(order)
    for i in range(1, BAND_LATS):
        lat = lat + (order >= i * NLON).astype(jnp.int32)
    rows = jnp.pad(order + lat * (LON_PAD - NLON), (0, ORDER_PAD - BAND_COLS))
    own_units = column_units[lev].reshape(1)
    padded = jnp.pad(order, (0, SLOTS_PAD))
    own = lax.dynamic_slice(padded, (TUBE_COLS * starts[lev],), (SLOTS_PAD,))
    own_lat = jnp.zeros_like(own)
    for i in range(1, BAND_LATS):
        own_lat = own_lat + (own >= i * NLON).astype(jnp.int32)
    own_north = (own_lat >= BAND_LATS // 2).astype(jnp.int32).reshape(SLOT_BLOCKS, LANES)
    own_lon = own - own_lat * NLON
    own_rows = (own_lat * 6 + own_lon // 512) * LANES + own_lon % LANES
    own_sel = ((own_lon // LANES) % 4).reshape(SLOT_BLOCKS, LANES)
    zero = jnp.zeros((SPECIES, 1), f32)
    lower = jnp.concatenate([zero, eddy_coupling[:, 1:]], 1)
    upper = jnp.concatenate([eddy_coupling[:, 1:], zero], 1)
    inv = 1.0 / (1.0 + lower + upper)
    coefs = jnp.stack([lower * inv, upper * inv, inv]).reshape(3, SPECIES, 8, 8)
    table, own_weights, coefs = prepare(
        own_units,
        tube_owner[lev, :, 0],
        own_rows,
        own_sel,
        pair_weight.reshape(PAIRS * BAND_LATS, NLON),
        jnp.swapaxes(coefs, 2, 3).reshape(-1, 1),
    )

    inside = interior(neutrals, winds)
    density, *halo = faces(side, neutrals, inside, winds, first_halo, first_halo, False)
    inside = interior(density, winds)
    (mine,) = faces(side, density, inside, winds, exchange(*halo), first_halo, True)
    owners = lax.axis_size("lev")
    other = swap(mine, "lev", 0)
    columns = own_table(mine)

    core = (lev % 2).reshape(1)
    parity = [[2 * i + c for i in range(owners // 2)] for c in range(2)]
    outgoing = pack(core, starts, column_units, rows, other, columns)
    got = lax.all_to_all(
        outgoing.reshape(16, PEER_ROWS, LANES), "lev", 0, 0, axis_index_groups=parity, tiled=True
    ).reshape(16 * PEER_ROWS, LANES)
    column_state, items = solve(core, own_units, table, got, coefs, own_weights, own_north)

    items = lax.all_to_all(
        items.reshape(PEERS, ITEM_ROWS, LANES), ("band", "lev"), 0, 0, tiled=True
    ).reshape(PEERS * ITEM_ROWS, LANES)
    return column_state, lines(items, ion_yield, ion_spread, ion_loss)


def solution(mesh):
    placed = (
        P(None, "lev", "band", None),
        P("lev", "band", None),
        P("lev", "band", None),
        P("lev", "band", None),
        P(),
        P(None, "band", None),
        P(),
        P(),
        P(),
        P("band", None),
        P(),
        P(),
    )

    return jax.shard_map(
        on_device,
        mesh=mesh,
        in_specs=placed,
        out_specs=(P("band", "lev", None, None, None), P(("band", "lev"), None, None, None)),
        check_vma=False,
    )
```

```python
import functools

import jax
import jax.numpy as jnp
import numpy as np
from jax import lax
from jax.experimental import pallas as pl
from jax.experimental.pallas import tpu as pltpu
from jax.sharding import PartitionSpec as P


SPECIES = 5
IONS = 7
NLON = 2880
NLEV = 64
PAIRS = 32
BAND_LATS = 8
SWEEPS = 8
SECTIONS = 20
TUBE_COLS = 4
PEERS = 128
PEER_SLOTS = 3
COL_CAP = 1080
BAND_COLS = BAND_LATS * NLON
LINE_PTS = 512

LANES = 128
LON_BLOCKS = 23
LON_PAD = LON_BLOCKS * LANES
PITCH = 9
LEVEL_PITCH = 257
PLANES = 12
GROUPS = 6
PIECE = 64
PEER_ROWS = 3 * PIECE
SLOT_BLOCKS = 9
SLOTS_PAD = SLOT_BLOCKS * LANES
ORDER_PAD = BAND_COLS + 4 * LANES
UNROLL = 64
ZERO_TUBE = SLOT_BLOCKS * 32
ITEM_ROWS = 16

f32 = jnp.float32
VMEM = pl.BlockSpec(memory_space=pltpu.VMEM)
HELD = pl.BlockSpec(memory_space=pltpu.VMEM)
SMEM = pl.BlockSpec(memory_space=pltpu.SMEM)
HBM = pl.BlockSpec(memory_space=pltpu.HBM)


def on_chip(shape, dtype=f32):
    return pltpu.VMEM(shape, dtype)


def call(kernel, out_shape, in_specs, out_specs, scratch=(), flops=0, vmem=16, aliases=()):
    run = pl.pallas_call(
        kernel,
        out_shape=out_shape,
        in_specs=in_specs,
        out_specs=out_specs,
        scratch_shapes=list(scratch),
        input_output_aliases=dict(aliases),
        cost_estimate=pl.CostEstimate(flops=flops, bytes_accessed=1 << 20, transcendentals=0),
        compiler_params=pltpu.CompilerParams(vmem_limit_bytes=vmem * 1024 * 1024),
    )

    def place(x, spec):
        space = pltpu.VMEM if spec is HELD else pltpu.HBM if spec is HBM else None
        return x if space is None else pltpu.with_memory_space_constraint(x, space)

    def placed(*args):
        return run(*(place(x, spec) for x, spec in zip(args, in_specs)))

    return placed


def sds(shape, dtype=f32):
    return jax.ShapeDtypeStruct(shape, dtype)


def upwind(courant, upstream, downstream):
    return courant * jnp.where(courant > 0.0, upstream, downstream)


def edges_kernel(
    side_ref, n_hbm, wlon_hbm, wlat_hbm, wlev_hbm,
    n_ref, wlon_ref, wlat_ref, wlev_ref, inner_ref, outer_ref, row_ref, far_row_ref, sems,
):
    fetches = [
        pltpu.make_async_copy(n_hbm.at[s], n_ref.at[s], sems.at[s]) for s in range(SPECIES)
    ]
    fetches.append(pltpu.make_async_copy(wlat_hbm, wlat_ref, sems.at[SPECIES]))
    fetches.append(pltpu.make_async_copy(wlev_hbm, wlev_ref, sems.at[SPECIES + 1]))
    fetches.append(pltpu.make_async_copy(wlon_hbm, wlon_ref, sems.at[SPECIES + 2]))
    for fetch in fetches:
        fetch.start()
    for fetch in fetches[:-1]:
        fetch.wait()
    core, odd = side_ref[0], side_ref[1] == 1
    inner_ref[SPECIES] = wlev_ref[0]
    outer_ref[SPECIES] = wlev_ref[0]
    for j in range(2):
        row_ref[SPECIES, j] = wlat_ref[j, :1]
        far_row_ref[SPECIES, j] = wlat_ref[j, :1]

    @pl.loop(0, SPECIES)
    def _(s):
        inner_ref[s] = n_ref[s, 1 - core]
        outer_ref[s] = n_ref[s, core]
        for j in range(2):
            first, last = n_ref[s, j, :1], n_ref[s, j, BAND_LATS - 1 :]
            row_ref[s, j] = jnp.where(odd, first, last)
            far_row_ref[s, j] = jnp.where(odd, last, first)

    fetches[-1].wait()


def edges(side, density, wind_lon, wind_lat, wind_lev):
    return call(
        edges_kernel,
        (
            on_chip(density.shape),
            on_chip(wind_lon.shape),
            on_chip(wind_lat.shape),
            on_chip(wind_lev.shape),
            on_chip((SPECIES + 1, BAND_LATS, NLON)),
            on_chip((SPECIES + 1, BAND_LATS, NLON)),
            on_chip((SPECIES + 1, 2, 1, NLON)),
            on_chip((SPECIES + 1, 2, 1, NLON)),
        ),
        [SMEM] + [HBM] * 4,
        (VMEM,) * 8,
        [pltpu.SemaphoreType.DMA((SPECIES + 3,))],
        flops=1_000_000,
    )(side, density, wind_lon, wind_lat, wind_lev)


def interior_kernel(n_ref, wlon_ref, wlat_ref, wlev_ref, *refs):
    out_ref = refs[-1]
    row = lax.broadcasted_iota(jnp.int32, (BAND_LATS, NLON), 0)

    @pl.loop(0, SPECIES)
    def _(s):
        for j in range(2):
            x = n_ref[s, j]
            west = jnp.concatenate([x[:, NLON - 1 :], x[:, : NLON - 1]], axis=1)
            flux = upwind(wlon_ref[j], west, x)
            total = x + (flux - jnp.concatenate([flux[:, 1:], flux[:, :1]], axis=1))
            flux = upwind(wlat_ref[j], pltpu.roll(x, 1, axis=0), x)
            flux = jnp.where(row == 0, 0.0, flux)
            total = total + (flux - pltpu.roll(flux, BAND_LATS - 1, axis=0))
            flux = upwind(wlev_ref[1], n_ref[s, 0], n_ref[s, 1])
            out_ref[s, j] = total + flux if j else total - flux


def interior(density, winds, ready=()):
    return call(
        interior_kernel,
        on_chip((SPECIES, 2, BAND_LATS, NLON)),
        [HELD] * 4 + [HBM] * len(ready),
        VMEM,
        flops=8_000_000,
    )(density, *winds, *ready)


def faces_kernel(side_ref, n_ref, inside_ref, wlat_ref, wlev_ref, *refs, last):
    inner_ref, outer_ref, row_ref, far_row_ref = refs[:4]
    inner_wind, outer_wind, row_wind, far_row_wind = refs[4:8]
    outs = refs[8:]
    odd = side_ref[1] == 1
    row = lax.broadcasted_iota(jnp.int32, (BAND_LATS, NLON), 0)

    def advance(core):
        below_ref, above_ref, above_wind = (
            (outer_ref, inner_ref, inner_wind) if core == 0 else (inner_ref, outer_ref, outer_wind)
        )

        @pl.loop(0, SPECIES)
        def _(s):
            for j in range(2):
                x = n_ref[s, j]
                total = inside_ref[s, j]
                south = jnp.where(odd, row_ref[s, j], far_row_ref[s, j])
                north = jnp.where(odd, far_row_ref[s, j], row_ref[s, j])
                north_wind = jnp.where(odd, far_row_wind[SPECIES, j], row_wind[SPECIES, j])
                into = upwind(wlat_ref[j, :1], south, x[:1])
                out_of = upwind(north_wind, x[BAND_LATS - 1 :], north)
                total = total + jnp.where(row == 0, into, 0.0) - jnp.where(row == BAND_LATS - 1, out_of, 0.0)
                if j == 0:
                    total = total + upwind(wlev_ref[0], below_ref[s], x)
                else:
                    total = total - upwind(above_wind[SPECIES], x, above_ref[s])
                if last:
                    start = pl.multiple_of((j * SPECIES + s) * BAND_LATS, BAND_LATS)
                    for blk in range(LON_BLOCKS):
                        wide = min(LANES, NLON - blk * LANES)
                        outs[0][blk, pl.ds(start, BAND_LATS), :wide] = total[:, blk * LANES : blk * LANES + wide]
                    continue
                outs[0][s, j] = total
                outs[2 if j == core else 1][s] = total
                first, final = total[:1], total[BAND_LATS - 1 :]
                outs[3][s, j] = jnp.where(odd, first, final)
                outs[4][s, j] = jnp.where(odd, final, first)

    for core in range(2):
        pl.when(side_ref[0] == core)(functools.partial(advance, core))


def faces(side, density, inside, winds, halo, wind_halo, last):
    if last:
        out_shape = (on_chip((LON_BLOCKS, 2 * SPECIES * BAND_LATS, LANES)),)
    else:
        out_shape = (
            on_chip((SPECIES, 2, BAND_LATS, NLON)),
            on_chip((SPECIES, BAND_LATS, NLON)),
            on_chip((SPECIES, BAND_LATS, NLON)),
            on_chip((SPECIES, 2, 1, NLON)),
            on_chip((SPECIES, 2, 1, NLON)),
        )
    return call(
        functools.partial(faces_kernel, last=last),
        out_shape,
        [SMEM] + [HELD] * 12,
        (VMEM,) * len(out_shape),
        flops=2_000_000,
    )(side, density, inside, *winds[1:], *halo, *wind_halo)


def places_kernel(units_ref, order_ref, place_ref, starts_ref):
    def advance(owner, start):
        starts_ref[owner] = start
        return start + units_ref[owner]

    lax.fori_loop(0, units_ref.shape[0], advance, jnp.int32(0))
    order = order_ref[...]
    lat = jnp.zeros_like(order)
    for i in range(1, BAND_LATS):
        lat = lat + (order >= i * NLON).astype(jnp.int32)
    place_ref[:, :BAND_COLS] = order + lat * (LON_PAD - NLON)
    place_ref[:, BAND_COLS:] = jnp.zeros((1, ORDER_PAD - BAND_COLS), jnp.int32)


def list_places(units, order):
    places, starts = call(
        places_kernel,
        (sds((1, ORDER_PAD), jnp.int32), sds(units.shape, jnp.int32)),
        [SMEM, VMEM],
        (VMEM, SMEM),
        flops=1_000_000,
    )(units, order)
    return places.reshape(-1), starts


def prepare_kernel(
    units_ref, owner_ref, rows_ref, sel_ref, weight_ref, column_ref,
    table_ref, own_ref, coef_ref, count, blocks, table, picked,
):
    @pl.loop(0, PEERS * PEER_SLOTS // 8)
    def _(i):
        for k in range(8):
            table_ref[i * 8 + k] = ZERO_TUBE

    @pl.loop(0, PEERS // 8)
    def _(i):
        for k in range(8):
            count[i * 8 + k] = 0

    @pl.loop(0, units_ref[0])
    def _(u):
        dest = owner_ref[u]
        rank = count[dest]
        count[dest] = rank + 1
        table_ref[dest * PEER_SLOTS + rank] = u

    coef_ref[...] = jnp.broadcast_to(column_ref[...], coef_ref.shape)

    for blk in range(LON_BLOCKS):
        wide = min(LANES, NLON - blk * LANES)
        blocks[blk, :, :wide] = weight_ref[:, blk * LANES : blk * LANES + wide]

    @pl.loop(0, BAND_LATS)
    def _(lat):
        for g in range(6):
            parts = [
                blocks[min(4 * g + i, LON_BLOCKS - 1), pl.ds(lat + h * BAND_LATS, 8, stride=4 * BAND_LATS), :]
                for i in range(4)
                for h in range(4)
            ]
            start = pl.multiple_of((lat * 6 + g) * LANES, LANES)
            table[pl.ds(start, LANES), :] = jnp.concatenate(parts, axis=0).T

    @pl.loop(0, SLOTS_PAD // UNROLL)
    def _(step):
        base = pl.multiple_of(step * UNROLL, UNROLL)
        places = rows_ref.at[pl.ds(base, UNROLL)]
        for i in range(UNROLL):
            picked[pl.ds(base + i, 1), :] = table[pl.ds(places[i], 1), :]

    for blk in range(SLOT_BLOCKS):
        turned = picked[blk * LANES : (blk + 1) * LANES, :].T
        which = sel_ref[blk : blk + 1, :]
        kept = turned[:PAIRS]
        for i in range(1, 4):
            kept = jnp.where(which == i, turned[i * PAIRS : (i + 1) * PAIRS], kept)
        own_ref[blk] = kept


def prepare(units, owners, rows, sel, weights, column):
    return call(
        prepare_kernel,
        (
            sds((PEERS * PEER_SLOTS,), jnp.int32),
            on_chip((SLOT_BLOCKS, PAIRS, LANES)),
            on_chip((3 * SPECIES * NLEV, LANES)),
        ),
        [SMEM, SMEM, SMEM, VMEM, VMEM, VMEM],
        (SMEM, VMEM, VMEM),
        [
            pltpu.SMEM((PEERS,), jnp.int32),
            pltpu.VMEM((LON_BLOCKS, PAIRS * BAND_LATS, LANES), f32),
            pltpu.VMEM((BAND_LATS * 6 * LANES, LANES), f32),
            pltpu.VMEM((SLOTS_PAD, LANES), f32),
        ],
        flops=20_000_000,
    )(units, owners, rows, sel, weights, column)


def fill_planes(planes, source_ref):
    @pl.loop(0, LON_BLOCKS)
    def _(blk):
        for j in range(2):
            for i in range(PLANES):
                from_row = (j * SPECIES + i % SPECIES) * BAND_LATS
                planes[blk, pl.ds((j * PLANES + i) * PITCH, BAND_LATS), :] = source_ref[
                    blk, from_row : from_row + BAND_LATS, :
                ]


def fill_table(planes, table_ref, lats):
    half = LANES // 2

    @pl.loop(0, LON_BLOCKS)
    def _(blk):
        for a in range(BAND_LATS // 2):
            parts = [
                planes[blk, pl.ds((j * PLANES + first) * PITCH + lat, 8, stride=PITCH), :]
                for lat in lats(a)
                for j in range(2)
                for first in (0, 3, 1, 4)
            ]
            rows = jnp.concatenate(parts, axis=0).T
            for side, lat in enumerate(lats(a)):
                start = pl.multiple_of((lat * LON_BLOCKS + blk) * LANES, LANES)
                lanes = slice(side * half, (side + 1) * half)
                table_ref[pl.ds(start, LANES), lanes] = rows[:, lanes]


def own_table_kernel(mine_ref, table_ref, planes):
    fill_planes(planes, mine_ref)
    fill_table(planes, table_ref, lambda a: (a, a + BAND_LATS // 2))


def own_table(mine):
    return call(
        own_table_kernel,
        on_chip((BAND_LATS * LON_PAD, LANES)),
        [HELD],
        VMEM,
        [pltpu.VMEM((LON_BLOCKS, 2 * PLANES * PITCH, LANES), f32)],
        flops=8_000_000,
    )(mine)


def pack_kernel(
    core_ref, starts_ref, units_ref, order_hbm, other_ref, _,
    out_hbm, table_ref, order_ref, planes, msg_ref, sems, order_sem,
):
    fetch = pltpu.make_async_copy(order_hbm, order_ref, order_sem)
    fetch.start()
    core = core_ref[0]
    fill_planes(planes, other_ref)
    fill_table(planes, table_ref, lambda a: (a + BAND_LATS // 2, a))

    lane = lax.broadcasted_iota(jnp.int32, (1, LANES), 1)
    group_of = lax.div(lax.rem(lane, 32), SPECIES)

    def send(peer):
        rows = pl.ds(pl.multiple_of(peer * PEER_ROWS, PEER_ROWS), PEER_ROWS)
        return pltpu.make_async_copy(msg_ref.at[rows, :], out_hbm.at[rows, :], sems.at[peer])

    fetch.wait()

    @pl.loop(0, 16)
    def _(peer):
        owner = 2 * peer + core
        first = TUBE_COLS * starts_ref[owner]
        pieces = lax.div(TUBE_COLS * units_ref[owner] + (PIECE - 1), PIECE)

        def copy(start, number):
            places = []
            for k in range(number):
                piece = start + k
                tail = piece >= 2 * GROUPS
                group = jnp.where(tail, piece - 2 * GROUPS, lax.div(piece, 2))
                row = peer * PEER_ROWS + jnp.where(tail, 2 * PIECE, PIECE * lax.rem(piece, 2))
                places.append((pl.multiple_of(row, PIECE), group_of == group))
            base = first + start * PIECE
            for i in range(number * PIECE):
                place = order_ref.at[pl.ds(i, ORDER_PAD - 2 * PIECE)][base]
                row, mask = places[i // PIECE]
                value = table_ref[pl.ds(place, 1), :]
                pltpu.store(msg_ref.at[pl.ds(row + i % PIECE, 1), :], value, mask=mask)

        @pl.loop(0, lax.div(pieces, 2))
        def _(pair):
            copy(2 * pair, 2)

        pl.when(lax.rem(pieces, 2) == 1)(functools.partial(copy, pieces - 1, 1))
        send(peer).start()

    @pl.loop(0, 16)
    def _(peer):
        send(peer).wait()


def pack(core, starts, units, order, other, table):
    outgoing, _ = call(
        pack_kernel,
        (sds((16 * PEER_ROWS, LANES)), on_chip((BAND_LATS * LON_PAD, LANES))),
        [SMEM, SMEM, SMEM, HBM, HELD, HELD],
        (HBM, VMEM),
        [
            pltpu.SMEM((ORDER_PAD,), jnp.int32),
            pltpu.VMEM((LON_BLOCKS, 2 * PLANES * PITCH, LANES), f32),
            pltpu.VMEM((16 * PEER_ROWS, LANES), f32),
            pltpu.SemaphoreType.DMA((16,)),
            pltpu.SemaphoreType.DMA,
        ],
        flops=30_000_000,
        aliases={5: 1},
    )(core, starts, units, order, other, table)
    return outgoing


def solve_kernel(
    core_ref, units_ref, table_ref, got_ref, coef_ref, weight_ref, north_ref, state_hbm, items_hbm,
    turned, natural, pairs, wide, tubes, state, items_ref, sems, item_sems,
):
    core = core_ref[0]
    live = TUBE_COLS * units_ref[0]
    lane = lax.broadcasted_iota(jnp.int32, (1, LANES), 1)
    low = lane < 64
    quarter = lax.div(lane, 32)

    @pl.loop(0, 8)
    def _(i):
        for side in range(2):
            out = i * LEVEL_PITCH + side * LANES
            row = pl.multiple_of((2 * i + side) * PEER_ROWS, PIECE)
            tail = got_ref[pl.ds(row + LANES, PIECE), :]
            for part, rows in enumerate((got_ref[pl.ds(row, LANES), :], jnp.concatenate([tail] * 2, axis=0))):
                flipped = rows.T
                turned[part, pl.ds(out + 64 * core, 64), :] = flipped[:64]
                turned[part, pl.ds(out + 64 - 64 * core, 64), :] = flipped[64:]

    def leave(s):
        return pltpu.make_async_copy(state.at[s], state_hbm.at[0, 0, s], sems.at[s])

    @pl.loop(0, SPECIES)
    def _(s):
        def coefs(which):
            row = pl.multiple_of((which * SPECIES + s) * NLEV, NLEV)
            return [coef_ref[pl.ds(row + 8 * v, 8), :] for v in range(8)]

        lower, upper, inv = coefs(0), coefs(1), coefs(2)
        for blk in range(SLOT_BLOCKS):
            i = blk % 3

            def levels(part, group, v):
                return turned[part, pl.ds(32 * v + group * SPECIES + s, 8, stride=LEVEL_PITCH), :]

            if blk < GROUPS:
                raw = [levels(0, blk, v) for v in range(8)]
            else:
                raw = [jnp.where(low, levels(1, 2 * i, v), levels(1, 2 * i + 1, v)) for v in range(8)]
            north = north_ref[blk : blk + 1, :] == 1
            rhs = [jnp.where(north, raw[v ^ 2], raw[v]) for v in range(8)]
            scaled = [rhs[v] * inv[v] for v in range(8)]
            x = rhs
            for _ in range(SWEEPS):
                beneath = [pltpu.roll(x[7], 1, axis=0)] + x[:7]
                overhead = x[1:] + [pltpu.roll(x[0], 7, axis=0)]
                x = [scaled[v] + lower[v] * beneath[v] + upper[v] * overhead[v] for v in range(8)]
            keep = lane + blk * LANES < live
            for v in range(8):
                natural[i, pl.ds(v, 8, stride=PITCH), :] = jnp.where(keep, x[v], 0.0)
            width = min(LANES, COL_CAP - blk * LANES)
            for g in range(8):
                state[s, g * 8 : g * 8 + 8, blk * LANES : blk * LANES + width] = natural[
                    i, g * PITCH : g * PITCH + 8, :width
                ]
            for h in range(4):
                weight = weight_ref[blk, 8 * h : 8 * h + 8, :]
                paired = weight * x[2 * h] + (1.0 - weight) * x[2 * h + 1]
                pairs[i, pl.ds(h, 8, stride=4), :] = paired
            wide[i] = jnp.concatenate([pairs[i]] * 4, axis=0).T
            item = wide[i, pl.ds(0, 32, stride=TUBE_COLS), :]
            for c in range(1, TUBE_COLS):
                item = jnp.where(quarter == c, wide[i, pl.ds(c, 32, stride=TUBE_COLS), :], item)
            tubes[pl.ds(blk * 256 + s, 32, stride=8), :] = item
        leave(s).start()

    tubes[ZERO_TUBE * 8 :, :] = jnp.zeros((8, LANES), f32)
    sub = lax.broadcasted_iota(jnp.int32, (8, LANES), 0)

    def send(quarter):
        rows = pl.ds(quarter * PEERS // 4 * ITEM_ROWS, PEERS // 4 * ITEM_ROWS)
        return pltpu.make_async_copy(items_ref.at[rows, :], items_hbm.at[rows, :], item_sems.at[quarter])

    for part in range(4):

        @pl.loop(part * PEERS // 16, (part + 1) * PEERS // 16)
        def _(step):
            for i in range(4):
                d = step * 4 + i
                tiles = [
                    tubes[pl.ds(pl.multiple_of(table_ref[d * PEER_SLOTS + r] * 8, 8), 8), :]
                    for r in range(PEER_SLOTS)
                ]
                mid = pltpu.roll(tiles[1], 5, axis=0)
                top = pltpu.roll(tiles[2], 2, axis=0)
                row = pl.multiple_of(d * ITEM_ROWS, ITEM_ROWS)
                items_ref[pl.ds(row, 8), :] = jnp.where(sub < 5, tiles[0], mid)
                items_ref[pl.ds(row + 8, 8), :] = jnp.where(sub < 2, mid, jnp.where(sub < 7, top, 0.0))

        send(part).start()

    for part in range(4):
        send(part).wait()
    for s in range(SPECIES):
        leave(s).wait()


def solve(core, units, table, got, coefs, weights, north):
    return call(
        solve_kernel,
        (sds((1, 1, SPECIES, NLEV, COL_CAP)), sds((PEERS * ITEM_ROWS, LANES))),
        [SMEM, SMEM, SMEM] + [HELD] * 4,
        (HBM, HBM),
        [
            pltpu.VMEM((2, 8 * LEVEL_PITCH, LANES), f32),
            pltpu.VMEM((3, 8 * PITCH, LANES), f32),
            pltpu.VMEM((3, PAIRS, LANES), f32),
            pltpu.VMEM((3, LANES, LANES), f32),
            pltpu.VMEM((ZERO_TUBE * 8 + 8, LANES), f32),
            pltpu.VMEM((SPECIES, NLEV, COL_CAP), f32),
            pltpu.VMEM((PEERS * ITEM_ROWS, LANES), f32),
            pltpu.SemaphoreType.DMA((SPECIES,)),
            pltpu.SemaphoreType.DMA((4,)),
        ],
        flops=40_000_000,
    )(core, units, table, got, coefs, weights, north)


def halves(x):
    high = x.astype(jnp.bfloat16)
    return high, (x - high.astype(f32)).astype(jnp.bfloat16)


def product(x, high, low):
    x_high, x_low = halves(x)
    dot = functools.partial(jnp.dot, preferred_element_type=f32)
    return dot(x_high, high) + (dot(x_low, high) + dot(x_high, low))


def lines_kernel(
    items_ref, yield_ref, rates_ref, waves_ref, fwd_high, fwd_low, inv_high, inv_low, out_hbm,
    spec_in, spec, mixed, done, sems,
):
    tubes = 32 * PEER_SLOTS
    for b in range(4):
        for s in range(SPECIES):
            for r in range(PEER_SLOTS):
                rows = items_ref[pl.ds(b * 32 * ITEM_ROWS + r * SPECIES + s, 32, stride=ITEM_ROWS), :]
                spec_in[b, pl.ds(s * tubes + r, 32, stride=PEER_SLOTS), :] = rows

    half = SPECIES * tubes // 2
    for step in range(2):
        row = step * half
        x = jnp.concatenate([spec_in[b, pl.ds(row, half), :] for b in range(4)], axis=1)
        spec[pl.ds(row, half), :] = product(x, fwd_high[...], fwd_low[...])

    waves = waves_ref[...]
    for i in range(IONS):
        keep = (1.0 - rates_ref[IONS + i]) + rates_ref[i] * waves
        gain = jnp.ones_like(waves)
        for _ in range(SECTIONS - 1):
            gain = gain * keep + 1.0
        total = (yield_ref[i * SPECIES] * gain) * spec[:tubes, :]
        for s in range(1, SPECIES):
            total = total + (yield_ref[i * SPECIES + s] * gain) * spec[s * tubes : (s + 1) * tubes, :]
        mixed[i] = total

    def leave(i):
        return pltpu.make_async_copy(done.at[i], out_hbm.at[0, i], sems.at[i])

    for i in range(0, IONS, 2):
        j = min(i + 2, IONS)
        back = product(mixed[i:j].reshape((j - i) * tubes, LINE_PTS), inv_high[...], inv_low[...])
        done[i:j] = back.reshape(j - i, tubes, LINE_PTS)
        for k in range(i, j):
            leave(k).start()

    for i in range(IONS):
        leave(i).wait()


def cosine_basis():
    k = np.arange(LINE_PTS)[:, None]
    n = np.arange(LINE_PTS)[None, :]
    basis = np.cos(np.pi * k * (n + 0.5) / LINE_PTS) * np.sqrt(2.0 / LINE_PTS)
    basis[0] *= np.sqrt(0.5)
    waves = 2.0 * np.cos(np.pi * np.arange(LINE_PTS) / LINE_PTS) - 2.0
    return basis, waves


def lines(items, ion_yield, ion_spread, ion_loss):
    basis, waves = cosine_basis()

    def parts(matrix):
        matrix = matrix.astype(np.float32)
        high = matrix.astype(jnp.bfloat16)
        low = (matrix - high.astype(np.float32)).astype(jnp.bfloat16)
        return jnp.asarray(high), jnp.asarray(low)

    waves = jnp.asarray(waves.astype(np.float32))[None]
    tubes = 32 * PEER_SLOTS
    by_ion = call(
        lines_kernel,
        sds((1, IONS, tubes, LINE_PTS)),
        [HELD, SMEM, SMEM] + [HELD] * 5,
        HBM,
        [
            pltpu.VMEM((4, SPECIES * tubes, LANES), f32),
            pltpu.VMEM((SPECIES * tubes, LINE_PTS), f32),
            pltpu.VMEM((IONS, tubes, LINE_PTS), f32),
            pltpu.VMEM((IONS, tubes, LINE_PTS), f32),
            pltpu.SemaphoreType.DMA((IONS,)),
        ],
        flops=2_000_000_000,
    )(items, ion_yield.reshape(-1), jnp.concatenate([ion_spread, ion_loss]), waves, *parts(basis.T), *parts(basis))
    return jnp.swapaxes(by_ion, 1, 2)


def swap(x, axis, offset):
    count = lax.axis_size(axis)
    lows = range(offset, count - 1, 2)
    return lax.ppermute(x, axis, [(i, i + 1) for i in lows] + [(i + 1, i) for i in lows])


def exchange(inner, outer, row, far_row):
    outer = swap(outer, "lev", 1)
    row = swap(row, "band", 0)
    far_row = swap(far_row, "band", 1)
    inner = swap(inner, "lev", 0)
    return inner, outer, row, far_row


def on_device(
    neutrals,
    wind_lon,
    wind_lat,
    wind_lev,
    eddy_coupling,
    pair_weight,
    ion_yield,
    ion_spread,
    ion_loss,
    column_order,
    column_units,
    tube_owner,
):
    lev = lax.axis_index("lev")

    side = jnp.stack([lev % 2, lax.axis_index("band") % 2]).astype(jnp.int32)
    neutrals, *rest = edges(side, neutrals, wind_lon, wind_lat, wind_lev)
    winds, first_halo = rest[:3], exchange(*rest[3:])

    places, starts = list_places(column_units, column_order)
    order = column_order[0]
    own_units = column_units[lev].reshape(1)
    padded = jnp.pad(order, (0, SLOTS_PAD))
    own = lax.dynamic_slice(padded, (TUBE_COLS * starts[lev],), (SLOTS_PAD,))
    own_lat = jnp.zeros_like(own)
    for i in range(1, BAND_LATS):
        own_lat = own_lat + (own >= i * NLON).astype(jnp.int32)
    own_north = (own_lat >= BAND_LATS // 2).astype(jnp.int32).reshape(SLOT_BLOCKS, LANES)
    own_lon = own - own_lat * NLON
    own_rows = (own_lat * 6 + own_lon // 512) * LANES + own_lon % LANES
    own_sel = ((own_lon // LANES) % 4).reshape(SLOT_BLOCKS, LANES)
    zero = jnp.zeros((SPECIES, 1), f32)
    lower = jnp.concatenate([zero, eddy_coupling[:, 1:]], 1)
    upper = jnp.concatenate([eddy_coupling[:, 1:], zero], 1)
    inv = 1.0 / (1.0 + lower + upper)
    coefs = jnp.stack([lower * inv, upper * inv, inv]).reshape(3, SPECIES, 8, 8)
    table, own_weights, coefs = prepare(
        own_units,
        tube_owner[lev, :, 0],
        own_rows,
        own_sel,
        pair_weight.reshape(PAIRS * BAND_LATS, NLON),
        jnp.swapaxes(coefs, 2, 3).reshape(-1, 1),
    )

    inside = interior(neutrals, winds)
    density, *halo = faces(side, neutrals, inside, winds, first_halo, first_halo, False)
    inside = interior(density, winds, (places, starts))
    (mine,) = faces(side, density, inside, winds, exchange(*halo), first_halo, True)
    owners = lax.axis_size("lev")
    other = swap(mine, "lev", 0)
    columns = own_table(mine)

    core = (lev % 2).reshape(1)
    parity = [[2 * i + c for i in range(owners // 2)] for c in range(2)]
    outgoing = pack(core, starts, column_units, places, other, columns)
    got = lax.all_to_all(
        outgoing.reshape(16, PEER_ROWS, LANES), "lev", 0, 0, axis_index_groups=parity, tiled=True
    ).reshape(16 * PEER_ROWS, LANES)
    column_state, items = solve(core, own_units, table, got, coefs, own_weights, own_north)

    items = lax.all_to_all(
        items.reshape(PEERS, ITEM_ROWS, LANES), ("band", "lev"), 0, 0, tiled=True
    ).reshape(PEERS * ITEM_ROWS, LANES)
    return column_state, lines(items, ion_yield, ion_spread, ion_loss)


def solution(mesh):
    placed = (
        P(None, "lev", "band", None),
        P("lev", "band", None),
        P("lev", "band", None),
        P("lev", "band", None),
        P(),
        P(None, "band", None),
        P(),
        P(),
        P(),
        P("band", None),
        P(),
        P(),
    )

    return jax.shard_map(
        on_device,
        mesh=mesh,
        in_specs=placed,
        out_specs=(P("band", "lev", None, None, None), P(("band", "lev"), None, None, None)),
        check_vma=False,
    )
```

```python
import functools

import jax
import jax.numpy as jnp
import numpy as np
from jax import lax
from jax.experimental import pallas as pl
from jax.experimental.pallas import tpu as pltpu
from jax.sharding import PartitionSpec as P


SPECIES = 5
IONS = 7
NLON = 2880
NLEV = 64
PAIRS = 32
BAND_LATS = 8
SWEEPS = 8
SECTIONS = 20
TUBE_COLS = 4
PEERS = 128
PEER_SLOTS = 3
COL_CAP = 1080
BAND_COLS = BAND_LATS * NLON
LINE_PTS = 512

LANES = 128
LON_BLOCKS = 23
LON_PAD = LON_BLOCKS * LANES
PITCH = 9
LEVEL_PITCH = 257
PLANES = 12
GROUPS = 6
PIECE = 64
PEER_ROWS = 3 * PIECE
SLOT_BLOCKS = 9
SLOTS_PAD = SLOT_BLOCKS * LANES
ORDER_PAD = BAND_COLS + 4 * LANES
UNROLL = 64
ZERO_TUBE = SLOT_BLOCKS * 32
ITEM_ROWS = 16

f32 = jnp.float32
VMEM = pl.BlockSpec(memory_space=pltpu.VMEM)
HELD = pl.BlockSpec(memory_space=pltpu.VMEM)
SMEM = pl.BlockSpec(memory_space=pltpu.SMEM)
HBM = pl.BlockSpec(memory_space=pltpu.HBM)


def on_chip(shape, dtype=f32):
    return pltpu.VMEM(shape, dtype)


def call(kernel, out_shape, in_specs, out_specs, scratch=(), flops=0, vmem=16, aliases=()):
    run = pl.pallas_call(
        kernel,
        out_shape=out_shape,
        in_specs=in_specs,
        out_specs=out_specs,
        scratch_shapes=list(scratch),
        input_output_aliases=dict(aliases),
        cost_estimate=pl.CostEstimate(flops=flops, bytes_accessed=1 << 20, transcendentals=0),
        compiler_params=pltpu.CompilerParams(vmem_limit_bytes=vmem * 1024 * 1024),
    )

    def place(x, spec):
        space = pltpu.VMEM if spec is HELD else pltpu.HBM if spec is HBM else None
        return x if space is None else pltpu.with_memory_space_constraint(x, space)

    def placed(*args):
        return run(*(place(x, spec) for x, spec in zip(args, in_specs)))

    return placed


def sds(shape, dtype=f32):
    return jax.ShapeDtypeStruct(shape, dtype)


def upwind(courant, upstream, downstream):
    return courant * jnp.where(courant > 0.0, upstream, downstream)


def edges_kernel(
    side_ref, n_hbm, wlon_hbm, wlat_hbm, wlev_hbm,
    n_ref, wlon_ref, wlat_ref, wlev_ref, inner_ref, outer_ref, row_ref, far_row_ref, sems,
):
    fetches = [
        pltpu.make_async_copy(n_hbm.at[s], n_ref.at[s], sems.at[s]) for s in range(SPECIES)
    ]
    fetches.append(pltpu.make_async_copy(wlat_hbm, wlat_ref, sems.at[SPECIES]))
    fetches.append(pltpu.make_async_copy(wlev_hbm, wlev_ref, sems.at[SPECIES + 1]))
    fetches.append(pltpu.make_async_copy(wlon_hbm, wlon_ref, sems.at[SPECIES + 2]))
    for fetch in fetches:
        fetch.start()
    for fetch in fetches[:-1]:
        fetch.wait()
    core, odd = side_ref[0], side_ref[1] == 1
    inner_ref[SPECIES] = wlev_ref[0]
    outer_ref[SPECIES] = wlev_ref[0]
    for j in range(2):
        row_ref[SPECIES, j] = wlat_ref[j, :1]
        far_row_ref[SPECIES, j] = wlat_ref[j, :1]

    @pl.loop(0, SPECIES)
    def _(s):
        inner_ref[s] = n_ref[s, 1 - core]
        outer_ref[s] = n_ref[s, core]
        for j in range(2):
            first, last = n_ref[s, j, :1], n_ref[s, j, BAND_LATS - 1 :]
            row_ref[s, j] = jnp.where(odd, first, last)
            far_row_ref[s, j] = jnp.where(odd, last, first)

    fetches[-1].wait()


def edges(side, density, wind_lon, wind_lat, wind_lev):
    return call(
        edges_kernel,
        (
            on_chip(density.shape),
            on_chip(wind_lon.shape),
            on_chip(wind_lat.shape),
            on_chip(wind_lev.shape),
            on_chip((SPECIES + 1, BAND_LATS, NLON)),
            on_chip((SPECIES + 1, BAND_LATS, NLON)),
            on_chip((SPECIES + 1, 2, 1, NLON)),
            on_chip((SPECIES + 1, 2, 1, NLON)),
        ),
        [SMEM] + [HBM] * 4,
        (VMEM,) * 8,
        [pltpu.SemaphoreType.DMA((SPECIES + 3,))],
        flops=1_000_000,
    )(side, density, wind_lon, wind_lat, wind_lev)


def interior_kernel(n_ref, wlon_ref, wlat_ref, wlev_ref, *refs):
    out_ref = refs[-1]
    row = lax.broadcasted_iota(jnp.int32, (BAND_LATS, NLON), 0)

    @pl.loop(0, SPECIES)
    def _(s):
        for j in range(2):
            x = n_ref[s, j]
            west = jnp.concatenate([x[:, NLON - 1 :], x[:, : NLON - 1]], axis=1)
            flux = upwind(wlon_ref[j], west, x)
            total = x + (flux - jnp.concatenate([flux[:, 1:], flux[:, :1]], axis=1))
            flux = upwind(wlat_ref[j], pltpu.roll(x, 1, axis=0), x)
            flux = jnp.where(row == 0, 0.0, flux)
            total = total + (flux - pltpu.roll(flux, BAND_LATS - 1, axis=0))
            flux = upwind(wlev_ref[1], n_ref[s, 0], n_ref[s, 1])
            out_ref[s, j] = total + flux if j else total - flux


def interior(density, winds, ready=()):
    return call(
        interior_kernel,
        on_chip((SPECIES, 2, BAND_LATS, NLON)),
        [HELD] * (4 + len(ready)),
        VMEM,
        flops=8_000_000,
    )(density, *winds, *ready)


def faces_kernel(side_ref, n_ref, inside_ref, wlat_ref, wlev_ref, *refs, last):
    inner_ref, outer_ref, row_ref, far_row_ref = refs[:4]
    inner_wind, outer_wind, row_wind, far_row_wind = refs[4:8]
    outs = refs[8:]
    odd = side_ref[1] == 1
    row = lax.broadcasted_iota(jnp.int32, (BAND_LATS, NLON), 0)

    def advance(core):
        below_ref, above_ref, above_wind = (
            (outer_ref, inner_ref, inner_wind) if core == 0 else (inner_ref, outer_ref, outer_wind)
        )

        @pl.loop(0, SPECIES)
        def _(s):
            for j in range(2):
                x = n_ref[s, j]
                total = inside_ref[s, j]
                south = jnp.where(odd, row_ref[s, j], far_row_ref[s, j])
                north = jnp.where(odd, far_row_ref[s, j], row_ref[s, j])
                north_wind = jnp.where(odd, far_row_wind[SPECIES, j], row_wind[SPECIES, j])
                into = upwind(wlat_ref[j, :1], south, x[:1])
                out_of = upwind(north_wind, x[BAND_LATS - 1 :], north)
                total = total + jnp.where(row == 0, into, 0.0) - jnp.where(row == BAND_LATS - 1, out_of, 0.0)
                if j == 0:
                    total = total + upwind(wlev_ref[0], below_ref[s], x)
                else:
                    total = total - upwind(above_wind[SPECIES], x, above_ref[s])
                if last:
                    start = pl.multiple_of((j * SPECIES + s) * BAND_LATS, BAND_LATS)
                    for blk in range(LON_BLOCKS):
                        wide = min(LANES, NLON - blk * LANES)
                        outs[0][blk, pl.ds(start, BAND_LATS), :wide] = total[:, blk * LANES : blk * LANES + wide]
                    continue
                outs[0][s, j] = total
                outs[2 if j == core else 1][s] = total
                first, final = total[:1], total[BAND_LATS - 1 :]
                outs[3][s, j] = jnp.where(odd, first, final)
                outs[4][s, j] = jnp.where(odd, final, first)

    for core in range(2):
        pl.when(side_ref[0] == core)(functools.partial(advance, core))


def faces(side, density, inside, winds, halo, wind_halo, last):
    if last:
        out_shape = (on_chip((LON_BLOCKS, 2 * SPECIES * BAND_LATS, LANES)),)
    else:
        out_shape = (
            on_chip((SPECIES, 2, BAND_LATS, NLON)),
            on_chip((SPECIES, BAND_LATS, NLON)),
            on_chip((SPECIES, BAND_LATS, NLON)),
            on_chip((SPECIES, 2, 1, NLON)),
            on_chip((SPECIES, 2, 1, NLON)),
        )
    return call(
        functools.partial(faces_kernel, last=last),
        out_shape,
        [SMEM] + [HELD] * 12,
        (VMEM,) * len(out_shape),
        flops=2_000_000,
    )(side, density, inside, *winds[1:], *halo, *wind_halo)


def places_kernel(units_ref, order_ref, place_ref, starts_ref):
    def advance(owner, start):
        starts_ref[owner] = start
        return start + units_ref[owner]

    lax.fori_loop(0, units_ref.shape[0], advance, jnp.int32(0))
    order = order_ref[...]
    lat = jnp.zeros_like(order)
    for i in range(1, BAND_LATS):
        lat = lat + (order >= i * NLON).astype(jnp.int32)
    place_ref[:, :BAND_COLS] = order + lat * (LON_PAD - NLON)
    place_ref[:, BAND_COLS:] = jnp.zeros((1, ORDER_PAD - BAND_COLS), jnp.int32)


def list_places(units, order):
    places, starts = call(
        places_kernel,
        (on_chip((1, ORDER_PAD), jnp.int32), sds(units.shape, jnp.int32)),
        [SMEM, VMEM],
        (VMEM, SMEM),
        flops=1_000_000,
    )(units, order)
    return places.reshape(-1), starts


def prepare_kernel(
    units_ref, owner_ref, rows_ref, sel_ref, weight_ref, column_ref,
    table_ref, own_ref, coef_ref, count, blocks, table, picked,
):
    @pl.loop(0, PEERS * PEER_SLOTS // 8)
    def _(i):
        for k in range(8):
            table_ref[i * 8 + k] = ZERO_TUBE

    @pl.loop(0, PEERS // 8)
    def _(i):
        for k in range(8):
            count[i * 8 + k] = 0

    @pl.loop(0, units_ref[0])
    def _(u):
        dest = owner_ref[u]
        rank = count[dest]
        count[dest] = rank + 1
        table_ref[dest * PEER_SLOTS + rank] = u

    coef_ref[...] = jnp.broadcast_to(column_ref[...], coef_ref.shape)

    for blk in range(LON_BLOCKS):
        wide = min(LANES, NLON - blk * LANES)
        blocks[blk, :, :wide] = weight_ref[:, blk * LANES : blk * LANES + wide]

    @pl.loop(0, BAND_LATS)
    def _(lat):
        for g in range(6):
            parts = [
                blocks[min(4 * g + i, LON_BLOCKS - 1), pl.ds(lat + h * BAND_LATS, 8, stride=4 * BAND_LATS), :]
                for i in range(4)
                for h in range(4)
            ]
            start = pl.multiple_of((lat * 6 + g) * LANES, LANES)
            table[pl.ds(start, LANES), :] = jnp.concatenate(parts, axis=0).T

    @pl.loop(0, SLOTS_PAD // UNROLL)
    def _(step):
        base = pl.multiple_of(step * UNROLL, UNROLL)
        places = rows_ref.at[pl.ds(base, UNROLL)]
        for i in range(UNROLL):
            picked[pl.ds(base + i, 1), :] = table[pl.ds(places[i], 1), :]

    for blk in range(SLOT_BLOCKS):
        turned = picked[blk * LANES : (blk + 1) * LANES, :].T
        which = sel_ref[blk : blk + 1, :]
        kept = turned[:PAIRS]
        for i in range(1, 4):
            kept = jnp.where(which == i, turned[i * PAIRS : (i + 1) * PAIRS], kept)
        own_ref[blk] = kept


def prepare(units, owners, rows, sel, weights, column):
    return call(
        prepare_kernel,
        (
            sds((PEERS * PEER_SLOTS,), jnp.int32),
            on_chip((SLOT_BLOCKS, PAIRS, LANES)),
            on_chip((3 * SPECIES * NLEV, LANES)),
        ),
        [SMEM, SMEM, SMEM, VMEM, VMEM, VMEM],
        (SMEM, VMEM, VMEM),
        [
            pltpu.SMEM((PEERS,), jnp.int32),
            pltpu.VMEM((LON_BLOCKS, PAIRS * BAND_LATS, LANES), f32),
            pltpu.VMEM((BAND_LATS * 6 * LANES, LANES), f32),
            pltpu.VMEM((SLOTS_PAD, LANES), f32),
        ],
        flops=20_000_000,
    )(units, owners, rows, sel, weights, column)


def fill_planes(planes, source_ref):
    @pl.loop(0, LON_BLOCKS)
    def _(blk):
        for j in range(2):
            for i in range(PLANES):
                from_row = (j * SPECIES + i % SPECIES) * BAND_LATS
                planes[blk, pl.ds((j * PLANES + i) * PITCH, BAND_LATS), :] = source_ref[
                    blk, from_row : from_row + BAND_LATS, :
                ]


def fill_table(planes, table_ref, lats):
    half = LANES // 2

    @pl.loop(0, LON_BLOCKS)
    def _(blk):
        for a in range(BAND_LATS // 2):
            parts = [
                planes[blk, pl.ds((j * PLANES + first) * PITCH + lat, 8, stride=PITCH), :]
                for lat in lats(a)
                for j in range(2)
                for first in (0, 3, 1, 4)
            ]
            rows = jnp.concatenate(parts, axis=0).T
            for side, lat in enumerate(lats(a)):
                start = pl.multiple_of((lat * LON_BLOCKS + blk) * LANES, LANES)
                lanes = slice(side * half, (side + 1) * half)
                table_ref[pl.ds(start, LANES), lanes] = rows[:, lanes]


def own_table_kernel(mine_ref, table_ref, planes):
    fill_planes(planes, mine_ref)
    fill_table(planes, table_ref, lambda a: (a, a + BAND_LATS // 2))


def own_table(mine):
    return call(
        own_table_kernel,
        on_chip((BAND_LATS * LON_PAD, LANES)),
        [HELD],
        VMEM,
        [pltpu.VMEM((LON_BLOCKS, 2 * PLANES * PITCH, LANES), f32)],
        flops=8_000_000,
    )(mine)


def pack_kernel(
    core_ref, starts_ref, units_ref, list_ref, other_ref, _,
    out_hbm, table_ref, order_ref, planes, msg_ref, sems, order_sem,
):
    fetch = pltpu.make_async_copy(list_ref, order_ref, order_sem)
    fetch.start()
    core = core_ref[0]
    fill_planes(planes, other_ref)
    fill_table(planes, table_ref, lambda a: (a + BAND_LATS // 2, a))

    lane = lax.broadcasted_iota(jnp.int32, (1, LANES), 1)
    group_of = lax.div(lax.rem(lane, 32), SPECIES)

    def send(peer):
        rows = pl.ds(pl.multiple_of(peer * PEER_ROWS, PEER_ROWS), PEER_ROWS)
        return pltpu.make_async_copy(msg_ref.at[rows, :], out_hbm.at[rows, :], sems.at[peer])

    fetch.wait()

    @pl.loop(0, 16)
    def _(peer):
        owner = 2 * peer + core
        first = TUBE_COLS * starts_ref[owner]
        pieces = lax.div(TUBE_COLS * units_ref[owner] + (PIECE - 1), PIECE)

        def copy(start, number):
            places = []
            for k in range(number):
                piece = start + k
                tail = piece >= 2 * GROUPS
                group = jnp.where(tail, piece - 2 * GROUPS, lax.div(piece, 2))
                row = peer * PEER_ROWS + jnp.where(tail, 2 * PIECE, PIECE * lax.rem(piece, 2))
                places.append((pl.multiple_of(row, PIECE), group_of == group))
            base = first + start * PIECE
            for i in range(number * PIECE):
                place = order_ref.at[pl.ds(i, ORDER_PAD - 2 * PIECE)][base]
                row, mask = places[i // PIECE]
                value = table_ref[pl.ds(place, 1), :]
                pltpu.store(msg_ref.at[pl.ds(row + i % PIECE, 1), :], value, mask=mask)

        @pl.loop(0, lax.div(pieces, 2))
        def _(pair):
            copy(2 * pair, 2)

        pl.when(lax.rem(pieces, 2) == 1)(functools.partial(copy, pieces - 1, 1))
        send(peer).start()

    @pl.loop(0, 16)
    def _(peer):
        send(peer).wait()


def pack(core, starts, units, order, other, table):
    outgoing, _ = call(
        pack_kernel,
        (sds((16 * PEER_ROWS, LANES)), on_chip((BAND_LATS * LON_PAD, LANES))),
        [SMEM, SMEM, SMEM, HELD, HELD, HELD],
        (HBM, VMEM),
        [
            pltpu.SMEM((ORDER_PAD,), jnp.int32),
            pltpu.VMEM((LON_BLOCKS, 2 * PLANES * PITCH, LANES), f32),
            pltpu.VMEM((16 * PEER_ROWS, LANES), f32),
            pltpu.SemaphoreType.DMA((16,)),
            pltpu.SemaphoreType.DMA,
        ],
        flops=30_000_000,
        aliases={5: 1},
    )(core, starts, units, order, other, table)
    return outgoing


def solve_kernel(
    core_ref, units_ref, table_ref, got_ref, coef_ref, weight_ref, north_ref, state_hbm, items_hbm,
    turned, natural, pairs, wide, tubes, state, items_ref, sems, item_sems,
):
    core = core_ref[0]
    live = TUBE_COLS * units_ref[0]
    lane = lax.broadcasted_iota(jnp.int32, (1, LANES), 1)
    low = lane < 64
    quarter = lax.div(lane, 32)

    @pl.loop(0, 8)
    def _(i):
        for side in range(2):
            out = i * LEVEL_PITCH + side * LANES
            row = pl.multiple_of((2 * i + side) * PEER_ROWS, PIECE)
            tail = got_ref[pl.ds(row + LANES, PIECE), :]
            for part, rows in enumerate((got_ref[pl.ds(row, LANES), :], jnp.concatenate([tail] * 2, axis=0))):
                flipped = rows.T
                turned[part, pl.ds(out + 64 * core, 64), :] = flipped[:64]
                turned[part, pl.ds(out + 64 - 64 * core, 64), :] = flipped[64:]

    def leave(s):
        return pltpu.make_async_copy(state.at[s], state_hbm.at[0, 0, s], sems.at[s])

    @pl.loop(0, SPECIES)
    def _(s):
        def coefs(which):
            row = pl.multiple_of((which * SPECIES + s) * NLEV, NLEV)
            return [coef_ref[pl.ds(row + 8 * v, 8), :] for v in range(8)]

        lower, upper, inv = coefs(0), coefs(1), coefs(2)
        for blk in range(SLOT_BLOCKS):
            i = blk % 3

            def levels(part, group, v):
                return turned[part, pl.ds(32 * v + group * SPECIES + s, 8, stride=LEVEL_PITCH), :]

            if blk < GROUPS:
                raw = [levels(0, blk, v) for v in range(8)]
            else:
                raw = [jnp.where(low, levels(1, 2 * i, v), levels(1, 2 * i + 1, v)) for v in range(8)]
            north = north_ref[blk : blk + 1, :] == 1
            rhs = [jnp.where(north, raw[v ^ 2], raw[v]) for v in range(8)]
            scaled = [rhs[v] * inv[v] for v in range(8)]
            x = rhs
            for _ in range(SWEEPS):
                beneath = [pltpu.roll(x[7], 1, axis=0)] + x[:7]
                overhead = x[1:] + [pltpu.roll(x[0], 7, axis=0)]
                x = [scaled[v] + lower[v] * beneath[v] + upper[v] * overhead[v] for v in range(8)]
            keep = lane + blk * LANES < live
            for v in range(8):
                natural[i, pl.ds(v, 8, stride=PITCH), :] = jnp.where(keep, x[v], 0.0)
            width = min(LANES, COL_CAP - blk * LANES)
            for g in range(8):
                state[s, g * 8 : g * 8 + 8, blk * LANES : blk * LANES + width] = natural[
                    i, g * PITCH : g * PITCH + 8, :width
                ]
            for h in range(4):
                weight = weight_ref[blk, 8 * h : 8 * h + 8, :]
                paired = weight * x[2 * h] + (1.0 - weight) * x[2 * h + 1]
                pairs[i, pl.ds(h, 8, stride=4), :] = paired
            wide[i] = jnp.concatenate([pairs[i]] * 4, axis=0).T
            item = wide[i, pl.ds(0, 32, stride=TUBE_COLS), :]
            for c in range(1, TUBE_COLS):
                item = jnp.where(quarter == c, wide[i, pl.ds(c, 32, stride=TUBE_COLS), :], item)
            tubes[pl.ds(blk * 256 + s, 32, stride=8), :] = item
        leave(s).start()

    tubes[ZERO_TUBE * 8 :, :] = jnp.zeros((8, LANES), f32)
    sub = lax.broadcasted_iota(jnp.int32, (8, LANES), 0)

    def send(quarter):
        rows = pl.ds(quarter * PEERS // 4 * ITEM_ROWS, PEERS // 4 * ITEM_ROWS)
        return pltpu.make_async_copy(items_ref.at[rows, :], items_hbm.at[rows, :], item_sems.at[quarter])

    for part in range(4):

        @pl.loop(part * PEERS // 16, (part + 1) * PEERS // 16)
        def _(step):
            for i in range(4):
                d = step * 4 + i
                tiles = [
                    tubes[pl.ds(pl.multiple_of(table_ref[d * PEER_SLOTS + r] * 8, 8), 8), :]
                    for r in range(PEER_SLOTS)
                ]
                mid = pltpu.roll(tiles[1], 5, axis=0)
                top = pltpu.roll(tiles[2], 2, axis=0)
                row = pl.multiple_of(d * ITEM_ROWS, ITEM_ROWS)
                items_ref[pl.ds(row, 8), :] = jnp.where(sub < 5, tiles[0], mid)
                items_ref[pl.ds(row + 8, 8), :] = jnp.where(sub < 2, mid, jnp.where(sub < 7, top, 0.0))

        send(part).start()

    for part in range(4):
        send(part).wait()
    for s in range(SPECIES):
        leave(s).wait()


def solve(core, units, table, got, coefs, weights, north):
    return call(
        solve_kernel,
        (sds((1, 1, SPECIES, NLEV, COL_CAP)), sds((PEERS * ITEM_ROWS, LANES))),
        [SMEM, SMEM, SMEM] + [HELD] * 4,
        (HBM, HBM),
        [
            pltpu.VMEM((2, 8 * LEVEL_PITCH, LANES), f32),
            pltpu.VMEM((3, 8 * PITCH, LANES), f32),
            pltpu.VMEM((3, PAIRS, LANES), f32),
            pltpu.VMEM((3, LANES, LANES), f32),
            pltpu.VMEM((ZERO_TUBE * 8 + 8, LANES), f32),
            pltpu.VMEM((SPECIES, NLEV, COL_CAP), f32),
            pltpu.VMEM((PEERS * ITEM_ROWS, LANES), f32),
            pltpu.SemaphoreType.DMA((SPECIES,)),
            pltpu.SemaphoreType.DMA((4,)),
        ],
        flops=40_000_000,
    )(core, units, table, got, coefs, weights, north)


def halves(x):
    high = x.astype(jnp.bfloat16)
    return high, (x - high.astype(f32)).astype(jnp.bfloat16)


def product(x, high, low):
    x_high, x_low = halves(x)
    dot = functools.partial(jnp.dot, preferred_element_type=f32)
    return dot(x_high, high) + (dot(x_low, high) + dot(x_high, low))


def lines_kernel(
    items_ref, yield_ref, rates_ref, waves_ref, fwd_high, fwd_low, inv_high, inv_low, out_hbm,
    spec_in, spec, mixed, done, sems,
):
    tubes = 32 * PEER_SLOTS
    for b in range(4):
        for s in range(SPECIES):
            for r in range(PEER_SLOTS):
                rows = items_ref[pl.ds(b * 32 * ITEM_ROWS + r * SPECIES + s, 32, stride=ITEM_ROWS), :]
                spec_in[b, pl.ds(s * tubes + r, 32, stride=PEER_SLOTS), :] = rows

    half = SPECIES * tubes // 2
    for step in range(2):
        row = step * half
        x = jnp.concatenate([spec_in[b, pl.ds(row, half), :] for b in range(4)], axis=1)
        spec[pl.ds(row, half), :] = product(x, fwd_high[...], fwd_low[...])

    waves = waves_ref[...]
    for i in range(IONS):
        keep = (1.0 - rates_ref[IONS + i]) + rates_ref[i] * waves
        gain = jnp.ones_like(waves)
        for _ in range(SECTIONS - 1):
            gain = gain * keep + 1.0
        total = (yield_ref[i * SPECIES] * gain) * spec[:tubes, :]
        for s in range(1, SPECIES):
            total = total + (yield_ref[i * SPECIES + s] * gain) * spec[s * tubes : (s + 1) * tubes, :]
        mixed[i] = total

    def leave(i):
        return pltpu.make_async_copy(done.at[i], out_hbm.at[0, i], sems.at[i])

    for i in range(0, IONS, 2):
        j = min(i + 2, IONS)
        back = product(mixed[i:j].reshape((j - i) * tubes, LINE_PTS), inv_high[...], inv_low[...])
        done[i:j] = back.reshape(j - i, tubes, LINE_PTS)
        for k in range(i, j):
            leave(k).start()

    for i in range(IONS):
        leave(i).wait()


def cosine_basis():
    k = np.arange(LINE_PTS)[:, None]
    n = np.arange(LINE_PTS)[None, :]
    basis = np.cos(np.pi * k * (n + 0.5) / LINE_PTS) * np.sqrt(2.0 / LINE_PTS)
    basis[0] *= np.sqrt(0.5)
    waves = 2.0 * np.cos(np.pi * np.arange(LINE_PTS) / LINE_PTS) - 2.0
    return basis, waves


def lines(items, ion_yield, ion_spread, ion_loss):
    basis, waves = cosine_basis()

    def parts(matrix):
        matrix = matrix.astype(np.float32)
        high = matrix.astype(jnp.bfloat16)
        low = (matrix - high.astype(np.float32)).astype(jnp.bfloat16)
        return jnp.asarray(high), jnp.asarray(low)

    waves = jnp.asarray(waves.astype(np.float32))[None]
    tubes = 32 * PEER_SLOTS
    by_ion = call(
        lines_kernel,
        sds((1, IONS, tubes, LINE_PTS)),
        [HELD, SMEM, SMEM] + [HELD] * 5,
        HBM,
        [
            pltpu.VMEM((4, SPECIES * tubes, LANES), f32),
            pltpu.VMEM((SPECIES * tubes, LINE_PTS), f32),
            pltpu.VMEM((IONS, tubes, LINE_PTS), f32),
            pltpu.VMEM((IONS, tubes, LINE_PTS), f32),
            pltpu.SemaphoreType.DMA((IONS,)),
        ],
        flops=2_000_000_000,
    )(items, ion_yield.reshape(-1), jnp.concatenate([ion_spread, ion_loss]), waves, *parts(basis.T), *parts(basis))
    return jnp.swapaxes(by_ion, 1, 2)


def swap(x, axis, offset):
    count = lax.axis_size(axis)
    lows = range(offset, count - 1, 2)
    return lax.ppermute(x, axis, [(i, i + 1) for i in lows] + [(i + 1, i) for i in lows])


def exchange(inner, outer, row, far_row):
    outer = swap(outer, "lev", 1)
    row = swap(row, "band", 0)
    far_row = swap(far_row, "band", 1)
    inner = swap(inner, "lev", 0)
    return inner, outer, row, far_row


def on_device(
    neutrals,
    wind_lon,
    wind_lat,
    wind_lev,
    eddy_coupling,
    pair_weight,
    ion_yield,
    ion_spread,
    ion_loss,
    column_order,
    column_units,
    tube_owner,
):
    lev = lax.axis_index("lev")

    side = jnp.stack([lev % 2, lax.axis_index("band") % 2]).astype(jnp.int32)
    neutrals, *rest = edges(side, neutrals, wind_lon, wind_lat, wind_lev)
    winds, first_halo = rest[:3], exchange(*rest[3:])

    places, starts = list_places(column_units, column_order)
    order = column_order[0]
    own_units = column_units[lev].reshape(1)
    padded = jnp.pad(order, (0, SLOTS_PAD))
    own = lax.dynamic_slice(padded, (TUBE_COLS * starts[lev],), (SLOTS_PAD,))
    own_lat = jnp.zeros_like(own)
    for i in range(1, BAND_LATS):
        own_lat = own_lat + (own >= i * NLON).astype(jnp.int32)
    own_north = (own_lat >= BAND_LATS // 2).astype(jnp.int32).reshape(SLOT_BLOCKS, LANES)
    own_lon = own - own_lat * NLON
    own_rows = (own_lat * 6 + own_lon // 512) * LANES + own_lon % LANES
    own_sel = ((own_lon // LANES) % 4).reshape(SLOT_BLOCKS, LANES)
    zero = jnp.zeros((SPECIES, 1), f32)
    lower = jnp.concatenate([zero, eddy_coupling[:, 1:]], 1)
    upper = jnp.concatenate([eddy_coupling[:, 1:], zero], 1)
    inv = 1.0 / (1.0 + lower + upper)
    coefs = jnp.stack([lower * inv, upper * inv, inv]).reshape(3, SPECIES, 8, 8)
    table, own_weights, coefs = prepare(
        own_units,
        tube_owner[lev, :, 0],
        own_rows,
        own_sel,
        pair_weight.reshape(PAIRS * BAND_LATS, NLON),
        jnp.swapaxes(coefs, 2, 3).reshape(-1, 1),
    )

    inside = interior(neutrals, winds, (places,))
    density, *halo = faces(side, neutrals, inside, winds, first_halo, first_halo, False)
    inside = interior(density, winds)
    (mine,) = faces(side, density, inside, winds, exchange(*halo), first_halo, True)
    owners = lax.axis_size("lev")
    other = swap(mine, "lev", 0)
    columns = own_table(mine)

    core = (lev % 2).reshape(1)
    parity = [[2 * i + c for i in range(owners // 2)] for c in range(2)]
    outgoing = pack(core, starts, column_units, places, other, columns)
    got = lax.all_to_all(
        outgoing.reshape(16, PEER_ROWS, LANES), "lev", 0, 0, axis_index_groups=parity, tiled=True
    ).reshape(16 * PEER_ROWS, LANES)
    column_state, items = solve(core, own_units, table, got, coefs, own_weights, own_north)

    items = lax.all_to_all(
        items.reshape(PEERS, ITEM_ROWS, LANES), ("band", "lev"), 0, 0, tiled=True
    ).reshape(PEERS * ITEM_ROWS, LANES)
    return column_state, lines(items, ion_yield, ion_spread, ion_loss)


def solution(mesh):
    placed = (
        P(None, "lev", "band", None),
        P("lev", "band", None),
        P("lev", "band", None),
        P("lev", "band", None),
        P(),
        P(None, "band", None),
        P(),
        P(),
        P(),
        P("band", None),
        P(),
        P(),
    )

    return jax.shard_map(
        on_device,
        mesh=mesh,
        in_specs=placed,
        out_specs=(P("band", "lev", None, None, None), P(("band", "lev"), None, None, None)),
        check_vma=False,
    )
```

```python
import functools

import jax
import jax.numpy as jnp
import numpy as np
from jax import lax
from jax.experimental import pallas as pl
from jax.experimental.pallas import tpu as pltpu
from jax.sharding import PartitionSpec as P


SPECIES = 5
IONS = 7
NLON = 2880
NLEV = 64
PAIRS = 32
BAND_LATS = 8
SWEEPS = 8
SECTIONS = 20
TUBE_COLS = 4
PEERS = 128
PEER_SLOTS = 3
COL_CAP = 1080
BAND_COLS = BAND_LATS * NLON
LINE_PTS = 512

LANES = 128
LON_BLOCKS = 23
LON_PAD = LON_BLOCKS * LANES
PITCH = 9
LEVEL_PITCH = 257
PLANES = 12
GROUPS = 6
PIECE = 64
PEER_ROWS = 3 * PIECE
SLOT_BLOCKS = 9
SLOTS_PAD = SLOT_BLOCKS * LANES
ORDER_PAD = BAND_COLS + 4 * LANES
UNROLL = 64
ZERO_TUBE = SLOT_BLOCKS * 32
ITEM_ROWS = 16

f32 = jnp.float32
VMEM = pl.BlockSpec(memory_space=pltpu.VMEM)
HELD = pl.BlockSpec(memory_space=pltpu.VMEM)
SMEM = pl.BlockSpec(memory_space=pltpu.SMEM)
HBM = pl.BlockSpec(memory_space=pltpu.HBM)


def on_chip(shape, dtype=f32):
    return pltpu.VMEM(shape, dtype)


def call(kernel, out_shape, in_specs, out_specs, scratch=(), flops=0, vmem=16, aliases=()):
    run = pl.pallas_call(
        kernel,
        out_shape=out_shape,
        in_specs=in_specs,
        out_specs=out_specs,
        scratch_shapes=list(scratch),
        input_output_aliases=dict(aliases),
        cost_estimate=pl.CostEstimate(flops=flops, bytes_accessed=1 << 20, transcendentals=0),
        compiler_params=pltpu.CompilerParams(vmem_limit_bytes=vmem * 1024 * 1024),
    )

    def place(x, spec):
        space = pltpu.VMEM if spec is HELD else pltpu.HBM if spec is HBM else None
        return x if space is None else pltpu.with_memory_space_constraint(x, space)

    def placed(*args):
        return run(*(place(x, spec) for x, spec in zip(args, in_specs)))

    return placed


def sds(shape, dtype=f32):
    return jax.ShapeDtypeStruct(shape, dtype)


def upwind(courant, upstream, downstream):
    return courant * jnp.where(courant > 0.0, upstream, downstream)


def own_core():
    return lax.rem(lax.axis_index("lev"), 2)


def in_odd_band():
    return lax.rem(lax.axis_index("band"), 2) == 1


def edges_kernel(
    n_hbm, wlon_hbm, wlat_hbm, wlev_hbm,
    n_ref, wlon_ref, wlat_ref, wlev_ref, inner_ref, outer_ref, row_ref, far_row_ref, sems,
):
    fetches = [
        pltpu.make_async_copy(n_hbm.at[s], n_ref.at[s], sems.at[s]) for s in range(SPECIES)
    ]
    fetches.append(pltpu.make_async_copy(wlat_hbm, wlat_ref, sems.at[SPECIES]))
    fetches.append(pltpu.make_async_copy(wlev_hbm, wlev_ref, sems.at[SPECIES + 1]))
    fetches.append(pltpu.make_async_copy(wlon_hbm, wlon_ref, sems.at[SPECIES + 2]))
    for fetch in fetches:
        fetch.start()
    for fetch in fetches[:-1]:
        fetch.wait()
    core, odd = own_core(), in_odd_band()
    inner_ref[SPECIES] = wlev_ref[0]
    outer_ref[SPECIES] = wlev_ref[0]
    for j in range(2):
        row_ref[SPECIES, j] = wlat_ref[j, :1]
        far_row_ref[SPECIES, j] = wlat_ref[j, :1]

    @pl.loop(0, SPECIES)
    def _(s):
        inner_ref[s] = n_ref[s, 1 - core]
        outer_ref[s] = n_ref[s, core]
        for j in range(2):
            first, last = n_ref[s, j, :1], n_ref[s, j, BAND_LATS - 1 :]
            row_ref[s, j] = jnp.where(odd, first, last)
            far_row_ref[s, j] = jnp.where(odd, last, first)

    fetches[-1].wait()


def edges(density, wind_lon, wind_lat, wind_lev):
    return call(
        edges_kernel,
        (
            on_chip(density.shape),
            on_chip(wind_lon.shape),
            on_chip(wind_lat.shape),
            on_chip(wind_lev.shape),
            on_chip((SPECIES + 1, BAND_LATS, NLON)),
            on_chip((SPECIES + 1, BAND_LATS, NLON)),
            on_chip((SPECIES + 1, 2, 1, NLON)),
            on_chip((SPECIES + 1, 2, 1, NLON)),
        ),
        [HBM] * 4,
        (VMEM,) * 8,
        [pltpu.SemaphoreType.DMA((SPECIES + 3,))],
        flops=1_000_000,
    )(density, wind_lon, wind_lat, wind_lev)


def interior_kernel(n_ref, wlon_ref, wlat_ref, wlev_ref, *refs):
    out_ref = refs[-1]
    row = lax.broadcasted_iota(jnp.int32, (BAND_LATS, NLON), 0)

    @pl.loop(0, SPECIES)
    def _(s):
        for j in range(2):
            x = n_ref[s, j]
            west = jnp.concatenate([x[:, NLON - 1 :], x[:, : NLON - 1]], axis=1)
            flux = upwind(wlon_ref[j], west, x)
            total = x + (flux - jnp.concatenate([flux[:, 1:], flux[:, :1]], axis=1))
            flux = upwind(wlat_ref[j], pltpu.roll(x, 1, axis=0), x)
            flux = jnp.where(row == 0, 0.0, flux)
            total = total + (flux - pltpu.roll(flux, BAND_LATS - 1, axis=0))
            flux = upwind(wlev_ref[1], n_ref[s, 0], n_ref[s, 1])
            out_ref[s, j] = total + flux if j else total - flux


def interior(density, winds, ready=()):
    return call(
        interior_kernel,
        on_chip((SPECIES, 2, BAND_LATS, NLON)),
        [HELD] * (4 + len(ready)),
        VMEM,
        flops=8_000_000,
    )(density, *winds, *ready)


def faces_kernel(n_ref, inside_ref, wlat_ref, wlev_ref, *refs, last):
    inner_ref, outer_ref, row_ref, far_row_ref = refs[:4]
    inner_wind, outer_wind, row_wind, far_row_wind = refs[4:8]
    outs = refs[8:]
    odd = in_odd_band()
    row = lax.broadcasted_iota(jnp.int32, (BAND_LATS, NLON), 0)

    def advance(core):
        below_ref, above_ref, above_wind = (
            (outer_ref, inner_ref, inner_wind) if core == 0 else (inner_ref, outer_ref, outer_wind)
        )

        @pl.loop(0, SPECIES)
        def _(s):
            for j in range(2):
                x = n_ref[s, j]
                total = inside_ref[s, j]
                south = jnp.where(odd, row_ref[s, j], far_row_ref[s, j])
                north = jnp.where(odd, far_row_ref[s, j], row_ref[s, j])
                north_wind = jnp.where(odd, far_row_wind[SPECIES, j], row_wind[SPECIES, j])
                into = upwind(wlat_ref[j, :1], south, x[:1])
                out_of = upwind(north_wind, x[BAND_LATS - 1 :], north)
                total = total + jnp.where(row == 0, into, 0.0) - jnp.where(row == BAND_LATS - 1, out_of, 0.0)
                if j == 0:
                    total = total + upwind(wlev_ref[0], below_ref[s], x)
                else:
                    total = total - upwind(above_wind[SPECIES], x, above_ref[s])
                if last:
                    start = pl.multiple_of((j * SPECIES + s) * BAND_LATS, BAND_LATS)
                    for blk in range(LON_BLOCKS):
                        wide = min(LANES, NLON - blk * LANES)
                        outs[0][blk, pl.ds(start, BAND_LATS), :wide] = total[:, blk * LANES : blk * LANES + wide]
                    continue
                outs[0][s, j] = total
                outs[2 if j == core else 1][s] = total
                first, final = total[:1], total[BAND_LATS - 1 :]
                outs[3][s, j] = jnp.where(odd, first, final)
                outs[4][s, j] = jnp.where(odd, final, first)

    for core in range(2):
        pl.when(own_core() == core)(functools.partial(advance, core))


def faces(density, inside, winds, halo, wind_halo, last):
    if last:
        out_shape = (on_chip((LON_BLOCKS, 2 * SPECIES * BAND_LATS, LANES)),)
    else:
        out_shape = (
            on_chip((SPECIES, 2, BAND_LATS, NLON)),
            on_chip((SPECIES, BAND_LATS, NLON)),
            on_chip((SPECIES, BAND_LATS, NLON)),
            on_chip((SPECIES, 2, 1, NLON)),
            on_chip((SPECIES, 2, 1, NLON)),
        )
    return call(
        functools.partial(faces_kernel, last=last),
        out_shape,
        [HELD] * 12,
        (VMEM,) * len(out_shape),
        flops=2_000_000,
    )(density, inside, *winds[1:], *halo, *wind_halo)


def places_kernel(units_ref, order_ref, place_ref, starts_ref):
    def advance(owner, start):
        starts_ref[owner] = start
        return start + units_ref[owner]

    lax.fori_loop(0, units_ref.shape[0], advance, jnp.int32(0))
    order = order_ref[...]
    lat = jnp.zeros_like(order)
    for i in range(1, BAND_LATS):
        lat = lat + (order >= i * NLON).astype(jnp.int32)
    place_ref[:, :BAND_COLS] = order + lat * (LON_PAD - NLON)
    place_ref[:, BAND_COLS:] = jnp.zeros((1, ORDER_PAD - BAND_COLS), jnp.int32)


def list_places(units, order):
    places, starts = call(
        places_kernel,
        (on_chip((1, ORDER_PAD), jnp.int32), sds(units.shape, jnp.int32)),
        [SMEM, VMEM],
        (VMEM, SMEM),
        flops=1_000_000,
    )(units, order)
    return places.reshape(-1), starts


def prepare_kernel(
    units_ref, owner_ref, rows_ref, sel_ref, weight_ref, column_ref,
    table_ref, own_ref, coef_ref, count, blocks, table, picked,
):
    @pl.loop(0, PEERS * PEER_SLOTS // 8)
    def _(i):
        for k in range(8):
            table_ref[i * 8 + k] = ZERO_TUBE

    @pl.loop(0, PEERS // 8)
    def _(i):
        for k in range(8):
            count[i * 8 + k] = 0

    @pl.loop(0, units_ref[0])
    def _(u):
        dest = owner_ref[u]
        rank = count[dest]
        count[dest] = rank + 1
        table_ref[dest * PEER_SLOTS + rank] = u

    coef_ref[...] = jnp.broadcast_to(column_ref[...], coef_ref.shape)

    for blk in range(LON_BLOCKS):
        wide = min(LANES, NLON - blk * LANES)
        blocks[blk, :, :wide] = weight_ref[:, blk * LANES : blk * LANES + wide]

    @pl.loop(0, BAND_LATS)
    def _(lat):
        for g in range(6):
            parts = [
                blocks[min(4 * g + i, LON_BLOCKS - 1), pl.ds(lat + h * BAND_LATS, 8, stride=4 * BAND_LATS), :]
                for i in range(4)
                for h in range(4)
            ]
            start = pl.multiple_of((lat * 6 + g) * LANES, LANES)
            table[pl.ds(start, LANES), :] = jnp.concatenate(parts, axis=0).T

    @pl.loop(0, SLOTS_PAD // UNROLL)
    def _(step):
        base = pl.multiple_of(step * UNROLL, UNROLL)
        places = rows_ref.at[pl.ds(base, UNROLL)]
        for i in range(UNROLL):
            picked[pl.ds(base + i, 1), :] = table[pl.ds(places[i], 1), :]

    for blk in range(SLOT_BLOCKS):
        turned = picked[blk * LANES : (blk + 1) * LANES, :].T
        which = sel_ref[blk : blk + 1, :]
        kept = turned[:PAIRS]
        for i in range(1, 4):
            kept = jnp.where(which == i, turned[i * PAIRS : (i + 1) * PAIRS], kept)
        own_ref[blk] = kept


def prepare(units, owners, rows, sel, weights, column):
    return call(
        prepare_kernel,
        (
            sds((PEERS * PEER_SLOTS,), jnp.int32),
            on_chip((SLOT_BLOCKS, PAIRS, LANES)),
            on_chip((3 * SPECIES * NLEV, LANES)),
        ),
        [SMEM, SMEM, SMEM, VMEM, VMEM, VMEM],
        (SMEM, VMEM, VMEM),
        [
            pltpu.SMEM((PEERS,), jnp.int32),
            pltpu.VMEM((LON_BLOCKS, PAIRS * BAND_LATS, LANES), f32),
            pltpu.VMEM((BAND_LATS * 6 * LANES, LANES), f32),
            pltpu.VMEM((SLOTS_PAD, LANES), f32),
        ],
        flops=20_000_000,
    )(units, owners, rows, sel, weights, column)


def fill_planes(planes, source_ref):
    @pl.loop(0, LON_BLOCKS)
    def _(blk):
        for j in range(2):
            for i in range(PLANES):
                from_row = (j * SPECIES + i % SPECIES) * BAND_LATS
                planes[blk, pl.ds((j * PLANES + i) * PITCH, BAND_LATS), :] = source_ref[
                    blk, from_row : from_row + BAND_LATS, :
                ]


def fill_table(planes, table_ref, lats):
    half = LANES // 2

    @pl.loop(0, LON_BLOCKS)
    def _(blk):
        for a in range(BAND_LATS // 2):
            parts = [
                planes[blk, pl.ds((j * PLANES + first) * PITCH + lat, 8, stride=PITCH), :]
                for lat in lats(a)
                for j in range(2)
                for first in (0, 3, 1, 4)
            ]
            rows = jnp.concatenate(parts, axis=0).T
            for side, lat in enumerate(lats(a)):
                start = pl.multiple_of((lat * LON_BLOCKS + blk) * LANES, LANES)
                lanes = slice(side * half, (side + 1) * half)
                table_ref[pl.ds(start, LANES), lanes] = rows[:, lanes]


def own_table_kernel(mine_ref, table_ref, planes):
    fill_planes(planes, mine_ref)
    fill_table(planes, table_ref, lambda a: (a, a + BAND_LATS // 2))


def own_table(mine):
    return call(
        own_table_kernel,
        on_chip((BAND_LATS * LON_PAD, LANES)),
        [HELD],
        VMEM,
        [pltpu.VMEM((LON_BLOCKS, 2 * PLANES * PITCH, LANES), f32)],
        flops=8_000_000,
    )(mine)


def pack_kernel(
    starts_ref, units_ref, list_ref, other_ref, _,
    out_hbm, table_ref, order_ref, planes, msg_ref, sems, order_sem,
):
    fetch = pltpu.make_async_copy(list_ref, order_ref, order_sem)
    fetch.start()
    core = own_core()
    fill_planes(planes, other_ref)
    fill_table(planes, table_ref, lambda a: (a + BAND_LATS // 2, a))

    lane = lax.broadcasted_iota(jnp.int32, (1, LANES), 1)
    group_of = lax.div(lax.rem(lane, 32), SPECIES)

    def send(peer):
        rows = pl.ds(pl.multiple_of(peer * PEER_ROWS, PEER_ROWS), PEER_ROWS)
        return pltpu.make_async_copy(msg_ref.at[rows, :], out_hbm.at[rows, :], sems.at[peer])

    fetch.wait()

    @pl.loop(0, 16)
    def _(peer):
        owner = 2 * peer + core
        first = TUBE_COLS * starts_ref[owner]
        pieces = lax.div(TUBE_COLS * units_ref[owner] + (PIECE - 1), PIECE)

        def copy(start, number):
            places = []
            for k in range(number):
                piece = start + k
                tail = piece >= 2 * GROUPS
                group = jnp.where(tail, piece - 2 * GROUPS, lax.div(piece, 2))
                row = peer * PEER_ROWS + jnp.where(tail, 2 * PIECE, PIECE * lax.rem(piece, 2))
                places.append((pl.multiple_of(row, PIECE), group_of == group))
            base = first + start * PIECE
            for i in range(number * PIECE):
                place = order_ref.at[pl.ds(i, ORDER_PAD - 2 * PIECE)][base]
                row, mask = places[i // PIECE]
                value = table_ref[pl.ds(place, 1), :]
                pltpu.store(msg_ref.at[pl.ds(row + i % PIECE, 1), :], value, mask=mask)

        @pl.loop(0, lax.div(pieces, 2))
        def _(pair):
            copy(2 * pair, 2)

        pl.when(lax.rem(pieces, 2) == 1)(functools.partial(copy, pieces - 1, 1))
        send(peer).start()

    @pl.loop(0, 16)
    def _(peer):
        send(peer).wait()


def pack(starts, units, order, other, table):
    outgoing, _ = call(
        pack_kernel,
        (sds((16 * PEER_ROWS, LANES)), on_chip((BAND_LATS * LON_PAD, LANES))),
        [SMEM, SMEM, HELD, HELD, HELD],
        (HBM, VMEM),
        [
            pltpu.SMEM((ORDER_PAD,), jnp.int32),
            pltpu.VMEM((LON_BLOCKS, 2 * PLANES * PITCH, LANES), f32),
            pltpu.VMEM((16 * PEER_ROWS, LANES), f32),
            pltpu.SemaphoreType.DMA((16,)),
            pltpu.SemaphoreType.DMA,
        ],
        flops=30_000_000,
        aliases={4: 1},
    )(starts, units, order, other, table)
    return outgoing


def solve_kernel(
    units_ref, table_ref, got_ref, coef_ref, weight_ref, north_ref, state_hbm, items_hbm,
    turned, natural, pairs, wide, tubes, state, items_ref, sems, item_sems,
):
    core = own_core()
    live = TUBE_COLS * units_ref[0]
    lane = lax.broadcasted_iota(jnp.int32, (1, LANES), 1)
    low = lane < 64
    quarter = lax.div(lane, 32)

    @pl.loop(0, 8)
    def _(i):
        for side in range(2):
            out = i * LEVEL_PITCH + side * LANES
            row = pl.multiple_of((2 * i + side) * PEER_ROWS, PIECE)
            tail = got_ref[pl.ds(row + LANES, PIECE), :]
            for part, rows in enumerate((got_ref[pl.ds(row, LANES), :], jnp.concatenate([tail] * 2, axis=0))):
                flipped = rows.T
                turned[part, pl.ds(out + 64 * core, 64), :] = flipped[:64]
                turned[part, pl.ds(out + 64 - 64 * core, 64), :] = flipped[64:]

    def leave(s):
        return pltpu.make_async_copy(state.at[s], state_hbm.at[0, 0, s], sems.at[s])

    @pl.loop(0, SPECIES)
    def _(s):
        def coefs(which):
            row = pl.multiple_of((which * SPECIES + s) * NLEV, NLEV)
            return [coef_ref[pl.ds(row + 8 * v, 8), :] for v in range(8)]

        lower, upper, inv = coefs(0), coefs(1), coefs(2)
        for blk in range(SLOT_BLOCKS):
            i = blk % 3

            def levels(part, group, v):
                return turned[part, pl.ds(32 * v + group * SPECIES + s, 8, stride=LEVEL_PITCH), :]

            if blk < GROUPS:
                raw = [levels(0, blk, v) for v in range(8)]
            else:
                raw = [jnp.where(low, levels(1, 2 * i, v), levels(1, 2 * i + 1, v)) for v in range(8)]
            north = north_ref[blk : blk + 1, :] == 1
            rhs = [jnp.where(north, raw[v ^ 2], raw[v]) for v in range(8)]
            scaled = [rhs[v] * inv[v] for v in range(8)]
            x = rhs
            for _ in range(SWEEPS):
                beneath = [pltpu.roll(x[7], 1, axis=0)] + x[:7]
                overhead = x[1:] + [pltpu.roll(x[0], 7, axis=0)]
                x = [scaled[v] + lower[v] * beneath[v] + upper[v] * overhead[v] for v in range(8)]
            keep = lane + blk * LANES < live
            for v in range(8):
                natural[i, pl.ds(v, 8, stride=PITCH), :] = jnp.where(keep, x[v], 0.0)
            width = min(LANES, COL_CAP - blk * LANES)
            for g in range(8):
                state[s, g * 8 : g * 8 + 8, blk * LANES : blk * LANES + width] = natural[
                    i, g * PITCH : g * PITCH + 8, :width
                ]
            for h in range(4):
                weight = weight_ref[blk, 8 * h : 8 * h + 8, :]
                paired = weight * x[2 * h] + (1.0 - weight) * x[2 * h + 1]
                pairs[i, pl.ds(h, 8, stride=4), :] = paired
            wide[i] = jnp.concatenate([pairs[i]] * 4, axis=0).T
            item = wide[i, pl.ds(0, 32, stride=TUBE_COLS), :]
            for c in range(1, TUBE_COLS):
                item = jnp.where(quarter == c, wide[i, pl.ds(c, 32, stride=TUBE_COLS), :], item)
            tubes[pl.ds(blk * 256 + s, 32, stride=8), :] = item
        leave(s).start()

    tubes[ZERO_TUBE * 8 :, :] = jnp.zeros((8, LANES), f32)
    sub = lax.broadcasted_iota(jnp.int32, (8, LANES), 0)

    def send(quarter):
        rows = pl.ds(quarter * PEERS // 4 * ITEM_ROWS, PEERS // 4 * ITEM_ROWS)
        return pltpu.make_async_copy(items_ref.at[rows, :], items_hbm.at[rows, :], item_sems.at[quarter])

    for part in range(4):

        @pl.loop(part * PEERS // 16, (part + 1) * PEERS // 16)
        def _(step):
            for i in range(4):
                d = step * 4 + i
                tiles = [
                    tubes[pl.ds(pl.multiple_of(table_ref[d * PEER_SLOTS + r] * 8, 8), 8), :]
                    for r in range(PEER_SLOTS)
                ]
                mid = pltpu.roll(tiles[1], 5, axis=0)
                top = pltpu.roll(tiles[2], 2, axis=0)
                row = pl.multiple_of(d * ITEM_ROWS, ITEM_ROWS)
                items_ref[pl.ds(row, 8), :] = jnp.where(sub < 5, tiles[0], mid)
                items_ref[pl.ds(row + 8, 8), :] = jnp.where(sub < 2, mid, jnp.where(sub < 7, top, 0.0))

        send(part).start()

    for part in range(4):
        send(part).wait()
    for s in range(SPECIES):
        leave(s).wait()


def solve(units, table, got, coefs, weights, north):
    return call(
        solve_kernel,
        (sds((1, 1, SPECIES, NLEV, COL_CAP)), sds((PEERS * ITEM_ROWS, LANES))),
        [SMEM, SMEM] + [HELD] * 4,
        (HBM, HBM),
        [
            pltpu.VMEM((2, 8 * LEVEL_PITCH, LANES), f32),
            pltpu.VMEM((3, 8 * PITCH, LANES), f32),
            pltpu.VMEM((3, PAIRS, LANES), f32),
            pltpu.VMEM((3, LANES, LANES), f32),
            pltpu.VMEM((ZERO_TUBE * 8 + 8, LANES), f32),
            pltpu.VMEM((SPECIES, NLEV, COL_CAP), f32),
            pltpu.VMEM((PEERS * ITEM_ROWS, LANES), f32),
            pltpu.SemaphoreType.DMA((SPECIES,)),
            pltpu.SemaphoreType.DMA((4,)),
        ],
        flops=40_000_000,
    )(units, table, got, coefs, weights, north)


def halves(x):
    high = x.astype(jnp.bfloat16)
    return high, (x - high.astype(f32)).astype(jnp.bfloat16)


def product(x, high, low):
    x_high, x_low = halves(x)
    dot = functools.partial(jnp.dot, preferred_element_type=f32)
    return dot(x_high, high) + (dot(x_low, high) + dot(x_high, low))


def lines_kernel(
    items_ref, yield_ref, rates_ref, waves_ref, fwd_high, fwd_low, inv_high, inv_low, out_hbm,
    spec_in, spec, mixed, done, sems,
):
    tubes = 32 * PEER_SLOTS
    for b in range(4):
        for s in range(SPECIES):
            for r in range(PEER_SLOTS):
                rows = items_ref[pl.ds(b * 32 * ITEM_ROWS + r * SPECIES + s, 32, stride=ITEM_ROWS), :]
                spec_in[b, pl.ds(s * tubes + r, 32, stride=PEER_SLOTS), :] = rows

    half = SPECIES * tubes // 2
    for step in range(2):
        row = step * half
        x = jnp.concatenate([spec_in[b, pl.ds(row, half), :] for b in range(4)], axis=1)
        spec[pl.ds(row, half), :] = product(x, fwd_high[...], fwd_low[...])

    waves = waves_ref[...]
    for i in range(IONS):
        keep = (1.0 - rates_ref[IONS + i]) + rates_ref[i] * waves
        gain = jnp.ones_like(waves)
        for _ in range(SECTIONS - 1):
            gain = gain * keep + 1.0
        total = (yield_ref[i * SPECIES] * gain) * spec[:tubes, :]
        for s in range(1, SPECIES):
            total = total + (yield_ref[i * SPECIES + s] * gain) * spec[s * tubes : (s + 1) * tubes, :]
        mixed[i] = total

    def leave(i):
        return pltpu.make_async_copy(done.at[i], out_hbm.at[0, i], sems.at[i])

    for i in range(0, IONS, 2):
        j = min(i + 2, IONS)
        back = product(mixed[i:j].reshape((j - i) * tubes, LINE_PTS), inv_high[...], inv_low[...])
        done[i:j] = back.reshape(j - i, tubes, LINE_PTS)
        for k in range(i, j):
            leave(k).start()

    for i in range(IONS):
        leave(i).wait()


def cosine_basis():
    k = np.arange(LINE_PTS)[:, None]
    n = np.arange(LINE_PTS)[None, :]
    basis = np.cos(np.pi * k * (n + 0.5) / LINE_PTS) * np.sqrt(2.0 / LINE_PTS)
    basis[0] *= np.sqrt(0.5)
    waves = 2.0 * np.cos(np.pi * np.arange(LINE_PTS) / LINE_PTS) - 2.0
    return basis, waves


def lines(items, ion_yield, ion_spread, ion_loss):
    basis, waves = cosine_basis()

    def parts(matrix):
        matrix = matrix.astype(np.float32)
        high = matrix.astype(jnp.bfloat16)
        low = (matrix - high.astype(np.float32)).astype(jnp.bfloat16)
        return jnp.asarray(high), jnp.asarray(low)

    waves = jnp.asarray(waves.astype(np.float32))[None]
    tubes = 32 * PEER_SLOTS
    by_ion = call(
        lines_kernel,
        sds((1, IONS, tubes, LINE_PTS)),
        [HELD, SMEM, SMEM] + [HELD] * 5,
        HBM,
        [
            pltpu.VMEM((4, SPECIES * tubes, LANES), f32),
            pltpu.VMEM((SPECIES * tubes, LINE_PTS), f32),
            pltpu.VMEM((IONS, tubes, LINE_PTS), f32),
            pltpu.VMEM((IONS, tubes, LINE_PTS), f32),
            pltpu.SemaphoreType.DMA((IONS,)),
        ],
        flops=2_000_000_000,
    )(items, ion_yield.reshape(-1), jnp.concatenate([ion_spread, ion_loss]), waves, *parts(basis.T), *parts(basis))
    return jnp.swapaxes(by_ion, 1, 2)


def swap(x, axis, offset):
    count = lax.axis_size(axis)
    lows = range(offset, count - 1, 2)
    return lax.ppermute(x, axis, [(i, i + 1) for i in lows] + [(i + 1, i) for i in lows])


def exchange(inner, outer, row, far_row):
    outer = swap(outer, "lev", 1)
    row = swap(row, "band", 0)
    far_row = swap(far_row, "band", 1)
    inner = swap(inner, "lev", 0)
    return inner, outer, row, far_row


def on_device(
    neutrals,
    wind_lon,
    wind_lat,
    wind_lev,
    eddy_coupling,
    pair_weight,
    ion_yield,
    ion_spread,
    ion_loss,
    column_order,
    column_units,
    tube_owner,
):
    lev = lax.axis_index("lev")

    neutrals, *rest = edges(neutrals, wind_lon, wind_lat, wind_lev)
    winds, first_halo = rest[:3], exchange(*rest[3:])

    places, starts = list_places(column_units, column_order)
    order = column_order[0]
    own_units = column_units[lev].reshape(1)
    padded = jnp.pad(order, (0, SLOTS_PAD))
    own = lax.dynamic_slice(padded, (TUBE_COLS * starts[lev],), (SLOTS_PAD,))
    own_lat = jnp.zeros_like(own)
    for i in range(1, BAND_LATS):
        own_lat = own_lat + (own >= i * NLON).astype(jnp.int32)
    own_north = (own_lat >= BAND_LATS // 2).astype(jnp.int32).reshape(SLOT_BLOCKS, LANES)
    own_lon = own - own_lat * NLON
    own_rows = (own_lat * 6 + own_lon // 512) * LANES + own_lon % LANES
    own_sel = ((own_lon // LANES) % 4).reshape(SLOT_BLOCKS, LANES)
    zero = jnp.zeros((SPECIES, 1), f32)
    lower = jnp.concatenate([zero, eddy_coupling[:, 1:]], 1)
    upper = jnp.concatenate([eddy_coupling[:, 1:], zero], 1)
    inv = 1.0 / (1.0 + lower + upper)
    coefs = jnp.stack([lower * inv, upper * inv, inv]).reshape(3, SPECIES, 8, 8)
    table, own_weights, coefs = prepare(
        own_units,
        tube_owner[lev, :, 0],
        own_rows,
        own_sel,
        pair_weight.reshape(PAIRS * BAND_LATS, NLON),
        jnp.swapaxes(coefs, 2, 3).reshape(-1, 1),
    )

    inside = interior(neutrals, winds, (places,))
    density, *halo = faces(neutrals, inside, winds, first_halo, first_halo, False)
    inside = interior(density, winds)
    (mine,) = faces(density, inside, winds, exchange(*halo), first_halo, True)
    owners = lax.axis_size("lev")
    other = swap(mine, "lev", 0)
    columns = own_table(mine)

    parity = [[2 * i + c for i in range(owners // 2)] for c in range(2)]
    outgoing = pack(starts, column_units, places, other, columns)
    got = lax.all_to_all(
        outgoing.reshape(16, PEER_ROWS, LANES), "lev", 0, 0, axis_index_groups=parity, tiled=True
    ).reshape(16 * PEER_ROWS, LANES)
    column_state, items = solve(own_units, table, got, coefs, own_weights, own_north)

    items = lax.all_to_all(
        items.reshape(PEERS, ITEM_ROWS, LANES), ("band", "lev"), 0, 0, tiled=True
    ).reshape(PEERS * ITEM_ROWS, LANES)
    return column_state, lines(items, ion_yield, ion_spread, ion_loss)


def solution(mesh):
    placed = (
        P(None, "lev", "band", None),
        P("lev", "band", None),
        P("lev", "band", None),
        P("lev", "band", None),
        P(),
        P(None, "band", None),
        P(),
        P(),
        P(),
        P("band", None),
        P(),
        P(),
    )

    return jax.shard_map(
        on_device,
        mesh=mesh,
        in_specs=placed,
        out_specs=(P("band", "lev", None, None, None), P(("band", "lev"), None, None, None)),
        check_vma=False,
    )
```

```python
import functools

import jax
import jax.numpy as jnp
import numpy as np
from jax import lax
from jax.experimental import pallas as pl
from jax.experimental.pallas import tpu as pltpu
from jax.sharding import PartitionSpec as P


SPECIES = 5
IONS = 7
NLON = 2880
NLEV = 64
PAIRS = 32
BAND_LATS = 8
SWEEPS = 8
SECTIONS = 20
TUBE_COLS = 4
PEERS = 128
PEER_SLOTS = 3
COL_CAP = 1080
BAND_COLS = BAND_LATS * NLON
LINE_PTS = 512

LANES = 128
LON_BLOCKS = 23
LON_PAD = LON_BLOCKS * LANES
PITCH = 9
LEVEL_PITCH = 257
PLANES = 12
GROUPS = 6
PIECE = 64
PEER_ROWS = 3 * PIECE
SLOT_BLOCKS = 9
SLOTS_PAD = SLOT_BLOCKS * LANES
ORDER_PAD = BAND_COLS + 4 * LANES
UNROLL = 64
ZERO_TUBE = SLOT_BLOCKS * 32
ITEM_ROWS = 16

f32 = jnp.float32
VMEM = pl.BlockSpec(memory_space=pltpu.VMEM)
HELD = pl.BlockSpec(memory_space=pltpu.VMEM)
SMEM = pl.BlockSpec(memory_space=pltpu.SMEM)
HBM = pl.BlockSpec(memory_space=pltpu.HBM)
ANY = pl.BlockSpec(memory_space=pl.ANY)


def on_chip(shape, dtype=f32):
    return pltpu.VMEM(shape, dtype)


def call(kernel, out_shape, in_specs, out_specs, scratch=(), flops=0, vmem=16, aliases=()):
    run = pl.pallas_call(
        kernel,
        out_shape=out_shape,
        in_specs=in_specs,
        out_specs=out_specs,
        scratch_shapes=list(scratch),
        input_output_aliases=dict(aliases),
        cost_estimate=pl.CostEstimate(flops=flops, bytes_accessed=1 << 20, transcendentals=0),
        compiler_params=pltpu.CompilerParams(vmem_limit_bytes=vmem * 1024 * 1024),
    )

    def place(x, spec):
        space = pltpu.VMEM if spec is HELD else pltpu.HBM if spec is HBM else None
        return x if space is None else pltpu.with_memory_space_constraint(x, space)

    def placed(*args):
        return run(*(place(x, spec) for x, spec in zip(args, in_specs)))

    return placed


def sds(shape, dtype=f32):
    return jax.ShapeDtypeStruct(shape, dtype)


def upwind(courant, upstream, downstream):
    return courant * jnp.where(courant > 0.0, upstream, downstream)


def own_core():
    return lax.rem(lax.axis_index("lev"), 2)


def in_odd_band():
    return lax.rem(lax.axis_index("band"), 2) == 1


def edges_kernel(
    n_hbm, wlon_hbm, wlat_hbm, wlev_hbm,
    n_ref, wlon_ref, wlat_ref, wlev_ref, inner_ref, outer_ref, row_ref, far_row_ref, sems,
):
    fetches = [
        pltpu.make_async_copy(n_hbm.at[s], n_ref.at[s], sems.at[s]) for s in range(SPECIES)
    ]
    fetches.append(pltpu.make_async_copy(wlat_hbm, wlat_ref, sems.at[SPECIES]))
    fetches.append(pltpu.make_async_copy(wlev_hbm, wlev_ref, sems.at[SPECIES + 1]))
    fetches.append(pltpu.make_async_copy(wlon_hbm, wlon_ref, sems.at[SPECIES + 2]))
    for fetch in fetches:
        fetch.start()
    for fetch in fetches[:-1]:
        fetch.wait()
    core, odd = own_core(), in_odd_band()
    inner_ref[SPECIES] = wlev_ref[0]
    outer_ref[SPECIES] = wlev_ref[0]
    for j in range(2):
        row_ref[SPECIES, j] = wlat_ref[j, :1]
        far_row_ref[SPECIES, j] = wlat_ref[j, :1]

    @pl.loop(0, SPECIES)
    def _(s):
        inner_ref[s] = n_ref[s, 1 - core]
        outer_ref[s] = n_ref[s, core]
        for j in range(2):
            first, last = n_ref[s, j, :1], n_ref[s, j, BAND_LATS - 1 :]
            row_ref[s, j] = jnp.where(odd, first, last)
            far_row_ref[s, j] = jnp.where(odd, last, first)

    fetches[-1].wait()


def edges(density, wind_lon, wind_lat, wind_lev):
    return call(
        edges_kernel,
        (
            on_chip(density.shape),
            on_chip(wind_lon.shape),
            on_chip(wind_lat.shape),
            on_chip(wind_lev.shape),
            on_chip((SPECIES + 1, BAND_LATS, NLON)),
            on_chip((SPECIES + 1, BAND_LATS, NLON)),
            on_chip((SPECIES + 1, 2, 1, NLON)),
            on_chip((SPECIES + 1, 2, 1, NLON)),
        ),
        [HBM] * 4,
        (VMEM,) * 8,
        [pltpu.SemaphoreType.DMA((SPECIES + 3,))],
        flops=1_000_000,
    )(density, wind_lon, wind_lat, wind_lev)


def interior_kernel(n_ref, wlon_ref, wlat_ref, wlev_ref, *refs):
    out_ref = refs[-1]
    row = lax.broadcasted_iota(jnp.int32, (BAND_LATS, NLON), 0)

    @pl.loop(0, SPECIES)
    def _(s):
        for j in range(2):
            x = n_ref[s, j]
            west = jnp.concatenate([x[:, NLON - 1 :], x[:, : NLON - 1]], axis=1)
            flux = upwind(wlon_ref[j], west, x)
            total = x + (flux - jnp.concatenate([flux[:, 1:], flux[:, :1]], axis=1))
            flux = upwind(wlat_ref[j], pltpu.roll(x, 1, axis=0), x)
            flux = jnp.where(row == 0, 0.0, flux)
            total = total + (flux - pltpu.roll(flux, BAND_LATS - 1, axis=0))
            flux = upwind(wlev_ref[1], n_ref[s, 0], n_ref[s, 1])
            out_ref[s, j] = total + flux if j else total - flux


def interior(density, winds, ready=()):
    return call(
        interior_kernel,
        on_chip((SPECIES, 2, BAND_LATS, NLON)),
        [HELD] * (4 + len(ready)),
        VMEM,
        flops=8_000_000,
    )(density, *winds, *ready)


def faces_kernel(n_ref, inside_ref, wlat_ref, wlev_ref, *refs, last):
    inner_ref, outer_ref, row_ref, far_row_ref = refs[:4]
    inner_wind, outer_wind, row_wind, far_row_wind = refs[4:8]
    outs = refs[8:]
    odd = in_odd_band()
    row = lax.broadcasted_iota(jnp.int32, (BAND_LATS, NLON), 0)

    def advance(core):
        below_ref, above_ref, above_wind = (
            (outer_ref, inner_ref, inner_wind) if core == 0 else (inner_ref, outer_ref, outer_wind)
        )

        @pl.loop(0, SPECIES)
        def _(s):
            for j in range(2):
                x = n_ref[s, j]
                total = inside_ref[s, j]
                south = jnp.where(odd, row_ref[s, j], far_row_ref[s, j])
                north = jnp.where(odd, far_row_ref[s, j], row_ref[s, j])
                north_wind = jnp.where(odd, far_row_wind[SPECIES, j], row_wind[SPECIES, j])
                into = upwind(wlat_ref[j, :1], south, x[:1])
                out_of = upwind(north_wind, x[BAND_LATS - 1 :], north)
                total = total + jnp.where(row == 0, into, 0.0) - jnp.where(row == BAND_LATS - 1, out_of, 0.0)
                if j == 0:
                    total = total + upwind(wlev_ref[0], below_ref[s], x)
                else:
                    total = total - upwind(above_wind[SPECIES], x, above_ref[s])
                if last:
                    start = pl.multiple_of((j * SPECIES + s) * BAND_LATS, BAND_LATS)
                    for blk in range(LON_BLOCKS):
                        wide = min(LANES, NLON - blk * LANES)
                        outs[0][blk, pl.ds(start, BAND_LATS), :wide] = total[:, blk * LANES : blk * LANES + wide]
                    continue
                outs[0][s, j] = total
                outs[2 if j == core else 1][s] = total
                first, final = total[:1], total[BAND_LATS - 1 :]
                outs[3][s, j] = jnp.where(odd, first, final)
                outs[4][s, j] = jnp.where(odd, final, first)

    for core in range(2):
        pl.when(own_core() == core)(functools.partial(advance, core))


def faces(density, inside, winds, halo, wind_halo, last):
    if last:
        out_shape = (on_chip((LON_BLOCKS, 2 * SPECIES * BAND_LATS, LANES)),)
    else:
        out_shape = (
            on_chip((SPECIES, 2, BAND_LATS, NLON)),
            on_chip((SPECIES, BAND_LATS, NLON)),
            on_chip((SPECIES, BAND_LATS, NLON)),
            on_chip((SPECIES, 2, 1, NLON)),
            on_chip((SPECIES, 2, 1, NLON)),
        )
    return call(
        functools.partial(faces_kernel, last=last),
        out_shape,
        [HELD] * 12,
        (VMEM,) * len(out_shape),
        flops=2_000_000,
    )(density, inside, *winds[1:], *halo, *wind_halo)


def places_kernel(units_ref, order_ref, place_ref, starts_ref):
    def advance(owner, start):
        starts_ref[owner] = start
        return start + units_ref[owner]

    lax.fori_loop(0, units_ref.shape[0], advance, jnp.int32(0))
    order = order_ref[...]
    lat = jnp.zeros_like(order)
    for i in range(1, BAND_LATS):
        lat = lat + (order >= i * NLON).astype(jnp.int32)
    place_ref[:, :BAND_COLS] = order + lat * (LON_PAD - NLON)
    place_ref[:, BAND_COLS:] = jnp.zeros((1, ORDER_PAD - BAND_COLS), jnp.int32)


def list_places(units, order):
    places, starts = call(
        places_kernel,
        (on_chip((1, ORDER_PAD), jnp.int32), sds(units.shape, jnp.int32)),
        [SMEM, VMEM],
        (VMEM, SMEM),
        flops=1_000_000,
    )(units, order)
    return places.reshape(-1), starts


def prepare_kernel(
    units_ref, owner_ref, rows_ref, sel_ref, weight_ref, column_ref,
    table_ref, own_ref, coef_ref, count, blocks, table, picked,
):
    @pl.loop(0, PEERS * PEER_SLOTS // 8)
    def _(i):
        for k in range(8):
            table_ref[i * 8 + k] = ZERO_TUBE

    @pl.loop(0, PEERS // 8)
    def _(i):
        for k in range(8):
            count[i * 8 + k] = 0

    @pl.loop(0, units_ref[0])
    def _(u):
        dest = owner_ref[u]
        rank = count[dest]
        count[dest] = rank + 1
        table_ref[dest * PEER_SLOTS + rank] = u

    coef_ref[...] = jnp.broadcast_to(column_ref[...], coef_ref.shape)

    for blk in range(LON_BLOCKS):
        wide = min(LANES, NLON - blk * LANES)
        blocks[blk, :, :wide] = weight_ref[:, blk * LANES : blk * LANES + wide]

    @pl.loop(0, BAND_LATS)
    def _(lat):
        for g in range(6):
            parts = [
                blocks[min(4 * g + i, LON_BLOCKS - 1), pl.ds(lat + h * BAND_LATS, 8, stride=4 * BAND_LATS), :]
                for i in range(4)
                for h in range(4)
            ]
            start = pl.multiple_of((lat * 6 + g) * LANES, LANES)
            table[pl.ds(start, LANES), :] = jnp.concatenate(parts, axis=0).T

    @pl.loop(0, SLOTS_PAD // UNROLL)
    def _(step):
        base = pl.multiple_of(step * UNROLL, UNROLL)
        places = rows_ref.at[pl.ds(base, UNROLL)]
        for i in range(UNROLL):
            picked[pl.ds(base + i, 1), :] = table[pl.ds(places[i], 1), :]

    for blk in range(SLOT_BLOCKS):
        turned = picked[blk * LANES : (blk + 1) * LANES, :].T
        which = sel_ref[blk : blk + 1, :]
        kept = turned[:PAIRS]
        for i in range(1, 4):
            kept = jnp.where(which == i, turned[i * PAIRS : (i + 1) * PAIRS], kept)
        own_ref[blk] = kept


def prepare(units, owners, rows, sel, weights, column):
    return call(
        prepare_kernel,
        (
            sds((PEERS * PEER_SLOTS,), jnp.int32),
            on_chip((SLOT_BLOCKS, PAIRS, LANES)),
            on_chip((3 * SPECIES * NLEV, LANES)),
        ),
        [SMEM, SMEM, SMEM, VMEM, VMEM, VMEM],
        (SMEM, VMEM, VMEM),
        [
            pltpu.SMEM((PEERS,), jnp.int32),
            pltpu.VMEM((LON_BLOCKS, PAIRS * BAND_LATS, LANES), f32),
            pltpu.VMEM((BAND_LATS * 6 * LANES, LANES), f32),
            pltpu.VMEM((SLOTS_PAD, LANES), f32),
        ],
        flops=20_000_000,
    )(units, owners, rows, sel, weights, column)


def fill_planes(planes, source_ref):
    @pl.loop(0, LON_BLOCKS)
    def _(blk):
        for j in range(2):
            for i in range(PLANES):
                from_row = (j * SPECIES + i % SPECIES) * BAND_LATS
                planes[blk, pl.ds((j * PLANES + i) * PITCH, BAND_LATS), :] = source_ref[
                    blk, from_row : from_row + BAND_LATS, :
                ]


def fill_table(planes, table_ref, lats):
    half = LANES // 2

    @pl.loop(0, LON_BLOCKS)
    def _(blk):
        for a in range(BAND_LATS // 2):
            parts = [
                planes[blk, pl.ds((j * PLANES + first) * PITCH + lat, 8, stride=PITCH), :]
                for lat in lats(a)
                for j in range(2)
                for first in (0, 3, 1, 4)
            ]
            rows = jnp.concatenate(parts, axis=0).T
            for side, lat in enumerate(lats(a)):
                start = pl.multiple_of((lat * LON_BLOCKS + blk) * LANES, LANES)
                lanes = slice(side * half, (side + 1) * half)
                table_ref[pl.ds(start, LANES), lanes] = rows[:, lanes]


def own_table_kernel(mine_ref, table_ref, planes):
    fill_planes(planes, mine_ref)
    fill_table(planes, table_ref, lambda a: (a, a + BAND_LATS // 2))


def own_table(mine):
    return call(
        own_table_kernel,
        on_chip((BAND_LATS * LON_PAD, LANES)),
        [HELD],
        VMEM,
        [pltpu.VMEM((LON_BLOCKS, 2 * PLANES * PITCH, LANES), f32)],
        flops=8_000_000,
    )(mine)


def pack_kernel(
    starts_any, units_any, list_ref, other_ref, _,
    out_hbm, table_ref, starts_ref, units_ref, order_ref, planes, msg_ref, sems, fetch_sems,
):
    fetches = [
        pltpu.make_async_copy(source, target, fetch_sems.at[i])
        for i, (source, target) in enumerate(
            ((starts_any, starts_ref), (units_any, units_ref), (list_ref, order_ref))
        )
    ]
    for fetch in fetches:
        fetch.start()
    core = own_core()
    fill_planes(planes, other_ref)
    fill_table(planes, table_ref, lambda a: (a + BAND_LATS // 2, a))

    lane = lax.broadcasted_iota(jnp.int32, (1, LANES), 1)
    group_of = lax.div(lax.rem(lane, 32), SPECIES)

    def send(peer):
        rows = pl.ds(pl.multiple_of(peer * PEER_ROWS, PEER_ROWS), PEER_ROWS)
        return pltpu.make_async_copy(msg_ref.at[rows, :], out_hbm.at[rows, :], sems.at[peer])

    for fetch in fetches:
        fetch.wait()

    @pl.loop(0, 16)
    def _(peer):
        owner = 2 * peer + core
        first = TUBE_COLS * starts_ref[owner]
        pieces = lax.div(TUBE_COLS * units_ref[owner] + (PIECE - 1), PIECE)

        def copy(start, number):
            places = []
            for k in range(number):
                piece = start + k
                tail = piece >= 2 * GROUPS
                group = jnp.where(tail, piece - 2 * GROUPS, lax.div(piece, 2))
                row = peer * PEER_ROWS + jnp.where(tail, 2 * PIECE, PIECE * lax.rem(piece, 2))
                places.append((pl.multiple_of(row, PIECE), group_of == group))
            base = first + start * PIECE
            for i in range(number * PIECE):
                place = order_ref.at[pl.ds(i, ORDER_PAD - 2 * PIECE)][base]
                row, mask = places[i // PIECE]
                value = table_ref[pl.ds(place, 1), :]
                pltpu.store(msg_ref.at[pl.ds(row + i % PIECE, 1), :], value, mask=mask)

        @pl.loop(0, lax.div(pieces, 2))
        def _(pair):
            copy(2 * pair, 2)

        pl.when(lax.rem(pieces, 2) == 1)(functools.partial(copy, pieces - 1, 1))
        send(peer).start()

    @pl.loop(0, 16)
    def _(peer):
        send(peer).wait()


def pack(starts, units, order, other, table):
    outgoing, _ = call(
        pack_kernel,
        (sds((16 * PEER_ROWS, LANES)), on_chip((BAND_LATS * LON_PAD, LANES))),
        [ANY, ANY, HELD, HELD, HELD],
        (HBM, VMEM),
        [
            pltpu.SMEM(starts.shape, jnp.int32),
            pltpu.SMEM(units.shape, jnp.int32),
            pltpu.SMEM((ORDER_PAD,), jnp.int32),
            pltpu.VMEM((LON_BLOCKS, 2 * PLANES * PITCH, LANES), f32),
            pltpu.VMEM((16 * PEER_ROWS, LANES), f32),
            pltpu.SemaphoreType.DMA((16,)),
            pltpu.SemaphoreType.DMA((3,)),
        ],
        flops=30_000_000,
        aliases={4: 1},
    )(starts, units, order, other, table)
    return outgoing


def solve_kernel(
    units_any, table_any, got_ref, coef_ref, weight_ref, north_ref, state_hbm, items_hbm,
    units_ref, table_ref, turned, natural, pairs, wide, tubes, state, items_ref, sems, item_sems, fetch_sems,
):
    fetches = [
        pltpu.make_async_copy(units_any, units_ref, fetch_sems.at[0]),
        pltpu.make_async_copy(table_any, table_ref, fetch_sems.at[1]),
    ]
    for fetch in fetches:
        fetch.start()
    core = own_core()
    lane = lax.broadcasted_iota(jnp.int32, (1, LANES), 1)
    low = lane < 64
    quarter = lax.div(lane, 32)

    @pl.loop(0, 8)
    def _(i):
        for side in range(2):
            out = i * LEVEL_PITCH + side * LANES
            row = pl.multiple_of((2 * i + side) * PEER_ROWS, PIECE)
            tail = got_ref[pl.ds(row + LANES, PIECE), :]
            for part, rows in enumerate((got_ref[pl.ds(row, LANES), :], jnp.concatenate([tail] * 2, axis=0))):
                flipped = rows.T
                turned[part, pl.ds(out + 64 * core, 64), :] = flipped[:64]
                turned[part, pl.ds(out + 64 - 64 * core, 64), :] = flipped[64:]

    for fetch in fetches:
        fetch.wait()
    live = TUBE_COLS * units_ref[0]

    def leave(s):
        return pltpu.make_async_copy(state.at[s], state_hbm.at[0, 0, s], sems.at[s])

    @pl.loop(0, SPECIES)
    def _(s):
        def coefs(which):
            row = pl.multiple_of((which * SPECIES + s) * NLEV, NLEV)
            return [coef_ref[pl.ds(row + 8 * v, 8), :] for v in range(8)]

        lower, upper, inv = coefs(0), coefs(1), coefs(2)
        for blk in range(SLOT_BLOCKS):
            i = blk % 3

            def levels(part, group, v):
                return turned[part, pl.ds(32 * v + group * SPECIES + s, 8, stride=LEVEL_PITCH), :]

            if blk < GROUPS:
                raw = [levels(0, blk, v) for v in range(8)]
            else:
                raw = [jnp.where(low, levels(1, 2 * i, v), levels(1, 2 * i + 1, v)) for v in range(8)]
            north = north_ref[blk : blk + 1, :] == 1
            rhs = [jnp.where(north, raw[v ^ 2], raw[v]) for v in range(8)]
            scaled = [rhs[v] * inv[v] for v in range(8)]
            x = rhs
            for _ in range(SWEEPS):
                beneath = [pltpu.roll(x[7], 1, axis=0)] + x[:7]
                overhead = x[1:] + [pltpu.roll(x[0], 7, axis=0)]
                x = [scaled[v] + lower[v] * beneath[v] + upper[v] * overhead[v] for v in range(8)]
            keep = lane + blk * LANES < live
            for v in range(8):
                natural[i, pl.ds(v, 8, stride=PITCH), :] = jnp.where(keep, x[v], 0.0)
            width = min(LANES, COL_CAP - blk * LANES)
            for g in range(8):
                state[s, g * 8 : g * 8 + 8, blk * LANES : blk * LANES + width] = natural[
                    i, g * PITCH : g * PITCH + 8, :width
                ]
            for h in range(4):
                weight = weight_ref[blk, 8 * h : 8 * h + 8, :]
                paired = weight * x[2 * h] + (1.0 - weight) * x[2 * h + 1]
                pairs[i, pl.ds(h, 8, stride=4), :] = paired
            wide[i] = jnp.concatenate([pairs[i]] * 4, axis=0).T
            item = wide[i, pl.ds(0, 32, stride=TUBE_COLS), :]
            for c in range(1, TUBE_COLS):
                item = jnp.where(quarter == c, wide[i, pl.ds(c, 32, stride=TUBE_COLS), :], item)
            tubes[pl.ds(blk * 256 + s, 32, stride=8), :] = item
        leave(s).start()

    tubes[ZERO_TUBE * 8 :, :] = jnp.zeros((8, LANES), f32)
    sub = lax.broadcasted_iota(jnp.int32, (8, LANES), 0)

    def send(quarter):
        rows = pl.ds(quarter * PEERS // 4 * ITEM_ROWS, PEERS // 4 * ITEM_ROWS)
        return pltpu.make_async_copy(items_ref.at[rows, :], items_hbm.at[rows, :], item_sems.at[quarter])

    for part in range(4):

        @pl.loop(part * PEERS // 16, (part + 1) * PEERS // 16)
        def _(step):
            for i in range(4):
                d = step * 4 + i
                tiles = [
                    tubes[pl.ds(pl.multiple_of(table_ref[d * PEER_SLOTS + r] * 8, 8), 8), :]
                    for r in range(PEER_SLOTS)
                ]
                mid = pltpu.roll(tiles[1], 5, axis=0)
                top = pltpu.roll(tiles[2], 2, axis=0)
                row = pl.multiple_of(d * ITEM_ROWS, ITEM_ROWS)
                items_ref[pl.ds(row, 8), :] = jnp.where(sub < 5, tiles[0], mid)
                items_ref[pl.ds(row + 8, 8), :] = jnp.where(sub < 2, mid, jnp.where(sub < 7, top, 0.0))

        send(part).start()

    for part in range(4):
        send(part).wait()
    for s in range(SPECIES):
        leave(s).wait()


def solve(units, table, got, coefs, weights, north):
    return call(
        solve_kernel,
        (sds((1, 1, SPECIES, NLEV, COL_CAP)), sds((PEERS * ITEM_ROWS, LANES))),
        [ANY, ANY] + [HELD] * 4,
        (HBM, HBM),
        [
            pltpu.SMEM(units.shape, jnp.int32),
            pltpu.SMEM(table.shape, jnp.int32),
            pltpu.VMEM((2, 8 * LEVEL_PITCH, LANES), f32),
            pltpu.VMEM((3, 8 * PITCH, LANES), f32),
            pltpu.VMEM((3, PAIRS, LANES), f32),
            pltpu.VMEM((3, LANES, LANES), f32),
            pltpu.VMEM((ZERO_TUBE * 8 + 8, LANES), f32),
            pltpu.VMEM((SPECIES, NLEV, COL_CAP), f32),
            pltpu.VMEM((PEERS * ITEM_ROWS, LANES), f32),
            pltpu.SemaphoreType.DMA((SPECIES,)),
            pltpu.SemaphoreType.DMA((4,)),
            pltpu.SemaphoreType.DMA((2,)),
        ],
        flops=40_000_000,
    )(units, table, got, coefs, weights, north)


def halves(x):
    high = x.astype(jnp.bfloat16)
    return high, (x - high.astype(f32)).astype(jnp.bfloat16)


def product(x, high, low):
    x_high, x_low = halves(x)
    dot = functools.partial(jnp.dot, preferred_element_type=f32)
    return dot(x_high, high) + (dot(x_low, high) + dot(x_high, low))


def lines_kernel(
    items_ref, yield_any, rates_any, waves_ref, fwd_high, fwd_low, inv_high, inv_low, out_hbm,
    yield_ref, rates_ref, spec_in, spec, mixed, done, sems, fetch_sems,
):
    fetches = [
        pltpu.make_async_copy(yield_any, yield_ref, fetch_sems.at[0]),
        pltpu.make_async_copy(rates_any, rates_ref, fetch_sems.at[1]),
    ]
    for fetch in fetches:
        fetch.start()
    tubes = 32 * PEER_SLOTS
    for b in range(4):
        for s in range(SPECIES):
            for r in range(PEER_SLOTS):
                rows = items_ref[pl.ds(b * 32 * ITEM_ROWS + r * SPECIES + s, 32, stride=ITEM_ROWS), :]
                spec_in[b, pl.ds(s * tubes + r, 32, stride=PEER_SLOTS), :] = rows

    half = SPECIES * tubes // 2
    for step in range(2):
        row = step * half
        x = jnp.concatenate([spec_in[b, pl.ds(row, half), :] for b in range(4)], axis=1)
        spec[pl.ds(row, half), :] = product(x, fwd_high[...], fwd_low[...])

    for fetch in fetches:
        fetch.wait()
    waves = waves_ref[...]
    for i in range(IONS):
        keep = (1.0 - rates_ref[IONS + i]) + rates_ref[i] * waves
        gain = jnp.ones_like(waves)
        for _ in range(SECTIONS - 1):
            gain = gain * keep + 1.0
        total = (yield_ref[i * SPECIES] * gain) * spec[:tubes, :]
        for s in range(1, SPECIES):
            total = total + (yield_ref[i * SPECIES + s] * gain) * spec[s * tubes : (s + 1) * tubes, :]
        mixed[i] = total

    def leave(i):
        return pltpu.make_async_copy(done.at[i], out_hbm.at[0, i], sems.at[i])

    for i in range(0, IONS, 2):
        j = min(i + 2, IONS)
        back = product(mixed[i:j].reshape((j - i) * tubes, LINE_PTS), inv_high[...], inv_low[...])
        done[i:j] = back.reshape(j - i, tubes, LINE_PTS)
        for k in range(i, j):
            leave(k).start()

    for i in range(IONS):
        leave(i).wait()


def cosine_basis():
    k = np.arange(LINE_PTS)[:, None]
    n = np.arange(LINE_PTS)[None, :]
    basis = np.cos(np.pi * k * (n + 0.5) / LINE_PTS) * np.sqrt(2.0 / LINE_PTS)
    basis[0] *= np.sqrt(0.5)
    waves = 2.0 * np.cos(np.pi * np.arange(LINE_PTS) / LINE_PTS) - 2.0
    return basis, waves


def lines(items, ion_yield, ion_spread, ion_loss):
    basis, waves = cosine_basis()

    def parts(matrix):
        matrix = matrix.astype(np.float32)
        high = matrix.astype(jnp.bfloat16)
        low = (matrix - high.astype(np.float32)).astype(jnp.bfloat16)
        return jnp.asarray(high), jnp.asarray(low)

    waves = jnp.asarray(waves.astype(np.float32))[None]
    tubes = 32 * PEER_SLOTS
    by_ion = call(
        lines_kernel,
        sds((1, IONS, tubes, LINE_PTS)),
        [HELD, ANY, ANY] + [HELD] * 5,
        HBM,
        [
            pltpu.SMEM((IONS * SPECIES,), f32),
            pltpu.SMEM((2 * IONS,), f32),
            pltpu.VMEM((4, SPECIES * tubes, LANES), f32),
            pltpu.VMEM((SPECIES * tubes, LINE_PTS), f32),
            pltpu.VMEM((IONS, tubes, LINE_PTS), f32),
            pltpu.VMEM((IONS, tubes, LINE_PTS), f32),
            pltpu.SemaphoreType.DMA((IONS,)),
            pltpu.SemaphoreType.DMA((2,)),
        ],
        flops=2_000_000_000,
    )(items, ion_yield.reshape(-1), jnp.concatenate([ion_spread, ion_loss]), waves, *parts(basis.T), *parts(basis))
    return jnp.swapaxes(by_ion, 1, 2)


def swap(x, axis, offset):
    count = lax.axis_size(axis)
    lows = range(offset, count - 1, 2)
    return lax.ppermute(x, axis, [(i, i + 1) for i in lows] + [(i + 1, i) for i in lows])


def exchange(inner, outer, row, far_row):
    outer = swap(outer, "lev", 1)
    row = swap(row, "band", 0)
    far_row = swap(far_row, "band", 1)
    inner = swap(inner, "lev", 0)
    return inner, outer, row, far_row


def on_device(
    neutrals,
    wind_lon,
    wind_lat,
    wind_lev,
    eddy_coupling,
    pair_weight,
    ion_yield,
    ion_spread,
    ion_loss,
    column_order,
    column_units,
    tube_owner,
):
    lev = lax.axis_index("lev")

    neutrals, *rest = edges(neutrals, wind_lon, wind_lat, wind_lev)
    winds, first_halo = rest[:3], exchange(*rest[3:])

    places, starts = list_places(column_units, column_order)
    order = column_order[0]
    own_units = column_units[lev].reshape(1)
    padded = jnp.pad(order, (0, SLOTS_PAD))
    own = lax.dynamic_slice(padded, (TUBE_COLS * starts[lev],), (SLOTS_PAD,))
    own_lat = jnp.zeros_like(own)
    for i in range(1, BAND_LATS):
        own_lat = own_lat + (own >= i * NLON).astype(jnp.int32)
    own_north = (own_lat >= BAND_LATS // 2).astype(jnp.int32).reshape(SLOT_BLOCKS, LANES)
    own_lon = own - own_lat * NLON
    own_rows = (own_lat * 6 + own_lon // 512) * LANES + own_lon % LANES
    own_sel = ((own_lon // LANES) % 4).reshape(SLOT_BLOCKS, LANES)
    zero = jnp.zeros((SPECIES, 1), f32)
    lower = jnp.concatenate([zero, eddy_coupling[:, 1:]], 1)
    upper = jnp.concatenate([eddy_coupling[:, 1:], zero], 1)
    inv = 1.0 / (1.0 + lower + upper)
    coefs = jnp.stack([lower * inv, upper * inv, inv]).reshape(3, SPECIES, 8, 8)
    table, own_weights, coefs = prepare(
        own_units,
        tube_owner[lev, :, 0],
        own_rows,
        own_sel,
        pair_weight.reshape(PAIRS * BAND_LATS, NLON),
        jnp.swapaxes(coefs, 2, 3).reshape(-1, 1),
    )

    inside = interior(neutrals, winds, (places,))
    density, *halo = faces(neutrals, inside, winds, first_halo, first_halo, False)
    inside = interior(density, winds)
    (mine,) = faces(density, inside, winds, exchange(*halo), first_halo, True)
    owners = lax.axis_size("lev")
    other = swap(mine, "lev", 0)
    columns = own_table(mine)

    parity = [[2 * i + c for i in range(owners // 2)] for c in range(2)]
    outgoing = pack(starts, column_units, places, other, columns)
    got = lax.all_to_all(
        outgoing.reshape(16, PEER_ROWS, LANES), "lev", 0, 0, axis_index_groups=parity, tiled=True
    ).reshape(16 * PEER_ROWS, LANES)
    column_state, items = solve(own_units, table, got, coefs, own_weights, own_north)

    items = lax.all_to_all(
        items.reshape(PEERS, ITEM_ROWS, LANES), ("band", "lev"), 0, 0, tiled=True
    ).reshape(PEERS * ITEM_ROWS, LANES)
    return column_state, lines(items, ion_yield, ion_spread, ion_loss)


def solution(mesh):
    placed = (
        P(None, "lev", "band", None),
        P("lev", "band", None),
        P("lev", "band", None),
        P("lev", "band", None),
        P(),
        P(None, "band", None),
        P(),
        P(),
        P(),
        P("band", None),
        P(),
        P(),
    )

    return jax.shard_map(
        on_device,
        mesh=mesh,
        in_specs=placed,
        out_specs=(P("band", "lev", None, None, None), P(("band", "lev"), None, None, None)),
        check_vma=False,
    )
```

```python
import functools

import jax
import jax.numpy as jnp
import numpy as np
from jax import lax
from jax.experimental import pallas as pl
from jax.experimental.pallas import tpu as pltpu
from jax.sharding import PartitionSpec as P


SPECIES = 5
IONS = 7
NLON = 2880
NLEV = 64
PAIRS = 32
BAND_LATS = 8
SWEEPS = 8
SECTIONS = 20
TUBE_COLS = 4
PEERS = 128
PEER_SLOTS = 3
COL_CAP = 1080
BAND_COLS = BAND_LATS * NLON
LINE_PTS = 512

LANES = 128
LON_BLOCKS = 23
LON_PAD = LON_BLOCKS * LANES
PITCH = 9
LEVEL_PITCH = 257
PLANES = 12
GROUPS = 6
PIECE = 64
PEER_ROWS = 3 * PIECE
SLOT_BLOCKS = 9
SLOTS_PAD = SLOT_BLOCKS * LANES
ORDER_PAD = BAND_COLS + 4 * LANES
UNROLL = 64
ZERO_TUBE = SLOT_BLOCKS * 32
ITEM_ROWS = 16

f32 = jnp.float32
VMEM = pl.BlockSpec(memory_space=pltpu.VMEM)
HELD = pl.BlockSpec(memory_space=pltpu.VMEM)
SMEM = pl.BlockSpec(memory_space=pltpu.SMEM)
HBM = pl.BlockSpec(memory_space=pltpu.HBM)
ANY = pl.BlockSpec(memory_space=pl.ANY)


def on_chip(shape, dtype=f32):
    return pltpu.VMEM(shape, dtype)


def call(kernel, out_shape, in_specs, out_specs, scratch=(), flops=0, vmem=16, aliases=()):
    run = pl.pallas_call(
        kernel,
        out_shape=out_shape,
        in_specs=in_specs,
        out_specs=out_specs,
        scratch_shapes=list(scratch),
        input_output_aliases=dict(aliases),
        cost_estimate=pl.CostEstimate(flops=flops, bytes_accessed=1 << 20, transcendentals=0),
        compiler_params=pltpu.CompilerParams(vmem_limit_bytes=vmem * 1024 * 1024),
    )

    def place(x, spec):
        space = pltpu.VMEM if spec is HELD else pltpu.HBM if spec is HBM else None
        return x if space is None else pltpu.with_memory_space_constraint(x, space)

    def placed(*args):
        return run(*(place(x, spec) for x, spec in zip(args, in_specs)))

    return placed


def sds(shape, dtype=f32):
    return jax.ShapeDtypeStruct(shape, dtype)


def upwind(courant, upstream, downstream):
    return courant * jnp.where(courant > 0.0, upstream, downstream)


def own_core():
    return lax.rem(lax.axis_index("lev"), 2)


def in_odd_band():
    return lax.rem(lax.axis_index("band"), 2) == 1


def edges_kernel(
    n_hbm, wlon_hbm, wlat_hbm, wlev_hbm,
    n_ref, wlon_ref, wlat_ref, wlev_ref, inner_ref, outer_ref, row_ref, far_row_ref, sems,
):
    fetches = [
        pltpu.make_async_copy(n_hbm.at[s], n_ref.at[s], sems.at[s]) for s in range(SPECIES)
    ]
    fetches.append(pltpu.make_async_copy(wlat_hbm, wlat_ref, sems.at[SPECIES]))
    fetches.append(pltpu.make_async_copy(wlev_hbm, wlev_ref, sems.at[SPECIES + 1]))
    fetches.append(pltpu.make_async_copy(wlon_hbm, wlon_ref, sems.at[SPECIES + 2]))
    for fetch in fetches:
        fetch.start()
    for fetch in fetches[:-1]:
        fetch.wait()
    core, odd = own_core(), in_odd_band()
    inner_ref[SPECIES] = wlev_ref[0]
    outer_ref[SPECIES] = wlev_ref[0]
    for j in range(2):
        row_ref[SPECIES, j] = wlat_ref[j, :1]
        far_row_ref[SPECIES, j] = wlat_ref[j, :1]

    @pl.loop(0, SPECIES)
    def _(s):
        inner_ref[s] = n_ref[s, 1 - core]
        outer_ref[s] = n_ref[s, core]
        for j in range(2):
            first, last = n_ref[s, j, :1], n_ref[s, j, BAND_LATS - 1 :]
            row_ref[s, j] = jnp.where(odd, first, last)
            far_row_ref[s, j] = jnp.where(odd, last, first)

    fetches[-1].wait()


def edges(density, wind_lon, wind_lat, wind_lev):
    return call(
        edges_kernel,
        (
            on_chip(density.shape),
            on_chip(wind_lon.shape),
            on_chip(wind_lat.shape),
            on_chip(wind_lev.shape),
            on_chip((SPECIES + 1, BAND_LATS, NLON)),
            on_chip((SPECIES + 1, BAND_LATS, NLON)),
            on_chip((SPECIES + 1, 2, 1, NLON)),
            on_chip((SPECIES + 1, 2, 1, NLON)),
        ),
        [HBM] * 4,
        (VMEM,) * 8,
        [pltpu.SemaphoreType.DMA((SPECIES + 3,))],
        flops=1_000_000,
    )(density, wind_lon, wind_lat, wind_lev)


def interior_kernel(n_ref, wlon_ref, wlat_ref, wlev_ref, *refs):
    out_ref = refs[-1]
    row = lax.broadcasted_iota(jnp.int32, (BAND_LATS, NLON), 0)

    @pl.loop(0, SPECIES)
    def _(s):
        for j in range(2):
            x = n_ref[s, j]
            west = jnp.concatenate([x[:, NLON - 1 :], x[:, : NLON - 1]], axis=1)
            flux = upwind(wlon_ref[j], west, x)
            total = x + (flux - jnp.concatenate([flux[:, 1:], flux[:, :1]], axis=1))
            flux = upwind(wlat_ref[j], pltpu.roll(x, 1, axis=0), x)
            flux = jnp.where(row == 0, 0.0, flux)
            total = total + (flux - pltpu.roll(flux, BAND_LATS - 1, axis=0))
            flux = upwind(wlev_ref[1], n_ref[s, 0], n_ref[s, 1])
            out_ref[s, j] = total + flux if j else total - flux


def interior(density, winds, ready=()):
    return call(
        interior_kernel,
        on_chip((SPECIES, 2, BAND_LATS, NLON)),
        [HELD] * (4 + len(ready)),
        VMEM,
        flops=8_000_000,
    )(density, *winds, *ready)


def faces_kernel(n_ref, inside_ref, wlat_ref, wlev_ref, *refs, last):
    inner_ref, outer_ref, row_ref, far_row_ref = refs[:4]
    inner_wind, outer_wind, row_wind, far_row_wind = refs[4:8]
    outs = refs[8:]
    odd = in_odd_band()
    row = lax.broadcasted_iota(jnp.int32, (BAND_LATS, NLON), 0)

    def advance(core):
        below_ref, above_ref, above_wind = (
            (outer_ref, inner_ref, inner_wind) if core == 0 else (inner_ref, outer_ref, outer_wind)
        )

        @pl.loop(0, SPECIES)
        def _(s):
            for j in range(2):
                x = n_ref[s, j]
                total = inside_ref[s, j]
                south = jnp.where(odd, row_ref[s, j], far_row_ref[s, j])
                north = jnp.where(odd, far_row_ref[s, j], row_ref[s, j])
                north_wind = jnp.where(odd, far_row_wind[SPECIES, j], row_wind[SPECIES, j])
                into = upwind(wlat_ref[j, :1], south, x[:1])
                out_of = upwind(north_wind, x[BAND_LATS - 1 :], north)
                total = total + jnp.where(row == 0, into, 0.0) - jnp.where(row == BAND_LATS - 1, out_of, 0.0)
                if j == 0:
                    total = total + upwind(wlev_ref[0], below_ref[s], x)
                else:
                    total = total - upwind(above_wind[SPECIES], x, above_ref[s])
                if last:
                    start = pl.multiple_of((j * SPECIES + s) * BAND_LATS, BAND_LATS)
                    for blk in range(LON_BLOCKS):
                        wide = min(LANES, NLON - blk * LANES)
                        outs[0][blk, pl.ds(start, BAND_LATS), :wide] = total[:, blk * LANES : blk * LANES + wide]
                    continue
                outs[0][s, j] = total
                outs[2 if j == core else 1][s] = total
                first, final = total[:1], total[BAND_LATS - 1 :]
                outs[3][s, j] = jnp.where(odd, first, final)
                outs[4][s, j] = jnp.where(odd, final, first)

    for core in range(2):
        pl.when(own_core() == core)(functools.partial(advance, core))


def faces(density, inside, winds, halo, wind_halo, last):
    if last:
        out_shape = (on_chip((LON_BLOCKS, 2 * SPECIES * BAND_LATS, LANES)),)
    else:
        out_shape = (
            on_chip((SPECIES, 2, BAND_LATS, NLON)),
            on_chip((SPECIES, BAND_LATS, NLON)),
            on_chip((SPECIES, BAND_LATS, NLON)),
            on_chip((SPECIES, 2, 1, NLON)),
            on_chip((SPECIES, 2, 1, NLON)),
        )
    return call(
        functools.partial(faces_kernel, last=last),
        out_shape,
        [HELD] * 12,
        (VMEM,) * len(out_shape),
        flops=2_000_000,
    )(density, inside, *winds[1:], *halo, *wind_halo)


def places_kernel(units_any, order_ref, place_ref, starts_ref, units_ref, sem):
    fetch = pltpu.make_async_copy(units_any, units_ref, sem)
    fetch.start()
    order = order_ref[...]
    lat = ((order >> 6) * 1457) >> 16
    place_ref[:, :BAND_COLS] = order + lat * (LON_PAD - NLON)
    place_ref[:, BAND_COLS:] = jnp.zeros((1, ORDER_PAD - BAND_COLS), jnp.int32)
    fetch.wait()

    start = jnp.int32(0)
    for owner in range(units_ref.shape[0]):
        starts_ref[owner] = start
        start = start + units_ref[owner]


def list_places(units, order):
    places, starts = call(
        places_kernel,
        (on_chip((1, ORDER_PAD), jnp.int32), sds(units.shape, jnp.int32)),
        [HBM, VMEM],
        (VMEM, SMEM),
        [pltpu.SMEM(units.shape, jnp.int32), pltpu.SemaphoreType.DMA],
        flops=1_000_000,
    )(units, order)
    return places.reshape(-1), starts


def prepare_kernel(
    units_ref, owner_ref, rows_ref, sel_ref, weight_ref, column_ref,
    table_ref, own_ref, coef_ref, count, blocks, table, picked,
):
    @pl.loop(0, PEERS * PEER_SLOTS // 8)
    def _(i):
        for k in range(8):
            table_ref[i * 8 + k] = ZERO_TUBE

    @pl.loop(0, PEERS // 8)
    def _(i):
        for k in range(8):
            count[i * 8 + k] = 0

    @pl.loop(0, units_ref[0])
    def _(u):
        dest = owner_ref[u]
        rank = count[dest]
        count[dest] = rank + 1
        table_ref[dest * PEER_SLOTS + rank] = u

    coef_ref[...] = jnp.broadcast_to(column_ref[...], coef_ref.shape)

    for blk in range(LON_BLOCKS):
        wide = min(LANES, NLON - blk * LANES)
        blocks[blk, :, :wide] = weight_ref[:, blk * LANES : blk * LANES + wide]

    @pl.loop(0, BAND_LATS)
    def _(lat):
        for g in range(6):
            parts = [
                blocks[min(4 * g + i, LON_BLOCKS - 1), pl.ds(lat + h * BAND_LATS, 8, stride=4 * BAND_LATS), :]
                for i in range(4)
                for h in range(4)
            ]
            start = pl.multiple_of((lat * 6 + g) * LANES, LANES)
            table[pl.ds(start, LANES), :] = jnp.concatenate(parts, axis=0).T

    @pl.loop(0, SLOTS_PAD // UNROLL)
    def _(step):
        base = pl.multiple_of(step * UNROLL, UNROLL)
        places = rows_ref.at[pl.ds(base, UNROLL)]
        for i in range(UNROLL):
            picked[pl.ds(base + i, 1), :] = table[pl.ds(places[i], 1), :]

    for blk in range(SLOT_BLOCKS):
        turned = picked[blk * LANES : (blk + 1) * LANES, :].T
        which = sel_ref[blk : blk + 1, :]
        kept = turned[:PAIRS]
        for i in range(1, 4):
            kept = jnp.where(which == i, turned[i * PAIRS : (i + 1) * PAIRS], kept)
        own_ref[blk] = kept


def prepare(units, owners, rows, sel, weights, column):
    return call(
        prepare_kernel,
        (
            sds((PEERS * PEER_SLOTS,), jnp.int32),
            on_chip((SLOT_BLOCKS, PAIRS, LANES)),
            on_chip((3 * SPECIES * NLEV, LANES)),
        ),
        [SMEM, SMEM, SMEM, VMEM, VMEM, VMEM],
        (SMEM, VMEM, VMEM),
        [
            pltpu.SMEM((PEERS,), jnp.int32),
            pltpu.VMEM((LON_BLOCKS, PAIRS * BAND_LATS, LANES), f32),
            pltpu.VMEM((BAND_LATS * 6 * LANES, LANES), f32),
            pltpu.VMEM((SLOTS_PAD, LANES), f32),
        ],
        flops=20_000_000,
    )(units, owners, rows, sel, weights, column)


def fill_planes(planes, source_ref):
    @pl.loop(0, LON_BLOCKS)
    def _(blk):
        for j in range(2):
            for i in range(PLANES):
                from_row = (j * SPECIES + i % SPECIES) * BAND_LATS
                planes[blk, pl.ds((j * PLANES + i) * PITCH, BAND_LATS), :] = source_ref[
                    blk, from_row : from_row + BAND_LATS, :
                ]


def fill_table(planes, table_ref, lats):
    half = LANES // 2

    @pl.loop(0, LON_BLOCKS)
    def _(blk):
        for a in range(BAND_LATS // 2):
            parts = [
                planes[blk, pl.ds((j * PLANES + first) * PITCH + lat, 8, stride=PITCH), :]
                for lat in lats(a)
                for j in range(2)
                for first in (0, 3, 1, 4)
            ]
            rows = jnp.concatenate(parts, axis=0).T
            for side, lat in enumerate(lats(a)):
                start = pl.multiple_of((lat * LON_BLOCKS + blk) * LANES, LANES)
                lanes = slice(side * half, (side + 1) * half)
                table_ref[pl.ds(start, LANES), lanes] = rows[:, lanes]


def own_table_kernel(mine_ref, table_ref, planes):
    fill_planes(planes, mine_ref)
    fill_table(planes, table_ref, lambda a: (a, a + BAND_LATS // 2))


def own_table(mine):
    return call(
        own_table_kernel,
        on_chip((BAND_LATS * LON_PAD, LANES)),
        [HELD],
        VMEM,
        [pltpu.VMEM((LON_BLOCKS, 2 * PLANES * PITCH, LANES), f32)],
        flops=8_000_000,
    )(mine)


def pack_kernel(
    starts_any, units_any, list_ref, other_ref, _,
    out_hbm, table_ref, starts_ref, units_ref, order_ref, planes, msg_ref, sems, fetch_sems,
):
    fetches = [
        pltpu.make_async_copy(source, target, fetch_sems.at[i])
        for i, (source, target) in enumerate(
            ((starts_any, starts_ref), (units_any, units_ref), (list_ref, order_ref))
        )
    ]
    for fetch in fetches:
        fetch.start()
    core = own_core()
    fill_planes(planes, other_ref)
    fill_table(planes, table_ref, lambda a: (a + BAND_LATS // 2, a))

    lane = lax.broadcasted_iota(jnp.int32, (1, LANES), 1)
    group_of = lax.div(lax.rem(lane, 32), SPECIES)

    def send(peer):
        rows = pl.ds(pl.multiple_of(peer * PEER_ROWS, PEER_ROWS), PEER_ROWS)
        return pltpu.make_async_copy(msg_ref.at[rows, :], out_hbm.at[rows, :], sems.at[peer])

    for fetch in fetches:
        fetch.wait()

    @pl.loop(0, 16)
    def _(peer):
        owner = 2 * peer + core
        first = TUBE_COLS * starts_ref[owner]
        pieces = lax.div(TUBE_COLS * units_ref[owner] + (PIECE - 1), PIECE)

        def copy(start, number):
            places = []
            for k in range(number):
                piece = start + k
                tail = piece >= 2 * GROUPS
                group = jnp.where(tail, piece - 2 * GROUPS, lax.div(piece, 2))
                row = peer * PEER_ROWS + jnp.where(tail, 2 * PIECE, PIECE * lax.rem(piece, 2))
                places.append((pl.multiple_of(row, PIECE), group_of == group))
            base = first + start * PIECE
            for i in range(number * PIECE):
                place = order_ref.at[pl.ds(i, ORDER_PAD - 2 * PIECE)][base]
                row, mask = places[i // PIECE]
                value = table_ref[pl.ds(place, 1), :]
                pltpu.store(msg_ref.at[pl.ds(row + i % PIECE, 1), :], value, mask=mask)

        @pl.loop(0, lax.div(pieces, 2))
        def _(pair):
            copy(2 * pair, 2)

        pl.when(lax.rem(pieces, 2) == 1)(functools.partial(copy, pieces - 1, 1))
        send(peer).start()

    @pl.loop(0, 16)
    def _(peer):
        send(peer).wait()


def pack(starts, units, order, other, table):
    outgoing, _ = call(
        pack_kernel,
        (sds((16 * PEER_ROWS, LANES)), on_chip((BAND_LATS * LON_PAD, LANES))),
        [ANY, ANY, HELD, HELD, HELD],
        (HBM, VMEM),
        [
            pltpu.SMEM(starts.shape, jnp.int32),
            pltpu.SMEM(units.shape, jnp.int32),
            pltpu.SMEM((ORDER_PAD,), jnp.int32),
            pltpu.VMEM((LON_BLOCKS, 2 * PLANES * PITCH, LANES), f32),
            pltpu.VMEM((16 * PEER_ROWS, LANES), f32),
            pltpu.SemaphoreType.DMA((16,)),
            pltpu.SemaphoreType.DMA((3,)),
        ],
        flops=30_000_000,
        aliases={4: 1},
    )(starts, units, order, other, table)
    return outgoing


def solve_kernel(
    units_any, table_any, got_ref, coef_ref, weight_ref, north_ref, state_hbm, items_hbm,
    units_ref, table_ref, turned, natural, pairs, wide, tubes, state, items_ref, sems, item_sems, fetch_sems,
):
    fetches = [
        pltpu.make_async_copy(units_any, units_ref, fetch_sems.at[0]),
        pltpu.make_async_copy(table_any, table_ref, fetch_sems.at[1]),
    ]
    for fetch in fetches:
        fetch.start()
    core = own_core()
    lane = lax.broadcasted_iota(jnp.int32, (1, LANES), 1)
    low = lane < 64
    quarter = lax.div(lane, 32)

    @pl.loop(0, 8)
    def _(i):
        for side in range(2):
            out = i * LEVEL_PITCH + side * LANES
            row = pl.multiple_of((2 * i + side) * PEER_ROWS, PIECE)
            tail = got_ref[pl.ds(row + LANES, PIECE), :]
            for part, rows in enumerate((got_ref[pl.ds(row, LANES), :], jnp.concatenate([tail] * 2, axis=0))):
                flipped = rows.T
                turned[part, pl.ds(out + 64 * core, 64), :] = flipped[:64]
                turned[part, pl.ds(out + 64 - 64 * core, 64), :] = flipped[64:]

    for fetch in fetches:
        fetch.wait()
    live = TUBE_COLS * units_ref[0]

    def leave(s):
        return pltpu.make_async_copy(state.at[s], state_hbm.at[0, 0, s], sems.at[s])

    @pl.loop(0, SPECIES)
    def _(s):
        def coefs(which):
            row = pl.multiple_of((which * SPECIES + s) * NLEV, NLEV)
            return [coef_ref[pl.ds(row + 8 * v, 8), :] for v in range(8)]

        lower, upper, inv = coefs(0), coefs(1), coefs(2)
        for blk in range(SLOT_BLOCKS):
            i = blk % 3

            def levels(part, group, v):
                return turned[part, pl.ds(32 * v + group * SPECIES + s, 8, stride=LEVEL_PITCH), :]

            if blk < GROUPS:
                raw = [levels(0, blk, v) for v in range(8)]
            else:
                raw = [jnp.where(low, levels(1, 2 * i, v), levels(1, 2 * i + 1, v)) for v in range(8)]
            north = north_ref[blk : blk + 1, :] == 1
            rhs = [jnp.where(north, raw[v ^ 2], raw[v]) for v in range(8)]
            scaled = [rhs[v] * inv[v] for v in range(8)]
            x = rhs
            for _ in range(SWEEPS):
                beneath = [pltpu.roll(x[7], 1, axis=0)] + x[:7]
                overhead = x[1:] + [pltpu.roll(x[0], 7, axis=0)]
                x = [scaled[v] + lower[v] * beneath[v] + upper[v] * overhead[v] for v in range(8)]
            keep = lane + blk * LANES < live
            for v in range(8):
                natural[i, pl.ds(v, 8, stride=PITCH), :] = jnp.where(keep, x[v], 0.0)
            width = min(LANES, COL_CAP - blk * LANES)
            for g in range(8):
                state[s, g * 8 : g * 8 + 8, blk * LANES : blk * LANES + width] = natural[
                    i, g * PITCH : g * PITCH + 8, :width
                ]
            for h in range(4):
                weight = weight_ref[blk, 8 * h : 8 * h + 8, :]
                paired = weight * x[2 * h] + (1.0 - weight) * x[2 * h + 1]
                pairs[i, pl.ds(h, 8, stride=4), :] = paired
            wide[i] = jnp.concatenate([pairs[i]] * 4, axis=0).T
            item = wide[i, pl.ds(0, 32, stride=TUBE_COLS), :]
            for c in range(1, TUBE_COLS):
                item = jnp.where(quarter == c, wide[i, pl.ds(c, 32, stride=TUBE_COLS), :], item)
            tubes[pl.ds(blk * 256 + s, 32, stride=8), :] = item
        leave(s).start()

    tubes[ZERO_TUBE * 8 :, :] = jnp.zeros((8, LANES), f32)
    sub = lax.broadcasted_iota(jnp.int32, (8, LANES), 0)

    def send(quarter):
        rows = pl.ds(quarter * PEERS // 4 * ITEM_ROWS, PEERS // 4 * ITEM_ROWS)
        return pltpu.make_async_copy(items_ref.at[rows, :], items_hbm.at[rows, :], item_sems.at[quarter])

    for part in range(4):

        @pl.loop(part * PEERS // 16, (part + 1) * PEERS // 16)
        def _(step):
            for i in range(4):
                d = step * 4 + i
                tiles = [
                    tubes[pl.ds(pl.multiple_of(table_ref[d * PEER_SLOTS + r] * 8, 8), 8), :]
                    for r in range(PEER_SLOTS)
                ]
                mid = pltpu.roll(tiles[1], 5, axis=0)
                top = pltpu.roll(tiles[2], 2, axis=0)
                row = pl.multiple_of(d * ITEM_ROWS, ITEM_ROWS)
                items_ref[pl.ds(row, 8), :] = jnp.where(sub < 5, tiles[0], mid)
                items_ref[pl.ds(row + 8, 8), :] = jnp.where(sub < 2, mid, jnp.where(sub < 7, top, 0.0))

        send(part).start()

    for part in range(4):
        send(part).wait()
    for s in range(SPECIES):
        leave(s).wait()


def solve(units, table, got, coefs, weights, north):
    return call(
        solve_kernel,
        (sds((1, 1, SPECIES, NLEV, COL_CAP)), sds((PEERS * ITEM_ROWS, LANES))),
        [ANY, ANY] + [HELD] * 4,
        (HBM, HBM),
        [
            pltpu.SMEM(units.shape, jnp.int32),
            pltpu.SMEM(table.shape, jnp.int32),
            pltpu.VMEM((2, 8 * LEVEL_PITCH, LANES), f32),
            pltpu.VMEM((3, 8 * PITCH, LANES), f32),
            pltpu.VMEM((3, PAIRS, LANES), f32),
            pltpu.VMEM((3, LANES, LANES), f32),
            pltpu.VMEM((ZERO_TUBE * 8 + 8, LANES), f32),
            pltpu.VMEM((SPECIES, NLEV, COL_CAP), f32),
            pltpu.VMEM((PEERS * ITEM_ROWS, LANES), f32),
            pltpu.SemaphoreType.DMA((SPECIES,)),
            pltpu.SemaphoreType.DMA((4,)),
            pltpu.SemaphoreType.DMA((2,)),
        ],
        flops=40_000_000,
    )(units, table, got, coefs, weights, north)


def halves(x):
    high = x.astype(jnp.bfloat16)
    return high, (x - high.astype(f32)).astype(jnp.bfloat16)


def product(x, high, low):
    x_high, x_low = halves(x)
    dot = functools.partial(jnp.dot, preferred_element_type=f32)
    return dot(x_high, high) + (dot(x_low, high) + dot(x_high, low))


def lines_kernel(
    items_ref, yield_any, rates_any, waves_ref, fwd_high, fwd_low, inv_high, inv_low, out_hbm,
    yield_ref, rates_ref, spec_in, spec, mixed, done, sems, fetch_sems,
):
    fetches = [
        pltpu.make_async_copy(yield_any, yield_ref, fetch_sems.at[0]),
        pltpu.make_async_copy(rates_any, rates_ref, fetch_sems.at[1]),
    ]
    for fetch in fetches:
        fetch.start()
    tubes = 32 * PEER_SLOTS
    for b in range(4):
        for s in range(SPECIES):
            for r in range(PEER_SLOTS):
                rows = items_ref[pl.ds(b * 32 * ITEM_ROWS + r * SPECIES + s, 32, stride=ITEM_ROWS), :]
                spec_in[b, pl.ds(s * tubes + r, 32, stride=PEER_SLOTS), :] = rows

    half = SPECIES * tubes // 2
    for step in range(2):
        row = step * half
        x = jnp.concatenate([spec_in[b, pl.ds(row, half), :] for b in range(4)], axis=1)
        spec[pl.ds(row, half), :] = product(x, fwd_high[...], fwd_low[...])

    for fetch in fetches:
        fetch.wait()
    waves = waves_ref[...]
    for i in range(IONS):
        keep = (1.0 - rates_ref[IONS + i]) + rates_ref[i] * waves
        gain = jnp.ones_like(waves)
        for _ in range(SECTIONS - 1):
            gain = gain * keep + 1.0
        total = (yield_ref[i * SPECIES] * gain) * spec[:tubes, :]
        for s in range(1, SPECIES):
            total = total + (yield_ref[i * SPECIES + s] * gain) * spec[s * tubes : (s + 1) * tubes, :]
        mixed[i] = total

    def leave(i):
        return pltpu.make_async_copy(done.at[i], out_hbm.at[0, i], sems.at[i])

    for i in range(0, IONS, 2):
        j = min(i + 2, IONS)
        back = product(mixed[i:j].reshape((j - i) * tubes, LINE_PTS), inv_high[...], inv_low[...])
        done[i:j] = back.reshape(j - i, tubes, LINE_PTS)
        for k in range(i, j):
            leave(k).start()

    for i in range(IONS):
        leave(i).wait()


def cosine_basis():
    k = np.arange(LINE_PTS)[:, None]
    n = np.arange(LINE_PTS)[None, :]
    basis = np.cos(np.pi * k * (n + 0.5) / LINE_PTS) * np.sqrt(2.0 / LINE_PTS)
    basis[0] *= np.sqrt(0.5)
    waves = 2.0 * np.cos(np.pi * np.arange(LINE_PTS) / LINE_PTS) - 2.0
    return basis, waves


def lines(items, ion_yield, ion_spread, ion_loss):
    basis, waves = cosine_basis()

    def parts(matrix):
        matrix = matrix.astype(np.float32)
        high = matrix.astype(jnp.bfloat16)
        low = (matrix - high.astype(np.float32)).astype(jnp.bfloat16)
        return jnp.asarray(high), jnp.asarray(low)

    waves = jnp.asarray(waves.astype(np.float32))[None]
    tubes = 32 * PEER_SLOTS
    by_ion = call(
        lines_kernel,
        sds((1, IONS, tubes, LINE_PTS)),
        [HELD, ANY, ANY] + [HELD] * 5,
        HBM,
        [
            pltpu.SMEM((IONS * SPECIES,), f32),
            pltpu.SMEM((2 * IONS,), f32),
            pltpu.VMEM((4, SPECIES * tubes, LANES), f32),
            pltpu.VMEM((SPECIES * tubes, LINE_PTS), f32),
            pltpu.VMEM((IONS, tubes, LINE_PTS), f32),
            pltpu.VMEM((IONS, tubes, LINE_PTS), f32),
            pltpu.SemaphoreType.DMA((IONS,)),
            pltpu.SemaphoreType.DMA((2,)),
        ],
        flops=2_000_000_000,
    )(items, ion_yield.reshape(-1), jnp.concatenate([ion_spread, ion_loss]), waves, *parts(basis.T), *parts(basis))
    return jnp.swapaxes(by_ion, 1, 2)


def swap(x, axis, offset):
    count = lax.axis_size(axis)
    lows = range(offset, count - 1, 2)
    return lax.ppermute(x, axis, [(i, i + 1) for i in lows] + [(i + 1, i) for i in lows])


def exchange(inner, outer, row, far_row):
    outer = swap(outer, "lev", 1)
    row = swap(row, "band", 0)
    far_row = swap(far_row, "band", 1)
    inner = swap(inner, "lev", 0)
    return inner, outer, row, far_row


def on_device(
    neutrals,
    wind_lon,
    wind_lat,
    wind_lev,
    eddy_coupling,
    pair_weight,
    ion_yield,
    ion_spread,
    ion_loss,
    column_order,
    column_units,
    tube_owner,
):
    lev = lax.axis_index("lev")

    neutrals, *rest = edges(neutrals, wind_lon, wind_lat, wind_lev)
    winds, first_halo = rest[:3], exchange(*rest[3:])

    places, starts = list_places(column_units, column_order)
    order = column_order[0]
    own_units = column_units[lev].reshape(1)
    padded = jnp.pad(order, (0, SLOTS_PAD))
    own = lax.dynamic_slice(padded, (TUBE_COLS * starts[lev],), (SLOTS_PAD,))
    own_lat = jnp.zeros_like(own)
    for i in range(1, BAND_LATS):
        own_lat = own_lat + (own >= i * NLON).astype(jnp.int32)
    own_north = (own_lat >= BAND_LATS // 2).astype(jnp.int32).reshape(SLOT_BLOCKS, LANES)
    own_lon = own - own_lat * NLON
    own_rows = (own_lat * 6 + own_lon // 512) * LANES + own_lon % LANES
    own_sel = ((own_lon // LANES) % 4).reshape(SLOT_BLOCKS, LANES)
    zero = jnp.zeros((SPECIES, 1), f32)
    lower = jnp.concatenate([zero, eddy_coupling[:, 1:]], 1)
    upper = jnp.concatenate([eddy_coupling[:, 1:], zero], 1)
    inv = 1.0 / (1.0 + lower + upper)
    coefs = jnp.stack([lower * inv, upper * inv, inv]).reshape(3, SPECIES, 8, 8)
    table, own_weights, coefs = prepare(
        own_units,
        tube_owner[lev, :, 0],
        own_rows,
        own_sel,
        pair_weight.reshape(PAIRS * BAND_LATS, NLON),
        jnp.swapaxes(coefs, 2, 3).reshape(-1, 1),
    )

    inside = interior(neutrals, winds, (places,))
    density, *halo = faces(neutrals, inside, winds, first_halo, first_halo, False)
    inside = interior(density, winds)
    (mine,) = faces(density, inside, winds, exchange(*halo), first_halo, True)
    owners = lax.axis_size("lev")
    other = swap(mine, "lev", 0)
    columns = own_table(mine)

    parity = [[2 * i + c for i in range(owners // 2)] for c in range(2)]
    outgoing = pack(starts, column_units, places, other, columns)
    got = lax.all_to_all(
        outgoing.reshape(16, PEER_ROWS, LANES), "lev", 0, 0, axis_index_groups=parity, tiled=True
    ).reshape(16 * PEER_ROWS, LANES)
    column_state, items = solve(own_units, table, got, coefs, own_weights, own_north)

    items = lax.all_to_all(
        items.reshape(PEERS, ITEM_ROWS, LANES), ("band", "lev"), 0, 0, tiled=True
    ).reshape(PEERS * ITEM_ROWS, LANES)
    return column_state, lines(items, ion_yield, ion_spread, ion_loss)


def solution(mesh):
    placed = (
        P(None, "lev", "band", None),
        P("lev", "band", None),
        P("lev", "band", None),
        P("lev", "band", None),
        P(),
        P(None, "band", None),
        P(),
        P(),
        P(),
        P("band", None),
        P(),
        P(),
    )

    return jax.shard_map(
        on_device,
        mesh=mesh,
        in_specs=placed,
        out_specs=(P("band", "lev", None, None, None), P(("band", "lev"), None, None, None)),
        check_vma=False,
    )
```
